32 devices in a mesh: ctx: 8 (over y, x, core), fsdp: 4 (over z).
Axes of the slice: x: 2, y: 2, z: 4, core: 2. Of those that a mesh axis runs over, the one named last changes fastest.
Arguments:
- hidden_in: bfloat16 [4, 2048, 768], P('fsdp', 'ctx'), may hold values from -6 to 6
- norm1_gain: bfloat16 [768], P('fsdp'), may hold values from 0.099609375 to 1.8984375
- attention_norm_bias: bfloat16 [768], P('fsdp'), may hold values from -1.5 to 1.5
- qkv_weight: bfloat16 [768, 2304], P('fsdp'), as said below
- qkv_bias: bfloat16 [2304], P('fsdp'), may hold values from -0.29882812 to 0.29882812
- out_weight: bfloat16 [768, 768], P('fsdp'), may hold values from -1.75 to 1.75
- out_bias: bfloat16 [768], P('fsdp'), may hold values from -1.5 to 1.5
- norm2_gain: bfloat16 [768], P('fsdp'), may hold values from 0.099609375 to 1.8984375
- feedforward_norm_bias: bfloat16 [768], P('fsdp'), may hold values from -1.5 to 1.5
- up_weight: bfloat16 [768, 3072], P('fsdp'), may hold values from -0.21875 to 0.21875
- up_bias: bfloat16 [3072], P('fsdp'), may hold values from -2.5 to 2.5
- down_weight: bfloat16 [3072, 768], P('fsdp'), may hold values from -0.109375 to 0.109375
- down_bias: bfloat16 [768], P('fsdp'), may hold values from -1.5 to 1.5
- cotangent: bfloat16 [4, 2048, 768], P('fsdp', 'ctx'), may hold values from -6 to 6
- block_order: int32 [16], replicated, may hold values from 0 to 15, as said below
Outputs:
- hidden_out: bfloat16 [4, 2048, 768], P('fsdp', 'ctx')
- hidden_grad: float32 [4, 2048, 768], P('fsdp', 'ctx')
- grad_norm1_gain: float32 [768], P('fsdp')
- grad_norm1_shift: float32 [768], P('fsdp')
- grad_qkv_weight: float32 [768, 2304], P('fsdp')
- grad_qkv_bias: float32 [2304], P('fsdp')
- grad_out_weight: float32 [768, 768], P('fsdp')
- grad_out_bias: float32 [768], P('fsdp')
- grad_norm2_gain: float32 [768], P('fsdp')
- grad_norm2_shift: float32 [768], P('fsdp')
- grad_up_weight: float32 [768, 3072], P('fsdp')
- grad_up_bias: float32 [3072], P('fsdp')
- grad_down_weight: float32 [3072, 768], P('fsdp')
- grad_down_bias: float32 [768], P('fsdp')
The draws below stay inside these ranges and needn't reach their ends.
Inputs may be any that keep to these rules, and one draw needn't show every extreme that they name: `qkv_weight`: the query, key and value projections side by side. `block_order`: each block number appears once; entries 2 j and 2 j + 1 are b and 15 - b.
All inputs are finite; a program needn't handle non-finite values.
Results may differ from the reference program's by a relative error of at most 0.014.
Values may be sent and summed in bfloat16 or wider, within the bound.
A program may use at most 192 MiB of HBM per device.

```python
import math
import jax
import jax.numpy as jnp
from jax import lax

D = 768
H = 12
HD = 64
FF = 3072
ROT = 16
BLK = 128
SEQ_LEN = 2048
SEQS = 4
NBLK = 16


def draw_qkv_weight(key, part):
    base_draw = jax.random.normal(key, (D, 3 * D), jnp.float32) / math.sqrt(D)
    return base_draw.astype(jnp.bfloat16)


def draw_block_order(key, part):
    pair_count = NBLK // 2
    chosen = jax.random.permutation(key, pair_count).astype(jnp.int32)
    paired = jnp.stack([chosen, NBLK - 1 - chosen], axis=1)
    return paired.reshape(NBLK).astype(jnp.int32)


def steps_of(own_key, extent, split, least, top_value):
    level, own = 1.0, jax.random.fold_in(own_key, 6)
    for dim, blocks in split:
        steps = jnp.exp(jax.random.uniform(jax.random.fold_in(own, dim), (blocks,), jnp.float32, least / len(split), top_value / len(split)))
        level = level * jnp.repeat(steps, extent[dim] // blocks).reshape([-1 if axis == dim else 1 for axis in range(len(extent))])
    return level


def bell_draw(rng, extent, deviation, reach, shards=(), kind=jnp.bfloat16):
    array = jax.random.normal(rng, extent, jnp.float32) * deviation
    if len(shards) > 0:
        array = steps_of(rng, extent, shards, -0.22, 0.18) * array
    return jnp.clip(array, min=-reach, max=reach).astype(kind)


def setup_inputs(seed: int = 0) -> dict:
    key_list = jax.random.split(jax.random.key(seed), 16)
    return {
        "hidden_in": bell_draw(key_list[0], (SEQS, SEQ_LEN, D), 1.0, 6.0, ((0, 4), (1, 8))),
        "norm1_gain": jnp.clip(1.0 + 0.18 * jax.random.normal(key_list[1], (D,), jnp.float32), 0.099609375, 1.8984375).astype(jnp.bfloat16),
        "attention_norm_bias": bell_draw(key_list[2], (D,), 0.3, 1.5, ((0, 4),)),
        "qkv_weight": draw_qkv_weight(jax.random.fold_in(key_list[15], 71), 0),
        "qkv_bias": bell_draw(key_list[4], (3 * D,), 0.05, 0.29882812, ((0, 4),)),
        "out_weight": bell_draw(key_list[5], (D, D), (D // 64) ** -0.5, 1.75, ((0, 4),)),
        "out_bias": bell_draw(key_list[6], (D,), 0.3, 1.5, ((0, 4),)),
        "norm2_gain": jnp.clip(1.0 + 0.18 * jax.random.normal(key_list[7], (D,), jnp.float32), 0.099609375, 1.8984375).astype(jnp.bfloat16),
        "feedforward_norm_bias": bell_draw(key_list[8], (D,), 0.3, 1.5, ((0, 4),)),
        "up_weight": bell_draw(key_list[9], (D, FF), D ** -0.5, 0.21875, ((0, 4),)),
        "up_bias": bell_draw(key_list[10], (FF,), 0.5, 2.5, ((0, 4),)),
        "down_weight": bell_draw(key_list[11], (FF, D), FF ** -0.5, 0.109375, ((0, 4),)),
        "down_bias": bell_draw(key_list[12], (D,), 0.3, 1.5, ((0, 4),)),
        "cotangent": bell_draw(key_list[13], (SEQS, SEQ_LEN, D), 1.0, 6.0, ((0, 4), (1, 8))),
        "block_order": draw_block_order(jax.random.fold_in(key_list[15], 71), 0),
    }


EPS = 1e-05
NEG = -1e+30
SQRT_HALF = 0.7071067811865476
INV_ROOT_TWO_PI = 0.3989422804014327

def apply_layer_norm(values_in, norm_gain, norm_bias):
    centre = lax.optimization_barrier(jnp.mean(values_in, axis=-1, keepdims=True))
    mean_removed = values_in - centre
    inverse_deviation = lax.rsqrt(lax.optimization_barrier(jnp.mean(mean_removed * mean_removed, axis=-1, keepdims=True)) + EPS)
    standardized = mean_removed * inverse_deviation
    return (standardized * norm_gain + norm_bias, standardized, inverse_deviation)

def layer_norm_backward(output_gradient, standardized, inverse_deviation, norm_gain):
    gain_scaled = output_gradient * norm_gain
    return inverse_deviation * (gain_scaled - lax.optimization_barrier(jnp.mean(gain_scaled, axis=-1, keepdims=True)) - standardized * lax.optimization_barrier(jnp.mean(gain_scaled * standardized, axis=-1, keepdims=True)))

def gelu_exact(values_in):
    return 0.5 * values_in * (1.0 + lax.erf(values_in * SQRT_HALF))

def gelu_slope(values_in):
    return 0.5 * (1.0 + lax.erf(values_in * SQRT_HALF)) + values_in * jnp.exp(-0.5 * values_in * values_in) * INV_ROOT_TWO_PI

def rotary_tables(position_list):
    half_rot = ROT // 2
    inverse = jnp.power(jnp.float32(10000.0), -2.0 * jnp.arange(half_rot, dtype=jnp.float32) / ROT)
    angle = position_list.astype(jnp.float32)[:, None] * inverse[None, :]
    return (jnp.cos(angle)[:, None, :], jnp.sin(angle)[:, None, :])

def rotate(tensor, cosine, sine):
    half_rot = ROT // 2
    first_half = tensor[..., :half_rot]
    second_half = tensor[..., half_rot:ROT]
    return jnp.concatenate([first_half * cosine - second_half * sine, second_half * cosine + first_half * sine, tensor[..., ROT:]], axis=-1)

def rotate_back(tensor, cosine, sine):
    half_rot = ROT // 2
    first_half = tensor[..., :half_rot]
    second_half = tensor[..., half_rot:ROT]
    return jnp.concatenate([first_half * cosine + second_half * sine, second_half * cosine - first_half * sine, tensor[..., ROT:]], axis=-1)

def attention_forward(query, key_rows, value_rows, position_list):
    seq_rows = query.shape[0]
    qstep = min(512, seq_rows)
    block_count = seq_rows // qstep
    keys_wide = key_rows.astype(jnp.float32)
    values_wide = value_rows.astype(jnp.float32)
    scale = 1.0 / math.sqrt(HD)

    def one_block(block_args):
        query_block, query_pos = block_args
        logits = jnp.einsum('qhd,khd->hqk', query_block.astype(jnp.float32), keys_wide) * scale
        logits = jnp.where(position_list[None, None, :] <= query_pos[None, :, None], logits, NEG)
        peak_value = lax.optimization_barrier(jnp.max(logits, axis=-1, keepdims=True))
        log_total = peak_value[..., 0] + jnp.log(lax.optimization_barrier(jnp.sum(jnp.exp(logits - peak_value), axis=-1)))
        attn_probs = jnp.exp(logits - log_total[:, :, None]).astype(jnp.bfloat16)
        weighted = jnp.einsum('hqk,khd->qhd', attn_probs.astype(jnp.float32), values_wide)
        return (weighted, log_total.T)
    weighted, log_total = lax.map(one_block, (query.reshape(block_count, qstep, H, HD), position_list.reshape(block_count, qstep)))
    return (weighted.reshape(seq_rows, H, HD), log_total.reshape(seq_rows, H))

def attention_backward(query, key_rows, value_rows, position_list, d_att, log_total, delta):
    seq_rows = query.shape[0]
    qstep = min(512, seq_rows)
    block_count = seq_rows // qstep
    keys_wide = key_rows.astype(jnp.float32)
    values_wide = value_rows.astype(jnp.float32)
    scale = 1.0 / math.sqrt(HD)

    def one_block(state_in, block_args):
        key_grads, value_grads = state_in
        query_block, dout_block, total_block, delta_block, query_pos = block_args
        logits = jnp.einsum('qhd,khd->hqk', query_block.astype(jnp.float32), keys_wide) * scale
        logits = jnp.where(position_list[None, None, :] <= query_pos[None, :, None], logits, NEG)
        probs_wide = jnp.exp(logits - total_block.T[:, :, None])
        attn_probs = probs_wide.astype(jnp.bfloat16)
        dprobs = jnp.einsum('qhd,khd->hqk', dout_block.astype(jnp.float32), values_wide)
        d_logits = (probs_wide * (dprobs - delta_block.T[:, :, None]) * scale).astype(jnp.bfloat16)
        d_query = jnp.einsum('hqk,khd->qhd', d_logits.astype(jnp.float32), keys_wide)
        key_grads = key_grads + jnp.einsum('hqk,qhd->khd', d_logits.astype(jnp.float32), query_block.astype(jnp.float32))
        value_grads = value_grads + jnp.einsum('hqk,qhd->khd', attn_probs.astype(jnp.float32), dout_block.astype(jnp.float32))
        return ((key_grads, value_grads), d_query)
    zero_grads = jnp.zeros((seq_rows, H, HD), jnp.float32)
    block_args = (query.reshape(block_count, qstep, H, HD), d_att.reshape(block_count, qstep, H, HD), log_total.reshape(block_count, qstep, H), delta.reshape(block_count, qstep, H), position_list.reshape(block_count, qstep))
    (key_grads, value_grads), d_query = lax.scan(one_block, (zero_grads, zero_grads), block_args)
    return (d_query.reshape(seq_rows, H, HD), key_grads, value_grads)

def reference(hidden_in, norm1_gain, attention_norm_bias, qkv_weight, qkv_bias, out_weight, out_bias, norm2_gain, feedforward_norm_bias, up_weight, up_bias, down_weight, down_bias, cotangent, block_order):
    width = H * HD
    position_list = (block_order[:, None] * BLK + jnp.arange(BLK, dtype=jnp.int32)[None, :]).reshape(SEQ_LEN).astype(jnp.int32)
    cosine, sine = rotary_tables(position_list)
    attention_norm_gain = norm1_gain.astype(jnp.float32)
    feedforward_norm_gain = norm2_gain.astype(jnp.float32)

    def sequence_pass(grads_in, seq_args):
        hidden_seq, cotan_seq = seq_args
        seq_rows = hidden_seq.shape[0]
        residual_stream = hidden_seq.astype(jnp.float32)
        attention_normed, attention_standardized, attention_inverse_deviation = apply_layer_norm(residual_stream, attention_norm_gain, attention_norm_bias.astype(jnp.float32))
        normed1_b = attention_normed.astype(jnp.bfloat16)
        projected = jnp.dot(normed1_b, qkv_weight, preferred_element_type=jnp.float32) + qkv_bias.astype(jnp.float32)
        query = rotate(projected[:, :width].reshape(seq_rows, H, HD), cosine, sine).astype(jnp.bfloat16)
        key_rows = rotate(projected[:, width:2 * width].reshape(seq_rows, H, HD), cosine, sine).astype(jnp.bfloat16)
        value_rows = projected[:, 2 * width:].reshape(seq_rows, H, HD).astype(jnp.bfloat16)
        attended, log_total = attention_forward(query, key_rows, value_rows, position_list)
        attended_b = attended.reshape(seq_rows, width).astype(jnp.bfloat16)
        attn_out = jnp.dot(attended_b, out_weight, preferred_element_type=jnp.float32) + out_bias.astype(jnp.float32)
        feedforward_normed, feedforward_standardized, feedforward_inverse_deviation = apply_layer_norm(residual_stream, feedforward_norm_gain, feedforward_norm_bias.astype(jnp.float32))
        normed2_b = feedforward_normed.astype(jnp.bfloat16)
        up_rows = jnp.dot(normed2_b, up_weight, preferred_element_type=jnp.float32) + up_bias.astype(jnp.float32)
        act_b = gelu_exact(up_rows).astype(jnp.bfloat16)
        mlp_out = jnp.dot(act_b, down_weight, preferred_element_type=jnp.float32) + down_bias.astype(jnp.float32)
        hidden_out = (residual_stream + attn_out + mlp_out).astype(jnp.bfloat16)
        cotan_wide = cotan_seq.astype(jnp.float32)
        grad_wdown = jnp.dot(act_b.T, cotan_seq, preferred_element_type=jnp.float32)
        grad_bdown = lax.optimization_barrier(jnp.sum(cotan_wide, axis=0))
        d_up = jnp.dot(cotan_seq, down_weight.T, preferred_element_type=jnp.float32) * gelu_slope(up_rows)
        d_up16 = d_up.astype(jnp.bfloat16)
        grad_wup = jnp.dot(normed2_b.T, d_up16, preferred_element_type=jnp.float32)
        grad_bup = lax.optimization_barrier(jnp.sum(d_up, axis=0))
        grad_feedforward_normed = jnp.dot(d_up16, up_weight.T, preferred_element_type=jnp.float32)
        grad_feedforward_gain = lax.optimization_barrier(jnp.sum(grad_feedforward_normed * feedforward_standardized, axis=0))
        grad_shift2 = lax.optimization_barrier(jnp.sum(grad_feedforward_normed, axis=0))
        feedforward_branch_grad = layer_norm_backward(grad_feedforward_normed, feedforward_standardized, feedforward_inverse_deviation, feedforward_norm_gain)
        grad_wout = jnp.dot(attended_b.T, cotan_seq, preferred_element_type=jnp.float32)
        d_att = jnp.dot(cotan_seq, out_weight.T, preferred_element_type=jnp.float32).astype(jnp.bfloat16).reshape(seq_rows, H, HD)
        delta = lax.optimization_barrier(jnp.sum(d_att.astype(jnp.float32) * attended_b.reshape(seq_rows, H, HD).astype(jnp.float32), axis=-1))
        d_query, d_key, d_value = attention_backward(query, key_rows, value_rows, position_list, d_att, log_total, delta)
        d_query = rotate_back(d_query, cosine, sine)
        d_key = rotate_back(d_key, cosine, sine)
        d_qkv = jnp.concatenate([d_query.reshape(seq_rows, width), d_key.reshape(seq_rows, width), d_value.reshape(seq_rows, width)], axis=1)
        d_qkv16 = d_qkv.astype(jnp.bfloat16)
        grad_wqkv = jnp.dot(normed1_b.T, d_qkv16, preferred_element_type=jnp.float32)
        grad_bqkv = lax.optimization_barrier(jnp.sum(d_qkv, axis=0))
        grad_attention_normed = jnp.dot(d_qkv16, qkv_weight.T, preferred_element_type=jnp.float32)
        grad_attention_gain = lax.optimization_barrier(jnp.sum(grad_attention_normed * attention_standardized, axis=0))
        grad_shift1 = lax.optimization_barrier(jnp.sum(grad_attention_normed, axis=0))
        attention_branch_grad = layer_norm_backward(grad_attention_normed, attention_standardized, attention_inverse_deviation, attention_norm_gain)
        hidden_grad = cotan_wide + attention_branch_grad + feedforward_branch_grad
        terms = (grad_attention_gain, grad_shift1, grad_wqkv, grad_bqkv, grad_wout, grad_bdown, grad_feedforward_gain, grad_shift2, grad_wup, grad_bup, grad_wdown, grad_bdown)
        grads_out = jax.tree.map(lambda older, newer: older + newer, grads_in, terms)
        return (grads_out, (hidden_out, hidden_grad))
    zero_grads = (jnp.zeros((D,), jnp.float32), jnp.zeros((D,), jnp.float32), jnp.zeros((D, 3 * D), jnp.float32), jnp.zeros((3 * D,), jnp.float32), jnp.zeros((D, D), jnp.float32), jnp.zeros((D,), jnp.float32), jnp.zeros((D,), jnp.float32), jnp.zeros((D,), jnp.float32), jnp.zeros((D, FF), jnp.float32), jnp.zeros((FF,), jnp.float32), jnp.zeros((FF, D), jnp.float32), jnp.zeros((D,), jnp.float32))
    grads_all, (hidden_out, hidden_grad) = lax.scan(sequence_pass, zero_grads, (hidden_in, cotangent))
    return (hidden_out, hidden_grad, grads_all[0], grads_all[1], grads_all[2], grads_all[3], grads_all[4], grads_all[5], grads_all[6], grads_all[7], grads_all[8], grads_all[9], grads_all[10], grads_all[11])
```

```python
import functools
import math

import jax
import jax.numpy as jnp
from jax import lax
from jax.experimental import pallas as pl
from jax.experimental.pallas import tpu as pltpu
from jax.sharding import PartitionSpec as P

H = 12
HD = 64
ROT = 16
BLK = 128


EPS = 1e-05
NEG = -1e30
SQRT_HALF = 0.7071067811865476
INV_ROOT_TWO_PI = 0.3989422804014327


def apply_layer_norm(values_in, norm_gain, norm_bias):
    centre = jnp.mean(values_in, axis=-1, keepdims=True)
    mean_removed = values_in - centre
    inverse_deviation = lax.rsqrt(
        jnp.mean(mean_removed * mean_removed, axis=-1, keepdims=True) + EPS
    )
    standardized = mean_removed * inverse_deviation
    return (standardized * norm_gain + norm_bias, standardized, inverse_deviation)


def layer_norm_backward(output_gradient, standardized, inverse_deviation, norm_gain):
    gain_scaled = output_gradient * norm_gain
    return inverse_deviation * (
        gain_scaled
        - jnp.mean(gain_scaled, axis=-1, keepdims=True)
        - standardized * jnp.mean(gain_scaled * standardized, axis=-1, keepdims=True)
    )


def gelu_exact(values_in):
    return 0.5 * values_in * (1.0 + lax.erf(values_in * SQRT_HALF))


def gelu_slope(values_in):
    return (
        0.5 * (1.0 + lax.erf(values_in * SQRT_HALF))
        + values_in * jnp.exp(-0.5 * values_in * values_in) * INV_ROOT_TWO_PI
    )


def rotary_tables(position_list):
    half_rot = ROT // 2
    inverse = jnp.power(jnp.float32(10000.0), -2.0 * jnp.arange(half_rot, dtype=jnp.float32) / ROT)
    angle = position_list.astype(jnp.float32)[:, None] * inverse[None, :]
    return (jnp.cos(angle)[:, None, :], jnp.sin(angle)[:, None, :])


def rotate(tensor, cosine, sine):
    half_rot = ROT // 2
    first_half = tensor[..., :half_rot]
    second_half = tensor[..., half_rot:ROT]
    return jnp.concatenate(
        [
            first_half * cosine - second_half * sine,
            second_half * cosine + first_half * sine,
            tensor[..., ROT:],
        ],
        axis=-1,
    )


def rotate_back(tensor, cosine, sine):
    half_rot = ROT // 2
    first_half = tensor[..., :half_rot]
    second_half = tensor[..., half_rot:ROT]
    return jnp.concatenate(
        [
            first_half * cosine + second_half * sine,
            second_half * cosine - first_half * sine,
            tensor[..., ROT:],
        ],
        axis=-1,
    )


def masked_logits(query_block, key_block, query_pos, key_pos):
    logits = jnp.einsum(
        "qhd,khd->hqk", query_block, key_block, preferred_element_type=jnp.float32
    ) * (1.0 / math.sqrt(HD))
    return jnp.where(key_pos[None, None, :] <= query_pos[None, :, None], logits, NEG)


def block_terms(
    query_block, dout_block, total_t, delta_t, query_pos, key_block, value_block, key_pos
):
    logits = masked_logits(query_block, key_block, query_pos, key_pos)
    probs_wide = jnp.exp(logits - total_t[:, :, None])
    dprobs = jnp.einsum("qhd,khd->hqk", dout_block, value_block, preferred_element_type=jnp.float32)
    d_logits = (probs_wide * (dprobs - delta_t[:, :, None]) * (1.0 / math.sqrt(HD))).astype(
        jnp.bfloat16
    )
    return (probs_wide.astype(jnp.bfloat16), d_logits)


def keep_state(state_in):
    return state_in


def forward_attention(query, keys_all, values_all, own_pos, all_pos):
    local_rows = query.shape[0]
    seq_rows = keys_all.shape[0]
    qstep = min(512, local_rows)
    kstep = min(512, seq_rows)
    latest = jnp.max(own_pos)

    def stats_step(number, state_in):
        key_block = lax.dynamic_slice_in_dim(keys_all, number * kstep, kstep, 0)
        key_pos = lax.dynamic_slice_in_dim(all_pos, number * kstep, kstep, 0)

        def stats_live(state_now):
            running_max, running_sum = state_now
            logits = masked_logits(query, key_block, own_pos, key_pos)
            new_max = jnp.maximum(running_max, jnp.max(logits, axis=-1))
            running_sum = running_sum * jnp.exp(running_max - new_max) + jnp.sum(
                jnp.exp(logits - new_max[:, :, None]), axis=-1
            )
            return (new_max, running_sum)

        return lax.cond(jnp.min(key_pos) <= latest, stats_live, keep_state, state_in)

    start_state = (jnp.full((H, qstep), NEG, jnp.float32), jnp.zeros((H, qstep), jnp.float32))
    running_max, running_sum = lax.fori_loop(0, seq_rows // kstep, stats_step, start_state)
    total_t = running_max + jnp.log(running_sum)

    def value_step(number, state_in):
        key_block = lax.dynamic_slice_in_dim(keys_all, number * kstep, kstep, 0)
        value_block = lax.dynamic_slice_in_dim(values_all, number * kstep, kstep, 0)
        key_pos = lax.dynamic_slice_in_dim(all_pos, number * kstep, kstep, 0)

        def value_live(state_now):
            logits = masked_logits(query, key_block, own_pos, key_pos)
            attn_probs = jnp.exp(logits - total_t[:, :, None]).astype(jnp.bfloat16)
            return state_now + jnp.einsum(
                "hqk,khd->qhd", attn_probs, value_block, preferred_element_type=jnp.float32
            )

        return lax.cond(jnp.min(key_pos) <= latest, value_live, keep_state, state_in)

    weighted = lax.fori_loop(
        0, seq_rows // kstep, value_step, jnp.zeros((qstep, H, HD), jnp.float32)
    )
    totals = total_t.T
    return (weighted, totals)


def query_grads(query, d_att, log_total, delta, own_pos, keys_all, values_all, all_pos):
    local_rows = query.shape[0]
    seq_rows = keys_all.shape[0]
    qstep = min(512, local_rows)
    kstep = min(512, seq_rows)
    key_grads = jnp.zeros((seq_rows, H, HD), jnp.float32)
    value_grads = jnp.zeros((seq_rows, H, HD), jnp.float32)
    total_t = log_total.T
    delta_t = delta.T
    latest = jnp.max(own_pos)

    def key_step(number, state_in):
        offset = number * kstep
        key_block = lax.dynamic_slice_in_dim(keys_all, offset, kstep, 0)
        value_block = lax.dynamic_slice_in_dim(values_all, offset, kstep, 0)
        key_pos = lax.dynamic_slice_in_dim(all_pos, offset, kstep, 0)

        def key_live(state_now):
            attn_probs, d_logits = block_terms(
                query, d_att, total_t, delta_t, own_pos, key_block, value_block, key_pos
            )
            d_query = state_now[0] + jnp.einsum(
                "hqk,khd->qhd", d_logits, key_block, preferred_element_type=jnp.float32
            )
            key_acc = state_now[1]
            value_acc = state_now[2]
            key_part = jnp.einsum(
                "hqk,qhd->khd", d_logits, query, preferred_element_type=jnp.float32
            )
            value_part = jnp.einsum(
                "hqk,qhd->khd", attn_probs, d_att, preferred_element_type=jnp.float32
            )
            key_acc = lax.dynamic_update_slice_in_dim(
                key_acc, lax.dynamic_slice_in_dim(key_acc, offset, kstep, 0) + key_part, offset, 0
            )
            value_acc = lax.dynamic_update_slice_in_dim(
                value_acc,
                lax.dynamic_slice_in_dim(value_acc, offset, kstep, 0) + value_part,
                offset,
                0,
            )
            return (d_query, key_acc, value_acc)

        return lax.cond(jnp.min(key_pos) <= latest, key_live, keep_state, state_in)

    start_state = (jnp.zeros((qstep, H, HD), jnp.float32),) + (key_grads, value_grads)
    result = lax.fori_loop(0, seq_rows // kstep, key_step, start_state)
    pieces = result[0]
    key_grads = result[1]
    value_grads = result[2]
    return (pieces, key_grads, value_grads)


def whole_parameter_layer(
    hidden_in,
    norm1_gain,
    attention_norm_bias,
    qkv_weight,
    qkv_bias,
    out_weight,
    out_bias,
    norm2_gain,
    feedforward_norm_bias,
    up_weight,
    up_bias,
    down_weight,
    down_bias,
    cotangent,
    block_order,
):
    (
        attention_norm_gain,
        attention_bias_term,
        wqkv,
        bqkv,
        wout,
        bout,
        feedforward_norm_gain,
        feedforward_bias_term,
        wup,
        bup,
        wdown,
        bdown,
    ) = (
        lax.all_gather(norm1_gain, "fsdp", axis=0, tiled=True),
        lax.all_gather(attention_norm_bias, "fsdp", axis=0, tiled=True),
        lax.all_gather(qkv_weight, "fsdp", axis=0, tiled=True),
        lax.all_gather(qkv_bias, "fsdp", axis=0, tiled=True),
        lax.all_gather(out_weight, "fsdp", axis=0, tiled=True),
        lax.all_gather(out_bias, "fsdp", axis=0, tiled=True),
        lax.all_gather(norm2_gain, "fsdp", axis=0, tiled=True),
        lax.all_gather(feedforward_norm_bias, "fsdp", axis=0, tiled=True),
        lax.all_gather(up_weight, "fsdp", axis=0, tiled=True),
        lax.all_gather(up_bias, "fsdp", axis=0, tiled=True),
        lax.all_gather(down_weight, "fsdp", axis=0, tiled=True),
        lax.all_gather(down_bias, "fsdp", axis=0, tiled=True),
    )
    width = H * HD
    hidden_rows = hidden_in[0]
    cotan_rows = cotangent[0]
    local_rows = hidden_rows.shape[0]
    ctx_count = lax.axis_size("ctx")
    ctx_rank = lax.axis_index("ctx")
    seq_rows = local_rows * ctx_count
    all_pos = (block_order[:, None] * BLK + jnp.arange(BLK, dtype=jnp.int32)[None, :]).reshape(
        seq_rows
    )
    own_pos = lax.dynamic_slice_in_dim(all_pos, ctx_rank * local_rows, local_rows, 0)
    cosine, sine = rotary_tables(own_pos)
    attention_norm_gain = attention_norm_gain.astype(jnp.float32)
    feedforward_norm_gain = feedforward_norm_gain.astype(jnp.float32)
    residual_stream = hidden_rows.astype(jnp.float32)
    attention_normed, attention_standardized, attention_inverse_deviation = apply_layer_norm(
        residual_stream, attention_norm_gain, attention_bias_term.astype(jnp.float32)
    )
    normed1_b = attention_normed.astype(jnp.bfloat16)
    projected = jnp.dot(normed1_b, wqkv, preferred_element_type=jnp.float32) + bqkv.astype(
        jnp.float32
    )
    query = rotate(projected[:, :width].reshape(local_rows, H, HD), cosine, sine).astype(
        jnp.bfloat16
    )
    key_rows = rotate(
        projected[:, width : 2 * width].reshape(local_rows, H, HD), cosine, sine
    ).astype(jnp.bfloat16)
    value_rows = projected[:, 2 * width :].astype(jnp.bfloat16)
    keys_all, values_all = (
        lax.all_gather(key_rows.reshape(local_rows, width), "ctx", axis=0, tiled=True),
        lax.all_gather(value_rows, "ctx", axis=0, tiled=True),
    )
    keys_all = keys_all.reshape(seq_rows, H, HD)
    values_all = values_all.reshape(seq_rows, H, HD)
    attended, log_total = forward_attention(query, keys_all, values_all, own_pos, all_pos)
    attended_b = attended.reshape(local_rows, width).astype(jnp.bfloat16)
    attn_out = jnp.dot(attended_b, wout, preferred_element_type=jnp.float32) + bout.astype(
        jnp.float32
    )
    feedforward_normed, feedforward_standardized, feedforward_inverse_deviation = apply_layer_norm(
        residual_stream, feedforward_norm_gain, feedforward_bias_term.astype(jnp.float32)
    )
    normed2_b = feedforward_normed.astype(jnp.bfloat16)
    up_rows = jnp.dot(normed2_b, wup, preferred_element_type=jnp.float32) + bup.astype(jnp.float32)
    act_b = gelu_exact(up_rows).astype(jnp.bfloat16)
    mlp_out = jnp.dot(act_b, wdown, preferred_element_type=jnp.float32) + bdown.astype(jnp.float32)
    hidden_out = (residual_stream + attn_out + mlp_out).astype(jnp.bfloat16)
    cotan_wide = cotan_rows.astype(jnp.float32)
    grad_wdown = jnp.einsum("tk,tn->kn", act_b, cotan_rows, preferred_element_type=jnp.float32)
    grad_bdown = jnp.sum(cotan_wide, axis=0)
    d_up = jnp.einsum(
        "tn,kn->tk", cotan_rows, wdown, preferred_element_type=jnp.float32
    ) * gelu_slope(up_rows)
    d_up16 = d_up.astype(jnp.bfloat16)
    grad_wup = jnp.einsum("tk,tn->kn", normed2_b, d_up16, preferred_element_type=jnp.float32)
    grad_bup = jnp.sum(d_up, axis=0)
    grad_feedforward_normed = jnp.einsum(
        "tn,kn->tk", d_up16, wup, preferred_element_type=jnp.float32
    )
    grad_feedforward_gain = jnp.sum(grad_feedforward_normed * feedforward_standardized, axis=0)
    grad_shift2 = jnp.sum(grad_feedforward_normed, axis=0)
    feedforward_branch_grad = layer_norm_backward(
        grad_feedforward_normed,
        feedforward_standardized,
        feedforward_inverse_deviation,
        feedforward_norm_gain,
    )
    grad_wout = jnp.einsum("tk,tn->kn", attended_b, cotan_rows, preferred_element_type=jnp.float32)
    d_att = jnp.einsum("tn,kn->tk", cotan_rows, wout, preferred_element_type=jnp.float32).astype(
        jnp.bfloat16
    )
    delta = jnp.sum(
        d_att.reshape(local_rows, H, HD).astype(jnp.float32)
        * attended_b.reshape(local_rows, H, HD).astype(jnp.float32),
        axis=-1,
    )
    d_att3 = d_att.reshape(local_rows, H, HD)
    d_query, key_grads, value_grads = query_grads(
        query, d_att3, log_total, delta, own_pos, keys_all, values_all, all_pos
    )
    d_key, d_value = (
        lax.psum_scatter(
            key_grads.reshape(seq_rows, width), "ctx", scatter_dimension=0, tiled=True
        ),
        lax.psum_scatter(
            value_grads.reshape(seq_rows, width), "ctx", scatter_dimension=0, tiled=True
        ),
    )
    d_query = rotate_back(d_query, cosine, sine)
    d_key = rotate_back(d_key.reshape(local_rows, H, HD), cosine, sine)
    d_qkv = jnp.concatenate(
        [d_query.reshape(local_rows, width), d_key.reshape(local_rows, width), d_value], axis=1
    )
    d_qkv16 = d_qkv.astype(jnp.bfloat16)
    grad_wqkv = jnp.einsum("tk,tn->kn", normed1_b, d_qkv16, preferred_element_type=jnp.float32)
    grad_bqkv = jnp.sum(d_qkv, axis=0)
    grad_attention_normed = jnp.einsum(
        "tn,kn->tk", d_qkv16, wqkv, preferred_element_type=jnp.float32
    )
    grad_attention_gain = jnp.sum(grad_attention_normed * attention_standardized, axis=0)
    grad_shift1 = jnp.sum(grad_attention_normed, axis=0)
    attention_branch_grad = layer_norm_backward(
        grad_attention_normed,
        attention_standardized,
        attention_inverse_deviation,
        attention_norm_gain,
    )
    hidden_grad = cotan_wide + attention_branch_grad + feedforward_branch_grad
    terms = (
        grad_attention_gain,
        grad_shift1,
        grad_wqkv,
        grad_bqkv,
        grad_wout,
        grad_bdown,
        grad_feedforward_gain,
        grad_shift2,
        grad_wup,
        grad_bup,
        grad_wdown,
        grad_bdown,
    )
    shares = (
        lax.psum_scatter(terms[0], "fsdp", scatter_dimension=0, tiled=True),
        lax.psum_scatter(terms[1], "fsdp", scatter_dimension=0, tiled=True),
        lax.psum_scatter(terms[2], "fsdp", scatter_dimension=0, tiled=True),
        lax.psum_scatter(terms[3], "fsdp", scatter_dimension=0, tiled=True),
        lax.psum_scatter(terms[4], "fsdp", scatter_dimension=0, tiled=True),
        lax.psum_scatter(terms[5], "fsdp", scatter_dimension=0, tiled=True),
        lax.psum_scatter(terms[6], "fsdp", scatter_dimension=0, tiled=True),
        lax.psum_scatter(terms[7], "fsdp", scatter_dimension=0, tiled=True),
        lax.psum_scatter(terms[8], "fsdp", scatter_dimension=0, tiled=True),
        lax.psum_scatter(terms[9], "fsdp", scatter_dimension=0, tiled=True),
        lax.psum_scatter(terms[10], "fsdp", scatter_dimension=0, tiled=True),
        lax.psum_scatter(terms[11], "fsdp", scatter_dimension=0, tiled=True),
    )
    shares = lax.psum(
        (
            shares[0],
            shares[1],
            shares[2],
            shares[3],
            shares[4],
            shares[5],
            shares[6],
            shares[7],
            shares[8],
            shares[9],
            shares[10],
            shares[11],
        ),
        "ctx",
    )
    return (
        hidden_out[None],
        hidden_grad[None],
        shares[0],
        shares[1],
        shares[2],
        shares[3],
        shares[4],
        shares[5],
        shares[6],
        shares[7],
        shares[8],
        shares[9],
        shares[10],
        shares[11],
    )


MESH_IDS = pl.DeviceIdType.MESH


def flip(index, bit):
    return index + bit - 2 * bit * ((index // bit) % 2)


class Copies:
    def __init__(self, send_sems, recv_sems):
        self.send_sems, self.recv_sems = send_sems, recv_sems
        self.count, self.started, self.numbers = 0, [], {}

    def make(self, source, target, device, when=None, like=None):
        if like is None:
            number = self.count
            self.count += 1
        else:
            number = self.numbers[id(like)]
        copy = pltpu.make_async_remote_copy(
            src_ref=source,
            dst_ref=target,
            send_sem=self.send_sems.at[number],
            recv_sem=self.recv_sems.at[number],
            device_id=device,
            device_id_type=MESH_IDS,
        )
        self.started.append((copy, when))
        self.numbers[id(copy)] = number
        return copy

    def finish(self):
        for copy, when in self.started:
            run_when(when, copy.wait_send)


def run_when(condition, action):
    if condition is None:
        action()
    else:
        pl.when(condition)(action)


def greet(peers):
    barrier = pltpu.get_barrier_semaphore()
    total = 0
    for device, condition in peers:
        run_when(
            condition,
            functools.partial(
                pl.semaphore_signal, barrier, inc=1, device_id=device, device_id_type=MESH_IDS
            ),
        )
        total = total + (1 if condition is None else condition.astype(jnp.int32))
    pl.semaphore_wait(barrier, total)


def plane_gather(copies, source, same, other, slot, chip_of, rows, ids):
    c, z, xn, yn, pn = ids
    half = rows // 2
    top, bottom = pl.ds(0, half), pl.ds(half, half)
    t = chip_of
    to_x = copies.make(source, same.at[slot(t)], (xn, z))
    to_y = copies.make(source, same.at[slot(t)], (yn, z))
    to_x.start()
    to_y.start()
    swaps = []

    def swap(tt, part=None):
        if other is None:
            return
        here, there = same.at[slot(tt)], other.at[slot(tt)]
        if part is not None:
            here, there = here.at[part], there.at[part]
        copy = copies.make(here, there, (pn, z))
        copy.start()
        swaps.append(copy)

    if other is not None:
        copy = copies.make(source, other.at[slot(t)], (pn, z))
        copy.start()
        swaps.append(copy)
    tx, ty, td = flip(t, 1), flip(t, 2), flip(flip(t, 1), 2)

    def on_x():
        to_x.wait_recv()
        forward = copies.make(same.at[slot(tx)].at[top], same.at[slot(tx)].at[top], (yn, z))
        forward.start()
        swap(tx)
        return forward

    def on_y():
        to_y.wait_recv()
        forward = copies.make(same.at[slot(ty)].at[bottom], same.at[slot(ty)].at[bottom], (xn, z))
        forward.start()
        swap(ty)
        return forward

    def on_diagonal(from_y, from_x):
        from_y.wait_recv()
        swap(td, top)
        from_x.wait_recv()
        swap(td, bottom)

    return on_x, on_y, on_diagonal, swaps


def line_gather(copies, source, gathered, nz, ids, half_of):
    c, z, xn, yn, pn = ids
    steps = []
    rows = gathered.shape[1] // 2
    mine = pl.ds(half_of * rows, rows)
    forwards = {}
    for step in range(nz - 1):
        for sign in (1, -1):
            shard = z - sign * step
            target = z + sign
            ok = (shard >= 0) & (shard < nz) & (target >= 0) & (target < nz)
            from_here = source.at[mine] if step == 0 else gathered.at[jnp.clip(shard, 0, nz - 1), mine]
            place = gathered.at[jnp.clip(shard, 0, nz - 1), mine]
            copy = copies.make(from_here, place, (c, jnp.clip(target, 0, nz - 1)), when=ok)
            forwards[step, sign] = (copy, ok)
    for sign in (1, -1):
        copy, ok = forwards[0, sign]
        run_when(ok, copy.start)
    swaps = []

    def advance(step):
        for sign in (1, -1):
            arrived = z - sign * (step + 1)
            ok = (arrived >= 0) & (arrived < nz)
            copy, _ = forwards[step, sign]
            run_when(ok, copy.wait_recv)
            if step + 1 < nz - 1:
                following, following_ok = forwards[step + 1, sign]
                run_when(following_ok, following.start)
            place = gathered.at[jnp.clip(arrived, 0, nz - 1), mine]
            swap = copies.make(place, place, (pn, z), when=ok)
            run_when(ok, swap.start)
            swaps.append((swap, ok))

    return advance, swaps


def gather_kernel(
    nz,
    h_ref,
    g_ref,
    wq_ref,
    wu_ref,
    wd_ref,
    wo_ref,
    sm_ref,
    hall_ref,
    gall_ref,
    wq4_ref,
    wu4_ref,
    wd4_ref,
    wo1_ref,
    sm4_ref,
    send_sems,
    recv_sems,
    local_sems,
):
    c, z = lax.axis_index("ctx"), lax.axis_index("fsdp")
    k, t = c % 2, c // 2
    xn, yn, pn = flip(c, 2), flip(c, 4), flip(c, 1)
    ids = (c, z, xn, yn, pn)
    others = [(z + d) % nz for d in range(1, nz)]
    greet(
        [((xn, z), None), ((yn, z), None), ((pn, z), None)] + [((c, other), None) for other in others]
    )
    copies = Copies(send_sems, recv_sems)
    local_copies = []

    def keep(source, target):
        copy = pltpu.make_async_copy(source, target, local_sems.at[len(local_copies)])
        copy.start()
        local_copies.append(copy)

    rows = h_ref.shape[0]
    shard = wq_ref.shape[0]
    wd_own = wd_ref.at[pl.ds(t * shard, shard)]
    small = [copies.make(sm_ref, sm4_ref.at[z], (c, other)) for other in others]
    for copy in small:
        copy.start()
    wq_step, wq_swaps = line_gather(copies, wq_ref, wq4_ref, nz, ids, k)
    h_x, h_y, h_d, h_swaps = plane_gather(
        copies, h_ref, hall_ref.at[0], hall_ref.at[1], lambda i: i, t, rows, ids
    )
    wu_step, wu_swaps = line_gather(copies, wu_ref, wu4_ref, nz, ids, k)
    wd_step, wd_swaps = line_gather(copies, wd_own, wd4_ref, nz, ids, k)
    g_x, g_y, g_d, _ = plane_gather(copies, g_ref, gall_ref, None, lambda i: i, t, rows, ids)
    keep(h_ref, hall_ref.at[0, t])
    keep(g_ref, gall_ref.at[t])
    keep(wq_ref, wq4_ref.at[z])
    keep(wu_ref, wu4_ref.at[z])
    keep(wd_own, wd4_ref.at[z])
    keep(sm_ref, sm4_ref.at[z])
    own_slice = z == t
    half = shard // 2
    mine = pl.ds(k * half, half)
    whole = pltpu.make_async_copy(wo_ref, wo1_ref, local_sems.at[len(local_copies)])
    pl.when(own_slice)(whole.start)
    wo_up = copies.make(
        wo_ref.at[mine], wo1_ref.at[mine], (c, jnp.minimum(z + 1, nz - 1)), when=own_slice & (z < nz - 1)
    )
    wo_down = copies.make(
        wo_ref.at[mine], wo1_ref.at[mine], (c, jnp.maximum(z - 1, 0)), when=own_slice & (z > 0)
    )
    pl.when(own_slice & (z < nz - 1))(wo_up.start)
    pl.when(own_slice & (z > 0))(wo_down.start)

    from_x = h_x()
    from_y = h_y()
    wq_step(0)
    h_d(from_x, from_y)
    wq_step(1)
    wu_step(0)
    g_from_x = g_x()
    g_from_y = g_y()
    wq_step(2)
    wd_step(0)
    wu_step(1)
    above, below = z > t, z < t
    relay_up, relay_down = above & (z < nz - 1), below & (z > 0)
    pl.when(above)(wo_up.wait_recv)
    pl.when(below)(wo_down.wait_recv)
    wo_on_up = copies.make(
        wo1_ref.at[mine], wo1_ref.at[mine], (c, jnp.minimum(z + 1, nz - 1)), when=relay_up, like=wo_up
    )
    wo_on_down = copies.make(
        wo1_ref.at[mine], wo1_ref.at[mine], (c, jnp.maximum(z - 1, 0)), when=relay_down, like=wo_down
    )
    pl.when(relay_up)(wo_on_up.start)
    pl.when(relay_down)(wo_on_down.start)
    wo_swap = copies.make(wo1_ref.at[mine], wo1_ref.at[mine], (pn, z), when=above | below)
    pl.when(above | below)(wo_swap.start)
    wd_step(1)
    wu_step(2)
    wd_step(2)
    g_from_x.wait_recv()
    g_from_y.wait_recv()
    for copy in small:
        copy.wait_recv()
    for copy in h_swaps:
        copy.wait_recv()
    for swaps in (wq_swaps, wu_swaps, wd_swaps):
        for swap, ok in swaps:
            run_when(ok, swap.wait_recv)
    pl.when(above | below)(wo_swap.wait_recv)
    for copy in local_copies:
        copy.wait()
    pl.when(own_slice)(whole.wait)
    copies.finish()


def reduce_kernel(
    nz,
    e_ref,
    o_ref,
    gq_ref,
    gu_ref,
    gd_ref,
    go_ref,
    vec_ref,
    eall_ref,
    oall_ref,
    fq_ref,
    fu_ref,
    fd_ref,
    fo_ref,
    vsum_ref,
    rq_ref,
    ru_ref,
    rd_ref,
    ro_ref,
    uq_ref,
    uu_ref,
    ud_ref,
    uo_ref,
    dq_ref,
    du_ref,
    dd_ref,
    do_ref,
    vz_ref,
    vs_ref,
    vp_ref,
    send_sems,
    recv_sems,
    local_sems,
):
    c, z = lax.axis_index("ctx"), lax.axis_index("fsdp")
    k, t = c % 2, c // 2
    xn, yn, pn = flip(c, 2), flip(c, 4), flip(c, 1)
    dn = flip(xn, 4)
    above_id, below_id = jnp.minimum(z + 1, nz - 1), jnp.maximum(z - 1, 0)
    others = [(z + d) % nz for d in range(1, nz)]
    plane = [xn, yn, dn, pn, flip(xn, 1), flip(yn, 1), flip(dn, 1)]
    greet([((peer, z), None) for peer in plane] + [((c, other), None) for other in others])
    copies = Copies(send_sems, recv_sems)
    arrays = (
        (gq_ref, rq_ref, uq_ref, dq_ref, fq_ref),
        (gu_ref, ru_ref, uu_ref, du_ref, fu_ref),
        (gd_ref, rd_ref, ud_ref, dd_ref, fd_ref),
    )
    half = gq_ref.shape[1] // 2
    mine = pl.ds(k * half, half)
    theirs = pl.ds((1 - k) * half, half)

    exchanged = []
    for source, received, _, _, _ in arrays:
        copy = copies.make(source.at[:, theirs], received, (pn, z))
        copy.start()
        exchanged.append(copy)
    o_exchanged = copies.make(go_ref.at[theirs], ro_ref, (pn, z))
    o_exchanged.start()
    vec_out = [copies.make(vec_ref.at[other], vz_ref.at[z], (c, other)) for other in others]
    for copy in vec_out:
        copy.start()
    scattered = []
    for source, target in ((o_ref, oall_ref), (e_ref, eall_ref)):
        for peer in (xn, yn, dn):
            copy = copies.make(source.at[peer // 2], target.at[t], (peer, z))
            copy.start()
            scattered.append(copy)
    own_e = pltpu.make_async_copy(e_ref.at[t], eall_ref.at[t], local_sems.at[0])
    own_o = pltpu.make_async_copy(o_ref.at[t], oall_ref.at[t], local_sems.at[1])
    own_e.start()
    own_o.start()

    for copy, (source, received, _, _, _) in zip(exchanged, arrays):
        copy.wait_recv()
        for zz in range(nz):
            received[zz] = (
                received[zz].astype(jnp.float32) + source[zz, mine].astype(jnp.float32)
            ).astype(jnp.bfloat16)
    o_exchanged.wait_recv()
    ro_ref[...] = (ro_ref[...].astype(jnp.float32) + go_ref[mine].astype(jnp.float32)).astype(
        jnp.bfloat16
    )

    chains = []
    for _, total, up, down, _ in arrays:
        chains.append((total, up, down))
    up_sends, down_sends = {}, {}
    for number, (total, up, down) in enumerate(chains):
        for owner in range(nz):
            up_sends[number, owner] = copies.make(
                total.at[owner], up.at[owner], (c, above_id), when=z < owner
            )
            down_sends[number, owner] = copies.make(
                total.at[owner], down.at[owner], (c, below_id), when=z > owner
            )
    order = list(range(len(chains)))

    def add_into(total, incoming, owner):
        total[owner] = (
            total[owner].astype(jnp.float32) + incoming[owner].astype(jnp.float32)
        ).astype(jnp.bfloat16)

    for place in range(nz):

        @pl.when(z == place)
        def _():
            events = []
            for owner in range(place, nz):
                if place > 0 or owner > place:
                    events.append((nz - 1 - owner + place, 0, owner))
            for owner in range(place + 1):
                if place < nz - 1 or owner < place:
                    events.append((owner + nz - 1 - place, 1, owner))
            for time, way, owner in sorted(events):
                for number in order:
                    total, up, down = chains[number]
                    if way == 0:
                        if place > 0:
                            up_sends[number, owner].wait_recv()
                            add_into(total, up, owner)
                        if owner > place:
                            up_sends[number, owner].start()
                    else:
                        if place < nz - 1:
                            down_sends[number, owner].wait_recv()
                            add_into(total, down, owner)
                        if owner < place:
                            down_sends[number, owner].start()

    o_up = copies.make(ro_ref, uo_ref, (c, above_id), when=z < t)
    o_down = copies.make(ro_ref, do_ref, (c, below_id), when=z > t)

    def take(incoming):
        ro_ref[...] = (ro_ref[...].astype(jnp.float32) + incoming[...].astype(jnp.float32)).astype(
            jnp.bfloat16
        )

    @pl.when((z <= t) & (z > 0))
    def _():
        o_up.wait_recv()
        take(uo_ref)

    pl.when(z < t)(o_up.start)

    @pl.when((z >= t) & (z < nz - 1))
    def _():
        o_down.wait_recv()
        take(do_ref)

    pl.when(z > t)(o_down.start)

    for copy in vec_out:
        copy.wait_recv()
    total = vec_ref[z]
    for other in others:
        total = total + vz_ref[other]
    vs_ref[...] = total
    vec_plane = [copies.make(vs_ref, vp_ref.at[c], (peer, z)) for peer in plane]
    for copy in vec_plane:
        copy.start()

    ids = (c, z, xn, yn, pn)
    kept = 2
    stages = []
    for total, (_, _, _, _, final) in zip((rq_ref, ru_ref, rd_ref), arrays):
        own = total.at[z]
        copy = pltpu.make_async_copy(own, final.at[k, t], local_sems.at[kept])
        copy.start()
        kept += 1
        stages.append((plane_share(copies, own, final, ids, k, t, half), copy))
    source_here = t == z
    source_x, source_y, source_d = flip(t, 1) == z, flip(t, 2) == z, flip(flip(t, 1), 2) == z
    o_own = pltpu.make_async_copy(ro_ref, fo_ref.at[k], local_sems.at[kept])
    top, bottom = pl.ds(0, half // 2), pl.ds(half // 2, half // 2)
    o_x = copies.make(ro_ref, fo_ref.at[k], (xn, z), when=source_here)
    o_y = copies.make(ro_ref, fo_ref.at[k], (yn, z), when=source_here)

    @pl.when(source_here)
    def _():
        o_own.start()
        o_x.start()
        o_y.start()

    o_fx = copies.make(fo_ref.at[k, top], fo_ref.at[k, top], (yn, z), when=source_x)
    o_fy = copies.make(fo_ref.at[k, bottom], fo_ref.at[k, bottom], (xn, z), when=source_y)
    o_swap = copies.make(fo_ref.at[k], fo_ref.at[k], (pn, z))

    for (on_x, _, _, _), _ in stages:
        on_x()
    for (_, on_y, _, _), _ in stages:
        on_y()

    @pl.when(source_x)
    def _():
        o_x.wait_recv()
        o_fx.start()

    @pl.when(source_y)
    def _():
        o_y.wait_recv()
        o_fy.start()

    pl.when(source_here)(o_own.wait)

    @pl.when(source_d)
    def _():
        o_fx.wait_recv()
        o_fy.wait_recv()

    o_swap.start()
    for (_, _, on_diagonal, _), _ in stages:
        on_diagonal()
    for copy in vec_plane:
        copy.wait_recv()
    vsum = vs_ref[...]
    for peer in plane:
        vsum = vsum + vp_ref[peer]
    vsum_ref[...] = vsum
    for (_, _, _, swaps), copy in stages:
        for swap in swaps:
            swap.wait_recv()
        copy.wait()
    o_swap.wait_recv()
    for copy in scattered:
        copy.wait_recv()
    own_e.wait()
    own_o.wait()
    copies.finish()


def plane_share(copies, own, final, ids, k, t, rows):
    c, z, xn, yn, pn = ids
    top, bottom = pl.ds(0, rows // 2), pl.ds(rows // 2, rows // 2)
    tx, ty, td = flip(t, 1), flip(t, 2), flip(flip(t, 1), 2)
    to_x = copies.make(own, final.at[k, t], (xn, z))
    to_y = copies.make(own, final.at[k, t], (yn, z))
    to_p = copies.make(own, final.at[k, t], (pn, z))
    to_x.start()
    to_y.start()
    to_p.start()
    swaps = [to_p]
    hop_y = copies.make(final.at[k, tx, top], final.at[k, tx, top], (yn, z))
    hop_x = copies.make(final.at[k, ty, bottom], final.at[k, ty, bottom], (xn, z))

    def swap(place):
        copy = copies.make(place, place, (pn, z))
        copy.start()
        swaps.append(copy)

    def on_x():
        to_x.wait_recv()
        hop_y.start()
        swap(final.at[k, tx])

    def on_y():
        to_y.wait_recv()
        hop_x.start()
        swap(final.at[k, ty])

    def on_diagonal():
        hop_y.wait_recv()
        swap(final.at[k, td, top])
        hop_x.wait_recv()
        swap(final.at[k, td, bottom])

    return on_x, on_y, on_diagonal, swaps


NN = (((1,), (0,)), ((), ()))
NT = (((1,), (1,)), ((), ()))
TN = (((0,), (0,)), ((), ()))


def mm(left, right, dims=NN):
    return lax.dot_general(left, right, dims, preferred_element_type=jnp.float32)


def norm_rows(values_in):
    centre = jnp.mean(values_in, axis=-1, keepdims=True)
    mean_removed = values_in - centre
    inverse_deviation = lax.rsqrt(
        jnp.mean(mean_removed * mean_removed, axis=-1, keepdims=True) + EPS
    )
    return mean_removed * inverse_deviation, inverse_deviation


def slice_kernel(wqkv_ref, wup_ref, wq_ref, wu_ref):
    t = lax.axis_index("ctx") // 2
    part = wq_ref.shape[1] // 3
    chips = wqkv_ref.shape[1] // wq_ref.shape[1]
    for chip in range(chips):

        @pl.when(t == chip)
        def _():
            for source, target in ((wqkv_ref, wq_ref), (wup_ref, wu_ref)):
                for piece in range(target.shape[1] // part):
                    first = (piece * chips + chip) * part
                    target[:, piece * part : (piece + 1) * part] = source[:, first : first + part]


def qkv_kernel(pos_ref, h_ref, w_ref, b_ref, gain_ref, shift_ref, rope_ref, q_ref, k_ref, v_ref, kt_ref, vt_ref):
    step = pl.program_id(0)
    part = q_ref.shape[1]
    standardized, _ = norm_rows(h_ref[0].astype(jnp.float32))
    normed = (standardized * gain_ref[...] + shift_ref[...]).astype(jnp.bfloat16)
    projected = mm(normed, w_ref[...]) + b_ref[...]
    both = projected[:, : 2 * part]
    wide = both.shape[1]
    tables = [
        jnp.concatenate([rope_ref[:, 128 * n : 128 * n + 128]] * (wide // 128), axis=1)
        for n in range(3)
    ]
    turned = (
        both * tables[0]
        + pltpu.roll(both, wide - ROT // 2, 1) * tables[1]
        + pltpu.roll(both, ROT // 2, 1) * tables[2]
    )
    blocks = both.shape[0] // BLK
    for block in range(blocks):
        place = pl.ds(pl.multiple_of(pos_ref[step * blocks + block] * BLK, BLK), BLK)
        rows = slice(block * BLK, (block + 1) * BLK)
        q_ref[place, :] = (turned[rows, :part].astype(jnp.bfloat16) * (HD**-0.5)).astype(jnp.bfloat16)
        key_rows = turned[rows, part:]
        value_rows = projected[rows, 2 * part :]
        k_ref[place, :] = key_rows.astype(jnp.bfloat16)
        v_ref[place, :] = value_rows.astype(jnp.bfloat16)
        kt_ref[:, place] = key_rows.T.astype(jnp.bfloat16)
        vt_ref[:, place] = value_rows.T.astype(jnp.bfloat16)


def head_rows(rows, head):
    lanes = lax.broadcasted_iota(jnp.int32, rows.shape, 1)
    inside = (lanes >= head * HD) & (lanes < (head + 1) * HD)
    return jnp.where(inside, rows, jnp.zeros_like(rows))


def attention_kernel(pos_ref, q_ref, k_ref, vt_ref, o_ref, lse_ref):
    step = pl.program_id(0)
    part = k_ref.shape[1]
    heads = part // HD
    kstep = 2 * BLK
    position = pos_ref[step]
    query = q_ref[pl.ds(pl.multiple_of(position * BLK, BLK), BLK), :]
    per_head = [head_rows(query, head) for head in range(heads)]

    def visit(number, state, masked):
        place = pl.ds(pl.multiple_of(number * kstep, kstep), kstep)
        keys = k_ref[place, :]
        result = []
        for head in range(heads):
            top, total, acc = state[head]
            logits = mm(keys, per_head[head], NT)
            if masked:
                key_pos = number * kstep + lax.broadcasted_iota(jnp.int32, logits.shape, 0)
                query_pos = position * BLK + lax.broadcasted_iota(jnp.int32, logits.shape, 1)
                logits = jnp.where(key_pos <= query_pos, logits, NEG)
            new_top = jnp.maximum(top, jnp.max(logits, axis=0, keepdims=True))
            fade = jnp.exp(top - new_top)
            probs = jnp.exp(logits - new_top)
            total = total * fade + jnp.sum(probs, axis=0, keepdims=True)
            values = vt_ref[head * HD : (head + 1) * HD, place]
            acc = acc * fade + mm(values, probs.astype(jnp.bfloat16))
            result.append((new_top, total, acc))
        return tuple(result)

    start = tuple(
        (
            jnp.full((1, BLK), NEG, jnp.float32),
            jnp.zeros((1, BLK), jnp.float32),
            jnp.zeros((HD, BLK), jnp.float32),
        )
        for _ in range(heads)
    )
    last = position // 2
    state = lax.fori_loop(0, last, lambda n, s: visit(n, s, False), start)
    state = visit(last, state, True)
    rows = jnp.concatenate([acc / total for _, total, acc in state], axis=0)
    o_ref[...] = rows.T.astype(jnp.bfloat16)
    for head in range(heads):
        lse_ref[0, head : head + 1, :] = state[head][0] + jnp.log(state[head][1])


def attention_grad_kernel(
    pos_ref, order_ref, q_ref, k_ref, v_ref, kt_ref, do_ref, o_ref, lse_ref, dq_ref, own_ref, sent_ref, dk_ref, dv_ref
):
    step = pl.program_id(0)
    part = k_ref.shape[1]
    heads = part // HD
    kstep = 2 * BLK
    position = pos_ref[step]

    @pl.when(step == 0)
    def _():
        dk_ref[...] = jnp.zeros_like(dk_ref)
        dv_ref[...] = jnp.zeros_like(dv_ref)

    query = q_ref[pl.ds(pl.multiple_of(position * BLK, BLK), BLK), :]
    d_out = do_ref[...]
    queries = jnp.concatenate([head_rows(query, head) for head in range(heads)], axis=0)
    d_outs = jnp.concatenate([head_rows(d_out, head) for head in range(heads)], axis=0)
    product = d_out.astype(jnp.float32) * o_ref[...].astype(jnp.float32)
    head_of = lax.broadcasted_iota(jnp.int32, (8, part), 1) // HD
    pick = (head_of == lax.broadcasted_iota(jnp.int32, (8, part), 0)).astype(jnp.float32)
    delta = lax.dot_general(
        pick, product, NT, precision=lax.Precision.HIGHEST, preferred_element_type=jnp.float32
    )
    log_total = lse_ref[0]

    def visit(number, state, masked):
        place = pl.ds(pl.multiple_of(number * kstep, kstep), kstep)
        keys, values = k_ref[place, :], v_ref[place, :]
        probs_all, d_logits_all, result = [], [], []
        for head in range(heads):
            rows = slice(head * BLK, (head + 1) * BLK)
            logits = mm(keys, queries[rows], NT)
            probs = jnp.exp(logits - log_total[head : head + 1, :])
            if masked:
                key_pos = number * kstep + lax.broadcasted_iota(jnp.int32, logits.shape, 0)
                query_pos = position * BLK + lax.broadcasted_iota(jnp.int32, logits.shape, 1)
                probs = jnp.where(key_pos <= query_pos, probs, 0.0)
            d_probs = mm(values, d_outs[rows], NT)
            d_logits = (probs * (d_probs - delta[head : head + 1, :])).astype(jnp.bfloat16)
            probs_all.append(probs.astype(jnp.bfloat16))
            d_logits_all.append(d_logits)
            result.append(state[head] + mm(kt_ref[head * HD : (head + 1) * HD, place], d_logits))
        dv_ref[place, :] += mm(jnp.concatenate(probs_all, axis=1), d_outs)
        dk_ref[place, :] += mm(jnp.concatenate(d_logits_all, axis=1), queries)
        return tuple(result)

    start = tuple(jnp.zeros((HD, BLK), jnp.float32) for _ in range(heads))
    last = position // 2
    state = lax.fori_loop(0, last, lambda n, s: visit(n, s, False), start)
    state = visit(last, state, True)
    dq_ref[...] = jnp.concatenate(state, axis=0).T * (HD**-0.5)

    @pl.when(step == pl.num_programs(0) - 1)
    def _():
        blocks = own_ref.shape[0] // BLK
        for block in range(2 * blocks):
            place = pl.ds(pl.multiple_of(order_ref[block] * BLK, BLK), BLK)
            if block < blocks:
                rows = slice(block * BLK, (block + 1) * BLK)
                own_ref[rows, :part] = dk_ref[place, :]
                own_ref[rows, part:] = dv_ref[place, :]
            else:
                rows = slice((block - blocks) * BLK, (block - blocks + 1) * BLK)
                sent_ref[rows, :part] = dk_ref[place, :].astype(jnp.bfloat16)
                sent_ref[rows, part:] = dv_ref[place, :].astype(jnp.bfloat16)


def swap_kernel(source_ref, target_ref, send_sem, recv_sem):
    c, z = lax.axis_index("ctx"), lax.axis_index("fsdp")
    partner = (flip(c, 1), z)
    greet([(partner, None)])
    copy = pltpu.make_async_remote_copy(
        src_ref=source_ref,
        dst_ref=target_ref,
        send_sem=send_sem,
        recv_sem=recv_sem,
        device_id=partner,
        device_id_type=MESH_IDS,
    )
    copy.start()
    copy.wait()


def qkv_grad_kernel(
    h_ref, dq_ref, own_ref, got_ref, rope_ref, w_ref, gain_ref, shift_ref, gain2_ref, d2_ref,
    gq_ref, e_ref, bias_ref, norm_ref, acc_ref,
):
    step = pl.program_id(0)
    part = dq_ref.shape[1]

    @pl.when(step == 0)
    def _():
        acc_ref[...] = jnp.zeros_like(acc_ref)
        bias_ref[...] = jnp.zeros_like(bias_ref)
        norm_ref[...] = jnp.zeros_like(norm_ref)

    standardized, _ = norm_rows(h_ref[0].astype(jnp.float32))
    normed = (standardized * gain_ref[...] + shift_ref[...]).astype(jnp.bfloat16)
    key_value = own_ref[...] + got_ref[...].astype(jnp.float32)
    both = jnp.concatenate([dq_ref[...], key_value[:, :part]], axis=1)
    wide = both.shape[1]
    tables = [
        jnp.concatenate([rope_ref[:, 128 * n : 128 * n + 128]] * (wide // 128), axis=1)
        for n in range(3)
    ]
    turned = (
        both * tables[0]
        - pltpu.roll(both, wide - ROT // 2, 1) * tables[1]
        - pltpu.roll(both, ROT // 2, 1) * tables[2]
    )
    d_qkv = jnp.concatenate([turned, key_value[:, part:]], axis=1)
    d_qkv16 = d_qkv.astype(jnp.bfloat16)
    bias_ref[...] += jnp.sum(d_qkv, axis=0, keepdims=True)
    acc_ref[...] += mm(normed, d_qkv16, TN)
    d_normed = mm(d_qkv16, w_ref[...], NT)
    norm_ref[0:1, :] += jnp.sum(d_normed * standardized, axis=0, keepdims=True)
    norm_ref[1:2, :] += jnp.sum(d_normed, axis=0, keepdims=True)
    e_ref[...] = (d_normed * gain_ref[...] + d2_ref[...] * gain2_ref[...]).astype(jnp.bfloat16)

    @pl.when(step == pl.num_programs(0) - 1)
    def _():
        gq_ref[...] = acc_ref[...].astype(jnp.bfloat16)


def assemble_kernel(fq_ref, fu_ref, fd_ref, fo_ref, gq_ref, gu_ref, gd_ref, go_ref):
    cores, chips, half, _ = fq_ref.shape
    part = fq_ref.shape[3] // 3
    for core in range(cores):
        rows = slice(core * half, (core + 1) * half)
        go_ref[rows, :] = fo_ref[core].astype(jnp.float32)
        for chip in range(chips):
            for source, target in ((fq_ref, gq_ref), (fu_ref, gu_ref)):
                for piece in range(source.shape[3] // part):
                    first = (piece * chips + chip) * part
                    target[rows, first : first + part] = source[
                        core, chip, :, piece * part : (piece + 1) * part
                    ].astype(jnp.float32)
            first = chip * cores * half + core * half
            gd_ref[first : first + half, :] = fd_ref[core, chip].astype(jnp.float32)


def rotary_lanes(position_list):
    half_rot = ROT // 2
    inverse = jnp.power(jnp.float32(10000.0), -2.0 * jnp.arange(half_rot, dtype=jnp.float32) / ROT)
    angle = position_list.astype(jnp.float32)[:, None] * inverse[None, :]
    cosine, sine = jnp.cos(angle), jnp.sin(angle)
    rest = jnp.zeros((position_list.shape[0], HD - ROT), jnp.float32)
    nothing = jnp.zeros_like(sine)
    one = [cosine, cosine, rest + 1.0]
    upper = [-sine, nothing, rest]
    lower = [nothing, sine, rest]
    return jnp.concatenate((one + one) + (upper + upper) + (lower + lower), axis=1)


VMEM_SPEC = pl.BlockSpec(memory_space=pltpu.VMEM)
ANY_SPEC = pl.BlockSpec(memory_space=pl.ANY)
VMEM_LIMIT = 56 * 1024 * 1024


def shape_of(shape, kind=jnp.bfloat16):
    return jax.ShapeDtypeStruct(shape, kind)


def sliced_layer(
    nz,
    hidden_in,
    norm1_gain,
    attention_norm_bias,
    qkv_weight,
    qkv_bias,
    out_weight,
    out_bias,
    norm2_gain,
    feedforward_norm_bias,
    up_weight,
    up_bias,
    down_weight,
    down_bias,
    cotangent,
    block_order,
):
    f32, b16 = jnp.float32, jnp.bfloat16
    h, g = hidden_in[0], cotangent[0]
    local_rows, width = h.shape
    chips = lax.axis_size("ctx") // 2
    c, z = lax.axis_index("ctx"), lax.axis_index("fsdp")
    k, t = c % 2, c // 2
    shard = qkv_weight.shape[0]
    part = width // chips
    heads = part // HD
    hidden = up_weight.shape[1] // chips
    rows = chips * local_rows
    all_rows = 2 * rows
    sides = local_rows // BLK

    order = block_order.reshape(chips, 2, sides)
    order = jnp.stack([order[:, k], order[:, 1 - k]]).reshape(2 * chips * sides)
    own_order = order[: chips * sides]
    positions = (order[:, None] * BLK + jnp.arange(BLK, dtype=jnp.int32)[None, :]).reshape(all_rows)
    rope = rotary_lanes(positions)

    small = [norm1_gain, attention_norm_bias, norm2_gain, feedforward_norm_bias, out_bias, down_bias, qkv_bias, up_bias]
    cuts = [0]
    for vector in small:
        cuts.append(cuts[-1] + vector.shape[0])
    small_rows = -(-cuts[-1] // (16 * 128)) * 16
    sm = jnp.pad(jnp.concatenate(small), (0, small_rows * 128 - cuts[-1])).reshape(small_rows, 128)

    wq, wu = pl.pallas_call(
        slice_kernel,
        out_shape=(shape_of((shard, 3 * part)), shape_of((shard, hidden))),
        in_specs=[VMEM_SPEC] * 2,
        out_specs=(VMEM_SPEC,) * 2,
        name="slice_weights",
    )(qkv_weight, up_weight)

    hall, gall, wq4, wu4, wd4, wo1, sm4 = pl.pallas_call(
        functools.partial(gather_kernel, nz),
        out_shape=(
            shape_of((2, chips, local_rows, width)),
            shape_of((chips, local_rows, width)),
            shape_of((nz, shard, 3 * part)),
            shape_of((nz, shard, hidden)),
            shape_of((nz, shard, width)),
            shape_of((part, width)),
            shape_of((nz, small_rows, 128)),
        ),
        in_specs=[VMEM_SPEC] * 7,
        out_specs=(ANY_SPEC,) * 7,
        scratch_shapes=[
            pltpu.SemaphoreType.DMA((96,)),
            pltpu.SemaphoreType.DMA((96,)),
            pltpu.SemaphoreType.DMA((8,)),
        ],
        compiler_params=pltpu.CompilerParams(collective_id=0, has_side_effects=True),
        name="gather",
    )(h, g, wq, wu, down_weight, out_weight, sm)

    flat = sm4.reshape(nz, small_rows * 128).astype(f32)
    gain1, shift1, gain2, shift2, bout, bdown = (
        flat[:, cuts[n] : cuts[n + 1]].reshape(1, width) for n in range(6)
    )
    bq = lax.dynamic_slice_in_dim(
        flat[:, cuts[6] : cuts[7]].reshape(3, chips, part), t, 1, 1
    ).reshape(1, 3 * part)
    bu = lax.dynamic_slice_in_dim(
        flat[:, cuts[7] : cuts[8]].reshape(hidden // part, chips, part), t, 1, 1
    ).reshape(1, hidden)
    wq_full = wq4.reshape(width, 3 * part)
    wu_full = wu4.reshape(width, hidden)
    wd_full = wd4.reshape(hidden, width)
    h_blocks = hall.reshape(2 * chips, local_rows, width)

    def whole(*shape):
        return pl.BlockSpec(shape, lambda i, *_: (0,) * len(shape))

    q, key_rows, value_rows, keys_t, values_t = pl.pallas_call(
        qkv_kernel,
        grid_spec=pltpu.PrefetchScalarGridSpec(
            num_scalar_prefetch=1,
            grid=(2 * chips,),
            in_specs=[
                pl.BlockSpec((1, local_rows, width), lambda i, *_: (i, 0, 0)),
                whole(width, 3 * part),
                whole(1, 3 * part),
                whole(1, width),
                whole(1, width),
                pl.BlockSpec((local_rows, 384), lambda i, *_: (i, 0)),
            ],
            out_specs=(
                whole(all_rows, part),
                whole(all_rows, part),
                whole(all_rows, part),
                whole(part, all_rows),
                whole(part, all_rows),
            ),
        ),
        out_shape=(shape_of((all_rows, part)),) * 3 + (shape_of((part, all_rows)),) * 2,
        compiler_params=pltpu.CompilerParams(vmem_limit_bytes=VMEM_LIMIT),
        name="qkv",
    )(order, h_blocks, wq_full, bq, gain1, shift1, rope)

    attended, log_total = pl.pallas_call(
        attention_kernel,
        grid_spec=pltpu.PrefetchScalarGridSpec(
            num_scalar_prefetch=1,
            grid=(chips * sides,),
            in_specs=[whole(all_rows, part), whole(all_rows, part), whole(part, all_rows)],
            out_specs=(
                pl.BlockSpec((BLK, part), lambda i, *_: (i, 0)),
                pl.BlockSpec((1, 8, BLK), lambda i, *_: (i, 0, 0)),
            ),
        ),
        out_shape=(shape_of((rows, part)), shape_of((chips * sides, 8, BLK), f32)),
        compiler_params=pltpu.CompilerParams(vmem_limit_bytes=VMEM_LIMIT),
        name="attention",
    )(own_order, q, key_rows, values_t)

    h_own = hall[0].reshape(rows, width).astype(f32)
    g_own = gall.reshape(rows, width)
    standardized, _ = norm_rows(h_own)
    normed2 = (standardized * gain2 + shift2).astype(b16)
    up = mm(normed2, wu_full) + bu
    act = gelu_exact(up).astype(b16)
    d_up = mm(g_own, wd_full, NT) * gelu_slope(up)
    d_up16 = d_up.astype(b16)
    out_part = (mm(attended, wo1) + mm(act, wd_full)).astype(b16)
    grad_d = mm(act, g_own, TN).astype(b16)
    grad_u = mm(normed2, d_up16, TN).astype(b16)
    grad_bu = jnp.sum(d_up, axis=0)
    d_normed2 = mm(d_up16, wu_full, NT)
    grad_gain2 = jnp.sum(d_normed2 * standardized, axis=0)
    grad_shift2 = jnp.sum(d_normed2, axis=0)
    grad_o = mm(attended, g_own, TN).astype(b16)
    d_att = mm(g_own, wo1, NT).astype(b16)

    d_query, kv_own, kv_sent = pl.pallas_call(
        attention_grad_kernel,
        grid_spec=pltpu.PrefetchScalarGridSpec(
            num_scalar_prefetch=2,
            grid=(chips * sides,),
            in_specs=[
                whole(all_rows, part),
                whole(all_rows, part),
                whole(all_rows, part),
                whole(part, all_rows),
                pl.BlockSpec((BLK, part), lambda i, *_: (i, 0)),
                pl.BlockSpec((BLK, part), lambda i, *_: (i, 0)),
                pl.BlockSpec((1, 8, BLK), lambda i, *_: (i, 0, 0)),
            ],
            out_specs=(
                pl.BlockSpec((BLK, part), lambda i, *_: (i, 0)),
                whole(rows, 2 * part),
                whole(rows, 2 * part),
            ),
            scratch_shapes=[pltpu.VMEM((all_rows, part), f32), pltpu.VMEM((all_rows, part), f32)],
        ),
        out_shape=(
            shape_of((rows, part), f32),
            shape_of((rows, 2 * part), f32),
            shape_of((rows, 2 * part)),
        ),
        compiler_params=pltpu.CompilerParams(vmem_limit_bytes=VMEM_LIMIT),
        name="attention_grad",
    )(own_order, order, q, key_rows, value_rows, keys_t, d_att, attended, log_total)

    kv_got = pl.pallas_call(
        swap_kernel,
        out_shape=shape_of((rows, 2 * part)),
        in_specs=[ANY_SPEC],
        out_specs=ANY_SPEC,
        scratch_shapes=[pltpu.SemaphoreType.DMA, pltpu.SemaphoreType.DMA],
        compiler_params=pltpu.CompilerParams(collective_id=1, has_side_effects=True),
        name="swap",
    )(kv_sent)

    by_rows = lambda cols: pl.BlockSpec((local_rows, cols), lambda i, *_: (i, 0))
    grad_q, e_part, grad_bq, grad_norm1 = pl.pallas_call(
        qkv_grad_kernel,
        grid=(chips,),
        in_specs=[
            pl.BlockSpec((1, local_rows, width), lambda i: (i, 0, 0)),
            by_rows(part),
            by_rows(2 * part),
            by_rows(2 * part),
            by_rows(384),
            whole(width, 3 * part),
            whole(1, width),
            whole(1, width),
            whole(1, width),
            by_rows(width),
        ],
        out_specs=(
            whole(width, 3 * part),
            by_rows(width),
            whole(1, 3 * part),
            whole(8, width),
        ),
        out_shape=(
            shape_of((width, 3 * part)),
            shape_of((rows, width)),
            shape_of((1, 3 * part), f32),
            shape_of((8, width), f32),
        ),
        scratch_shapes=[pltpu.VMEM((width, 3 * part), f32)],
        compiler_params=pltpu.CompilerParams(vmem_limit_bytes=VMEM_LIMIT),
        name="qkv_grad",
    )(h_blocks, d_query, kv_own, kv_got, rope, wq_full, gain1, shift1, gain2, d_normed2)

    def spread(values, pieces):
        slots = jnp.arange(chips)[None, :, None] == t
        return jnp.where(slots, values.reshape(pieces, 1, part), 0.0).reshape(nz, -1)

    vectors = jnp.concatenate(
        [
            grad_norm1[0].reshape(nz, -1),
            grad_norm1[1].reshape(nz, -1),
            grad_gain2.reshape(nz, -1),
            grad_shift2.reshape(nz, -1),
            jnp.sum(g.astype(f32), axis=0).reshape(nz, -1),
            spread(grad_bq, 3),
            spread(grad_bu, hidden // part),
        ],
        axis=1,
    )
    vec_used = vectors.shape[1]
    vec_rows = -(-vec_used // (8 * 128)) * 8
    vectors = jnp.pad(vectors, ((0, 0), (0, vec_rows * 128 - vec_used))).reshape(nz, vec_rows, 128)

    half = shard // 2
    widths = (3 * part, hidden, width)
    grads = (
        grad_q.reshape(nz, shard, 3 * part),
        grad_u.reshape(nz, shard, hidden),
        grad_d.reshape(nz, shard, width),
    )
    eall, oall, fq, fu, fd, fo, vsum = pl.pallas_call(
        functools.partial(reduce_kernel, nz),
        out_shape=(
            shape_of((chips, local_rows, width)),
            shape_of((chips, local_rows, width)),
        )
        + tuple(shape_of((2, chips, half, cols)) for cols in widths)
        + (shape_of((2, half, width)), shape_of((vec_rows, 128), f32)),
        in_specs=[VMEM_SPEC] * 7,
        out_specs=(ANY_SPEC,) * 6 + (VMEM_SPEC,),
        scratch_shapes=[pltpu.VMEM((nz, half, cols), b16) for cols in widths]
        + [pltpu.VMEM((half, width), b16)]
        + [pltpu.VMEM((nz, half, cols), b16) for cols in widths]
        + [pltpu.VMEM((half, width), b16)]
        + [pltpu.VMEM((nz, half, cols), b16) for cols in widths]
        + [pltpu.VMEM((half, width), b16)]
        + [
            pltpu.VMEM((nz, vec_rows, 128), f32),
            pltpu.VMEM((vec_rows, 128), f32),
            pltpu.VMEM((2 * chips, vec_rows, 128), f32),
            pltpu.SemaphoreType.DMA((96,)),
            pltpu.SemaphoreType.DMA((96,)),
            pltpu.SemaphoreType.DMA((8,)),
        ],
        compiler_params=pltpu.CompilerParams(
            collective_id=2, has_side_effects=True, vmem_limit_bytes=VMEM_LIMIT
        ),
        name="reduce",
    )(
        e_part.reshape(chips, local_rows, width),
        out_part.reshape(chips, local_rows, width),
        *grads,
        grad_o,
        vectors,
    )

    grad_qkv, grad_up, grad_down, grad_out = pl.pallas_call(
        assemble_kernel,
        out_shape=(
            shape_of(qkv_weight.shape, f32),
            shape_of(up_weight.shape, f32),
            shape_of(down_weight.shape, f32),
            shape_of(out_weight.shape, f32),
        ),
        in_specs=[VMEM_SPEC] * 4,
        out_specs=(VMEM_SPEC,) * 4,
        compiler_params=pltpu.CompilerParams(vmem_limit_bytes=VMEM_LIMIT),
        name="assemble",
    )(fq, fu, fd, fo)

    residual = h.astype(f32)
    own_standardized, own_deviation = norm_rows(residual)
    hidden_out = (residual + bout + bdown + jnp.sum(oall.astype(f32), axis=0)).astype(b16)
    e_total = jnp.sum(eall.astype(f32), axis=0)
    hidden_grad = g.astype(f32) + own_deviation * (
        e_total
        - jnp.mean(e_total, axis=-1, keepdims=True)
        - own_standardized * jnp.mean(e_total * own_standardized, axis=-1, keepdims=True)
    )
    final = vsum.reshape(-1)
    sizes = [shard] * 5 + [qkv_bias.shape[0], up_bias.shape[0]]
    pieces, first = [], 0
    for size in sizes:
        pieces.append(final[first : first + size])
        first += size
    g_gain1, g_shift1, g_gain2, g_shift2, g_bias, g_bq, g_bu = pieces
    return (
        hidden_out[None],
        hidden_grad[None],
        g_gain1,
        g_shift1,
        grad_qkv,
        g_bq,
        grad_out,
        g_bias,
        g_gain2,
        g_shift2,
        grad_up,
        g_bu,
        grad_down,
        g_bias,
    )


def sliced_fits(mesh):
    return mesh.shape["ctx"] == 8 and mesh.shape["fsdp"] == 4


def solution(mesh):
    in_specs = (
        P("fsdp", "ctx", None),
        P("fsdp"),
        P("fsdp"),
        P("fsdp", None),
        P("fsdp"),
        P("fsdp", None),
        P("fsdp"),
        P("fsdp"),
        P("fsdp"),
        P("fsdp", None),
        P("fsdp"),
        P("fsdp", None),
        P("fsdp"),
        P("fsdp", "ctx", None),
        P(),
    )
    out_specs = (
        P("fsdp", "ctx", None),
        P("fsdp", "ctx", None),
        P("fsdp"),
        P("fsdp"),
        P("fsdp", None),
        P("fsdp"),
        P("fsdp", None),
        P("fsdp"),
        P("fsdp"),
        P("fsdp"),
        P("fsdp", None),
        P("fsdp"),
        P("fsdp", None),
        P("fsdp"),
    )
    local = whole_parameter_layer
    if sliced_fits(mesh):
        local = functools.partial(sliced_layer, mesh.shape["fsdp"])
    return jax.shard_map(local, mesh=mesh, in_specs=in_specs, out_specs=out_specs, check_vma=False)
```

```python
import functools
import math
import types

import jax
import jax.numpy as jnp
import numpy as np
from jax import lax
from jax.experimental import pallas as pl
from jax.experimental.pallas import tpu as pltpu
from jax.sharding import PartitionSpec as P

H = 12
HD = 64
ROT = 16
BLK = 128


EPS = 1e-05
NEG = -1e30
SQRT_HALF = 0.7071067811865476
INV_ROOT_TWO_PI = 0.3989422804014327


def apply_layer_norm(values_in, norm_gain, norm_bias):
    centre = jnp.mean(values_in, axis=-1, keepdims=True)
    mean_removed = values_in - centre
    inverse_deviation = lax.rsqrt(
        jnp.mean(mean_removed * mean_removed, axis=-1, keepdims=True) + EPS
    )
    standardized = mean_removed * inverse_deviation
    return (standardized * norm_gain + norm_bias, standardized, inverse_deviation)


def layer_norm_backward(output_gradient, standardized, inverse_deviation, norm_gain):
    gain_scaled = output_gradient * norm_gain
    return inverse_deviation * (
        gain_scaled
        - jnp.mean(gain_scaled, axis=-1, keepdims=True)
        - standardized * jnp.mean(gain_scaled * standardized, axis=-1, keepdims=True)
    )


def gelu_exact(values_in):
    return 0.5 * values_in * (1.0 + lax.erf(values_in * SQRT_HALF))


def gelu_slope(values_in):
    return (
        0.5 * (1.0 + lax.erf(values_in * SQRT_HALF))
        + values_in * jnp.exp(-0.5 * values_in * values_in) * INV_ROOT_TWO_PI
    )


def rotary_tables(position_list):
    half_rot = ROT // 2
    inverse = jnp.power(jnp.float32(10000.0), -2.0 * jnp.arange(half_rot, dtype=jnp.float32) / ROT)
    angle = position_list.astype(jnp.float32)[:, None] * inverse[None, :]
    return (jnp.cos(angle)[:, None, :], jnp.sin(angle)[:, None, :])


def rotate(tensor, cosine, sine):
    half_rot = ROT // 2
    first_half = tensor[..., :half_rot]
    second_half = tensor[..., half_rot:ROT]
    return jnp.concatenate(
        [
            first_half * cosine - second_half * sine,
            second_half * cosine + first_half * sine,
            tensor[..., ROT:],
        ],
        axis=-1,
    )


def rotate_back(tensor, cosine, sine):
    half_rot = ROT // 2
    first_half = tensor[..., :half_rot]
    second_half = tensor[..., half_rot:ROT]
    return jnp.concatenate(
        [
            first_half * cosine + second_half * sine,
            second_half * cosine - first_half * sine,
            tensor[..., ROT:],
        ],
        axis=-1,
    )


def masked_logits(query_block, key_block, query_pos, key_pos):
    logits = jnp.einsum(
        "qhd,khd->hqk", query_block, key_block, preferred_element_type=jnp.float32
    ) * (1.0 / math.sqrt(HD))
    return jnp.where(key_pos[None, None, :] <= query_pos[None, :, None], logits, NEG)


def block_terms(
    query_block, dout_block, total_t, delta_t, query_pos, key_block, value_block, key_pos
):
    logits = masked_logits(query_block, key_block, query_pos, key_pos)
    probs_wide = jnp.exp(logits - total_t[:, :, None])
    dprobs = jnp.einsum("qhd,khd->hqk", dout_block, value_block, preferred_element_type=jnp.float32)
    d_logits = (probs_wide * (dprobs - delta_t[:, :, None]) * (1.0 / math.sqrt(HD))).astype(
        jnp.bfloat16
    )
    return (probs_wide.astype(jnp.bfloat16), d_logits)


def keep_state(state_in):
    return state_in


def forward_attention(query, keys_all, values_all, own_pos, all_pos):
    local_rows = query.shape[0]
    seq_rows = keys_all.shape[0]
    qstep = min(512, local_rows)
    kstep = min(512, seq_rows)
    latest = jnp.max(own_pos)

    def stats_step(number, state_in):
        key_block = lax.dynamic_slice_in_dim(keys_all, number * kstep, kstep, 0)
        key_pos = lax.dynamic_slice_in_dim(all_pos, number * kstep, kstep, 0)

        def stats_live(state_now):
            running_max, running_sum = state_now
            logits = masked_logits(query, key_block, own_pos, key_pos)
            new_max = jnp.maximum(running_max, jnp.max(logits, axis=-1))
            running_sum = running_sum * jnp.exp(running_max - new_max) + jnp.sum(
                jnp.exp(logits - new_max[:, :, None]), axis=-1
            )
            return (new_max, running_sum)

        return lax.cond(jnp.min(key_pos) <= latest, stats_live, keep_state, state_in)

    start_state = (jnp.full((H, qstep), NEG, jnp.float32), jnp.zeros((H, qstep), jnp.float32))
    running_max, running_sum = lax.fori_loop(0, seq_rows // kstep, stats_step, start_state)
    total_t = running_max + jnp.log(running_sum)

    def value_step(number, state_in):
        key_block = lax.dynamic_slice_in_dim(keys_all, number * kstep, kstep, 0)
        value_block = lax.dynamic_slice_in_dim(values_all, number * kstep, kstep, 0)
        key_pos = lax.dynamic_slice_in_dim(all_pos, number * kstep, kstep, 0)

        def value_live(state_now):
            logits = masked_logits(query, key_block, own_pos, key_pos)
            attn_probs = jnp.exp(logits - total_t[:, :, None]).astype(jnp.bfloat16)
            return state_now + jnp.einsum(
                "hqk,khd->qhd", attn_probs, value_block, preferred_element_type=jnp.float32
            )

        return lax.cond(jnp.min(key_pos) <= latest, value_live, keep_state, state_in)

    weighted = lax.fori_loop(
        0, seq_rows // kstep, value_step, jnp.zeros((qstep, H, HD), jnp.float32)
    )
    totals = total_t.T
    return (weighted, totals)


def query_grads(query, d_att, log_total, delta, own_pos, keys_all, values_all, all_pos):
    local_rows = query.shape[0]
    seq_rows = keys_all.shape[0]
    qstep = min(512, local_rows)
    kstep = min(512, seq_rows)
    key_grads = jnp.zeros((seq_rows, H, HD), jnp.float32)
    value_grads = jnp.zeros((seq_rows, H, HD), jnp.float32)
    total_t = log_total.T
    delta_t = delta.T
    latest = jnp.max(own_pos)

    def key_step(number, state_in):
        offset = number * kstep
        key_block = lax.dynamic_slice_in_dim(keys_all, offset, kstep, 0)
        value_block = lax.dynamic_slice_in_dim(values_all, offset, kstep, 0)
        key_pos = lax.dynamic_slice_in_dim(all_pos, offset, kstep, 0)

        def key_live(state_now):
            attn_probs, d_logits = block_terms(
                query, d_att, total_t, delta_t, own_pos, key_block, value_block, key_pos
            )
            d_query = state_now[0] + jnp.einsum(
                "hqk,khd->qhd", d_logits, key_block, preferred_element_type=jnp.float32
            )
            key_acc = state_now[1]
            value_acc = state_now[2]
            key_part = jnp.einsum(
                "hqk,qhd->khd", d_logits, query, preferred_element_type=jnp.float32
            )
            value_part = jnp.einsum(
                "hqk,qhd->khd", attn_probs, d_att, preferred_element_type=jnp.float32
            )
            key_acc = lax.dynamic_update_slice_in_dim(
                key_acc, lax.dynamic_slice_in_dim(key_acc, offset, kstep, 0) + key_part, offset, 0
            )
            value_acc = lax.dynamic_update_slice_in_dim(
                value_acc,
                lax.dynamic_slice_in_dim(value_acc, offset, kstep, 0) + value_part,
                offset,
                0,
            )
            return (d_query, key_acc, value_acc)

        return lax.cond(jnp.min(key_pos) <= latest, key_live, keep_state, state_in)

    start_state = (jnp.zeros((qstep, H, HD), jnp.float32),) + (key_grads, value_grads)
    result = lax.fori_loop(0, seq_rows // kstep, key_step, start_state)
    pieces = result[0]
    key_grads = result[1]
    value_grads = result[2]
    return (pieces, key_grads, value_grads)


def whole_parameter_layer(
    hidden_in,
    norm1_gain,
    attention_norm_bias,
    qkv_weight,
    qkv_bias,
    out_weight,
    out_bias,
    norm2_gain,
    feedforward_norm_bias,
    up_weight,
    up_bias,
    down_weight,
    down_bias,
    cotangent,
    block_order,
):
    (
        attention_norm_gain,
        attention_bias_term,
        wqkv,
        bqkv,
        wout,
        bout,
        feedforward_norm_gain,
        feedforward_bias_term,
        wup,
        bup,
        wdown,
        bdown,
    ) = (
        lax.all_gather(norm1_gain, "fsdp", axis=0, tiled=True),
        lax.all_gather(attention_norm_bias, "fsdp", axis=0, tiled=True),
        lax.all_gather(qkv_weight, "fsdp", axis=0, tiled=True),
        lax.all_gather(qkv_bias, "fsdp", axis=0, tiled=True),
        lax.all_gather(out_weight, "fsdp", axis=0, tiled=True),
        lax.all_gather(out_bias, "fsdp", axis=0, tiled=True),
        lax.all_gather(norm2_gain, "fsdp", axis=0, tiled=True),
        lax.all_gather(feedforward_norm_bias, "fsdp", axis=0, tiled=True),
        lax.all_gather(up_weight, "fsdp", axis=0, tiled=True),
        lax.all_gather(up_bias, "fsdp", axis=0, tiled=True),
        lax.all_gather(down_weight, "fsdp", axis=0, tiled=True),
        lax.all_gather(down_bias, "fsdp", axis=0, tiled=True),
    )
    width = H * HD
    hidden_rows = hidden_in[0]
    cotan_rows = cotangent[0]
    local_rows = hidden_rows.shape[0]
    ctx_count = lax.axis_size("ctx")
    ctx_rank = lax.axis_index("ctx")
    seq_rows = local_rows * ctx_count
    all_pos = (block_order[:, None] * BLK + jnp.arange(BLK, dtype=jnp.int32)[None, :]).reshape(
        seq_rows
    )
    own_pos = lax.dynamic_slice_in_dim(all_pos, ctx_rank * local_rows, local_rows, 0)
    cosine, sine = rotary_tables(own_pos)
    attention_norm_gain = attention_norm_gain.astype(jnp.float32)
    feedforward_norm_gain = feedforward_norm_gain.astype(jnp.float32)
    residual_stream = hidden_rows.astype(jnp.float32)
    attention_normed, attention_standardized, attention_inverse_deviation = apply_layer_norm(
        residual_stream, attention_norm_gain, attention_bias_term.astype(jnp.float32)
    )
    normed1_b = attention_normed.astype(jnp.bfloat16)
    projected = jnp.dot(normed1_b, wqkv, preferred_element_type=jnp.float32) + bqkv.astype(
        jnp.float32
    )
    query = rotate(projected[:, :width].reshape(local_rows, H, HD), cosine, sine).astype(
        jnp.bfloat16
    )
    key_rows = rotate(
        projected[:, width : 2 * width].reshape(local_rows, H, HD), cosine, sine
    ).astype(jnp.bfloat16)
    value_rows = projected[:, 2 * width :].astype(jnp.bfloat16)
    keys_all, values_all = (
        lax.all_gather(key_rows.reshape(local_rows, width), "ctx", axis=0, tiled=True),
        lax.all_gather(value_rows, "ctx", axis=0, tiled=True),
    )
    keys_all = keys_all.reshape(seq_rows, H, HD)
    values_all = values_all.reshape(seq_rows, H, HD)
    attended, log_total = forward_attention(query, keys_all, values_all, own_pos, all_pos)
    attended_b = attended.reshape(local_rows, width).astype(jnp.bfloat16)
    attn_out = jnp.dot(attended_b, wout, preferred_element_type=jnp.float32) + bout.astype(
        jnp.float32
    )
    feedforward_normed, feedforward_standardized, feedforward_inverse_deviation = apply_layer_norm(
        residual_stream, feedforward_norm_gain, feedforward_bias_term.astype(jnp.float32)
    )
    normed2_b = feedforward_normed.astype(jnp.bfloat16)
    up_rows = jnp.dot(normed2_b, wup, preferred_element_type=jnp.float32) + bup.astype(jnp.float32)
    act_b = gelu_exact(up_rows).astype(jnp.bfloat16)
    mlp_out = jnp.dot(act_b, wdown, preferred_element_type=jnp.float32) + bdown.astype(jnp.float32)
    hidden_out = (residual_stream + attn_out + mlp_out).astype(jnp.bfloat16)
    cotan_wide = cotan_rows.astype(jnp.float32)
    grad_wdown = jnp.einsum("tk,tn->kn", act_b, cotan_rows, preferred_element_type=jnp.float32)
    grad_bdown = jnp.sum(cotan_wide, axis=0)
    d_up = jnp.einsum(
        "tn,kn->tk", cotan_rows, wdown, preferred_element_type=jnp.float32
    ) * gelu_slope(up_rows)
    d_up16 = d_up.astype(jnp.bfloat16)
    grad_wup = jnp.einsum("tk,tn->kn", normed2_b, d_up16, preferred_element_type=jnp.float32)
    grad_bup = jnp.sum(d_up, axis=0)
    grad_feedforward_normed = jnp.einsum(
        "tn,kn->tk", d_up16, wup, preferred_element_type=jnp.float32
    )
    grad_feedforward_gain = jnp.sum(grad_feedforward_normed * feedforward_standardized, axis=0)
    grad_shift2 = jnp.sum(grad_feedforward_normed, axis=0)
    feedforward_branch_grad = layer_norm_backward(
        grad_feedforward_normed,
        feedforward_standardized,
        feedforward_inverse_deviation,
        feedforward_norm_gain,
    )
    grad_wout = jnp.einsum("tk,tn->kn", attended_b, cotan_rows, preferred_element_type=jnp.float32)
    d_att = jnp.einsum("tn,kn->tk", cotan_rows, wout, preferred_element_type=jnp.float32).astype(
        jnp.bfloat16
    )
    delta = jnp.sum(
        d_att.reshape(local_rows, H, HD).astype(jnp.float32)
        * attended_b.reshape(local_rows, H, HD).astype(jnp.float32),
        axis=-1,
    )
    d_att3 = d_att.reshape(local_rows, H, HD)
    d_query, key_grads, value_grads = query_grads(
        query, d_att3, log_total, delta, own_pos, keys_all, values_all, all_pos
    )
    d_key, d_value = (
        lax.psum_scatter(
            key_grads.reshape(seq_rows, width), "ctx", scatter_dimension=0, tiled=True
        ),
        lax.psum_scatter(
            value_grads.reshape(seq_rows, width), "ctx", scatter_dimension=0, tiled=True
        ),
    )
    d_query = rotate_back(d_query, cosine, sine)
    d_key = rotate_back(d_key.reshape(local_rows, H, HD), cosine, sine)
    d_qkv = jnp.concatenate(
        [d_query.reshape(local_rows, width), d_key.reshape(local_rows, width), d_value], axis=1
    )
    d_qkv16 = d_qkv.astype(jnp.bfloat16)
    grad_wqkv = jnp.einsum("tk,tn->kn", normed1_b, d_qkv16, preferred_element_type=jnp.float32)
    grad_bqkv = jnp.sum(d_qkv, axis=0)
    grad_attention_normed = jnp.einsum(
        "tn,kn->tk", d_qkv16, wqkv, preferred_element_type=jnp.float32
    )
    grad_attention_gain = jnp.sum(grad_attention_normed * attention_standardized, axis=0)
    grad_shift1 = jnp.sum(grad_attention_normed, axis=0)
    attention_branch_grad = layer_norm_backward(
        grad_attention_normed,
        attention_standardized,
        attention_inverse_deviation,
        attention_norm_gain,
    )
    hidden_grad = cotan_wide + attention_branch_grad + feedforward_branch_grad
    terms = (
        grad_attention_gain,
        grad_shift1,
        grad_wqkv,
        grad_bqkv,
        grad_wout,
        grad_bdown,
        grad_feedforward_gain,
        grad_shift2,
        grad_wup,
        grad_bup,
        grad_wdown,
        grad_bdown,
    )
    shares = (
        lax.psum_scatter(terms[0], "fsdp", scatter_dimension=0, tiled=True),
        lax.psum_scatter(terms[1], "fsdp", scatter_dimension=0, tiled=True),
        lax.psum_scatter(terms[2], "fsdp", scatter_dimension=0, tiled=True),
        lax.psum_scatter(terms[3], "fsdp", scatter_dimension=0, tiled=True),
        lax.psum_scatter(terms[4], "fsdp", scatter_dimension=0, tiled=True),
        lax.psum_scatter(terms[5], "fsdp", scatter_dimension=0, tiled=True),
        lax.psum_scatter(terms[6], "fsdp", scatter_dimension=0, tiled=True),
        lax.psum_scatter(terms[7], "fsdp", scatter_dimension=0, tiled=True),
        lax.psum_scatter(terms[8], "fsdp", scatter_dimension=0, tiled=True),
        lax.psum_scatter(terms[9], "fsdp", scatter_dimension=0, tiled=True),
        lax.psum_scatter(terms[10], "fsdp", scatter_dimension=0, tiled=True),
        lax.psum_scatter(terms[11], "fsdp", scatter_dimension=0, tiled=True),
    )
    shares = lax.psum(
        (
            shares[0],
            shares[1],
            shares[2],
            shares[3],
            shares[4],
            shares[5],
            shares[6],
            shares[7],
            shares[8],
            shares[9],
            shares[10],
            shares[11],
        ),
        "ctx",
    )
    return (
        hidden_out[None],
        hidden_grad[None],
        shares[0],
        shares[1],
        shares[2],
        shares[3],
        shares[4],
        shares[5],
        shares[6],
        shares[7],
        shares[8],
        shares[9],
        shares[10],
        shares[11],
    )


MESH_IDS = pl.DeviceIdType.MESH
NN = (((1,), (0,)), ((), ()))
NT = (((1,), (1,)), ((), ()))
TN = (((0,), (0,)), ((), ()))
QTILE = 256
SEMAPHORES = 160


def mm(left, right, dims=NN):
    return lax.dot_general(left, right, dims, preferred_element_type=jnp.float32)


def flip(index, bit):
    return index + bit - 2 * bit * ((index // bit) % 2)


def run_when(condition, action):
    if condition is None:
        action()
    else:
        pl.when(condition)(action)


def narrow(values):
    return values.astype(jnp.bfloat16)


def wide(values):
    return values.astype(jnp.float32)


class Copies:
    def __init__(self, send_sems, recv_sems):
        self.send_sems, self.recv_sems = send_sems, recv_sems
        self.count, self.started, self.numbers = 0, [], {}

    def make(self, source, target, device, when=None, like=None):
        if like is None:
            number = self.count
            self.count += 1
        else:
            number = self.numbers[id(like)]
        copy = pltpu.make_async_remote_copy(
            src_ref=source,
            dst_ref=target,
            send_sem=self.send_sems.at[number],
            recv_sem=self.recv_sems.at[number],
            device_id=device,
            device_id_type=MESH_IDS,
        )
        self.started.append((copy, when))
        self.numbers[id(copy)] = number
        return copy

    def settle(self, chosen):
        numbers = {id(copy) for copy in chosen}
        for copy, when in self.started:
            if id(copy) in numbers:
                run_when(when, copy.wait_send)
        self.started = [entry for entry in self.started if id(entry[0]) not in numbers]

    def finish(self):
        for copy, when in self.started:
            run_when(when, copy.wait_send)


class Place:
    def __init__(self, nz):
        self.nz = nz
        self.c, self.z = lax.axis_index("ctx"), lax.axis_index("fsdp")
        self.k, self.t = self.c % 2, self.c // 2
        self.xn, self.yn, self.pn = flip(self.c, 2), flip(self.c, 4), flip(self.c, 1)
        self.dn = flip(self.xn, 4)
        self.tx, self.ty = flip(self.t, 1), flip(self.t, 2)
        self.td = flip(self.tx, 2)
        self.others = [(self.z + d) % nz for d in range(1, nz)]
        self.plane = [self.xn, self.yn, self.dn, self.pn] + [
            flip(peer, 1) for peer in (self.xn, self.yn, self.dn)
        ]
        self.above, self.below = jnp.minimum(self.z + 1, nz - 1), jnp.maximum(self.z - 1, 0)

    def on_plane(self, c):
        return (c, self.z)

    def on_line(self, z):
        return (self.c, z)

    def greet(self):
        barrier = pltpu.get_barrier_semaphore()
        peers = [self.on_plane(peer) for peer in self.plane] + [self.on_line(z) for z in self.others]
        for peer in peers:
            pl.semaphore_signal(barrier, inc=1, device_id=peer, device_id_type=MESH_IDS)
        pl.semaphore_wait(barrier, len(peers))


class PlaneShare:
    def __init__(self, copies, me, source, slot, rows):
        self.copies, self.me, self.slot = copies, me, slot
        self.top, self.bottom = pl.ds(0, rows // 2), pl.ds(rows // 2, rows // 2)
        own = slot(me.k, me.t)
        self.to_x = copies.make(source, own, me.on_plane(me.xn))
        self.to_y = copies.make(source, own, me.on_plane(me.yn))
        self.to_p = copies.make(source, own, me.on_plane(me.pn))
        self.swaps = [self.to_p]
        through_x, through_y = slot(me.k, me.tx).at[self.top], slot(me.k, me.ty).at[self.bottom]
        self.hop_y = copies.make(through_x, through_x, me.on_plane(me.yn))
        self.hop_x = copies.make(through_y, through_y, me.on_plane(me.xn))

    def start(self):
        self.to_x.start()
        self.to_y.start()
        self.to_p.start()

    def swap(self, place):
        copy = self.copies.make(place, place, self.me.on_plane(self.me.pn))
        copy.start()
        self.swaps.append(copy)

    def on_x(self):
        self.to_x.wait_recv()
        self.hop_y.start()
        self.swap(self.slot(self.me.k, self.me.tx))

    def on_y(self):
        self.to_y.wait_recv()
        self.hop_x.start()
        self.swap(self.slot(self.me.k, self.me.ty))

    def on_diagonal(self):
        diagonal = self.slot(self.me.k, self.me.td)
        self.hop_y.wait_recv()
        self.swap(diagonal.at[self.top])
        self.hop_x.wait_recv()
        self.swap(diagonal.at[self.bottom])

    def finish(self):
        for swap in self.swaps:
            swap.wait_recv()


class LineGather:
    def __init__(self, copies, me, source, gathered):
        self.copies, self.me, self.gathered = copies, me, gathered
        rows = gathered.shape[1] // 2
        self.mine = pl.ds(me.k * rows, rows)
        self.moves, self.swaps = {}, []
        for step in range(me.nz - 1):
            for sign in (1, -1):
                shard, target = me.z - sign * step, me.z + sign
                ok = (shard >= 0) & (shard < me.nz) & (target >= 0) & (target < me.nz)
                place = self.slot(shard)
                copy = copies.make(
                    source.at[self.mine] if step == 0 else place,
                    place,
                    me.on_line(jnp.clip(target, 0, me.nz - 1)),
                    when=ok,
                )
                self.moves[step, sign] = (copy, ok)

    def slot(self, shard):
        return self.gathered.at[jnp.clip(shard, 0, self.me.nz - 1), self.mine]

    def start(self):
        for sign in (1, -1):
            copy, ok = self.moves[0, sign]
            run_when(ok, copy.start)

    def advance(self, step):
        me = self.me
        for sign in (1, -1):
            arrived = me.z - sign * (step + 1)
            ok = (arrived >= 0) & (arrived < me.nz)
            run_when(ok, self.moves[step, sign][0].wait_recv)
            if step + 1 < me.nz - 1:
                copy, following = self.moves[step + 1, sign]
                run_when(following, copy.start)
            place = self.slot(arrived)
            swap = self.copies.make(place, place, me.on_plane(me.pn), when=ok)
            run_when(ok, swap.start)
            self.swaps.append((swap, ok))

    def finish(self):
        for swap, ok in self.swaps:
            run_when(ok, swap.wait_recv)


class LineSpread:
    def __init__(self, copies, me, source, target):
        self.me, self.source, self.target = me, source, target
        rows = target.shape[0] // 2
        mine = pl.ds(me.k * rows, rows)
        here, up, down = me.z == me.t, me.z > me.t, me.z < me.t
        self.here, self.up, self.down = here, up, down
        not_last, not_first = me.z < me.nz - 1, me.z > 0
        to_up, to_down = me.on_line(me.above), me.on_line(me.below)
        place = target.at[mine]
        self.first_up = copies.make(source.at[mine], place, to_up, when=here & not_last)
        self.first_down = copies.make(source.at[mine], place, to_down, when=here & not_first)
        self.next_up = copies.make(place, place, to_up, when=up & not_last, like=self.first_up)
        self.next_down = copies.make(place, place, to_down, when=down & not_first, like=self.first_down)
        self.not_last, self.not_first = not_last, not_first
        self.swap = copies.make(place, place, me.on_plane(me.pn), when=up | down)

    def start(self):
        pl.when(self.here & self.not_last)(self.first_up.start)
        pl.when(self.here & self.not_first)(self.first_down.start)

        @pl.when(self.here)
        def _():
            self.target[...] = self.source[...]

    def advance(self):
        pl.when(self.up)(self.first_up.wait_recv)
        pl.when(self.down)(self.first_down.wait_recv)
        pl.when(self.up & self.not_last)(self.next_up.start)
        pl.when(self.down & self.not_first)(self.next_down.start)
        pl.when(self.up | self.down)(self.swap.start)

    def finish(self):
        pl.when(self.up | self.down)(self.swap.wait_recv)


def add_narrow(target, index, incoming):
    target[index] = narrow(wide(target[index]) + wide(incoming[index]))


class LineReduce:
    def __init__(self, copies, me, source, total, up, down):
        self.me, self.source, self.total, self.up, self.down = me, source, total, up, down
        half = total.shape[1]
        self.mine, theirs = pl.ds(me.k * half, half), pl.ds((1 - me.k) * half, half)
        self.exchange = copies.make(source.at[:, theirs], total, me.on_plane(me.pn))
        self.sends = {}
        for owner in range(me.nz):
            self.sends[owner, 0] = copies.make(
                total.at[owner], up.at[owner], me.on_line(me.above), when=me.z < owner
            )
            self.sends[owner, 1] = copies.make(
                total.at[owner], down.at[owner], me.on_line(me.below), when=me.z > owner
            )

    def start(self):
        self.exchange.start()

    def pair(self):
        self.exchange.wait_recv()
        for owner in range(self.me.nz):
            self.total[owner] = narrow(
                wide(self.total[owner]) + wide(self.source[owner, self.mine])
            )

    def events(self, place):
        nz, found = self.me.nz, []
        for owner in range(place, nz):
            if place > 0 or owner > place:
                found.append((nz - 1 - owner + place, 0, owner))
        for owner in range(place + 1):
            if place < nz - 1 or owner < place:
                found.append((owner + nz - 1 - place, 1, owner))
        return sorted(found)

    def step(self, place, way, owner):
        incoming = (self.up, self.down)[way]
        send = self.sends[owner, way]
        if (way == 0 and place > 0) or (way == 1 and place < self.me.nz - 1):
            send.wait_recv()
            add_narrow(self.total, owner, incoming)
        if owner != place:
            send.start()


def reduce_along(me, reductions, time):
    for place in range(me.nz):
        found = [event for event in reductions[0].events(place) if event[0] == time]
        if not found:
            continue

        @pl.when(me.z == place)
        def _():
            for _, way, owner in found:
                for reduction in reductions:
                    reduction.step(place, way, owner)


class LineCollect:
    def __init__(self, copies, me, source, total, up, down):
        self.me, self.source, self.total, self.up, self.down = me, source, total, up, down
        half = total.shape[0]
        self.mine, theirs = pl.ds(me.k * half, half), pl.ds((1 - me.k) * half, half)
        self.exchange = copies.make(source.at[theirs], total, me.on_plane(me.pn))
        self.to_up = copies.make(total, up, me.on_line(me.above), when=me.z < me.t)
        self.to_down = copies.make(total, down, me.on_line(me.below), when=me.z > me.t)

    def start(self):
        self.exchange.start()

    def pair(self):
        self.exchange.wait_recv()
        self.total[...] = narrow(wide(self.total[...]) + wide(self.source[self.mine]))

    def take(self, incoming):
        self.total[...] = narrow(wide(self.total[...]) + wide(incoming[...]))

    def along(self, time):
        me = self.me
        for place in range(me.nz):

            @pl.when((me.z == place) & (me.t >= place))
            def _():
                if place == time:
                    if place > 0:
                        self.to_up.wait_recv()
                        self.take(self.up)
                    pl.when(me.t > place)(self.to_up.start)

            @pl.when((me.z == place) & (me.t <= place))
            def _():
                if me.nz - 1 - place == time:
                    if place < me.nz - 1:
                        self.to_down.wait_recv()
                        self.take(self.down)
                    pl.when(me.t < place)(self.to_down.start)


class PlaneSpread:
    def __init__(self, copies, me, source, target, rows):
        self.me, self.source, self.target = me, source, target
        top, bottom = pl.ds(0, rows // 2), pl.ds(rows // 2, rows // 2)
        place = target.at[me.k]
        self.here, self.from_x, self.from_y = me.t == me.z, me.tx == me.z, me.ty == me.z
        self.from_d = me.td == me.z
        self.to_x = copies.make(source, place, me.on_plane(me.xn), when=self.here)
        self.to_y = copies.make(source, place, me.on_plane(me.yn), when=self.here)
        self.to_p = copies.make(source, place, me.on_plane(me.pn), when=self.here)
        self.hop_y = copies.make(place.at[top], place.at[top], me.on_plane(me.yn), when=self.from_x)
        self.hop_x = copies.make(
            place.at[bottom], place.at[bottom], me.on_plane(me.xn), when=self.from_y
        )
        away = self.from_x | self.from_y | self.from_d
        self.away = away
        self.swap = copies.make(place, place, me.on_plane(me.pn), when=away, like=self.to_p)

    def start(self):
        @pl.when(self.here)
        def _():
            self.to_x.start()
            self.to_y.start()
            self.to_p.start()
            self.target[self.me.k] = self.source[...]

    def advance(self):
        @pl.when(self.from_x)
        def _():
            self.to_x.wait_recv()
            self.hop_y.start()
            self.swap.start()

        @pl.when(self.from_y)
        def _():
            self.to_y.wait_recv()
            self.hop_x.start()
            self.swap.start()

    def on_diagonal(self):
        @pl.when(self.from_d)
        def _():
            self.hop_y.wait_recv()
            self.hop_x.wait_recv()
            self.swap.start()

    def finish(self):
        self.to_p.wait_recv()

def norm_rows(values_in):
    centre = jnp.mean(values_in, axis=-1, keepdims=True)
    mean_removed = values_in - centre
    inverse_deviation = lax.rsqrt(
        jnp.mean(mean_removed * mean_removed, axis=-1, keepdims=True) + EPS
    )
    return mean_removed * inverse_deviation, inverse_deviation


def head_rows(rows, head):
    lanes = lax.broadcasted_iota(jnp.int32, rows.shape, 1)
    inside = (lanes >= head * HD) & (lanes < (head + 1) * HD)
    return jnp.where(inside, rows, jnp.zeros_like(rows))


def rope_lanes(r, first, blocks, columns, back):
    half_rot = ROT // 2
    tables = [[], [], []]
    row_cos, row_sin = r.rope_r[:, :128], r.rope_r[:, 128:]
    lane = lax.broadcasted_iota(jnp.int32, row_cos.shape, 1) % HD
    for block in range(blocks):
        both = r.rope_b[pl.ds(first + block, 1), :]
        block_cos, block_sin = both[:, :128], both[:, 128:]
        cosine = block_cos * row_cos - block_sin * row_sin
        sine = block_sin * row_cos + block_cos * row_sin
        if back:
            sine = -sine
        tables[0].append(cosine)
        tables[1].append(jnp.where(lane < half_rot, -sine, 0.0))
        tables[2].append(jnp.where(lane >= half_rot, sine, 0.0))
    stacked = [jnp.concatenate(table, axis=0) for table in tables]
    return [jnp.concatenate([table] * (columns // 128), axis=1) for table in stacked]


def turn(values, tables):
    columns, half_rot = values.shape[1], ROT // 2
    return (
        values * tables[0]
        + pltpu.roll(values, columns - half_rot, 1) * tables[1]
        + pltpu.roll(values, half_rot, 1) * tables[2]
    )


def slice_weights(r, me):
    part = r.wqs.shape[1] // 3
    chips = r.wqkv.shape[1] // r.wqs.shape[1]
    for chip in range(chips):

        @pl.when(me.t == chip)
        def _():
            for source, target in ((r.wqkv, r.wqs), (r.wup, r.wus)):
                for piece in range(target.shape[1] // part):
                    first = (piece * chips + chip) * part
                    target[:, piece * part : (piece + 1) * part] = source[:, first : first + part]


def read_vectors(r, me):
    nz, part = me.nz, r.vec.shape[1] // me.nz
    shards = [wide(r.sm4[z]) for z in range(nz)]
    for row in range(4):
        for z in range(nz):
            r.vec[row : row + 1, z * part : (z + 1) * part] = shards[z][
                0:1, row * part : (row + 1) * part
            ]
    for z in range(nz):
        r.vec[4:5, z * part : (z + 1) * part] = shards[z][1:2, :part] + shards[z][1:2, part : 2 * part]
    chips = nz
    for chip in range(chips):

        @pl.when(me.t == chip)
        def _():
            for piece in range(3):
                number = piece * chips + chip
                first = number % 3 * part
                r.vec[5:6, piece * part : (piece + 1) * part] = shards[number // 3][
                    2:3, first : first + part
                ]
            for z in range(nz):
                r.vec[6:7, z * part : (z + 1) * part] = shards[z][3:4, chip * part : (chip + 1) * part]


def sorted_rows(r, source, block, blocks):
    pieces = []
    for number in range(blocks):
        pieces.append(source[r.idx[block + number]])
    return jnp.concatenate(pieces, axis=0)


def put_blocks(target, tile, values):
    blocks = values.shape[0] // BLK
    target[pl.ds(tile * blocks, blocks)] = values.reshape(blocks, BLK, values.shape[1])


def project(r, tile):
    part = r.q.shape[1]
    blocks = QTILE // BLK
    standardized, _ = norm_rows(wide(sorted_rows(r, r.hall, tile * blocks, blocks)))
    normed = narrow(standardized * r.vec[0:1, :] + r.vec[1:2, :])
    weight = r.wq4[...].reshape(-1, 3 * part)
    projected = mm(normed, weight) + r.vec[5:6, : 3 * part]
    turned = turn(
        projected[:, : 2 * part], rope_lanes(r, tile * blocks, blocks, 2 * part, False)
    )
    place = pl.ds(pl.multiple_of(tile * QTILE, QTILE), QTILE)
    r.q[place, :] = narrow(wide(narrow(turned[:, :part])) * HD**-0.5)
    keys, values = turned[:, part:], projected[:, 2 * part :]
    r.k[place, :] = narrow(keys)
    r.v[place, :] = narrow(values)
    r.kt[:, place] = narrow(keys.T)
    r.vt[:, place] = narrow(values.T)


def tile_start(r, me, tile):
    quarter = r.k.shape[0] // 4
    low = tile < quarter // QTILE
    inside = tile * QTILE - jnp.where(low, 0, quarter)
    return jnp.where(low, quarter * me.k, 3 * quarter - quarter * me.k) + inside


def attend(r, me, tile):
    part = r.k.shape[1]
    heads = part // HD
    start = tile_start(r, me, tile)
    rows = slice(tile * QTILE, (tile + 1) * QTILE)
    query = r.q[pl.ds(pl.multiple_of(start, QTILE), QTILE), :]
    per_head = [head_rows(query, head) for head in range(heads)]

    def visit(number, state, masked):
        place = pl.ds(pl.multiple_of(number * QTILE, QTILE), QTILE)
        keys = r.k[place, :]
        result = []
        for head in range(heads):
            top, total, acc = state[head]
            logits = mm(keys, per_head[head], NT)
            if masked:
                key_row = lax.broadcasted_iota(jnp.int32, logits.shape, 0)
                query_row = lax.broadcasted_iota(jnp.int32, logits.shape, 1)
                logits = jnp.where(key_row <= query_row, logits, NEG)
            new_top = jnp.maximum(top, jnp.max(logits, axis=0, keepdims=True))
            fade = jnp.exp(top - new_top)
            probs = jnp.exp(logits - new_top)
            total = total * fade + jnp.sum(probs, axis=0, keepdims=True)
            values = r.vt[head * HD : (head + 1) * HD, place]
            acc = acc * fade + mm(values, narrow(probs))
            result.append((new_top, total, acc))
        return tuple(result)

    state = tuple(
        (
            jnp.full((1, QTILE), NEG, jnp.float32),
            jnp.zeros((1, QTILE), jnp.float32),
            jnp.zeros((HD, QTILE), jnp.float32),
        )
        for _ in range(heads)
    )
    last = start // QTILE
    state = lax.fori_loop(0, last, lambda n, s: visit(n, s, False), state)
    state = visit(last, state, True)
    merged = jnp.concatenate([acc / total for _, total, acc in state], axis=0)
    r.att[rows, :] = narrow(merged.T)
    for head in range(heads):
        r.lse[head : head + 1, rows] = state[head][0] + jnp.log(state[head][1])


def feed_forward(r, me, tile):
    place = pl.ds(pl.multiple_of(tile * QTILE, QTILE), QTILE)
    blocks = QTILE // BLK
    block = tile_start(r, me, tile) // BLK
    width = r.hall.shape[2]
    standardized, _ = norm_rows(wide(sorted_rows(r, r.hall, block, blocks)))
    cotan = sorted_rows(r, r.gall, block, blocks)
    gain2 = r.vec[2:3, :]
    normed = narrow(standardized * gain2 + r.vec[3:4, :])
    up_weight = r.wu4[...].reshape(width, -1)
    down_weight = r.wd4[...].reshape(-1, width)
    up = mm(normed, up_weight) + r.vec[6:7, :]
    below = 0.5 * (1.0 + lax.erf(up * SQRT_HALF))
    act = narrow(up * below)
    slope = below + up * jnp.exp(-0.5 * up * up) * INV_ROOT_TWO_PI
    d_up = mm(cotan, down_weight, NT) * slope
    d_up16 = narrow(d_up)
    attended = r.att[place, :]
    put_blocks(r.outb, tile, narrow(mm(act, down_weight) + mm(attended, r.wo1[...])))
    d_normed = mm(d_up16, up_weight, NT)
    r.sums[2:3, :] += jnp.sum(d_normed * standardized, axis=0, keepdims=True)
    r.sums[3:4, :] += jnp.sum(d_normed, axis=0, keepdims=True)
    r.sums[6:7, :] += jnp.sum(d_up, axis=0, keepdims=True)
    r.e2[place, :] = d_normed * gain2
    r.n[place, :] = normed
    r.gl[place, :] = cotan
    r.act[place, :] = act
    r.du[place, :] = d_up16
    d_att = narrow(mm(cotan, r.wo1[...], NT))
    r.datt[place, :] = d_att
    product = wide(d_att) * wide(attended)
    shape = (8, product.shape[1])
    picked = lax.broadcasted_iota(jnp.int32, shape, 1) // HD == lax.broadcasted_iota(
        jnp.int32, shape, 0
    )
    r.delta[:, place] = lax.dot_general(
        picked.astype(jnp.float32),
        product,
        NT,
        precision=lax.Precision.HIGHEST,
        preferred_element_type=jnp.float32,
    )


def weight_grad(target, left, right):
    rows, columns = left.shape[1], right.shape[1]
    shard = target.shape[1]
    values = right[...]
    for first in range(0, rows, QTILE):
        result = narrow(mm(left[:, first : first + QTILE], values, TN))
        at = first
        while at < first + QTILE:
            owner, inside = at // shard, at % shard
            until = min((owner + 1) * shard, first + QTILE)
            target[owner, inside : inside + until - at, :] = result[at - first : until - first, :]
            at = until


def attend_grad(r, me, tile):
    part = r.k.shape[1]
    heads = part // HD
    kstep = 2 * QTILE
    start = tile_start(r, me, tile)
    rows = slice(tile * QTILE, (tile + 1) * QTILE)
    query = r.q[pl.ds(pl.multiple_of(start, QTILE), QTILE), :]
    d_out = r.datt[rows, :]
    queries = jnp.concatenate([head_rows(query, head) for head in range(heads)], axis=0)
    d_outs = jnp.concatenate([head_rows(d_out, head) for head in range(heads)], axis=0)

    def visit(number, state, masked):
        place = pl.ds(pl.multiple_of(number * kstep, kstep), kstep)
        keys, values = r.k[place, :], r.v[place, :]
        probs_all, d_logits_all, result = [], [], []
        for head in range(heads):
            own = slice(head * QTILE, (head + 1) * QTILE)
            logits = mm(keys, queries[own], NT)
            probs = jnp.exp(logits - r.lse[head : head + 1, rows])
            if masked:
                key_row = number * kstep + lax.broadcasted_iota(jnp.int32, logits.shape, 0)
                query_row = start + lax.broadcasted_iota(jnp.int32, logits.shape, 1)
                probs = jnp.where(key_row <= query_row, probs, 0.0)
            d_probs = mm(values, d_outs[own], NT)
            d_logits = narrow(probs * (d_probs - r.delta[head : head + 1, rows]))
            probs_all.append(narrow(probs))
            d_logits_all.append(d_logits)
            result.append(state[head] + mm(r.kt[head * HD : (head + 1) * HD, place], d_logits))
        r.dv[place, :] += mm(jnp.concatenate(probs_all, axis=1), d_outs)
        r.dk[place, :] += mm(jnp.concatenate(d_logits_all, axis=1), queries)
        return tuple(result)

    state = tuple(jnp.zeros((HD, QTILE), jnp.float32) for _ in range(heads))
    last = start // kstep
    state = lax.fori_loop(0, last, lambda n, s: visit(n, s, False), state)
    state = visit(last, state, True)
    r.dqt[:, rows] = jnp.concatenate(state, axis=0)


def qkv_grad(r, me, tile):
    place = pl.ds(pl.multiple_of(tile * QTILE, QTILE), QTILE)
    part = r.k.shape[1]
    blocks = QTILE // BLK
    start = tile_start(r, me, tile)
    block = start // BLK
    held = pl.ds(pl.multiple_of(start, QTILE), QTILE)
    standardized, _ = norm_rows(wide(sorted_rows(r, r.hall, block, blocks)))
    gain1 = r.vec[0:1, :]
    r.n[place, :] = narrow(standardized * gain1 + r.vec[1:2, :])
    d_query = r.dqt[:, place].T * HD**-0.5
    d_key = r.dk[held, :] + wide(r.kvin[place, :part])
    d_value = r.dv[held, :] + wide(r.kvin[place, part:])
    turned = turn(
        jnp.concatenate([d_query, d_key], axis=1), rope_lanes(r, block, blocks, 2 * part, True)
    )
    d_qkv = jnp.concatenate([turned, d_value], axis=1)
    d_qkv16 = narrow(d_qkv)
    r.du[place, : 3 * part] = d_qkv16
    r.sums[5:6, : 3 * part] += jnp.sum(d_qkv, axis=0, keepdims=True)
    weight = r.wq4[...].reshape(-1, 3 * part)
    d_normed = mm(d_qkv16, weight, NT)
    r.sums[0:1, :] += jnp.sum(d_normed * standardized, axis=0, keepdims=True)
    r.sums[1:2, :] += jnp.sum(d_normed, axis=0, keepdims=True)
    put_blocks(r.outb, tile, narrow(d_normed * gain1 + r.e2[place, :]))


def flat_rows(values):
    return values.reshape(-1, values.shape[-1])


class Scatter:
    def __init__(self, copies, me, r, source, sent, got, landed):
        self.me, self.r, self.source, self.sent, self.got, self.landed = me, r, source, sent, got, landed
        self.chips, self.sides = landed.shape[0], landed.shape[1]
        self.first = r.k.shape[0] // BLK
        self.exchanges = [
            copies.make(self.piece(sent, chip), self.piece(got, chip), me.on_plane(me.pn))
            for chip in range(self.chips)
        ]
        self.moves = [
            copies.make(self.piece(got, chip), landed.at[me.t], me.on_plane(peer))
            for chip, peer in ((me.tx, me.xn), (me.ty, me.yn), (me.td, me.dn))
        ]

    def piece(self, array, chip):
        return array.at[pl.ds(chip * self.sides, self.sides)]

    def block(self, number):
        return self.source[self.r.idx[self.first + number]]

    def start(self):
        count = self.chips * self.sides
        for number in range(count):
            self.sent[number] = self.block(count + number)
        for exchange in self.exchanges:
            exchange.start()

    def spread(self):
        count = self.chips * self.sides
        for exchange in self.exchanges:
            exchange.wait_recv()
        for number in range(count):
            flag = self.r.idx[self.first + 2 * count + number // self.sides]
            own, other = wide(self.block(number)), wide(self.got[number])
            here = jnp.full(own.shape, flag, jnp.int32) > 0
            self.got[number] = narrow(jnp.where(here, own, other))
        for move in self.moves:
            move.start()

    def total(self):
        for move in self.moves:
            move.wait_recv()
        me = self.me
        result = wide(self.got[pl.ds(me.t * self.sides, self.sides)])
        for chip in (me.tx, me.ty, me.td):
            result = result + wide(self.landed[chip])
        return flat_rows(result)


def layer_kernel(nz, names, *refs):
    r = types.SimpleNamespace(**dict(zip(names, refs)))
    me = Place(nz)
    copies = Copies(r.send_sems, r.recv_sems)
    sides = r.h.shape[0]
    shard = r.wqs.shape[0]
    tiles = r.att.shape[0] // QTILE

    slice_weights(r, me)
    me.greet()

    def row_slot(array):
        return lambda core, chip: array.at[pl.ds((2 * chip + core) * sides, sides)]

    own_rows = pl.ds(me.c * sides, sides)
    h_share = PlaneShare(copies, me, r.h, row_slot(r.hall), sides)
    g_share = PlaneShare(copies, me, r.g, row_slot(r.gall), sides)
    wq = LineGather(copies, me, r.wqs, r.wq4)
    wu = LineGather(copies, me, r.wus, r.wu4)
    wd = LineGather(copies, me, r.wdown.at[pl.ds(me.t * shard, shard)], r.wd4)
    wo = LineSpread(copies, me, r.wout, r.wo1)
    small = [copies.make(r.sm, r.sm4.at[me.z], me.on_line(other)) for other in me.others]

    h_share.start()
    wq.start()
    for copy in small:
        copy.start()
    wu.start()
    r.hall[own_rows] = r.h[...]
    r.gall[own_rows] = r.g[...]
    r.wq4[me.z] = r.wqs[...]
    r.wu4[me.z] = r.wus[...]
    own_down = pltpu.make_async_copy(
        r.wdown.at[pl.ds(me.t * shard, shard)], r.wd4.at[me.z], r.local_sem
    )
    own_down.start()
    r.sm4[me.z] = r.sm[...]
    r.sums[...] = jnp.zeros_like(r.sums)
    r.vout[...] = jnp.zeros_like(r.vout)
    r.dk[...] = jnp.zeros_like(r.dk)
    r.dv[...] = jnp.zeros_like(r.dv)
    wq.advance(0)
    h_share.on_x()
    h_share.on_y()
    g_share.start()
    wq.advance(1)
    wd.start()
    wo.start()
    wq.advance(2)
    for copy in small:
        copy.wait_recv()
    read_vectors(r, me)
    wu.advance(0)
    h_share.on_diagonal()
    wq.finish()
    h_share.finish()

    @pl.loop(0, r.k.shape[0] // QTILE)
    def _(tile):
        project(r, tile)

    wd.advance(0)
    g_share.on_x()
    g_share.on_y()
    attend(r, me, 0)
    wu.advance(1)
    wd.advance(1)
    attend(r, me, 1)
    wo.advance()
    wu.advance(2)
    attend(r, me, 2)
    g_share.on_diagonal()
    wd.advance(2)
    for tile in range(3, tiles):
        attend(r, me, tile)
    own_down.wait()
    wu.finish()
    wd.finish()
    wo.finish()
    g_share.finish()
    copies.settle([g_share.hop_x, g_share.hop_y, *g_share.swaps[1:]])

    @pl.loop(0, tiles)
    def _(tile):
        feed_forward(r, me, tile)

    out_scatter = Scatter(copies, me, r, r.outb, r.osent, r.ogot, r.oland)
    out_scatter.start()
    up_reduce = LineReduce(copies, me, r.gu, r.tu, r.uu, r.du_in)
    down_reduce = LineReduce(copies, me, r.gd, r.td, r.ud, r.dd_in)
    out_reduce = LineCollect(copies, me, r.go, r.to, r.uo, r.do_in)
    weight_grad(r.gd, r.act, r.gl)
    down_reduce.start()
    weight_grad(r.gu, r.n, r.du)
    up_reduce.start()
    r.go[...] = narrow(mm(r.att[...], r.gl[...], TN))
    out_reduce.start()
    out_scatter.spread()
    down_reduce.pair()
    up_reduce.pair()
    out_reduce.pair()
    early = [down_reduce, up_reduce]
    reduce_along(me, early, 0)
    out_reduce.along(0)
    attend_grad(r, me, 0)
    reduce_along(me, early, 1)
    out_reduce.along(1)
    attend_grad(r, me, 1)
    reduce_along(me, early, 2)
    out_reduce.along(2)
    attend_grad(r, me, 2)
    reduce_along(me, early, 3)
    out_reduce.along(3)
    half = shard // 2
    d_share = PlaneShare(copies, me, r.td.at[me.z], lambda core, chip: r.fd.at[core, chip], half)
    u_share = PlaneShare(copies, me, r.tu.at[me.z], lambda core, chip: r.fu.at[core, chip], half)
    o_spread = PlaneSpread(copies, me, r.to, r.fo, half)
    d_share.start()
    u_share.start()
    o_spread.start()
    r.fd[me.k, me.t] = r.td[me.z]
    r.fu[me.k, me.t] = r.tu[me.z]
    for tile in range(3, tiles):
        attend_grad(r, me, tile)

    part = r.k.shape[1]
    quarter = r.k.shape[0] // 4
    kv_moves = []
    for number in range(2):
        first = quarter * (1 - me.k) if number == 0 else 3 * quarter - quarter * (1 - me.k)
        theirs = pl.ds(pl.multiple_of(first, quarter), quarter)
        rows = slice(number * quarter, (number + 1) * quarter)
        r.act[rows, :part] = narrow(r.dk[theirs, :])
        r.act[rows, part : 2 * part] = narrow(r.dv[theirs, :])
        copy = copies.make(r.act.at[rows, : 2 * part], r.kvin.at[rows], me.on_plane(me.pn))
        copy.start()
        kv_moves.append(copy)
    d_share.on_x()
    d_share.on_y()
    u_share.on_x()
    u_share.on_y()
    o_spread.advance()
    for copy in kv_moves:
        copy.wait_recv()

    @pl.loop(0, tiles)
    def _(tile):
        qkv_grad(r, me, tile)

    e_scatter = Scatter(
        copies, me, r, r.outb, r.gall.at[: r.outb.shape[0]], r.gall.at[r.outb.shape[0] :], r.eland
    )
    e_scatter.start()
    weight_grad(r.gq, r.n, r.du.at[:, : 3 * part])
    qkv_reduce = LineReduce(copies, me, r.gq, r.tq, r.uq, r.dq_in)
    qkv_reduce.start()
    e_scatter.spread()
    qkv_reduce.pair()
    reduce_along(me, [qkv_reduce], 0)

    vec_part = r.vec.shape[1] // nz
    r.sums[4:5, :] = jnp.sum(wide(flat_rows(r.g[...])), axis=0, keepdims=True)
    for z in range(nz):
        span = slice(z * vec_part, (z + 1) * vec_part)
        for row in range(4):
            r.vout[z, 0:1, row * vec_part : (row + 1) * vec_part] = r.sums[row : row + 1, span]
        r.vout[z, 1:2, :vec_part] = r.sums[4:5, span]
    for chip in range(nz):

        @pl.when(me.t == chip)
        def _():
            for piece in range(3):
                number = piece * nz + chip
                first = number % 3 * vec_part
                r.vout[number // 3, 2:3, first : first + vec_part] = r.sums[
                    5:6, piece * vec_part : (piece + 1) * vec_part
                ]
            for z in range(nz):
                r.vout[z, 3:4, chip * vec_part : (chip + 1) * vec_part] = r.sums[
                    6:7, z * vec_part : (z + 1) * vec_part
                ]

    vec_line = [
        copies.make(r.vout.at[other], r.vline.at[me.z], me.on_line(other)) for other in me.others
    ]
    for copy in vec_line:
        copy.start()
    d_share.on_diagonal()
    u_share.on_diagonal()
    o_spread.on_diagonal()
    reduce_along(me, [qkv_reduce], 1)
    for copy in vec_line:
        copy.wait_recv()
    vector = r.vout[me.z]
    for other in me.others:
        vector = vector + r.vline[other]
    r.vsend[...] = vector
    reduce_along(me, [qkv_reduce], 2)
    vec_plane = [copies.make(r.vsend, r.vplane.at[me.c], me.on_plane(peer)) for peer in me.plane]
    for copy in vec_plane:
        copy.start()
    reduce_along(me, [qkv_reduce], 3)
    q_share = PlaneShare(copies, me, r.tq.at[me.z], lambda core, chip: r.fq.at[core, chip], half)
    q_share.start()
    r.fq[me.k, me.t] = r.tq[me.z]

    residual = wide(flat_rows(r.h[...]))
    own_standardized, own_deviation = norm_rows(residual)
    r.hidden_out[...] = narrow(residual + r.vec[4:5, :] + out_scatter.total())
    q_share.on_x()
    q_share.on_y()
    e_total = e_scatter.total()
    r.hidden_grad[...] = wide(flat_rows(r.g[...])) + own_deviation * (
        e_total
        - jnp.mean(e_total, axis=-1, keepdims=True)
        - own_standardized * jnp.mean(e_total * own_standardized, axis=-1, keepdims=True)
    )
    for copy in vec_plane:
        copy.wait_recv()
    vector = r.vsend[...]
    for peer in me.plane:
        vector = vector + r.vplane[peer]
    r.vsum[...] = vector
    q_share.on_diagonal()
    d_share.finish()
    u_share.finish()
    o_spread.finish()
    q_share.finish()
    copies.finish()


def assemble_kernel(fq_ref, fu_ref, fd_ref, fo_ref, gq_ref, gu_ref, gd_ref, go_ref):
    cores, chips, half, _ = fq_ref.shape
    part = fq_ref.shape[3] // 3
    for core in range(cores):
        rows = slice(core * half, (core + 1) * half)
        go_ref[rows, :] = wide(fo_ref[core])
        for chip in range(chips):
            for source, target in ((fq_ref, gq_ref), (fu_ref, gu_ref)):
                for piece in range(source.shape[3] // part):
                    first = (piece * chips + chip) * part
                    target[rows, first : first + part] = wide(
                        source[core, chip, :, piece * part : (piece + 1) * part]
                    )
            first = chip * cores * half + core * half
            gd_ref[first : first + half, :] = wide(fd_ref[core, chip])


def rotary_parts(block_count):
    half_rot = ROT // 2
    lane = np.arange(128) % HD
    rate = np.where(lane < ROT, 10000.0 ** (-2.0 * (lane % half_rot) / ROT), 0.0)

    def table(places):
        angle = places[:, None].astype(np.float64) * rate[None, :]
        return np.concatenate([np.cos(angle), np.sin(angle)], axis=1).astype(np.float32)

    return table(np.arange(BLK)), table(np.arange(block_count) * BLK)


def block_table(block_order, chips, core):
    count = block_order.shape[0]
    quarter = count // 4
    places = jnp.arange(count, dtype=jnp.int32)
    gathered = jnp.sum(
        jnp.where(block_order[:, None] == places[None, :], places[:, None], 0), axis=0
    )
    pairs = block_order.reshape(chips, 2, count // (2 * chips))
    local = jnp.where(
        (pairs >= quarter * core) & (pairs < quarter * (core + 1)),
        pairs - quarter * core,
        jnp.clip(pairs - (3 * quarter - quarter * core) + quarter, 0, 2 * quarter - 1),
    )
    outer = (pairs[:, :, 0] < quarter) | (pairs[:, :, 0] >= 3 * quarter)
    here = outer == (core == 0)
    mine = jnp.where(core == 0, local[:, 0], local[:, 1])
    theirs = jnp.where(core == 0, local[:, 1], local[:, 0])
    flags = jnp.where(core == 0, here[:, 0], here[:, 1])
    return jnp.concatenate(
        [gathered, mine.reshape(-1), theirs.reshape(-1), flags.astype(jnp.int32)]
    ).astype(jnp.int32)


VMEM_SPEC = pl.BlockSpec(memory_space=pltpu.VMEM)
SPECS = {
    "idx": pl.BlockSpec(memory_space=pltpu.SMEM),
    "wdown": pl.BlockSpec(memory_space=pl.ANY),
}
VMEM_LIMIT = 63 * 1024 * 1024


def sliced_layer(
    nz,
    hidden_in,
    norm1_gain,
    attention_norm_bias,
    qkv_weight,
    qkv_bias,
    out_weight,
    out_bias,
    norm2_gain,
    feedforward_norm_bias,
    up_weight,
    up_bias,
    down_weight,
    down_bias,
    cotangent,
    block_order,
):
    f32, b16 = jnp.float32, jnp.bfloat16
    h, g = hidden_in[0], cotangent[0]
    local_rows, width = h.shape
    chips = lax.axis_size("ctx") // 2
    core = lax.axis_index("ctx") % 2
    shard = qkv_weight.shape[0]
    half = shard // 2
    part = width // chips
    hidden = up_weight.shape[1] // chips
    rows = chips * local_rows
    everyone = 2 * rows
    sides = local_rows // BLK

    idx = block_table(block_order, chips, core)
    first = jnp.concatenate([norm1_gain, attention_norm_bias, norm2_gain, feedforward_norm_bias])
    second = jnp.concatenate([out_bias, down_bias])
    lines = [
        jnp.pad(line, (0, width - line.shape[0])) for line in (first, second, qkv_bias, up_bias)
    ]
    sm = jnp.pad(jnp.stack(lines), ((0, 12), (0, 0)))
    rope_r, rope_b = rotary_parts(everyone // BLK)

    inputs = {
        "idx": idx,
        "h": h.reshape(sides, BLK, width),
        "g": g.reshape(sides, BLK, width),
        "wqkv": qkv_weight,
        "wup": up_weight,
        "wdown": down_weight,
        "wout": out_weight,
        "sm": sm,
        "rope_r": jnp.asarray(rope_r),
        "rope_b": jnp.asarray(rope_b),
    }
    outputs = {
        "hidden_out": ((local_rows, width), b16),
        "hidden_grad": ((local_rows, width), f32),
        "fq": ((2, chips, half, 3 * part), b16),
        "fu": ((2, chips, half, hidden), b16),
        "fd": ((2, chips, half, width), b16),
        "fo": ((2, half, width), b16),
        "vsum": ((8, width), f32),
    }
    scratch = {
        "hall": ((everyone // BLK, BLK, width), b16),
        "gall": ((everyone // BLK, BLK, width), b16),
        "wqs": ((shard, 3 * part), b16),
        "wus": ((shard, hidden), b16),
        "wq4": ((nz, shard, 3 * part), b16),
        "wu4": ((nz, shard, hidden), b16),
        "wd4": ((nz, shard, width), b16),
        "wo1": ((part, width), b16),
        "sm4": ((nz, 16, width), b16),
        "vec": ((8, width), f32),
        "sums": ((8, width), f32),
        "q": ((everyone, part), b16),
        "k": ((everyone, part), b16),
        "v": ((everyone, part), b16),
        "kt": ((part, everyone), b16),
        "vt": ((part, everyone), b16),
        "att": ((rows, part), b16),
        "lse": ((8, rows), f32),
        "delta": ((8, rows), f32),
        "datt": ((rows, part), b16),
        "act": ((rows, hidden), b16),
        "du": ((rows, hidden), b16),
        "n": ((rows, width), b16),
        "gl": ((rows, width), b16),
        "outb": ((rows // BLK, BLK, width), b16),
        "e2": ((rows, width), f32),
        "dk": ((everyone, part), f32),
        "dv": ((everyone, part), f32),
        "dqt": ((part, rows), f32),
        "kvin": ((rows, 2 * part), b16),
        "osent": ((rows // BLK, BLK, width), b16),
        "ogot": ((rows // BLK, BLK, width), b16),
        "oland": ((chips, sides, BLK, width), b16),
        "eland": ((chips, sides, BLK, width), b16),
        "gq": ((nz, shard, 3 * part), b16),
        "gu": ((nz, shard, hidden), b16),
        "gd": ((nz, shard, width), b16),
        "go": ((part, width), b16),
        "tq": ((nz, half, 3 * part), b16),
        "uq": ((nz, half, 3 * part), b16),
        "dq_in": ((nz, half, 3 * part), b16),
        "tu": ((nz, half, hidden), b16),
        "uu": ((nz, half, hidden), b16),
        "du_in": ((nz, half, hidden), b16),
        "td": ((nz, half, width), b16),
        "ud": ((nz, half, width), b16),
        "dd_in": ((nz, half, width), b16),
        "to": ((half, width), b16),
        "uo": ((half, width), b16),
        "do_in": ((half, width), b16),
        "vout": ((nz, 8, width), f32),
        "vline": ((nz, 8, width), f32),
        "vsend": ((8, width), f32),
        "vplane": ((2 * chips, 8, width), f32),
    }
    names = [*inputs, *outputs, *scratch, "send_sems", "recv_sems", "local_sem"]
    results = pl.pallas_call(
        functools.partial(layer_kernel, nz, names),
        out_shape=tuple(jax.ShapeDtypeStruct(*leaf) for leaf in outputs.values()),
        in_specs=[SPECS.get(name, VMEM_SPEC) for name in inputs],
        out_specs=(VMEM_SPEC,) * len(outputs),
        scratch_shapes=[pltpu.VMEM(*leaf) for leaf in scratch.values()]
        + [pltpu.SemaphoreType.DMA((SEMAPHORES,))] * 2
        + [pltpu.SemaphoreType.DMA],
        compiler_params=pltpu.CompilerParams(
            collective_id=0, has_side_effects=True, vmem_limit_bytes=VMEM_LIMIT
        ),
        name="layer",
    )(*inputs.values())
    hidden_out, hidden_grad, fq, fu, fd, fo, vsum = results

    grad_qkv, grad_up, grad_down, grad_out = pl.pallas_call(
        assemble_kernel,
        out_shape=tuple(
            jax.ShapeDtypeStruct(weight.shape, f32)
            for weight in (qkv_weight, up_weight, down_weight, out_weight)
        ),
        in_specs=[VMEM_SPEC] * 4,
        out_specs=(VMEM_SPEC,) * 4,
        compiler_params=pltpu.CompilerParams(vmem_limit_bytes=56 * 1024 * 1024),
        name="assemble",
    )(fq, fu, fd, fo)

    norms = vsum[0].reshape(nz, shard)
    bias = vsum[1, :shard]
    return (
        hidden_out[None],
        hidden_grad[None],
        norms[0],
        norms[1],
        grad_qkv,
        vsum[2, : qkv_bias.shape[0]],
        grad_out,
        bias,
        norms[2],
        norms[3],
        grad_up,
        vsum[3, : up_bias.shape[0]],
        grad_down,
        bias,
    )


def sliced_fits(mesh):
    return mesh.shape["ctx"] == 8 and mesh.shape["fsdp"] == 4


def solution(mesh):
    in_specs = (
        P("fsdp", "ctx", None),
        P("fsdp"),
        P("fsdp"),
        P("fsdp", None),
        P("fsdp"),
        P("fsdp", None),
        P("fsdp"),
        P("fsdp"),
        P("fsdp"),
        P("fsdp", None),
        P("fsdp"),
        P("fsdp", None),
        P("fsdp"),
        P("fsdp", "ctx", None),
        P(),
    )
    out_specs = (
        P("fsdp", "ctx", None),
        P("fsdp", "ctx", None),
        P("fsdp"),
        P("fsdp"),
        P("fsdp", None),
        P("fsdp"),
        P("fsdp", None),
        P("fsdp"),
        P("fsdp"),
        P("fsdp"),
        P("fsdp", None),
        P("fsdp"),
        P("fsdp", None),
        P("fsdp"),
    )
    local = whole_parameter_layer
    if sliced_fits(mesh):
        local = functools.partial(sliced_layer, mesh.shape["fsdp"])
    return jax.shard_map(local, mesh=mesh, in_specs=in_specs, out_specs=out_specs, check_vma=False)
```

```python
import functools
import math
import types

import jax
import jax.numpy as jnp
import numpy as np
from jax import lax
from jax.experimental import pallas as pl
from jax.experimental.pallas import tpu as pltpu
from jax.sharding import PartitionSpec as P

H = 12
HD = 64
ROT = 16
BLK = 128


EPS = 1e-05
NEG = -1e30
SQRT_HALF = 0.7071067811865476
INV_ROOT_TWO_PI = 0.3989422804014327


def apply_layer_norm(values_in, norm_gain, norm_bias):
    centre = jnp.mean(values_in, axis=-1, keepdims=True)
    mean_removed = values_in - centre
    inverse_deviation = lax.rsqrt(
        jnp.mean(mean_removed * mean_removed, axis=-1, keepdims=True) + EPS
    )
    standardized = mean_removed * inverse_deviation
    return (standardized * norm_gain + norm_bias, standardized, inverse_deviation)


def layer_norm_backward(output_gradient, standardized, inverse_deviation, norm_gain):
    gain_scaled = output_gradient * norm_gain
    return inverse_deviation * (
        gain_scaled
        - jnp.mean(gain_scaled, axis=-1, keepdims=True)
        - standardized * jnp.mean(gain_scaled * standardized, axis=-1, keepdims=True)
    )


def gelu_exact(values_in):
    return 0.5 * values_in * (1.0 + lax.erf(values_in * SQRT_HALF))


def gelu_slope(values_in):
    return (
        0.5 * (1.0 + lax.erf(values_in * SQRT_HALF))
        + values_in * jnp.exp(-0.5 * values_in * values_in) * INV_ROOT_TWO_PI
    )


def rotary_tables(position_list):
    half_rot = ROT // 2
    inverse = jnp.power(jnp.float32(10000.0), -2.0 * jnp.arange(half_rot, dtype=jnp.float32) / ROT)
    angle = position_list.astype(jnp.float32)[:, None] * inverse[None, :]
    return (jnp.cos(angle)[:, None, :], jnp.sin(angle)[:, None, :])


def rotate(tensor, cosine, sine):
    half_rot = ROT // 2
    first_half = tensor[..., :half_rot]
    second_half = tensor[..., half_rot:ROT]
    return jnp.concatenate(
        [
            first_half * cosine - second_half * sine,
            second_half * cosine + first_half * sine,
            tensor[..., ROT:],
        ],
        axis=-1,
    )


def rotate_back(tensor, cosine, sine):
    half_rot = ROT // 2
    first_half = tensor[..., :half_rot]
    second_half = tensor[..., half_rot:ROT]
    return jnp.concatenate(
        [
            first_half * cosine + second_half * sine,
            second_half * cosine - first_half * sine,
            tensor[..., ROT:],
        ],
        axis=-1,
    )


def masked_logits(query_block, key_block, query_pos, key_pos):
    logits = jnp.einsum(
        "qhd,khd->hqk", query_block, key_block, preferred_element_type=jnp.float32
    ) * (1.0 / math.sqrt(HD))
    return jnp.where(key_pos[None, None, :] <= query_pos[None, :, None], logits, NEG)


def block_terms(
    query_block, dout_block, total_t, delta_t, query_pos, key_block, value_block, key_pos
):
    logits = masked_logits(query_block, key_block, query_pos, key_pos)
    probs_wide = jnp.exp(logits - total_t[:, :, None])
    dprobs = jnp.einsum("qhd,khd->hqk", dout_block, value_block, preferred_element_type=jnp.float32)
    d_logits = (probs_wide * (dprobs - delta_t[:, :, None]) * (1.0 / math.sqrt(HD))).astype(
        jnp.bfloat16
    )
    return (probs_wide.astype(jnp.bfloat16), d_logits)


def keep_state(state_in):
    return state_in


def forward_attention(query, keys_all, values_all, own_pos, all_pos):
    local_rows = query.shape[0]
    seq_rows = keys_all.shape[0]
    qstep = min(512, local_rows)
    kstep = min(512, seq_rows)
    latest = jnp.max(own_pos)

    def stats_step(number, state_in):
        key_block = lax.dynamic_slice_in_dim(keys_all, number * kstep, kstep, 0)
        key_pos = lax.dynamic_slice_in_dim(all_pos, number * kstep, kstep, 0)

        def stats_live(state_now):
            running_max, running_sum = state_now
            logits = masked_logits(query, key_block, own_pos, key_pos)
            new_max = jnp.maximum(running_max, jnp.max(logits, axis=-1))
            running_sum = running_sum * jnp.exp(running_max - new_max) + jnp.sum(
                jnp.exp(logits - new_max[:, :, None]), axis=-1
            )
            return (new_max, running_sum)

        return lax.cond(jnp.min(key_pos) <= latest, stats_live, keep_state, state_in)

    start_state = (jnp.full((H, qstep), NEG, jnp.float32), jnp.zeros((H, qstep), jnp.float32))
    running_max, running_sum = lax.fori_loop(0, seq_rows // kstep, stats_step, start_state)
    total_t = running_max + jnp.log(running_sum)

    def value_step(number, state_in):
        key_block = lax.dynamic_slice_in_dim(keys_all, number * kstep, kstep, 0)
        value_block = lax.dynamic_slice_in_dim(values_all, number * kstep, kstep, 0)
        key_pos = lax.dynamic_slice_in_dim(all_pos, number * kstep, kstep, 0)

        def value_live(state_now):
            logits = masked_logits(query, key_block, own_pos, key_pos)
            attn_probs = jnp.exp(logits - total_t[:, :, None]).astype(jnp.bfloat16)
            return state_now + jnp.einsum(
                "hqk,khd->qhd", attn_probs, value_block, preferred_element_type=jnp.float32
            )

        return lax.cond(jnp.min(key_pos) <= latest, value_live, keep_state, state_in)

    weighted = lax.fori_loop(
        0, seq_rows // kstep, value_step, jnp.zeros((qstep, H, HD), jnp.float32)
    )
    totals = total_t.T
    return (weighted, totals)


def query_grads(query, d_att, log_total, delta, own_pos, keys_all, values_all, all_pos):
    local_rows = query.shape[0]
    seq_rows = keys_all.shape[0]
    qstep = min(512, local_rows)
    kstep = min(512, seq_rows)
    key_grads = jnp.zeros((seq_rows, H, HD), jnp.float32)
    value_grads = jnp.zeros((seq_rows, H, HD), jnp.float32)
    total_t = log_total.T
    delta_t = delta.T
    latest = jnp.max(own_pos)

    def key_step(number, state_in):
        offset = number * kstep
        key_block = lax.dynamic_slice_in_dim(keys_all, offset, kstep, 0)
        value_block = lax.dynamic_slice_in_dim(values_all, offset, kstep, 0)
        key_pos = lax.dynamic_slice_in_dim(all_pos, offset, kstep, 0)

        def key_live(state_now):
            attn_probs, d_logits = block_terms(
                query, d_att, total_t, delta_t, own_pos, key_block, value_block, key_pos
            )
            d_query = state_now[0] + jnp.einsum(
                "hqk,khd->qhd", d_logits, key_block, preferred_element_type=jnp.float32
            )
            key_acc = state_now[1]
            value_acc = state_now[2]
            key_part = jnp.einsum(
                "hqk,qhd->khd", d_logits, query, preferred_element_type=jnp.float32
            )
            value_part = jnp.einsum(
                "hqk,qhd->khd", attn_probs, d_att, preferred_element_type=jnp.float32
            )
            key_acc = lax.dynamic_update_slice_in_dim(
                key_acc, lax.dynamic_slice_in_dim(key_acc, offset, kstep, 0) + key_part, offset, 0
            )
            value_acc = lax.dynamic_update_slice_in_dim(
                value_acc,
                lax.dynamic_slice_in_dim(value_acc, offset, kstep, 0) + value_part,
                offset,
                0,
            )
            return (d_query, key_acc, value_acc)

        return lax.cond(jnp.min(key_pos) <= latest, key_live, keep_state, state_in)

    start_state = (jnp.zeros((qstep, H, HD), jnp.float32),) + (key_grads, value_grads)
    result = lax.fori_loop(0, seq_rows // kstep, key_step, start_state)
    pieces = result[0]
    key_grads = result[1]
    value_grads = result[2]
    return (pieces, key_grads, value_grads)


def whole_parameter_layer(
    hidden_in,
    norm1_gain,
    attention_norm_bias,
    qkv_weight,
    qkv_bias,
    out_weight,
    out_bias,
    norm2_gain,
    feedforward_norm_bias,
    up_weight,
    up_bias,
    down_weight,
    down_bias,
    cotangent,
    block_order,
):
    (
        attention_norm_gain,
        attention_bias_term,
        wqkv,
        bqkv,
        wout,
        bout,
        feedforward_norm_gain,
        feedforward_bias_term,
        wup,
        bup,
        wdown,
        bdown,
    ) = (
        lax.all_gather(norm1_gain, "fsdp", axis=0, tiled=True),
        lax.all_gather(attention_norm_bias, "fsdp", axis=0, tiled=True),
        lax.all_gather(qkv_weight, "fsdp", axis=0, tiled=True),
        lax.all_gather(qkv_bias, "fsdp", axis=0, tiled=True),
        lax.all_gather(out_weight, "fsdp", axis=0, tiled=True),
        lax.all_gather(out_bias, "fsdp", axis=0, tiled=True),
        lax.all_gather(norm2_gain, "fsdp", axis=0, tiled=True),
        lax.all_gather(feedforward_norm_bias, "fsdp", axis=0, tiled=True),
        lax.all_gather(up_weight, "fsdp", axis=0, tiled=True),
        lax.all_gather(up_bias, "fsdp", axis=0, tiled=True),
        lax.all_gather(down_weight, "fsdp", axis=0, tiled=True),
        lax.all_gather(down_bias, "fsdp", axis=0, tiled=True),
    )
    width = H * HD
    hidden_rows = hidden_in[0]
    cotan_rows = cotangent[0]
    local_rows = hidden_rows.shape[0]
    ctx_count = lax.axis_size("ctx")
    ctx_rank = lax.axis_index("ctx")
    seq_rows = local_rows * ctx_count
    all_pos = (block_order[:, None] * BLK + jnp.arange(BLK, dtype=jnp.int32)[None, :]).reshape(
        seq_rows
    )
    own_pos = lax.dynamic_slice_in_dim(all_pos, ctx_rank * local_rows, local_rows, 0)
    cosine, sine = rotary_tables(own_pos)
    attention_norm_gain = attention_norm_gain.astype(jnp.float32)
    feedforward_norm_gain = feedforward_norm_gain.astype(jnp.float32)
    residual_stream = hidden_rows.astype(jnp.float32)
    attention_normed, attention_standardized, attention_inverse_deviation = apply_layer_norm(
        residual_stream, attention_norm_gain, attention_bias_term.astype(jnp.float32)
    )
    normed1_b = attention_normed.astype(jnp.bfloat16)
    projected = jnp.dot(normed1_b, wqkv, preferred_element_type=jnp.float32) + bqkv.astype(
        jnp.float32
    )
    query = rotate(projected[:, :width].reshape(local_rows, H, HD), cosine, sine).astype(
        jnp.bfloat16
    )
    key_rows = rotate(
        projected[:, width : 2 * width].reshape(local_rows, H, HD), cosine, sine
    ).astype(jnp.bfloat16)
    value_rows = projected[:, 2 * width :].astype(jnp.bfloat16)
    keys_all, values_all = (
        lax.all_gather(key_rows.reshape(local_rows, width), "ctx", axis=0, tiled=True),
        lax.all_gather(value_rows, "ctx", axis=0, tiled=True),
    )
    keys_all = keys_all.reshape(seq_rows, H, HD)
    values_all = values_all.reshape(seq_rows, H, HD)
    attended, log_total = forward_attention(query, keys_all, values_all, own_pos, all_pos)
    attended_b = attended.reshape(local_rows, width).astype(jnp.bfloat16)
    attn_out = jnp.dot(attended_b, wout, preferred_element_type=jnp.float32) + bout.astype(
        jnp.float32
    )
    feedforward_normed, feedforward_standardized, feedforward_inverse_deviation = apply_layer_norm(
        residual_stream, feedforward_norm_gain, feedforward_bias_term.astype(jnp.float32)
    )
    normed2_b = feedforward_normed.astype(jnp.bfloat16)
    up_rows = jnp.dot(normed2_b, wup, preferred_element_type=jnp.float32) + bup.astype(jnp.float32)
    act_b = gelu_exact(up_rows).astype(jnp.bfloat16)
    mlp_out = jnp.dot(act_b, wdown, preferred_element_type=jnp.float32) + bdown.astype(jnp.float32)
    hidden_out = (residual_stream + attn_out + mlp_out).astype(jnp.bfloat16)
    cotan_wide = cotan_rows.astype(jnp.float32)
    grad_wdown = jnp.einsum("tk,tn->kn", act_b, cotan_rows, preferred_element_type=jnp.float32)
    grad_bdown = jnp.sum(cotan_wide, axis=0)
    d_up = jnp.einsum(
        "tn,kn->tk", cotan_rows, wdown, preferred_element_type=jnp.float32
    ) * gelu_slope(up_rows)
    d_up16 = d_up.astype(jnp.bfloat16)
    grad_wup = jnp.einsum("tk,tn->kn", normed2_b, d_up16, preferred_element_type=jnp.float32)
    grad_bup = jnp.sum(d_up, axis=0)
    grad_feedforward_normed = jnp.einsum(
        "tn,kn->tk", d_up16, wup, preferred_element_type=jnp.float32
    )
    grad_feedforward_gain = jnp.sum(grad_feedforward_normed * feedforward_standardized, axis=0)
    grad_shift2 = jnp.sum(grad_feedforward_normed, axis=0)
    feedforward_branch_grad = layer_norm_backward(
        grad_feedforward_normed,
        feedforward_standardized,
        feedforward_inverse_deviation,
        feedforward_norm_gain,
    )
    grad_wout = jnp.einsum("tk,tn->kn", attended_b, cotan_rows, preferred_element_type=jnp.float32)
    d_att = jnp.einsum("tn,kn->tk", cotan_rows, wout, preferred_element_type=jnp.float32).astype(
        jnp.bfloat16
    )
    delta = jnp.sum(
        d_att.reshape(local_rows, H, HD).astype(jnp.float32)
        * attended_b.reshape(local_rows, H, HD).astype(jnp.float32),
        axis=-1,
    )
    d_att3 = d_att.reshape(local_rows, H, HD)
    d_query, key_grads, value_grads = query_grads(
        query, d_att3, log_total, delta, own_pos, keys_all, values_all, all_pos
    )
    d_key, d_value = (
        lax.psum_scatter(
            key_grads.reshape(seq_rows, width), "ctx", scatter_dimension=0, tiled=True
        ),
        lax.psum_scatter(
            value_grads.reshape(seq_rows, width), "ctx", scatter_dimension=0, tiled=True
        ),
    )
    d_query = rotate_back(d_query, cosine, sine)
    d_key = rotate_back(d_key.reshape(local_rows, H, HD), cosine, sine)
    d_qkv = jnp.concatenate(
        [d_query.reshape(local_rows, width), d_key.reshape(local_rows, width), d_value], axis=1
    )
    d_qkv16 = d_qkv.astype(jnp.bfloat16)
    grad_wqkv = jnp.einsum("tk,tn->kn", normed1_b, d_qkv16, preferred_element_type=jnp.float32)
    grad_bqkv = jnp.sum(d_qkv, axis=0)
    grad_attention_normed = jnp.einsum(
        "tn,kn->tk", d_qkv16, wqkv, preferred_element_type=jnp.float32
    )
    grad_attention_gain = jnp.sum(grad_attention_normed * attention_standardized, axis=0)
    grad_shift1 = jnp.sum(grad_attention_normed, axis=0)
    attention_branch_grad = layer_norm_backward(
        grad_attention_normed,
        attention_standardized,
        attention_inverse_deviation,
        attention_norm_gain,
    )
    hidden_grad = cotan_wide + attention_branch_grad + feedforward_branch_grad
    terms = (
        grad_attention_gain,
        grad_shift1,
        grad_wqkv,
        grad_bqkv,
        grad_wout,
        grad_bdown,
        grad_feedforward_gain,
        grad_shift2,
        grad_wup,
        grad_bup,
        grad_wdown,
        grad_bdown,
    )
    shares = (
        lax.psum_scatter(terms[0], "fsdp", scatter_dimension=0, tiled=True),
        lax.psum_scatter(terms[1], "fsdp", scatter_dimension=0, tiled=True),
        lax.psum_scatter(terms[2], "fsdp", scatter_dimension=0, tiled=True),
        lax.psum_scatter(terms[3], "fsdp", scatter_dimension=0, tiled=True),
        lax.psum_scatter(terms[4], "fsdp", scatter_dimension=0, tiled=True),
        lax.psum_scatter(terms[5], "fsdp", scatter_dimension=0, tiled=True),
        lax.psum_scatter(terms[6], "fsdp", scatter_dimension=0, tiled=True),
        lax.psum_scatter(terms[7], "fsdp", scatter_dimension=0, tiled=True),
        lax.psum_scatter(terms[8], "fsdp", scatter_dimension=0, tiled=True),
        lax.psum_scatter(terms[9], "fsdp", scatter_dimension=0, tiled=True),
        lax.psum_scatter(terms[10], "fsdp", scatter_dimension=0, tiled=True),
        lax.psum_scatter(terms[11], "fsdp", scatter_dimension=0, tiled=True),
    )
    shares = lax.psum(
        (
            shares[0],
            shares[1],
            shares[2],
            shares[3],
            shares[4],
            shares[5],
            shares[6],
            shares[7],
            shares[8],
            shares[9],
            shares[10],
            shares[11],
        ),
        "ctx",
    )
    return (
        hidden_out[None],
        hidden_grad[None],
        shares[0],
        shares[1],
        shares[2],
        shares[3],
        shares[4],
        shares[5],
        shares[6],
        shares[7],
        shares[8],
        shares[9],
        shares[10],
        shares[11],
    )


MESH_IDS = pl.DeviceIdType.MESH
NN = (((1,), (0,)), ((), ()))
NT = (((1,), (1,)), ((), ()))
TN = (((0,), (0,)), ((), ()))
QTILE = 256
SEMAPHORES = 160


def mm(left, right, dims=NN):
    return lax.dot_general(left, right, dims, preferred_element_type=jnp.float32)


def flip(index, bit):
    return index + bit - 2 * bit * ((index // bit) % 2)


def run_when(condition, action):
    if condition is None:
        action()
    else:
        pl.when(condition)(action)


def narrow(values):
    return values.astype(jnp.bfloat16)


def wide(values):
    return values.astype(jnp.float32)


class Copies:
    def __init__(self, send_sems, recv_sems):
        self.send_sems, self.recv_sems = send_sems, recv_sems
        self.count, self.started, self.numbers = 0, [], {}

    def make(self, source, target, device, when=None, like=None):
        if like is None:
            number = self.count
            self.count += 1
        else:
            number = self.numbers[id(like)]
        copy = pltpu.make_async_remote_copy(
            src_ref=source,
            dst_ref=target,
            send_sem=self.send_sems.at[number],
            recv_sem=self.recv_sems.at[number],
            device_id=device,
            device_id_type=MESH_IDS,
        )
        self.started.append((copy, when))
        self.numbers[id(copy)] = number
        return copy

    def settle(self, chosen):
        numbers = {id(copy) for copy in chosen}
        for copy, when in self.started:
            if id(copy) in numbers:
                run_when(when, copy.wait_send)
        self.started = [entry for entry in self.started if id(entry[0]) not in numbers]

    def finish(self):
        for copy, when in self.started:
            run_when(when, copy.wait_send)


class Place:
    def __init__(self, nz):
        self.nz = nz
        self.c, self.z = lax.axis_index("ctx"), lax.axis_index("fsdp")
        self.k, self.t = self.c % 2, self.c // 2
        self.xn, self.yn, self.pn = flip(self.c, 2), flip(self.c, 4), flip(self.c, 1)
        self.dn = flip(self.xn, 4)
        self.tx, self.ty = flip(self.t, 1), flip(self.t, 2)
        self.td = flip(self.tx, 2)
        self.others = [(self.z + d) % nz for d in range(1, nz)]
        self.plane = [self.xn, self.yn, self.dn, self.pn] + [
            flip(peer, 1) for peer in (self.xn, self.yn, self.dn)
        ]
        self.above, self.below = jnp.minimum(self.z + 1, nz - 1), jnp.maximum(self.z - 1, 0)

    def on_plane(self, c):
        return (c, self.z)

    def on_line(self, z):
        return (self.c, z)

    def greet(self):
        barrier = pltpu.get_barrier_semaphore()
        peers = [self.on_plane(peer) for peer in self.plane] + [self.on_line(z) for z in self.others]
        for peer in peers:
            pl.semaphore_signal(barrier, inc=1, device_id=peer, device_id_type=MESH_IDS)
        pl.semaphore_wait(barrier, len(peers))


class PlaneShare:
    def __init__(self, copies, me, source, slot, rows):
        self.copies, self.me, self.slot = copies, me, slot
        top, bottom = pl.ds(0, rows // 2), pl.ds(rows // 2, rows // 2)
        own = slot(me.k, me.t)
        to_x, to_y = me.on_plane(me.xn), me.on_plane(me.yn)
        self.x_first = copies.make(source.at[top], own.at[top], to_x)
        self.y_first = copies.make(source.at[bottom], own.at[bottom], to_y)
        self.x_second = copies.make(source.at[bottom], own.at[bottom], to_x)
        self.y_second = copies.make(source.at[top], own.at[top], to_y)
        self.to_p = copies.make(source, own, me.on_plane(me.pn))
        through_x, through_y = slot(me.k, me.tx).at[top], slot(me.k, me.ty).at[bottom]
        self.hop_y = copies.make(through_x, through_x, to_y)
        self.hop_x = copies.make(through_y, through_y, to_x)
        self.swaps = []
        for chip in (me.tx, me.ty, me.td):
            place = slot(me.k, chip)
            self.swaps.append(copies.make(place, place, me.on_plane(me.pn)))

    def start(self):
        for copy in (self.x_first, self.y_first, self.x_second, self.y_second, self.to_p):
            copy.start()

    def relay(self):
        self.x_first.wait_recv()
        self.hop_y.start()
        self.y_first.wait_recv()
        self.hop_x.start()

    def swap(self):
        self.x_second.wait_recv()
        self.swaps[0].start()
        self.y_second.wait_recv()
        self.swaps[1].start()

    def on_diagonal(self):
        self.hop_y.wait_recv()
        self.hop_x.wait_recv()
        self.swaps[2].start()

    def finish(self):
        for copy in (self.to_p, *self.swaps):
            copy.wait_recv()


class LineGather:
    def __init__(self, copies, me, source, gathered):
        self.copies, self.me, self.gathered = copies, me, gathered
        rows = gathered.shape[1] // 2
        self.mine = pl.ds(me.k * rows, rows)
        self.moves, self.swaps = {}, []
        for step in range(me.nz - 1):
            for sign in (1, -1):
                shard, target = me.z - sign * step, me.z + sign
                ok = (shard >= 0) & (shard < me.nz) & (target >= 0) & (target < me.nz)
                place = self.slot(shard)
                copy = copies.make(
                    source.at[self.mine] if step == 0 else place,
                    place,
                    me.on_line(jnp.clip(target, 0, me.nz - 1)),
                    when=ok,
                )
                self.moves[step, sign] = (copy, ok)

    def slot(self, shard):
        return self.gathered.at[jnp.clip(shard, 0, self.me.nz - 1), self.mine]

    def start(self):
        for sign in (1, -1):
            copy, ok = self.moves[0, sign]
            run_when(ok, copy.start)

    def advance(self, step):
        me = self.me
        for sign in (1, -1):
            arrived = me.z - sign * (step + 1)
            ok = (arrived >= 0) & (arrived < me.nz)
            run_when(ok, self.moves[step, sign][0].wait_recv)
            if step + 1 < me.nz - 1:
                copy, following = self.moves[step + 1, sign]
                run_when(following, copy.start)
            place = self.slot(arrived)
            swap = self.copies.make(place, place, me.on_plane(me.pn), when=ok)
            run_when(ok, swap.start)
            self.swaps.append((swap, ok))

    def finish(self):
        for swap, ok in self.swaps:
            run_when(ok, swap.wait_recv)


class LineSpread:
    def __init__(self, copies, me, source, target):
        self.me, self.source, self.target = me, source, target
        rows = target.shape[0] // 2
        mine = pl.ds(me.k * rows, rows)
        self.here, self.away = me.z == me.t, me.z != me.t
        place = target.at[mine]
        self.sends, self.arrivals = [], []
        for distance in range(1, me.nz):
            target_z = (me.t + distance) % me.nz
            copy = copies.make(source.at[mine], place, me.on_line(target_z), when=self.here)
            self.sends.append(copy)
            self.arrivals.append(me.z == target_z)
        self.swap = copies.make(place, place, me.on_plane(me.pn), when=self.away)

    def start(self):
        @pl.when(self.here)
        def _():
            for copy in self.sends:
                copy.start()
            self.target[...] = self.source[...]

    def advance(self):
        for copy, arrives in zip(self.sends, self.arrivals):
            pl.when(arrives)(copy.wait_recv)
        pl.when(self.away)(self.swap.start)

    def finish(self):
        pl.when(self.away)(self.swap.wait_recv)


class LineReduce:
    def __init__(self, copies, me, source, total, landed):
        self.me, self.source, self.total, self.landed = me, source, total, landed
        half = total.shape[1]
        self.mine, theirs = pl.ds(me.k * half, half), pl.ds((1 - me.k) * half, half)
        self.exchange = copies.make(source.at[:, theirs], total, me.on_plane(me.pn))
        self.sends = [
            copies.make(total.at[other], landed.at[me.z], me.on_line(other)) for other in me.others
        ]

    def start(self):
        self.exchange.start()

    def pair(self):
        self.exchange.wait_recv()
        for owner in range(self.me.nz):
            self.total[owner] = narrow(
                wide(self.total[owner]) + wide(self.source[owner, self.mine])
            )
        for send in self.sends:
            send.start()

    def collect(self):
        me = self.me
        result = wide(self.total[me.z])
        for send in self.sends:
            send.wait_recv()
        for other in me.others:
            result = result + wide(self.landed[other])
        self.total[me.z] = narrow(result)


class LineCollect:
    def __init__(self, copies, me, source, total, landed):
        self.me, self.source, self.total, self.landed = me, source, total, landed
        half = total.shape[0]
        self.mine, theirs = pl.ds(me.k * half, half), pl.ds((1 - me.k) * half, half)
        self.exchange = copies.make(source.at[theirs], total, me.on_plane(me.pn))
        self.sends = []
        for distance in range(1, me.nz):
            leaves = (me.z + distance) % me.nz == me.t
            copy = copies.make(total, landed.at[me.z], me.on_line(me.t), when=leaves)
            self.sends.append((copy, leaves))

    def start(self):
        self.exchange.start()

    def pair(self):
        self.exchange.wait_recv()
        self.total[...] = narrow(wide(self.total[...]) + wide(self.source[self.mine]))
        for copy, leaves in self.sends:
            pl.when(leaves)(copy.start)

    def collect(self):
        me = self.me

        @pl.when(me.z == me.t)
        def _():
            result = wide(self.total[...])
            for copy, _ in self.sends:
                copy.wait_recv()
            for other in me.others:
                result = result + wide(self.landed[other])
            self.total[...] = narrow(result)


class PlaneSpread:
    def __init__(self, copies, me, source, target, rows):
        self.me, self.source, self.target = me, source, target
        top, bottom = pl.ds(0, rows // 2), pl.ds(rows // 2, rows // 2)
        place = target.at[me.k]
        self.here, self.from_x, self.from_y = me.t == me.z, me.tx == me.z, me.ty == me.z
        self.from_d = me.td == me.z
        self.to_x = copies.make(source, place, me.on_plane(me.xn), when=self.here)
        self.to_y = copies.make(source, place, me.on_plane(me.yn), when=self.here)
        self.to_p = copies.make(source, place, me.on_plane(me.pn), when=self.here)
        self.hop_y = copies.make(place.at[top], place.at[top], me.on_plane(me.yn), when=self.from_x)
        self.hop_x = copies.make(
            place.at[bottom], place.at[bottom], me.on_plane(me.xn), when=self.from_y
        )
        away = self.from_x | self.from_y | self.from_d
        self.away = away
        self.swap = copies.make(place, place, me.on_plane(me.pn), when=away, like=self.to_p)

    def start(self):
        @pl.when(self.here)
        def _():
            self.to_x.start()
            self.to_y.start()
            self.to_p.start()
            self.target[self.me.k] = self.source[...]

    def advance(self):
        @pl.when(self.from_x)
        def _():
            self.to_x.wait_recv()
            self.hop_y.start()
            self.swap.start()

        @pl.when(self.from_y)
        def _():
            self.to_y.wait_recv()
            self.hop_x.start()
            self.swap.start()

    def on_diagonal(self):
        @pl.when(self.from_d)
        def _():
            self.hop_y.wait_recv()
            self.hop_x.wait_recv()
            self.swap.start()

    def finish(self):
        self.to_p.wait_recv()

def norm_rows(values_in):
    centre = jnp.mean(values_in, axis=-1, keepdims=True)
    mean_removed = values_in - centre
    inverse_deviation = lax.rsqrt(
        jnp.mean(mean_removed * mean_removed, axis=-1, keepdims=True) + EPS
    )
    return mean_removed * inverse_deviation, inverse_deviation


def head_rows(rows, head):
    lanes = lax.broadcasted_iota(jnp.int32, rows.shape, 1)
    inside = (lanes >= head * HD) & (lanes < (head + 1) * HD)
    return jnp.where(inside, rows, jnp.zeros_like(rows))


def rope_lanes(r, first, blocks, columns, back):
    half_rot = ROT // 2
    tables = [[], [], []]
    row_cos, row_sin = r.rope_r[:, :128], r.rope_r[:, 128:]
    lane = lax.broadcasted_iota(jnp.int32, row_cos.shape, 1) % HD
    for block in range(blocks):
        both = r.rope_b[pl.ds(first + block, 1), :]
        block_cos, block_sin = both[:, :128], both[:, 128:]
        cosine = block_cos * row_cos - block_sin * row_sin
        sine = block_sin * row_cos + block_cos * row_sin
        if back:
            sine = -sine
        tables[0].append(cosine)
        tables[1].append(jnp.where(lane < half_rot, -sine, 0.0))
        tables[2].append(jnp.where(lane >= half_rot, sine, 0.0))
    stacked = [jnp.concatenate(table, axis=0) for table in tables]
    return [jnp.concatenate([table] * (columns // 128), axis=1) for table in stacked]


def turn(values, tables):
    columns, half_rot = values.shape[1], ROT // 2
    return (
        values * tables[0]
        + pltpu.roll(values, columns - half_rot, 1) * tables[1]
        + pltpu.roll(values, half_rot, 1) * tables[2]
    )


def slice_weights(r, me):
    part = r.wqs.shape[1] // 3
    chips = r.wqkv.shape[1] // r.wqs.shape[1]
    for chip in range(chips):

        @pl.when(me.t == chip)
        def _():
            for source, target in ((r.wqkv, r.wqs), (r.wup, r.wus)):
                for piece in range(target.shape[1] // part):
                    first = (piece * chips + chip) * part
                    target[:, piece * part : (piece + 1) * part] = source[:, first : first + part]


VECTORS = ("gain1", "shift1", "gain2", "shift2", "bout", "bdown", "bqkv", "bup")


def pack_vectors(r):
    first = 0
    for name in VECTORS:
        values = wide(getattr(r, name)[...])
        count = values.shape[0]
        r.sm[0:1, first : first + count] = values.reshape(1, count)
        first += count


def read_vectors(r, me):
    nz, part = me.nz, r.vec.shape[1] // me.nz

    def piece(z, number):
        return r.sm4[z, 0:1, number * part : (number + 1) * part]

    for z in range(nz):
        span = slice(z * part, (z + 1) * part)
        for row in range(4):
            r.vec[row : row + 1, span] = piece(z, row)
        r.vec[4:5, span] = piece(z, 4) + piece(z, 5)
    chips = nz
    for chip in range(chips):

        @pl.when(me.t == chip)
        def _():
            for number in range(3):
                held = number * chips + chip
                r.vec[5:6, number * part : (number + 1) * part] = piece(held // 3, 6 + held % 3)
            for z in range(nz):
                r.vec[6:7, z * part : (z + 1) * part] = piece(z, 9 + chip)


def block_table(r, me):
    count = r.order.shape[0]
    chips, quarter = me.nz, count // 4
    sides = count // (2 * chips)
    held = [r.order[number] for number in range(count)]
    for position in range(count):
        found = 0
        for number in range(1, count):
            found = jnp.where(held[number] == position, number, found)
        r.idx[position] = found
    for chip in range(chips):
        for owner, first in ((me.k, count), (1 - me.k, count + chips * sides)):
            for side in range(sides):
                position = r.order[(2 * chip + owner) * sides + side]
                low = (position >= quarter * me.k) & (position < quarter * (me.k + 1))
                high = position - 2 * quarter + quarter * me.k
                r.idx[first + chip * sides + side] = jnp.where(
                    low, position - quarter * me.k, jnp.clip(high, 0, 2 * quarter - 1)
                )
        position = r.order[(2 * chip + me.k) * sides]
        outer = jnp.where((position < quarter) | (position >= 3 * quarter), 0, 1)
        r.idx[count + 2 * chips * sides + chip] = jnp.where(outer == me.k, 1, 0)


def sorted_rows(r, source, block, blocks):
    pieces = []
    for number in range(blocks):
        pieces.append(source[r.idx[block + number]])
    return jnp.concatenate(pieces, axis=0)


def flat_rows(values):
    return values.reshape(-1, values.shape[-1])


def put_blocks(target, tile, values):
    blocks = values.shape[0] // BLK
    target[pl.ds(tile * blocks, blocks)] = values.reshape(blocks, BLK, values.shape[1])


def project(r, tile):
    part = r.q.shape[1]
    blocks = QTILE // BLK
    standardized, _ = norm_rows(wide(sorted_rows(r, r.hall, tile * blocks, blocks)))
    normed = narrow(standardized * r.vec[0:1, :] + r.vec[1:2, :])
    weight = r.wq4[...].reshape(-1, 3 * part)
    projected = mm(normed, weight) + r.vec[5:6, : 3 * part]
    turned = turn(
        projected[:, : 2 * part], rope_lanes(r, tile * blocks, blocks, 2 * part, False)
    )
    place = pl.ds(pl.multiple_of(tile * QTILE, QTILE), QTILE)
    r.q[place, :] = narrow(wide(narrow(turned[:, :part])) * HD**-0.5)
    keys, values = turned[:, part:], projected[:, 2 * part :]
    r.k[place, :] = narrow(keys)
    r.v[place, :] = narrow(values)
    r.kt[:, place] = narrow(keys.T)
    r.vt[:, place] = narrow(values.T)


def tile_start(r, me, tile):
    quarter = r.k.shape[0] // 4
    low = tile < quarter // QTILE
    inside = tile * QTILE - jnp.where(low, 0, quarter)
    return jnp.where(low, quarter * me.k, 3 * quarter - quarter * me.k) + inside


def attend(r, me, tile):
    part = r.k.shape[1]
    heads = part // HD
    start = tile_start(r, me, tile)
    rows = slice(tile * QTILE, (tile + 1) * QTILE)
    query = r.q[pl.ds(pl.multiple_of(start, QTILE), QTILE), :]
    per_head = [head_rows(query, head) for head in range(heads)]

    def visit(number, state, masked):
        place = pl.ds(pl.multiple_of(number * QTILE, QTILE), QTILE)
        keys = r.k[place, :]
        result = []
        for head in range(heads):
            top, total, acc = state[head]
            logits = mm(keys, per_head[head], NT)
            if masked:
                key_row = lax.broadcasted_iota(jnp.int32, logits.shape, 0)
                query_row = lax.broadcasted_iota(jnp.int32, logits.shape, 1)
                logits = jnp.where(key_row <= query_row, logits, NEG)
            new_top = jnp.maximum(top, jnp.max(logits, axis=0, keepdims=True))
            fade = jnp.exp(top - new_top)
            probs = jnp.exp(logits - new_top)
            total = total * fade + jnp.sum(probs, axis=0, keepdims=True)
            values = r.vt[head * HD : (head + 1) * HD, place]
            acc = acc * fade + mm(values, narrow(probs))
            result.append((new_top, total, acc))
        return tuple(result)

    state = tuple(
        (
            jnp.full((1, QTILE), NEG, jnp.float32),
            jnp.zeros((1, QTILE), jnp.float32),
            jnp.zeros((HD, QTILE), jnp.float32),
        )
        for _ in range(heads)
    )
    last = start // QTILE
    state = lax.fori_loop(0, last, lambda n, s: visit(n, s, False), state)
    state = visit(last, state, True)
    merged = jnp.concatenate([acc / total for _, total, acc in state], axis=0)
    r.att[rows, :] = narrow(merged.T)
    r.attt[:, rows] = narrow(merged)
    for head in range(heads):
        r.lse[head : head + 1, rows] = state[head][0] + jnp.log(state[head][1])


def feed_forward(r, me, tile):
    place = pl.ds(pl.multiple_of(tile * QTILE, QTILE), QTILE)
    blocks = QTILE // BLK
    block = tile_start(r, me, tile) // BLK
    width = r.hall.shape[2]
    standardized, _ = norm_rows(wide(sorted_rows(r, r.hall, block, blocks)))
    cotan = sorted_rows(r, r.gall, block, blocks)
    gain2 = r.vec[2:3, :]
    normed = narrow(standardized * gain2 + r.vec[3:4, :])
    up_weight = r.wu4[...].reshape(width, -1)
    down_weight = r.wd4[...].reshape(-1, width)
    up = mm(normed, up_weight) + r.vec[6:7, :]
    below = 0.5 * (1.0 + lax.erf(up * SQRT_HALF))
    act = narrow(up * below)
    slope = below + up * jnp.exp(-0.5 * up * up) * INV_ROOT_TWO_PI
    d_up = mm(cotan, down_weight, NT) * slope
    d_up16 = narrow(d_up)
    put_blocks(r.outb, tile, narrow(mm(act, down_weight)))
    d_normed = mm(d_up16, up_weight, NT)
    r.sums[2:3, :] += jnp.sum(d_normed * standardized, axis=0, keepdims=True)
    r.sums[3:4, :] += jnp.sum(d_normed, axis=0, keepdims=True)
    r.sums[6:7, :] += jnp.sum(d_up, axis=0, keepdims=True)
    r.e2[place, :] = d_normed * gain2
    r.n[place, :] = normed
    r.gl[place, :] = cotan
    r.act[place, :] = act
    r.du[place, :] = d_up16


def out_project(r, me, tile):
    place = pl.ds(pl.multiple_of(tile * QTILE, QTILE), QTILE)
    blocks = QTILE // BLK
    attended = r.att[place, :]
    mlp = flat_rows(r.outb[pl.ds(tile * blocks, blocks)])
    put_blocks(r.outb, tile, narrow(wide(mlp) + mm(attended, r.wo1[...])))
    cotan = r.gl[place, :]
    r.datt[place, :] = narrow(mm(cotan, r.wo1[...], NT))
    product = wide(narrow(mm(r.wo1[...], cotan, NT))) * wide(r.attt[:, place])
    for head in range(product.shape[0] // HD):
        r.delta[head : head + 1, place] = jnp.sum(
            product[head * HD : (head + 1) * HD], axis=0, keepdims=True
        )


def weight_grad(target, left, right):
    rows, columns = left.shape[1], right.shape[1]
    shard = target.shape[1]
    values = right[...]
    for first in range(0, rows, QTILE):
        result = narrow(mm(left[:, first : first + QTILE], values, TN))
        at = first
        while at < first + QTILE:
            owner, inside = at // shard, at % shard
            until = min((owner + 1) * shard, first + QTILE)
            target[owner, inside : inside + until - at, :] = result[at - first : until - first, :]
            at = until


def attend_grad(r, me, tile):
    part = r.k.shape[1]
    heads = part // HD
    kstep = 2 * QTILE
    start = tile_start(r, me, tile)
    rows = slice(tile * QTILE, (tile + 1) * QTILE)
    query = r.q[pl.ds(pl.multiple_of(start, QTILE), QTILE), :]
    d_out = r.datt[rows, :]
    queries = jnp.concatenate([head_rows(query, head) for head in range(heads)], axis=0)
    d_outs = jnp.concatenate([head_rows(d_out, head) for head in range(heads)], axis=0)

    def visit(number, state, masked):
        place = pl.ds(pl.multiple_of(number * kstep, kstep), kstep)
        keys, values = r.k[place, :], r.v[place, :]
        probs_all, d_logits_all, result = [], [], []
        for head in range(heads):
            own = slice(head * QTILE, (head + 1) * QTILE)
            logits = mm(keys, queries[own], NT)
            probs = jnp.exp(logits - r.lse[head : head + 1, rows])
            if masked:
                key_row = number * kstep + lax.broadcasted_iota(jnp.int32, logits.shape, 0)
                query_row = start + lax.broadcasted_iota(jnp.int32, logits.shape, 1)
                probs = jnp.where(key_row <= query_row, probs, 0.0)
            d_probs = mm(values, d_outs[own], NT)
            d_logits = narrow(probs * (d_probs - r.delta[head : head + 1, rows]))
            probs_all.append(narrow(probs))
            d_logits_all.append(d_logits)
            result.append(state[head] + mm(r.kt[head * HD : (head + 1) * HD, place], d_logits))
        r.dv[place, :] += mm(jnp.concatenate(probs_all, axis=1), d_outs)
        r.dk[place, :] += mm(jnp.concatenate(d_logits_all, axis=1), queries)
        return tuple(result)

    state = tuple(jnp.zeros((HD, QTILE), jnp.float32) for _ in range(heads))
    last = start // kstep
    state = lax.fori_loop(0, last, lambda n, s: visit(n, s, False), state)
    state = visit(last, state, True)
    r.dqt[:, rows] = jnp.concatenate(state, axis=0)


def qkv_grad(r, me, tile):
    place = pl.ds(pl.multiple_of(tile * QTILE, QTILE), QTILE)
    part = r.k.shape[1]
    blocks = QTILE // BLK
    start = tile_start(r, me, tile)
    block = start // BLK
    held = pl.ds(pl.multiple_of(start, QTILE), QTILE)
    standardized, _ = norm_rows(wide(sorted_rows(r, r.hall, block, blocks)))
    gain1 = r.vec[0:1, :]
    r.n[place, :] = narrow(standardized * gain1 + r.vec[1:2, :])
    d_query = r.dqt[:, place].T * HD**-0.5
    d_key = r.dk[held, :] + wide(r.kvin[place, :part])
    d_value = r.dv[held, :] + wide(r.kvin[place, part:])
    turned = turn(
        jnp.concatenate([d_query, d_key], axis=1), rope_lanes(r, block, blocks, 2 * part, True)
    )
    d_qkv = jnp.concatenate([turned, d_value], axis=1)
    d_qkv16 = narrow(d_qkv)
    r.du[place, : 3 * part] = d_qkv16
    r.sums[5:6, : 3 * part] += jnp.sum(d_qkv, axis=0, keepdims=True)
    weight = r.wq4[...].reshape(-1, 3 * part)
    d_normed = mm(d_qkv16, weight, NT)
    r.sums[0:1, :] += jnp.sum(d_normed * standardized, axis=0, keepdims=True)
    r.sums[1:2, :] += jnp.sum(d_normed, axis=0, keepdims=True)
    put_blocks(r.outb, tile, narrow(d_normed * gain1 + r.e2[place, :]))


class Scatter:
    def __init__(self, copies, me, r, source, sent, got, landed):
        self.me, self.r, self.source, self.sent, self.got, self.landed = me, r, source, sent, got, landed
        self.chips = me.nz
        self.sides = sent.shape[0] // self.chips
        self.first = r.k.shape[0] // BLK
        self.exchanges = [
            copies.make(self.piece(sent, chip), self.piece(got, chip), me.on_plane(me.pn))
            for chip in range(self.chips)
        ]
        self.steps = []
        for side, near, far, to_near, to_far in (
            (0, me.tx, me.ty, me.xn, me.yn),
            (1, me.ty, me.tx, me.yn, me.xn),
        ):
            first, last = self.place(near, side), self.place(far, side)
            self.steps.append(
                (
                    copies.make(got.at[self.place(me.td, side)], landed.at[3 * side], me.on_plane(to_near)),
                    copies.make(got.at[first], landed.at[3 * side + 1], me.on_plane(to_near)),
                    copies.make(got.at[last], landed.at[3 * side + 2], me.on_plane(to_far)),
                    last,
                )
            )

    def place(self, chip, side):
        return chip * self.sides + side

    def piece(self, array, chip):
        return array.at[pl.ds(chip * self.sides, self.sides)]

    def block(self, number):
        return self.source[self.r.idx[self.first + number]]

    def start(self):
        count = self.chips * self.sides
        for number in range(count):
            self.sent[number] = self.block(count + number)
        for exchange in self.exchanges:
            exchange.start()

    def spread(self):
        count = self.chips * self.sides
        for exchange in self.exchanges:
            exchange.wait_recv()
        for number in range(count):
            flag = self.r.idx[self.first + 2 * count + number // self.sides]
            own, other = wide(self.block(number)), wide(self.got[number])
            here = jnp.full(own.shape, flag, jnp.int32) > 0
            self.got[number] = narrow(jnp.where(here, own, other))
        for far, _, _, _ in self.steps:
            far.start()
        for _, near, _, _ in self.steps:
            near.start()

    def middle(self):
        for side, (far, _, on, last) in enumerate(self.steps):
            far.wait_recv()
            self.got[last] = narrow(wide(self.got[last]) + wide(self.landed[3 * side]))
            on.start()

    def total(self):
        pieces = []
        for side, (_, near, on, _) in enumerate(self.steps):
            near.wait_recv()
            on.wait_recv()
            pieces.append(
                wide(self.got[self.place(self.me.t, side)])
                + wide(self.landed[3 * side + 1])
                + wide(self.landed[3 * side + 2])
            )
        return jnp.concatenate(pieces, axis=0)


def layer_kernel(nz, names, *refs):
    r = types.SimpleNamespace(**dict(zip(names, refs)))
    me = Place(nz)
    copies = Copies(r.send_sems, r.recv_sems)
    sides = r.h.shape[0]
    shard = r.wqs.shape[0]
    tiles = r.att.shape[0] // QTILE

    slice_weights(r, me)
    pack_vectors(r)
    me.greet()

    def row_slot(array):
        return lambda core, chip: array.at[pl.ds((2 * chip + core) * sides, sides)]

    own_rows = pl.ds(me.c * sides, sides)
    h_share = PlaneShare(copies, me, r.h, row_slot(r.hall), sides)
    g_share = PlaneShare(copies, me, r.g, row_slot(r.gall), sides)
    wq = LineGather(copies, me, r.wqs, r.wq4)
    wu = LineGather(copies, me, r.wus, r.wu4)
    wd = LineGather(copies, me, r.wdown.at[pl.ds(me.t * shard, shard)], r.wd4)
    wo = LineSpread(copies, me, r.wout, r.wo1)
    small = [copies.make(r.sm, r.sm4.at[me.z], me.on_line(other)) for other in me.others]

    h_share.start()
    wq.start()
    for copy in small:
        copy.start()
    wu.start()
    own_down = pltpu.make_async_copy(
        r.wdown.at[pl.ds(me.t * shard, shard)], r.wd4.at[me.z], r.local_sem
    )
    own_down.start()
    r.hall[own_rows] = r.h[...]
    r.gall[own_rows] = r.g[...]
    r.wq4[me.z] = r.wqs[...]
    r.wu4[me.z] = r.wus[...]
    r.sm4[me.z] = r.sm[...]
    block_table(r, me)
    r.sums[...] = jnp.zeros_like(r.sums)
    r.vout[...] = jnp.zeros_like(r.vout)
    r.dk[...] = jnp.zeros_like(r.dk)
    r.dv[...] = jnp.zeros_like(r.dv)
    wq.advance(0)
    h_share.relay()
    wu.advance(0)
    wq.advance(1)
    wd.start()
    h_share.swap()
    g_share.start()
    for copy in small:
        copy.wait_recv()
    read_vectors(r, me)
    wq.advance(2)
    wu.advance(1)
    h_share.on_diagonal()
    wq.finish()
    h_share.finish()

    count = r.k.shape[0] // QTILE
    for first in (0, count // 2):

        @pl.loop(first, first + count // 2)
        def _(tile):
            project(r, tile)

        if first == 0:
            wd.advance(0)

    wu.advance(2)
    wd.advance(1)
    attend(r, me, 0)
    g_share.relay()
    attend(r, me, 1)
    wd.advance(2)
    wo.start()
    g_share.swap()
    attend(r, me, 2)
    g_share.on_diagonal()
    own_down.wait()
    wu.finish()
    wd.finish()
    g_share.finish()
    copies.settle([g_share.hop_x, g_share.hop_y, *g_share.swaps])

    @pl.loop(0, tiles)
    def _(tile):
        feed_forward(r, me, tile)

    half = shard // 2
    out_scatter = Scatter(copies, me, r, r.outb, r.osent, r.ogot, r.oland)
    up_reduce = LineReduce(copies, me, r.gu, r.tu, r.uu)
    down_reduce = LineReduce(copies, me, r.gd, r.td, r.ud)
    out_reduce = LineCollect(copies, me, r.go, r.to, r.uo)
    d_share = PlaneShare(copies, me, r.td.at[me.z], lambda core, chip: r.fd.at[core, chip], half)
    u_share = PlaneShare(copies, me, r.tu.at[me.z], lambda core, chip: r.fu.at[core, chip], half)
    o_spread = PlaneSpread(copies, me, r.to, r.fo, half)

    def share_down():
        d_share.start()
        r.fd[me.k, me.t] = r.td[me.z]

    def share_up():
        u_share.start()
        r.fu[me.k, me.t] = r.tu[me.z]

    weight_grad(r.gd, r.act, r.gl)
    down_reduce.start()
    weight_grad(r.gu, r.n, r.du)
    up_reduce.start()
    down_reduce.pair()
    wo.advance()
    up_reduce.pair()
    attend(r, me, 3)
    wo.finish()

    @pl.loop(0, tiles)
    def _(tile):
        out_project(r, me, tile)

    out_scatter.start()
    r.go[...] = narrow(mm(r.att[...], r.gl[...], TN))
    out_reduce.start()
    attend_grad(r, me, 0)
    out_scatter.spread()
    out_reduce.pair()
    attend_grad(r, me, 1)
    attend_grad(r, me, 2)
    down_reduce.collect()
    share_down()
    out_scatter.middle()
    attend_grad(r, me, 3)

    part = r.k.shape[1]
    quarter = r.k.shape[0] // 4
    kv_moves = []
    for number in range(2):
        first = quarter * (1 - me.k) if number == 0 else 3 * quarter - quarter * (1 - me.k)
        theirs = pl.ds(pl.multiple_of(first, quarter), quarter)
        rows = slice(number * quarter, (number + 1) * quarter)
        r.act[rows, :part] = narrow(r.dk[theirs, :])
        r.act[rows, part : 2 * part] = narrow(r.dv[theirs, :])
        copy = copies.make(r.act.at[rows, : 2 * part], r.kvin.at[rows], me.on_plane(me.pn))
        copy.start()
        kv_moves.append(copy)
    d_share.relay()
    up_reduce.collect()
    share_up()
    d_share.swap()
    out_reduce.collect()
    o_spread.start()
    for copy in kv_moves:
        copy.wait_recv()

    @pl.loop(0, tiles)
    def _(tile):
        qkv_grad(r, me, tile)

    e_scatter = Scatter(
        copies, me, r, r.outb, r.gall.at[: r.outb.shape[0]], r.gall.at[r.outb.shape[0] :], r.eland
    )
    e_scatter.start()
    u_share.relay()
    weight_grad(r.gq, r.n, r.du.at[:, : 3 * part])
    qkv_reduce = LineReduce(copies, me, r.gq, r.tq, r.uq)
    qkv_reduce.start()
    e_scatter.spread()
    qkv_reduce.pair()
    u_share.swap()
    o_spread.advance()

    vec_part = r.vec.shape[1] // nz
    r.sums[4:5, :] = jnp.sum(wide(flat_rows(r.g[...])), axis=0, keepdims=True)
    for z in range(nz):
        span = slice(z * vec_part, (z + 1) * vec_part)
        for row in range(4):
            r.vout[z, 0:1, row * vec_part : (row + 1) * vec_part] = r.sums[row : row + 1, span]
        r.vout[z, 1:2, :vec_part] = r.sums[4:5, span]
    for chip in range(nz):

        @pl.when(me.t == chip)
        def _():
            for piece in range(3):
                number = piece * nz + chip
                first = number % 3 * vec_part
                r.vout[number // 3, 2:3, first : first + vec_part] = r.sums[
                    5:6, piece * vec_part : (piece + 1) * vec_part
                ]
            for z in range(nz):
                r.vout[z, 3:4, chip * vec_part : (chip + 1) * vec_part] = r.sums[
                    6:7, z * vec_part : (z + 1) * vec_part
                ]

    vec_line = [
        copies.make(r.vout.at[other], r.vline.at[me.z], me.on_line(other)) for other in me.others
    ]
    for copy in vec_line:
        copy.start()
    d_share.on_diagonal()
    for copy in vec_line:
        copy.wait_recv()
    vector = r.vout[me.z]
    for other in me.others:
        vector = vector + r.vline[other]
    r.vsend[...] = vector
    e_scatter.middle()
    vec_plane = [copies.make(r.vsend, r.vplane.at[me.c], me.on_plane(peer)) for peer in me.plane]
    for copy in vec_plane:
        copy.start()
    u_share.on_diagonal()
    o_spread.on_diagonal()
    qkv_reduce.collect()
    q_share = PlaneShare(copies, me, r.tq.at[me.z], lambda core, chip: r.fq.at[core, chip], half)
    q_share.start()
    r.fq[me.k, me.t] = r.tq[me.z]

    residual = wide(flat_rows(r.h[...]))
    own_standardized, own_deviation = norm_rows(residual)
    r.hidden_out[...] = narrow(residual + r.vec[4:5, :] + out_scatter.total())
    q_share.relay()
    e_total = e_scatter.total()
    r.hidden_grad[...] = wide(flat_rows(r.g[...])) + own_deviation * (
        e_total
        - jnp.mean(e_total, axis=-1, keepdims=True)
        - own_standardized * jnp.mean(e_total * own_standardized, axis=-1, keepdims=True)
    )
    q_share.swap()
    for copy in vec_plane:
        copy.wait_recv()
    vector = r.vsend[...]
    for peer in me.plane:
        vector = vector + r.vplane[peer]
    r.vsum[...] = vector
    q_share.on_diagonal()
    d_share.finish()
    u_share.finish()
    o_spread.finish()
    q_share.finish()
    copies.finish()


def assemble_kernel(
    fq_ref, fu_ref, fd_ref, fo_ref, out_ref, grad_ref, vsum_ref,
    gq_ref, gu_ref, gd_ref, go_ref, hidden_out_ref, hidden_grad_ref, *vector_refs,
):
    _, chips, _, _ = fq_ref.shape
    part = fq_ref.shape[3] // 3
    hidden_out_ref[...] = out_ref[...]
    hidden_grad_ref[...] = grad_ref[...]
    go_ref[...] = wide(fo_ref[0])
    for chip in range(chips):
        for source, target in ((fq_ref, gq_ref), (fu_ref, gu_ref)):
            for piece in range(source.shape[3] // part):
                first = (piece * chips + chip) * part
                target[:, first : first + part] = wide(
                    source[0, chip, :, piece * part : (piece + 1) * part]
                )
        gd_ref[chip, 0] = wide(fd_ref[0, chip])

    @pl.when(pl.program_id(0) == 0)
    def _():
        places = [(0, n) for n in range(4)] + [(1, 0), (1, 0), (2, 0), (3, 0)]
        for target, (row, number) in zip(vector_refs, places):
            count = target.shape[0]
            target[...] = vsum_ref[row : row + 1, number * count : (number + 1) * count].reshape(count)


def rotary_parts(block_count):
    half_rot = ROT // 2
    lane = np.arange(128) % HD
    rate = np.where(lane < ROT, 10000.0 ** (-2.0 * (lane % half_rot) / ROT), 0.0)

    def table(places):
        angle = places[:, None].astype(np.float64) * rate[None, :]
        return np.concatenate([np.cos(angle), np.sin(angle)], axis=1).astype(np.float32)

    return table(np.arange(BLK)), table(np.arange(block_count) * BLK)


VMEM_SPEC = pl.BlockSpec(memory_space=pltpu.VMEM)
SPECS = {
    "order": pl.BlockSpec(memory_space=pltpu.SMEM),
    "wdown": pl.BlockSpec(memory_space=pl.ANY),
}
VMEM_LIMIT = 63 * 1024 * 1024


def sliced_layer(
    nz,
    hidden_in,
    norm1_gain,
    attention_norm_bias,
    qkv_weight,
    qkv_bias,
    out_weight,
    out_bias,
    norm2_gain,
    feedforward_norm_bias,
    up_weight,
    up_bias,
    down_weight,
    down_bias,
    cotangent,
    block_order,
):
    f32, b16 = jnp.float32, jnp.bfloat16
    h, g = hidden_in[0], cotangent[0]
    local_rows, width = h.shape
    chips = lax.axis_size("ctx") // 2
    shard = qkv_weight.shape[0]
    half = shard // 2
    part = width // chips
    hidden = up_weight.shape[1] // chips
    rows = chips * local_rows
    everyone = 2 * rows
    sides = local_rows // BLK

    small = 6 * shard + qkv_bias.shape[0] + up_bias.shape[0]
    rope_r, rope_b = rotary_parts(everyone // BLK)

    inputs = {
        "order": block_order,
        "h": h.reshape(sides, BLK, width),
        "g": g.reshape(sides, BLK, width),
        "wqkv": qkv_weight,
        "wup": up_weight,
        "wdown": down_weight,
        "wout": out_weight,
        **dict(
            zip(
                VECTORS,
                (norm1_gain, attention_norm_bias, norm2_gain, feedforward_norm_bias)
                + (out_bias, down_bias, qkv_bias, up_bias),
            )
        ),
        "rope_r": jnp.asarray(rope_r),
        "rope_b": jnp.asarray(rope_b),
    }
    outputs = {
        "hidden_out": ((local_rows, width), b16),
        "hidden_grad": ((local_rows, width), f32),
        "fq": ((2, chips, half, 3 * part), b16),
        "fu": ((2, chips, half, hidden), b16),
        "fd": ((2, chips, half, width), b16),
        "fo": ((2, half, width), b16),
        "vsum": ((8, width), f32),
    }
    scratch = {
        "hall": ((everyone // BLK, BLK, width), b16),
        "gall": ((everyone // BLK, BLK, width), b16),
        "wqs": ((shard, 3 * part), b16),
        "wus": ((shard, hidden), b16),
        "wq4": ((nz, shard, 3 * part), b16),
        "wu4": ((nz, shard, hidden), b16),
        "wd4": ((nz, shard, width), b16),
        "wo1": ((part, width), b16),
        "sm": ((1, small), f32),
        "sm4": ((nz, 1, small), f32),
        "vec": ((8, width), f32),
        "sums": ((8, width), f32),
        "q": ((everyone, part), b16),
        "k": ((everyone, part), b16),
        "v": ((everyone, part), b16),
        "kt": ((part, everyone), b16),
        "vt": ((part, everyone), b16),
        "att": ((rows, part), b16),
        "attt": ((part, rows), b16),
        "lse": ((8, rows), f32),
        "delta": ((8, rows), f32),
        "datt": ((rows, part), b16),
        "act": ((rows, hidden), b16),
        "du": ((rows, hidden), b16),
        "n": ((rows, width), b16),
        "gl": ((rows, width), b16),
        "outb": ((rows // BLK, BLK, width), b16),
        "e2": ((rows, width), f32),
        "dk": ((everyone, part), f32),
        "dv": ((everyone, part), f32),
        "dqt": ((part, rows), f32),
        "kvin": ((rows, 2 * part), b16),
        "osent": ((rows // BLK, BLK, width), b16),
        "ogot": ((rows // BLK, BLK, width), b16),
        "oland": ((6, BLK, width), b16),
        "eland": ((6, BLK, width), b16),
        "gq": ((nz, shard, 3 * part), b16),
        "gu": ((nz, shard, hidden), b16),
        "gd": ((nz, shard, width), b16),
        "go": ((part, width), b16),
        "tq": ((nz, half, 3 * part), b16),
        "uq": ((nz, half, 3 * part), b16),
        "tu": ((nz, half, hidden), b16),
        "uu": ((nz, half, hidden), b16),
        "td": ((nz, half, width), b16),
        "ud": ((nz, half, width), b16),
        "to": ((half, width), b16),
        "uo": ((nz, half, width), b16),
        "vout": ((nz, 8, width), f32),
        "vline": ((nz, 8, width), f32),
        "vsend": ((8, width), f32),
        "vplane": ((2 * chips, 8, width), f32),
    }
    names = [*inputs, *outputs, *scratch, "idx", "send_sems", "recv_sems", "local_sem"]
    results = pl.pallas_call(
        functools.partial(layer_kernel, nz, names),
        out_shape=tuple(jax.ShapeDtypeStruct(*leaf) for leaf in outputs.values()),
        in_specs=[SPECS.get(name, VMEM_SPEC) for name in inputs],
        out_specs=(VMEM_SPEC,) * len(outputs),
        scratch_shapes=[pltpu.VMEM(*leaf) for leaf in scratch.values()]
        + [pltpu.SMEM((64,), jnp.int32)]
        + [pltpu.SemaphoreType.DMA((SEMAPHORES,))] * 2
        + [pltpu.SemaphoreType.DMA],
        compiler_params=pltpu.CompilerParams(
            collective_id=0, has_side_effects=True, vmem_limit_bytes=VMEM_LIMIT
        ),
        name="layer",
    )(*inputs.values())
    hidden_out, hidden_grad, fq, fu, fd, fo, vsum = results

    steps = 4
    some, few = shard // steps, local_rows // steps
    inner = half // some

    def pieces(cols):
        return pl.BlockSpec((1, chips, some, cols), lambda i: (i // inner, 0, i % inner, 0))

    def lines(count, cols):
        return pl.BlockSpec((count, cols), lambda i: (i, 0))

    def vector(count):
        return pl.BlockSpec((count,), lambda i: (0,))

    sizes = [shard] * 6 + [qkv_bias.shape[0], up_bias.shape[0]]
    grad_qkv, grad_up, grad_down, grad_out, hidden_out, hidden_grad, *vectors = pl.pallas_call(
        assemble_kernel,
        grid=(steps,),
        out_shape=(
            jax.ShapeDtypeStruct(qkv_weight.shape, f32),
            jax.ShapeDtypeStruct(up_weight.shape, f32),
            jax.ShapeDtypeStruct((chips, steps, some, width), f32),
            jax.ShapeDtypeStruct(out_weight.shape, f32),
            jax.ShapeDtypeStruct(h.shape, b16),
            jax.ShapeDtypeStruct(h.shape, f32),
        )
        + tuple(jax.ShapeDtypeStruct((size,), f32) for size in sizes),
        in_specs=[
            pieces(3 * part),
            pieces(hidden),
            pieces(width),
            pl.BlockSpec((1, some, width), lambda i: (i // inner, i % inner, 0)),
            lines(few, width),
            lines(few, width),
            pl.BlockSpec((8, width), lambda i: (0, 0)),
        ],
        out_specs=(
            lines(some, qkv_weight.shape[1]),
            lines(some, up_weight.shape[1]),
            pl.BlockSpec((chips, 1, some, width), lambda i: (0, i, 0, 0)),
            lines(some, width),
            lines(few, width),
            lines(few, width),
        )
        + tuple(vector(size) for size in sizes),
        compiler_params=pltpu.CompilerParams(vmem_limit_bytes=56 * 1024 * 1024),
        name="assemble",
    )(fq, fu, fd, fo, hidden_out, hidden_grad, vsum)
    g_gain1, g_shift1, g_gain2, g_shift2, g_bout, g_bdown, g_bqkv, g_bup = vectors
    return (
        hidden_out[None],
        hidden_grad[None],
        g_gain1,
        g_shift1,
        grad_qkv,
        g_bqkv,
        grad_out,
        g_bout,
        g_gain2,
        g_shift2,
        grad_up,
        g_bup,
        grad_down.reshape(down_weight.shape),
        g_bdown,
    )


def sliced_fits(mesh):
    return mesh.shape["ctx"] == 8 and mesh.shape["fsdp"] == 4


def solution(mesh):
    in_specs = (
        P("fsdp", "ctx", None),
        P("fsdp"),
        P("fsdp"),
        P("fsdp", None),
        P("fsdp"),
        P("fsdp", None),
        P("fsdp"),
        P("fsdp"),
        P("fsdp"),
        P("fsdp", None),
        P("fsdp"),
        P("fsdp", None),
        P("fsdp"),
        P("fsdp", "ctx", None),
        P(),
    )
    out_specs = (
        P("fsdp", "ctx", None),
        P("fsdp", "ctx", None),
        P("fsdp"),
        P("fsdp"),
        P("fsdp", None),
        P("fsdp"),
        P("fsdp", None),
        P("fsdp"),
        P("fsdp"),
        P("fsdp"),
        P("fsdp", None),
        P("fsdp"),
        P("fsdp", None),
        P("fsdp"),
    )
    local = whole_parameter_layer
    if sliced_fits(mesh):
        local = functools.partial(sliced_layer, mesh.shape["fsdp"])
    return jax.shard_map(local, mesh=mesh, in_specs=in_specs, out_specs=out_specs, check_vma=False)
```

```python
import functools
import math
import types

import jax
import jax.numpy as jnp
import numpy as np
from jax import lax
from jax.experimental import pallas as pl
from jax.experimental.pallas import tpu as pltpu
from jax.sharding import PartitionSpec as P

H = 12
HD = 64
ROT = 16
BLK = 128


EPS = 1e-05
NEG = -1e30
SQRT_HALF = 0.7071067811865476
INV_ROOT_TWO_PI = 0.3989422804014327


def apply_layer_norm(values_in, norm_gain, norm_bias):
    centre = jnp.mean(values_in, axis=-1, keepdims=True)
    mean_removed = values_in - centre
    inverse_deviation = lax.rsqrt(
        jnp.mean(mean_removed * mean_removed, axis=-1, keepdims=True) + EPS
    )
    standardized = mean_removed * inverse_deviation
    return (standardized * norm_gain + norm_bias, standardized, inverse_deviation)


def layer_norm_backward(output_gradient, standardized, inverse_deviation, norm_gain):
    gain_scaled = output_gradient * norm_gain
    return inverse_deviation * (
        gain_scaled
        - jnp.mean(gain_scaled, axis=-1, keepdims=True)
        - standardized * jnp.mean(gain_scaled * standardized, axis=-1, keepdims=True)
    )


def gelu_exact(values_in):
    return 0.5 * values_in * (1.0 + lax.erf(values_in * SQRT_HALF))


def gelu_slope(values_in):
    return (
        0.5 * (1.0 + lax.erf(values_in * SQRT_HALF))
        + values_in * jnp.exp(-0.5 * values_in * values_in) * INV_ROOT_TWO_PI
    )


def rotary_tables(position_list):
    half_rot = ROT // 2
    inverse = jnp.power(jnp.float32(10000.0), -2.0 * jnp.arange(half_rot, dtype=jnp.float32) / ROT)
    angle = position_list.astype(jnp.float32)[:, None] * inverse[None, :]
    return (jnp.cos(angle)[:, None, :], jnp.sin(angle)[:, None, :])


def rotate(tensor, cosine, sine):
    half_rot = ROT // 2
    first_half = tensor[..., :half_rot]
    second_half = tensor[..., half_rot:ROT]
    return jnp.concatenate(
        [
            first_half * cosine - second_half * sine,
            second_half * cosine + first_half * sine,
            tensor[..., ROT:],
        ],
        axis=-1,
    )


def rotate_back(tensor, cosine, sine):
    half_rot = ROT // 2
    first_half = tensor[..., :half_rot]
    second_half = tensor[..., half_rot:ROT]
    return jnp.concatenate(
        [
            first_half * cosine + second_half * sine,
            second_half * cosine - first_half * sine,
            tensor[..., ROT:],
        ],
        axis=-1,
    )


def masked_logits(query_block, key_block, query_pos, key_pos):
    logits = jnp.einsum(
        "qhd,khd->hqk", query_block, key_block, preferred_element_type=jnp.float32
    ) * (1.0 / math.sqrt(HD))
    return jnp.where(key_pos[None, None, :] <= query_pos[None, :, None], logits, NEG)


def block_terms(
    query_block, dout_block, total_t, delta_t, query_pos, key_block, value_block, key_pos
):
    logits = masked_logits(query_block, key_block, query_pos, key_pos)
    probs_wide = jnp.exp(logits - total_t[:, :, None])
    dprobs = jnp.einsum("qhd,khd->hqk", dout_block, value_block, preferred_element_type=jnp.float32)
    d_logits = (probs_wide * (dprobs - delta_t[:, :, None]) * (1.0 / math.sqrt(HD))).astype(
        jnp.bfloat16
    )
    return (probs_wide.astype(jnp.bfloat16), d_logits)


def keep_state(state_in):
    return state_in


def forward_attention(query, keys_all, values_all, own_pos, all_pos):
    local_rows = query.shape[0]
    seq_rows = keys_all.shape[0]
    qstep = min(512, local_rows)
    kstep = min(512, seq_rows)
    latest = jnp.max(own_pos)

    def stats_step(number, state_in):
        key_block = lax.dynamic_slice_in_dim(keys_all, number * kstep, kstep, 0)
        key_pos = lax.dynamic_slice_in_dim(all_pos, number * kstep, kstep, 0)

        def stats_live(state_now):
            running_max, running_sum = state_now
            logits = masked_logits(query, key_block, own_pos, key_pos)
            new_max = jnp.maximum(running_max, jnp.max(logits, axis=-1))
            running_sum = running_sum * jnp.exp(running_max - new_max) + jnp.sum(
                jnp.exp(logits - new_max[:, :, None]), axis=-1
            )
            return (new_max, running_sum)

        return lax.cond(jnp.min(key_pos) <= latest, stats_live, keep_state, state_in)

    start_state = (jnp.full((H, qstep), NEG, jnp.float32), jnp.zeros((H, qstep), jnp.float32))
    running_max, running_sum = lax.fori_loop(0, seq_rows // kstep, stats_step, start_state)
    total_t = running_max + jnp.log(running_sum)

    def value_step(number, state_in):
        key_block = lax.dynamic_slice_in_dim(keys_all, number * kstep, kstep, 0)
        value_block = lax.dynamic_slice_in_dim(values_all, number * kstep, kstep, 0)
        key_pos = lax.dynamic_slice_in_dim(all_pos, number * kstep, kstep, 0)

        def value_live(state_now):
            logits = masked_logits(query, key_block, own_pos, key_pos)
            attn_probs = jnp.exp(logits - total_t[:, :, None]).astype(jnp.bfloat16)
            return state_now + jnp.einsum(
                "hqk,khd->qhd", attn_probs, value_block, preferred_element_type=jnp.float32
            )

        return lax.cond(jnp.min(key_pos) <= latest, value_live, keep_state, state_in)

    weighted = lax.fori_loop(
        0, seq_rows // kstep, value_step, jnp.zeros((qstep, H, HD), jnp.float32)
    )
    totals = total_t.T
    return (weighted, totals)


def query_grads(query, d_att, log_total, delta, own_pos, keys_all, values_all, all_pos):
    local_rows = query.shape[0]
    seq_rows = keys_all.shape[0]
    qstep = min(512, local_rows)
    kstep = min(512, seq_rows)
    key_grads = jnp.zeros((seq_rows, H, HD), jnp.float32)
    value_grads = jnp.zeros((seq_rows, H, HD), jnp.float32)
    total_t = log_total.T
    delta_t = delta.T
    latest = jnp.max(own_pos)

    def key_step(number, state_in):
        offset = number * kstep
        key_block = lax.dynamic_slice_in_dim(keys_all, offset, kstep, 0)
        value_block = lax.dynamic_slice_in_dim(values_all, offset, kstep, 0)
        key_pos = lax.dynamic_slice_in_dim(all_pos, offset, kstep, 0)

        def key_live(state_now):
            attn_probs, d_logits = block_terms(
                query, d_att, total_t, delta_t, own_pos, key_block, value_block, key_pos
            )
            d_query = state_now[0] + jnp.einsum(
                "hqk,khd->qhd", d_logits, key_block, preferred_element_type=jnp.float32
            )
            key_acc = state_now[1]
            value_acc = state_now[2]
            key_part = jnp.einsum(
                "hqk,qhd->khd", d_logits, query, preferred_element_type=jnp.float32
            )
            value_part = jnp.einsum(
                "hqk,qhd->khd", attn_probs, d_att, preferred_element_type=jnp.float32
            )
            key_acc = lax.dynamic_update_slice_in_dim(
                key_acc, lax.dynamic_slice_in_dim(key_acc, offset, kstep, 0) + key_part, offset, 0
            )
            value_acc = lax.dynamic_update_slice_in_dim(
                value_acc,
                lax.dynamic_slice_in_dim(value_acc, offset, kstep, 0) + value_part,
                offset,
                0,
            )
            return (d_query, key_acc, value_acc)

        return lax.cond(jnp.min(key_pos) <= latest, key_live, keep_state, state_in)

    start_state = (jnp.zeros((qstep, H, HD), jnp.float32),) + (key_grads, value_grads)
    result = lax.fori_loop(0, seq_rows // kstep, key_step, start_state)
    pieces = result[0]
    key_grads = result[1]
    value_grads = result[2]
    return (pieces, key_grads, value_grads)


def whole_parameter_layer(
    hidden_in,
    norm1_gain,
    attention_norm_bias,
    qkv_weight,
    qkv_bias,
    out_weight,
    out_bias,
    norm2_gain,
    feedforward_norm_bias,
    up_weight,
    up_bias,
    down_weight,
    down_bias,
    cotangent,
    block_order,
):
    (
        attention_norm_gain,
        attention_bias_term,
        wqkv,
        bqkv,
        wout,
        bout,
        feedforward_norm_gain,
        feedforward_bias_term,
        wup,
        bup,
        wdown,
        bdown,
    ) = (
        lax.all_gather(norm1_gain, "fsdp", axis=0, tiled=True),
        lax.all_gather(attention_norm_bias, "fsdp", axis=0, tiled=True),
        lax.all_gather(qkv_weight, "fsdp", axis=0, tiled=True),
        lax.all_gather(qkv_bias, "fsdp", axis=0, tiled=True),
        lax.all_gather(out_weight, "fsdp", axis=0, tiled=True),
        lax.all_gather(out_bias, "fsdp", axis=0, tiled=True),
        lax.all_gather(norm2_gain, "fsdp", axis=0, tiled=True),
        lax.all_gather(feedforward_norm_bias, "fsdp", axis=0, tiled=True),
        lax.all_gather(up_weight, "fsdp", axis=0, tiled=True),
        lax.all_gather(up_bias, "fsdp", axis=0, tiled=True),
        lax.all_gather(down_weight, "fsdp", axis=0, tiled=True),
        lax.all_gather(down_bias, "fsdp", axis=0, tiled=True),
    )
    width = H * HD
    hidden_rows = hidden_in[0]
    cotan_rows = cotangent[0]
    local_rows = hidden_rows.shape[0]
    ctx_count = lax.axis_size("ctx")
    ctx_rank = lax.axis_index("ctx")
    seq_rows = local_rows * ctx_count
    all_pos = (block_order[:, None] * BLK + jnp.arange(BLK, dtype=jnp.int32)[None, :]).reshape(
        seq_rows
    )
    own_pos = lax.dynamic_slice_in_dim(all_pos, ctx_rank * local_rows, local_rows, 0)
    cosine, sine = rotary_tables(own_pos)
    attention_norm_gain = attention_norm_gain.astype(jnp.float32)
    feedforward_norm_gain = feedforward_norm_gain.astype(jnp.float32)
    residual_stream = hidden_rows.astype(jnp.float32)
    attention_normed, attention_standardized, attention_inverse_deviation = apply_layer_norm(
        residual_stream, attention_norm_gain, attention_bias_term.astype(jnp.float32)
    )
    normed1_b = attention_normed.astype(jnp.bfloat16)
    projected = jnp.dot(normed1_b, wqkv, preferred_element_type=jnp.float32) + bqkv.astype(
        jnp.float32
    )
    query = rotate(projected[:, :width].reshape(local_rows, H, HD), cosine, sine).astype(
        jnp.bfloat16
    )
    key_rows = rotate(
        projected[:, width : 2 * width].reshape(local_rows, H, HD), cosine, sine
    ).astype(jnp.bfloat16)
    value_rows = projected[:, 2 * width :].astype(jnp.bfloat16)
    keys_all, values_all = (
        lax.all_gather(key_rows.reshape(local_rows, width), "ctx", axis=0, tiled=True),
        lax.all_gather(value_rows, "ctx", axis=0, tiled=True),
    )
    keys_all = keys_all.reshape(seq_rows, H, HD)
    values_all = values_all.reshape(seq_rows, H, HD)
    attended, log_total = forward_attention(query, keys_all, values_all, own_pos, all_pos)
    attended_b = attended.reshape(local_rows, width).astype(jnp.bfloat16)
    attn_out = jnp.dot(attended_b, wout, preferred_element_type=jnp.float32) + bout.astype(
        jnp.float32
    )
    feedforward_normed, feedforward_standardized, feedforward_inverse_deviation = apply_layer_norm(
        residual_stream, feedforward_norm_gain, feedforward_bias_term.astype(jnp.float32)
    )
    normed2_b = feedforward_normed.astype(jnp.bfloat16)
    up_rows = jnp.dot(normed2_b, wup, preferred_element_type=jnp.float32) + bup.astype(jnp.float32)
    act_b = gelu_exact(up_rows).astype(jnp.bfloat16)
    mlp_out = jnp.dot(act_b, wdown, preferred_element_type=jnp.float32) + bdown.astype(jnp.float32)
    hidden_out = (residual_stream + attn_out + mlp_out).astype(jnp.bfloat16)
    cotan_wide = cotan_rows.astype(jnp.float32)
    grad_wdown = jnp.einsum("tk,tn->kn", act_b, cotan_rows, preferred_element_type=jnp.float32)
    grad_bdown = jnp.sum(cotan_wide, axis=0)
    d_up = jnp.einsum(
        "tn,kn->tk", cotan_rows, wdown, preferred_element_type=jnp.float32
    ) * gelu_slope(up_rows)
    d_up16 = d_up.astype(jnp.bfloat16)
    grad_wup = jnp.einsum("tk,tn->kn", normed2_b, d_up16, preferred_element_type=jnp.float32)
    grad_bup = jnp.sum(d_up, axis=0)
    grad_feedforward_normed = jnp.einsum(
        "tn,kn->tk", d_up16, wup, preferred_element_type=jnp.float32
    )
    grad_feedforward_gain = jnp.sum(grad_feedforward_normed * feedforward_standardized, axis=0)
    grad_shift2 = jnp.sum(grad_feedforward_normed, axis=0)
    feedforward_branch_grad = layer_norm_backward(
        grad_feedforward_normed,
        feedforward_standardized,
        feedforward_inverse_deviation,
        feedforward_norm_gain,
    )
    grad_wout = jnp.einsum("tk,tn->kn", attended_b, cotan_rows, preferred_element_type=jnp.float32)
    d_att = jnp.einsum("tn,kn->tk", cotan_rows, wout, preferred_element_type=jnp.float32).astype(
        jnp.bfloat16
    )
    delta = jnp.sum(
        d_att.reshape(local_rows, H, HD).astype(jnp.float32)
        * attended_b.reshape(local_rows, H, HD).astype(jnp.float32),
        axis=-1,
    )
    d_att3 = d_att.reshape(local_rows, H, HD)
    d_query, key_grads, value_grads = query_grads(
        query, d_att3, log_total, delta, own_pos, keys_all, values_all, all_pos
    )
    d_key, d_value = (
        lax.psum_scatter(
            key_grads.reshape(seq_rows, width), "ctx", scatter_dimension=0, tiled=True
        ),
        lax.psum_scatter(
            value_grads.reshape(seq_rows, width), "ctx", scatter_dimension=0, tiled=True
        ),
    )
    d_query = rotate_back(d_query, cosine, sine)
    d_key = rotate_back(d_key.reshape(local_rows, H, HD), cosine, sine)
    d_qkv = jnp.concatenate(
        [d_query.reshape(local_rows, width), d_key.reshape(local_rows, width), d_value], axis=1
    )
    d_qkv16 = d_qkv.astype(jnp.bfloat16)
    grad_wqkv = jnp.einsum("tk,tn->kn", normed1_b, d_qkv16, preferred_element_type=jnp.float32)
    grad_bqkv = jnp.sum(d_qkv, axis=0)
    grad_attention_normed = jnp.einsum(
        "tn,kn->tk", d_qkv16, wqkv, preferred_element_type=jnp.float32
    )
    grad_attention_gain = jnp.sum(grad_attention_normed * attention_standardized, axis=0)
    grad_shift1 = jnp.sum(grad_attention_normed, axis=0)
    attention_branch_grad = layer_norm_backward(
        grad_attention_normed,
        attention_standardized,
        attention_inverse_deviation,
        attention_norm_gain,
    )
    hidden_grad = cotan_wide + attention_branch_grad + feedforward_branch_grad
    terms = (
        grad_attention_gain,
        grad_shift1,
        grad_wqkv,
        grad_bqkv,
        grad_wout,
        grad_bdown,
        grad_feedforward_gain,
        grad_shift2,
        grad_wup,
        grad_bup,
        grad_wdown,
        grad_bdown,
    )
    shares = (
        lax.psum_scatter(terms[0], "fsdp", scatter_dimension=0, tiled=True),
        lax.psum_scatter(terms[1], "fsdp", scatter_dimension=0, tiled=True),
        lax.psum_scatter(terms[2], "fsdp", scatter_dimension=0, tiled=True),
        lax.psum_scatter(terms[3], "fsdp", scatter_dimension=0, tiled=True),
        lax.psum_scatter(terms[4], "fsdp", scatter_dimension=0, tiled=True),
        lax.psum_scatter(terms[5], "fsdp", scatter_dimension=0, tiled=True),
        lax.psum_scatter(terms[6], "fsdp", scatter_dimension=0, tiled=True),
        lax.psum_scatter(terms[7], "fsdp", scatter_dimension=0, tiled=True),
        lax.psum_scatter(terms[8], "fsdp", scatter_dimension=0, tiled=True),
        lax.psum_scatter(terms[9], "fsdp", scatter_dimension=0, tiled=True),
        lax.psum_scatter(terms[10], "fsdp", scatter_dimension=0, tiled=True),
        lax.psum_scatter(terms[11], "fsdp", scatter_dimension=0, tiled=True),
    )
    shares = lax.psum(
        (
            shares[0],
            shares[1],
            shares[2],
            shares[3],
            shares[4],
            shares[5],
            shares[6],
            shares[7],
            shares[8],
            shares[9],
            shares[10],
            shares[11],
        ),
        "ctx",
    )
    return (
        hidden_out[None],
        hidden_grad[None],
        shares[0],
        shares[1],
        shares[2],
        shares[3],
        shares[4],
        shares[5],
        shares[6],
        shares[7],
        shares[8],
        shares[9],
        shares[10],
        shares[11],
    )


MESH_IDS = pl.DeviceIdType.MESH
NN = (((1,), (0,)), ((), ()))
NT = (((1,), (1,)), ((), ()))
TN = (((0,), (0,)), ((), ()))
QTILE = 256
SEMAPHORES = 160


def mm(left, right, dims=NN):
    return lax.dot_general(left, right, dims, preferred_element_type=jnp.float32)


def flip(index, bit):
    return index + bit - 2 * bit * ((index // bit) % 2)


def run_when(condition, action):
    if condition is None:
        action()
    else:
        pl.when(condition)(action)


def narrow(values):
    return values.astype(jnp.bfloat16)


def wide(values):
    return values.astype(jnp.float32)


class Copies:
    def __init__(self, send_sems, recv_sems):
        self.send_sems, self.recv_sems = send_sems, recv_sems
        self.count, self.started, self.numbers = 0, [], {}

    def make(self, source, target, device, when=None, like=None):
        if like is None:
            number = self.count
            self.count += 1
        else:
            number = self.numbers[id(like)]
        copy = pltpu.make_async_remote_copy(
            src_ref=source,
            dst_ref=target,
            send_sem=self.send_sems.at[number],
            recv_sem=self.recv_sems.at[number],
            device_id=device,
            device_id_type=MESH_IDS,
        )
        self.started.append((copy, when))
        self.numbers[id(copy)] = number
        return copy

    def settle(self, chosen):
        numbers = {id(copy) for copy in chosen}
        for copy, when in self.started:
            if id(copy) in numbers:
                run_when(when, copy.wait_send)
        self.started = [entry for entry in self.started if id(entry[0]) not in numbers]

    def finish(self):
        for copy, when in self.started:
            run_when(when, copy.wait_send)


class Place:
    def __init__(self, nz):
        self.nz = nz
        self.c, self.z = lax.axis_index("ctx"), lax.axis_index("fsdp")
        self.k, self.t = self.c % 2, self.c // 2
        self.xn, self.yn, self.pn = flip(self.c, 2), flip(self.c, 4), flip(self.c, 1)
        self.dn = flip(self.xn, 4)
        self.tx, self.ty = flip(self.t, 1), flip(self.t, 2)
        self.td = flip(self.tx, 2)
        self.others = [(self.z + d) % nz for d in range(1, nz)]
        self.plane = [self.xn, self.yn, self.dn, self.pn] + [
            flip(peer, 1) for peer in (self.xn, self.yn, self.dn)
        ]
        self.above, self.below = jnp.minimum(self.z + 1, nz - 1), jnp.maximum(self.z - 1, 0)

    def on_plane(self, c):
        return (c, self.z)

    def on_line(self, z):
        return (self.c, z)

    def greet(self):
        barrier = pltpu.get_barrier_semaphore()
        peers = [self.on_plane(peer) for peer in self.plane] + [self.on_line(z) for z in self.others]
        for peer in peers:
            pl.semaphore_signal(barrier, inc=1, device_id=peer, device_id_type=MESH_IDS)
        pl.semaphore_wait(barrier, len(peers))


class PlaneShare:
    def __init__(self, copies, me, source, slot, rows):
        self.copies, self.me, self.slot = copies, me, slot
        top, bottom = pl.ds(0, rows // 2), pl.ds(rows // 2, rows // 2)
        own = slot(me.k, me.t)
        to_x, to_y = me.on_plane(me.xn), me.on_plane(me.yn)
        self.x_first = copies.make(source.at[top], own.at[top], to_x)
        self.y_first = copies.make(source.at[bottom], own.at[bottom], to_y)
        self.x_second = copies.make(source.at[bottom], own.at[bottom], to_x)
        self.y_second = copies.make(source.at[top], own.at[top], to_y)
        self.to_p = copies.make(source, own, me.on_plane(me.pn))
        through_x, through_y = slot(me.k, me.tx).at[top], slot(me.k, me.ty).at[bottom]
        self.hop_y = copies.make(through_x, through_x, to_y)
        self.hop_x = copies.make(through_y, through_y, to_x)
        self.swaps = []
        for chip in (me.tx, me.ty, me.td):
            place = slot(me.k, chip)
            self.swaps.append(copies.make(place, place, me.on_plane(me.pn)))

    def start(self):
        for copy in (self.x_first, self.y_first, self.x_second, self.y_second, self.to_p):
            copy.start()

    def relay(self):
        self.x_first.wait_recv()
        self.hop_y.start()
        self.y_first.wait_recv()
        self.hop_x.start()

    def swap(self):
        self.x_second.wait_recv()
        self.swaps[0].start()
        self.y_second.wait_recv()
        self.swaps[1].start()

    def on_diagonal(self):
        self.hop_y.wait_recv()
        self.hop_x.wait_recv()
        self.swaps[2].start()

    def finish(self):
        for copy in (self.to_p, *self.swaps):
            copy.wait_recv()


class LineGather:
    def __init__(self, copies, me, source, gathered):
        self.copies, self.me, self.gathered = copies, me, gathered
        rows = gathered.shape[1] // 2
        self.mine = pl.ds(me.k * rows, rows)
        self.moves, self.swaps = {}, []
        for step in range(me.nz - 1):
            for sign in (1, -1):
                shard, target = me.z - sign * step, me.z + sign
                ok = (shard >= 0) & (shard < me.nz) & (target >= 0) & (target < me.nz)
                place = self.slot(shard)
                copy = copies.make(
                    source.at[self.mine] if step == 0 else place,
                    place,
                    me.on_line(jnp.clip(target, 0, me.nz - 1)),
                    when=ok,
                )
                self.moves[step, sign] = (copy, ok)

    def slot(self, shard):
        return self.gathered.at[jnp.clip(shard, 0, self.me.nz - 1), self.mine]

    def start(self):
        for sign in (1, -1):
            copy, ok = self.moves[0, sign]
            run_when(ok, copy.start)

    def advance(self, step):
        me = self.me
        for sign in (1, -1):
            arrived = me.z - sign * (step + 1)
            ok = (arrived >= 0) & (arrived < me.nz)
            run_when(ok, self.moves[step, sign][0].wait_recv)
            if step + 1 < me.nz - 1:
                copy, following = self.moves[step + 1, sign]
                run_when(following, copy.start)
            place = self.slot(arrived)
            swap = self.copies.make(place, place, me.on_plane(me.pn), when=ok)
            run_when(ok, swap.start)
            self.swaps.append((swap, ok))

    def finish(self):
        for swap, ok in self.swaps:
            run_when(ok, swap.wait_recv)


class LineSend:
    def __init__(self, copies, me, source, gathered):
        self.me = me
        rows = gathered.shape[1] // 2
        mine = pl.ds(me.k * rows, rows)
        self.sends, self.swaps = [], []
        for distance, other in enumerate(me.others, 1):
            self.sends.append(
                copies.make(source.at[mine], gathered.at[me.z, mine], me.on_line(other))
            )
            place = gathered.at[(me.z - distance) % me.nz, mine]
            self.swaps.append(copies.make(place, place, me.on_plane(me.pn)))

    def start(self):
        for send in self.sends:
            send.start()

    def advance(self):
        for send, swap in zip(self.sends, self.swaps):
            send.wait_recv()
            swap.start()

    def finish(self):
        for swap in self.swaps:
            swap.wait_recv()


class LineSpread:
    def __init__(self, copies, me, source, target):
        self.me, self.source, self.target = me, source, target
        rows = target.shape[0] // 2
        mine = pl.ds(me.k * rows, rows)
        self.here, self.away = me.z == me.t, me.z != me.t
        place = target.at[mine]
        self.sends, self.arrivals = [], []
        for distance in range(1, me.nz):
            target_z = (me.t + distance) % me.nz
            copy = copies.make(source.at[mine], place, me.on_line(target_z), when=self.here)
            self.sends.append(copy)
            self.arrivals.append(me.z == target_z)
        self.swap = copies.make(place, place, me.on_plane(me.pn), when=self.away)

    def start(self):
        @pl.when(self.here)
        def _():
            for copy in self.sends:
                copy.start()
            self.target[...] = self.source[...]

    def advance(self):
        for copy, arrives in zip(self.sends, self.arrivals):
            pl.when(arrives)(copy.wait_recv)
        pl.when(self.away)(self.swap.start)

    def finish(self):
        pl.when(self.away)(self.swap.wait_recv)


class LineReduce:
    def __init__(self, copies, me, source, total, landed):
        self.me, self.source, self.total, self.landed = me, source, total, landed
        half = total.shape[1]
        self.mine, theirs = pl.ds(me.k * half, half), pl.ds((1 - me.k) * half, half)
        self.exchange = copies.make(source.at[:, theirs], total, me.on_plane(me.pn))
        self.sends = [
            copies.make(total.at[other], landed.at[me.z], me.on_line(other)) for other in me.others
        ]

    def start(self):
        self.exchange.start()

    def pair(self):
        self.exchange.wait_recv()
        for owner in range(self.me.nz):
            self.total[owner] = narrow(
                wide(self.total[owner]) + wide(self.source[owner, self.mine])
            )
        for send in self.sends:
            send.start()

    def collect(self):
        me = self.me
        result = wide(self.total[me.z])
        for send in self.sends:
            send.wait_recv()
        for other in me.others:
            result = result + wide(self.landed[other])
        self.total[me.z] = narrow(result)


class LineCollect:
    def __init__(self, copies, me, source, total, landed):
        self.me, self.source, self.total, self.landed = me, source, total, landed
        half = total.shape[0]
        self.mine, theirs = pl.ds(me.k * half, half), pl.ds((1 - me.k) * half, half)
        self.exchange = copies.make(source.at[theirs], total, me.on_plane(me.pn))
        self.sends = []
        for distance in range(1, me.nz):
            leaves = (me.z + distance) % me.nz == me.t
            copy = copies.make(total, landed.at[me.z], me.on_line(me.t), when=leaves)
            self.sends.append((copy, leaves))

    def start(self):
        self.exchange.start()

    def pair(self):
        self.exchange.wait_recv()
        self.total[...] = narrow(wide(self.total[...]) + wide(self.source[self.mine]))
        for copy, leaves in self.sends:
            pl.when(leaves)(copy.start)

    def collect(self):
        me = self.me

        @pl.when(me.z == me.t)
        def _():
            result = wide(self.total[...])
            for copy, _ in self.sends:
                copy.wait_recv()
            for other in me.others:
                result = result + wide(self.landed[other])
            self.total[...] = narrow(result)


class PlaneSpread:
    def __init__(self, copies, me, source, target, rows):
        self.me, self.source, self.target = me, source, target
        top, bottom = pl.ds(0, rows // 2), pl.ds(rows // 2, rows // 2)
        place = target.at[me.k]
        self.here, self.from_x, self.from_y = me.t == me.z, me.tx == me.z, me.ty == me.z
        self.from_d = me.td == me.z
        self.to_x = copies.make(source, place, me.on_plane(me.xn), when=self.here)
        self.to_y = copies.make(source, place, me.on_plane(me.yn), when=self.here)
        self.to_p = copies.make(source, place, me.on_plane(me.pn), when=self.here)
        self.hop_y = copies.make(place.at[top], place.at[top], me.on_plane(me.yn), when=self.from_x)
        self.hop_x = copies.make(
            place.at[bottom], place.at[bottom], me.on_plane(me.xn), when=self.from_y
        )
        away = self.from_x | self.from_y | self.from_d
        self.away = away
        self.swap = copies.make(place, place, me.on_plane(me.pn), when=away, like=self.to_p)

    def start(self):
        @pl.when(self.here)
        def _():
            self.to_x.start()
            self.to_y.start()
            self.to_p.start()
            self.target[self.me.k] = self.source[...]

    def advance(self):
        @pl.when(self.from_x)
        def _():
            self.to_x.wait_recv()
            self.hop_y.start()
            self.swap.start()

        @pl.when(self.from_y)
        def _():
            self.to_y.wait_recv()
            self.hop_x.start()
            self.swap.start()

    def on_diagonal(self):
        @pl.when(self.from_d)
        def _():
            self.hop_y.wait_recv()
            self.hop_x.wait_recv()
            self.swap.start()

    def finish(self):
        self.to_p.wait_recv()

def norm_rows(values_in):
    centre = jnp.mean(values_in, axis=-1, keepdims=True)
    mean_removed = values_in - centre
    inverse_deviation = lax.rsqrt(
        jnp.mean(mean_removed * mean_removed, axis=-1, keepdims=True) + EPS
    )
    return mean_removed * inverse_deviation, inverse_deviation


def head_rows(rows, head):
    lanes = lax.broadcasted_iota(jnp.int32, rows.shape, 1)
    inside = (lanes >= head * HD) & (lanes < (head + 1) * HD)
    return jnp.where(inside, rows, jnp.zeros_like(rows))


def rope_lanes(r, blocks, columns, back):
    half_rot = ROT // 2
    tables = [[], [], []]
    row_cos, row_sin = r.rope_r[:, :128], r.rope_r[:, 128:]
    lane = lax.broadcasted_iota(jnp.int32, row_cos.shape, 1) % HD
    for block in blocks:
        both = r.rope_b[block]
        block_cos, block_sin = both[:, :128], both[:, 128:]
        cosine = block_cos * row_cos - block_sin * row_sin
        sine = block_sin * row_cos + block_cos * row_sin
        if back:
            sine = -sine
        tables[0].append(cosine)
        tables[1].append(jnp.where(lane < half_rot, -sine, 0.0))
        tables[2].append(jnp.where(lane >= half_rot, sine, 0.0))
    stacked = [jnp.concatenate(table, axis=0) for table in tables]
    return [jnp.concatenate([table] * (columns // 128), axis=1) for table in stacked]


def turn(values, tables):
    columns, half_rot = values.shape[1], ROT // 2
    return (
        values * tables[0]
        + pltpu.roll(values, columns - half_rot, 1) * tables[1]
        + pltpu.roll(values, half_rot, 1) * tables[2]
    )


def slice_weights(r, me):
    part = r.wqs.shape[1] // 3
    chips = r.wqkv.shape[1] // r.wqs.shape[1]
    for chip in range(chips):

        @pl.when(me.t == chip)
        def _():
            for source, target in ((r.wqkv, r.wqs), (r.wup, r.wus)):
                for piece in range(target.shape[1] // part):
                    first = (piece * chips + chip) * part
                    target[:, piece * part : (piece + 1) * part] = source[:, first : first + part]


VECTORS = ("gain1", "shift1", "gain2", "shift2", "bout", "bdown", "bqkv", "bup")


def pack_vectors(r):
    first = 0
    for name in VECTORS:
        values = wide(getattr(r, name)[...])
        count = values.shape[0]
        r.sm[0:1, first : first + count] = values.reshape(1, count)
        first += count


def read_vectors(r, me):
    nz, part = me.nz, r.vec.shape[1] // me.nz

    def piece(z, number):
        return r.sm4[z, 0:1, number * part : (number + 1) * part]

    for z in range(nz):
        span = slice(z * part, (z + 1) * part)
        for row in range(4):
            r.vec[row : row + 1, span] = piece(z, row)
        r.vec[4:5, span] = piece(z, 4) + piece(z, 5)
    chips = nz
    for chip in range(chips):

        @pl.when(me.t == chip)
        def _():
            for number in range(3):
                held = number * chips + chip
                r.vec[5:6, number * part : (number + 1) * part] = piece(held // 3, 6 + held % 3)
            for z in range(nz):
                r.vec[6:7, z * part : (z + 1) * part] = piece(z, 9 + chip)


def block_table(r, me):
    count = r.order.shape[0]
    chips, quarter = me.nz, count // 4
    sides = count // (2 * chips)
    held = [r.order[number] for number in range(count)]
    for position in range(count):
        found = 0
        for number in range(1, count):
            found = jnp.where(held[number] == position, number, found)
        r.idx[position] = found
    for chip in range(chips):
        for owner, first in ((me.k, count), (1 - me.k, count + chips * sides)):
            for side in range(sides):
                position = r.order[(2 * chip + owner) * sides + side]
                low = (position >= quarter * me.k) & (position < quarter * (me.k + 1))
                high = position - 2 * quarter + quarter * me.k
                r.idx[first + chip * sides + side] = jnp.where(
                    low, position - quarter * me.k, jnp.clip(high, 0, 2 * quarter - 1)
                )
        position = r.order[(2 * chip + me.k) * sides]
        outer = jnp.where((position < quarter) | (position >= 3 * quarter), 0, 1)
        r.idx[count + 2 * chips * sides + chip] = jnp.where(outer == me.k, 1, 0)


def sorted_rows(r, source, block, blocks):
    pieces = []
    for number in range(blocks):
        pieces.append(source[r.idx[block + number]])
    return jnp.concatenate(pieces, axis=0)


def flat_rows(values):
    return values.reshape(-1, values.shape[-1])


def put_blocks(target, tile, values):
    blocks = values.shape[0] // BLK
    target[pl.ds(tile * blocks, blocks)] = values.reshape(blocks, BLK, values.shape[1])


def project(r, me, chip):
    part = r.wqs.shape[1] // 3
    sides = r.h.shape[0]

    @pl.loop(0, 2)
    def _(number):
        first = (2 * chip + (me.k + number) % 2) * sides
        rows = flat_rows(r.hall[pl.ds(first, sides)])
        standardized, _ = norm_rows(wide(rows))
        normed = narrow(standardized * r.vec[0:1, :] + r.vec[1:2, :])
        weight = r.wq4[...].reshape(-1, 3 * part)
        projected = mm(normed, weight) + r.vec[5:6, : 3 * part]
        positions = [r.order[first + side] for side in range(sides)]
        turned = turn(projected[:, : 2 * part], rope_lanes(r, positions, 2 * part, False))
        keys, values = turned[:, part:], projected[:, 2 * part :]
        query = narrow(wide(narrow(turned[:, :part])) * HD**-0.5)
        for side in range(sides):
            own = slice(side * BLK, (side + 1) * BLK)
            r.q[first + side] = query[own]
            r.k[first + side] = narrow(keys[own])
            r.v[first + side] = narrow(values[own])
            r.kt[first + side] = narrow(keys[own].T)
            r.vt[first + side] = narrow(values[own].T)


def sorted_columns(r, source, head, block, blocks):
    lanes = slice(head * HD, (head + 1) * HD)
    return jnp.concatenate(
        [source[r.idx[block + number], lanes, :] for number in range(blocks)], axis=1
    )


def tile_start(r, me, tile):
    quarter = r.k.shape[0] * BLK // 4
    low = tile < quarter // QTILE
    inside = tile * QTILE - jnp.where(low, 0, quarter)
    return jnp.where(low, quarter * me.k, 3 * quarter - quarter * me.k) + inside


def attend(r, me, tile):
    part = r.k.shape[2]
    blocks = QTILE // BLK
    heads = part // HD
    start = tile_start(r, me, tile)
    rows = slice(tile * QTILE, (tile + 1) * QTILE)
    query = sorted_rows(r, r.q, start // BLK, blocks)
    per_head = [head_rows(query, head) for head in range(heads)]

    def visit(number, state, masked):
        keys = sorted_rows(r, r.k, number * blocks, blocks)
        result = []
        for head in range(heads):
            top, total, acc = state[head]
            logits = mm(keys, per_head[head], NT)
            if masked:
                key_row = lax.broadcasted_iota(jnp.int32, logits.shape, 0)
                query_row = lax.broadcasted_iota(jnp.int32, logits.shape, 1)
                logits = jnp.where(key_row <= query_row, logits, NEG)
            new_top = jnp.maximum(top, jnp.max(logits, axis=0, keepdims=True))
            fade = jnp.exp(top - new_top)
            probs = jnp.exp(logits - new_top)
            total = total * fade + jnp.sum(probs, axis=0, keepdims=True)
            values = sorted_columns(r, r.vt, head, number * blocks, blocks)
            acc = acc * fade + mm(values, narrow(probs))
            result.append((new_top, total, acc))
        return tuple(result)

    state = tuple(
        (
            jnp.full((1, QTILE), NEG, jnp.float32),
            jnp.zeros((1, QTILE), jnp.float32),
            jnp.zeros((HD, QTILE), jnp.float32),
        )
        for _ in range(heads)
    )
    last = start // QTILE
    state = lax.fori_loop(0, last, lambda n, s: visit(n, s, False), state)
    state = visit(last, state, True)
    merged = jnp.concatenate([acc / total for _, total, acc in state], axis=0)
    r.att[rows, :] = narrow(merged.T)
    r.attt[:, rows] = narrow(merged)
    for head in range(heads):
        r.lse[head : head + 1, rows] = state[head][0] + jnp.log(state[head][1])


def feed_forward(r, me, tile):
    place = pl.ds(pl.multiple_of(tile * QTILE, QTILE), QTILE)
    blocks = QTILE // BLK
    block = tile_start(r, me, tile) // BLK
    width = r.hall.shape[2]
    standardized, _ = norm_rows(wide(sorted_rows(r, r.hall, block, blocks)))
    cotan = sorted_rows(r, r.gall, block, blocks)
    gain2 = r.vec[2:3, :]
    normed = narrow(standardized * gain2 + r.vec[3:4, :])
    up_weight = r.wu4[...].reshape(width, -1)
    down_weight = r.wd4[...].reshape(-1, width)
    up = mm(normed, up_weight) + r.vec[6:7, :]
    below = 0.5 * (1.0 + lax.erf(up * SQRT_HALF))
    act = narrow(up * below)
    slope = below + up * jnp.exp(-0.5 * up * up) * INV_ROOT_TWO_PI
    d_up = mm(cotan, down_weight, NT) * slope
    d_up16 = narrow(d_up)
    put_blocks(r.outb, tile, narrow(mm(act, down_weight)))
    d_normed = mm(d_up16, up_weight, NT)
    r.sums[2:3, :] += jnp.sum(d_normed * standardized, axis=0, keepdims=True)
    r.sums[3:4, :] += jnp.sum(d_normed, axis=0, keepdims=True)
    r.sums[6:7, :] += jnp.sum(d_up, axis=0, keepdims=True)
    r.e2[place, :] = d_normed * gain2
    r.n[place, :] = normed
    r.gl[place, :] = cotan
    r.act[place, :] = act
    r.du[place, :] = d_up16


def out_project(r, me, tile):
    place = pl.ds(pl.multiple_of(tile * QTILE, QTILE), QTILE)
    blocks = QTILE // BLK
    attended = r.att[place, :]
    mlp = flat_rows(r.outb[pl.ds(tile * blocks, blocks)])
    put_blocks(r.outb, tile, narrow(wide(mlp) + mm(attended, r.wo1[...])))
    cotan = r.gl[place, :]
    r.datt[place, :] = narrow(mm(cotan, r.wo1[...], NT))
    product = wide(narrow(mm(r.wo1[...], cotan, NT))) * wide(r.attt[:, place])
    for head in range(product.shape[0] // HD):
        r.delta[head : head + 1, place] = jnp.sum(
            product[head * HD : (head + 1) * HD], axis=0, keepdims=True
        )


def weight_grad(target, left, right):
    rows, columns = left.shape[1], right.shape[1]
    shard = target.shape[1]
    values = right[...]
    for first in range(0, rows, QTILE):
        result = narrow(mm(left[:, first : first + QTILE], values, TN))
        at = first
        while at < first + QTILE:
            owner, inside = at // shard, at % shard
            until = min((owner + 1) * shard, first + QTILE)
            target[owner, inside : inside + until - at, :] = result[at - first : until - first, :]
            at = until


def attend_grad(r, me, tile):
    part = r.k.shape[2]
    heads = part // HD
    kstep = 2 * QTILE
    start = tile_start(r, me, tile)
    rows = slice(tile * QTILE, (tile + 1) * QTILE)
    blocks = kstep // BLK
    query = sorted_rows(r, r.q, start // BLK, QTILE // BLK)
    d_out = r.datt[rows, :]
    queries = jnp.concatenate([head_rows(query, head) for head in range(heads)], axis=0)
    d_outs = jnp.concatenate([head_rows(d_out, head) for head in range(heads)], axis=0)

    def visit(number, state, masked):
        place = pl.ds(pl.multiple_of(number * kstep, kstep), kstep)
        keys = sorted_rows(r, r.k, number * blocks, blocks)
        values = sorted_rows(r, r.v, number * blocks, blocks)
        probs_all, d_logits_all, result = [], [], []
        for head in range(heads):
            own = slice(head * QTILE, (head + 1) * QTILE)
            logits = mm(keys, queries[own], NT)
            probs = jnp.exp(logits - r.lse[head : head + 1, rows])
            if masked:
                key_row = number * kstep + lax.broadcasted_iota(jnp.int32, logits.shape, 0)
                query_row = start + lax.broadcasted_iota(jnp.int32, logits.shape, 1)
                probs = jnp.where(key_row <= query_row, probs, 0.0)
            d_probs = mm(values, d_outs[own], NT)
            d_logits = narrow(probs * (d_probs - r.delta[head : head + 1, rows]))
            probs_all.append(narrow(probs))
            d_logits_all.append(d_logits)
            columns = sorted_columns(r, r.kt, head, number * blocks, blocks)
            result.append(state[head] + mm(columns, d_logits))
        r.dv[place, :] += mm(jnp.concatenate(probs_all, axis=1), d_outs)
        r.dk[place, :] += mm(jnp.concatenate(d_logits_all, axis=1), queries)
        return tuple(result)

    state = tuple(jnp.zeros((HD, QTILE), jnp.float32) for _ in range(heads))
    last = start // kstep
    state = lax.fori_loop(0, last, lambda n, s: visit(n, s, False), state)
    state = visit(last, state, True)
    r.dqt[:, rows] = jnp.concatenate(state, axis=0)


def qkv_grad(r, me, tile):
    place = pl.ds(pl.multiple_of(tile * QTILE, QTILE), QTILE)
    part = r.k.shape[2]
    blocks = QTILE // BLK
    start = tile_start(r, me, tile)
    block = start // BLK
    held = pl.ds(pl.multiple_of(start, QTILE), QTILE)
    standardized, _ = norm_rows(wide(sorted_rows(r, r.hall, block, blocks)))
    gain1 = r.vec[0:1, :]
    r.n[place, :] = narrow(standardized * gain1 + r.vec[1:2, :])
    d_query = r.dqt[:, place].T * HD**-0.5
    d_key = r.dk[held, :] + wide(r.kvin[place, :part])
    d_value = r.dv[held, :] + wide(r.kvin[place, part:])
    turned = turn(
        jnp.concatenate([d_query, d_key], axis=1),
        rope_lanes(r, [block + n for n in range(blocks)], 2 * part, True),
    )
    d_qkv = jnp.concatenate([turned, d_value], axis=1)
    d_qkv16 = narrow(d_qkv)
    r.du[place, : 3 * part] = d_qkv16
    r.sums[5:6, : 3 * part] += jnp.sum(d_qkv, axis=0, keepdims=True)
    weight = r.wq4[...].reshape(-1, 3 * part)
    d_normed = mm(d_qkv16, weight, NT)
    r.sums[0:1, :] += jnp.sum(d_normed * standardized, axis=0, keepdims=True)
    r.sums[1:2, :] += jnp.sum(d_normed, axis=0, keepdims=True)
    put_blocks(r.outb, tile, narrow(d_normed * gain1 + r.e2[place, :]))


def gather_sums(r, me):
    nz, part = me.nz, r.vec.shape[1] // me.nz
    r.sums[4:5, :] = jnp.sum(wide(flat_rows(r.g[...])), axis=0, keepdims=True)

    def put(z, number, values):
        r.vout[z, 0:1, number * part : (number + 1) * part] = values

    for z in range(nz):
        for row in range(5):
            put(z, row, r.sums[row : row + 1, z * part : (z + 1) * part])
    for chip in range(nz):

        @pl.when(me.t == chip)
        def _():
            for number in range(3):
                held = number * nz + chip
                put(held // 3, 5 + held % 3, r.sums[5:6, number * part : (number + 1) * part])
            for z in range(nz):
                put(z, 8 + chip, r.sums[6:7, z * part : (z + 1) * part])


class Scatter:
    def __init__(self, copies, me, r, source, sent, got, landed):
        self.me, self.r, self.source, self.sent, self.got, self.landed = me, r, source, sent, got, landed
        self.chips = me.nz
        self.sides = sent.shape[0] // self.chips
        self.first = r.k.shape[0]
        self.exchanges = [
            copies.make(self.piece(sent, chip), self.piece(got, chip), me.on_plane(me.pn))
            for chip in range(self.chips)
        ]
        self.steps = []
        for side, near, far, to_near, to_far in (
            (0, me.tx, me.ty, me.xn, me.yn),
            (1, me.ty, me.tx, me.yn, me.xn),
        ):
            first, last = self.place(near, side), self.place(far, side)
            self.steps.append(
                (
                    copies.make(got.at[self.place(me.td, side)], landed.at[3 * side], me.on_plane(to_near)),
                    copies.make(got.at[first], landed.at[3 * side + 1], me.on_plane(to_near)),
                    copies.make(got.at[last], landed.at[3 * side + 2], me.on_plane(to_far)),
                    last,
                )
            )

    def place(self, chip, side):
        return chip * self.sides + side

    def piece(self, array, chip):
        return array.at[pl.ds(chip * self.sides, self.sides)]

    def block(self, number):
        return self.source[self.r.idx[self.first + number]]

    def start(self):
        count = self.chips * self.sides
        for number in range(count):
            self.sent[number] = self.block(count + number)
        for exchange in self.exchanges:
            exchange.start()

    def spread(self):
        count = self.chips * self.sides
        for exchange in self.exchanges:
            exchange.wait_recv()
        for number in range(count):
            flag = self.r.idx[self.first + 2 * count + number // self.sides]
            own, other = wide(self.block(number)), wide(self.got[number])
            here = jnp.full(own.shape, flag, jnp.int32) > 0
            self.got[number] = narrow(jnp.where(here, own, other))
        for far, _, _, _ in self.steps:
            far.start()
        for _, near, _, _ in self.steps:
            near.start()

    def middle(self):
        for side, (far, _, on, last) in enumerate(self.steps):
            far.wait_recv()
            self.got[last] = narrow(wide(self.got[last]) + wide(self.landed[3 * side]))
            on.start()

    def total(self):
        pieces = []
        for side, (_, near, on, _) in enumerate(self.steps):
            near.wait_recv()
            on.wait_recv()
            pieces.append(
                wide(self.got[self.place(self.me.t, side)])
                + wide(self.landed[3 * side + 1])
                + wide(self.landed[3 * side + 2])
            )
        return jnp.concatenate(pieces, axis=0)


def layer_kernel(nz, names, *refs):
    r = types.SimpleNamespace(**dict(zip(names, refs)))
    me = Place(nz)
    copies = Copies(r.send_sems, r.recv_sems)
    sides = r.h.shape[0]
    shard = r.wqs.shape[0]
    tiles = r.att.shape[0] // QTILE

    slice_weights(r, me)
    pack_vectors(r)
    me.greet()

    def row_slot(array):
        return lambda core, chip: array.at[pl.ds((2 * chip + core) * sides, sides)]

    own_rows = pl.ds(me.c * sides, sides)
    h_share = PlaneShare(copies, me, r.h, row_slot(r.hall), sides)
    g_share = PlaneShare(copies, me, r.g, row_slot(r.gall), sides)
    wq = LineSend(copies, me, r.wqs, r.wq4)
    wu = LineGather(copies, me, r.wus, r.wu4)
    wd = LineGather(copies, me, r.wdown.at[pl.ds(me.t * shard, shard)], r.wd4)
    wo = LineSpread(copies, me, r.wout, r.wo1)
    small = [copies.make(r.sm, r.sm4.at[me.z], me.on_line(other)) for other in me.others]

    h_share.start()
    wq.start()
    for copy in small:
        copy.start()
    wu.start()
    wd.start()
    own_down = pltpu.make_async_copy(
        r.wdown.at[pl.ds(me.t * shard, shard)], r.wd4.at[me.z], r.local_sem
    )
    own_down.start()
    r.hall[own_rows] = r.h[...]
    r.gall[own_rows] = r.g[...]
    r.wq4[me.z] = r.wqs[...]
    r.wu4[me.z] = r.wus[...]
    r.sm4[me.z] = r.sm[...]
    block_table(r, me)
    r.sums[...] = jnp.zeros_like(r.sums)
    r.vout[...] = jnp.zeros_like(r.vout)
    r.dk[...] = jnp.zeros_like(r.dk)
    r.dv[...] = jnp.zeros_like(r.dv)
    h_share.relay()
    h_share.swap()
    g_share.start()
    wq.advance()
    for copy in small:
        copy.wait_recv()
    read_vectors(r, me)
    wq.finish()
    h_share.to_p.wait_recv()
    project(r, me, me.t)
    wu.advance(0)
    h_share.swaps[0].wait_recv()
    h_share.on_diagonal()
    project(r, me, me.tx)
    wd.advance(0)
    h_share.swaps[1].wait_recv()
    project(r, me, me.ty)
    g_share.relay()
    wu.advance(1)
    h_share.swaps[2].wait_recv()
    project(r, me, me.td)
    attend(r, me, 1)
    wd.advance(1)
    g_share.swap()
    attend(r, me, 2)
    wu.advance(2)
    g_share.on_diagonal()
    attend(r, me, 0)
    wd.advance(2)
    wo.start()
    own_down.wait()
    wu.finish()
    wd.finish()
    g_share.finish()

    @pl.loop(0, tiles)
    def _(tile):
        feed_forward(r, me, tile)

    half = shard // 2
    out_scatter = Scatter(copies, me, r, r.outb, r.osent, r.ogot, r.oland)
    up_reduce = LineReduce(copies, me, r.gu, r.tu, r.uu)
    down_reduce = LineReduce(copies, me, r.gd, r.td, r.ud)
    out_reduce = LineCollect(copies, me, r.go, r.to, r.uo)
    d_share = PlaneShare(copies, me, r.td.at[me.z], lambda core, chip: r.fd.at[core, chip], half)
    u_share = PlaneShare(copies, me, r.tu.at[me.z], lambda core, chip: r.fu.at[core, chip], half)
    o_spread = PlaneSpread(copies, me, r.to, r.fo, half)

    def share_down():
        d_share.start()
        r.fd[me.k, me.t] = r.td[me.z]

    def share_up():
        u_share.start()
        r.fu[me.k, me.t] = r.tu[me.z]

    weight_grad(r.gd, r.act, r.gl)
    down_reduce.start()
    weight_grad(r.gu, r.n, r.du)
    up_reduce.start()
    wo.advance()
    down_reduce.pair()
    attend(r, me, 3)
    up_reduce.pair()
    wo.finish()

    @pl.loop(0, tiles)
    def _(tile):
        out_project(r, me, tile)

    out_scatter.start()
    r.go[...] = narrow(mm(r.att[...], r.gl[...], TN))
    out_reduce.start()
    attend_grad(r, me, 0)
    out_reduce.pair()
    out_scatter.spread()
    attend_grad(r, me, 3)
    out_scatter.middle()
    attend_grad(r, me, 1)
    down_reduce.collect()
    share_down()
    copies.settle([g_share.hop_x, g_share.hop_y, *g_share.swaps])
    attend_grad(r, me, 2)

    part = r.k.shape[2]
    quarter = r.k.shape[0] * BLK // 4
    kv_moves = []
    for number in range(2):
        first = quarter * (1 - me.k) if number == 0 else 3 * quarter - quarter * (1 - me.k)
        theirs = pl.ds(pl.multiple_of(first, quarter), quarter)
        rows = slice(number * quarter, (number + 1) * quarter)
        r.act[rows, :part] = narrow(r.dk[theirs, :])
        r.act[rows, part : 2 * part] = narrow(r.dv[theirs, :])
        copy = copies.make(r.act.at[rows, : 2 * part], r.kvin.at[rows], me.on_plane(me.pn))
        copy.start()
        kv_moves.append(copy)
    d_share.relay()
    up_reduce.collect()
    share_up()
    for copy in kv_moves:
        copy.wait_recv()

    @pl.loop(0, tiles)
    def _(tile):
        qkv_grad(r, me, tile)

    e_scatter = Scatter(
        copies, me, r, r.outb, r.gall.at[: r.outb.shape[0]], r.gall.at[r.outb.shape[0] :], r.eland
    )
    e_scatter.start()
    u_share.relay()
    d_share.swap()
    out_reduce.collect()
    o_spread.start()
    gather_sums(r, me)
    vec_line = [
        copies.make(r.vout.at[other], r.vline.at[me.z], me.on_line(other)) for other in me.others
    ]
    for copy in vec_line:
        copy.start()
    weight_grad(r.gq, r.n, r.du.at[:, : 3 * part])
    qkv_reduce = LineReduce(copies, me, r.gq, r.tq, r.uq)
    qkv_reduce.start()
    e_scatter.spread()
    qkv_reduce.pair()
    d_share.on_diagonal()
    u_share.swap()
    o_spread.advance()
    for copy in vec_line:
        copy.wait_recv()
    vector = r.vout[me.z]
    for other in me.others:
        vector = vector + r.vline[other]
    r.vsend[...] = vector
    e_scatter.middle()
    vec_plane = [copies.make(r.vsend, r.vplane.at[me.c], me.on_plane(peer)) for peer in me.plane]
    for copy in vec_plane:
        copy.start()
    u_share.on_diagonal()
    o_spread.on_diagonal()
    qkv_reduce.collect()
    q_share = PlaneShare(copies, me, r.tq.at[me.z], lambda core, chip: r.fq.at[core, chip], half)
    q_share.start()
    r.fq[me.k, me.t] = r.tq[me.z]

    residual = wide(flat_rows(r.h[...]))
    own_standardized, own_deviation = norm_rows(residual)
    r.hidden_out[...] = narrow(residual + r.vec[4:5, :] + out_scatter.total())
    e_total = e_scatter.total()
    r.hidden_grad[...] = wide(flat_rows(r.g[...])) + own_deviation * (
        e_total
        - jnp.mean(e_total, axis=-1, keepdims=True)
        - own_standardized * jnp.mean(e_total * own_standardized, axis=-1, keepdims=True)
    )
    q_share.relay()
    q_share.swap()
    for copy in vec_plane:
        copy.wait_recv()
    vector = r.vsend[...]
    for peer in me.plane:
        vector = vector + r.vplane[peer]
    r.vsum[...] = vector
    q_share.on_diagonal()
    for share in (d_share, u_share, o_spread, q_share):
        share.finish()
    copies.finish()


def assemble_kernel(
    fq_ref, fu_ref, fd_ref, fo_ref, out_ref, grad_ref, vsum_ref,
    gq_ref, gu_ref, gd_ref, go_ref, hidden_out_ref, hidden_grad_ref, *vector_refs,
):
    _, chips, _, _ = fq_ref.shape
    part = fq_ref.shape[3] // 3
    hidden_out_ref[...] = out_ref[...]
    hidden_grad_ref[...] = grad_ref[...]
    go_ref[...] = wide(fo_ref[0])
    for chip in range(chips):
        for source, target in ((fq_ref, gq_ref), (fu_ref, gu_ref)):
            for piece in range(source.shape[3] // part):
                first = (piece * chips + chip) * part
                target[:, first : first + part] = wide(
                    source[0, chip, :, piece * part : (piece + 1) * part]
                )
        gd_ref[chip, 0] = wide(fd_ref[0, chip])

    @pl.when(pl.program_id(0) == 0)
    def _():
        first = 0
        for number, target in enumerate(vector_refs):
            count = target.shape[0]
            if number == 5:
                first -= count
            target[...] = vsum_ref[0:1, first : first + count].reshape(count)
            first += count


def rotary_parts(block_count):
    half_rot = ROT // 2
    lane = np.arange(128) % HD
    rate = np.where(lane < ROT, 10000.0 ** (-2.0 * (lane % half_rot) / ROT), 0.0)

    def table(places):
        angle = places[:, None].astype(np.float64) * rate[None, :]
        return np.concatenate([np.cos(angle), np.sin(angle)], axis=1).astype(np.float32)

    return table(np.arange(BLK)), table(np.arange(block_count) * BLK)


VMEM_SPEC = pl.BlockSpec(memory_space=pltpu.VMEM)
SPECS = {
    "order": pl.BlockSpec(memory_space=pltpu.SMEM),
    "wdown": pl.BlockSpec(memory_space=pl.ANY),
}
VMEM_LIMIT = 63 * 1024 * 1024


def sliced_layer(
    nz,
    hidden_in,
    norm1_gain,
    attention_norm_bias,
    qkv_weight,
    qkv_bias,
    out_weight,
    out_bias,
    norm2_gain,
    feedforward_norm_bias,
    up_weight,
    up_bias,
    down_weight,
    down_bias,
    cotangent,
    block_order,
):
    f32, b16 = jnp.float32, jnp.bfloat16
    h, g = hidden_in[0], cotangent[0]
    local_rows, width = h.shape
    chips = lax.axis_size("ctx") // 2
    shard = qkv_weight.shape[0]
    half = shard // 2
    part = width // chips
    hidden = up_weight.shape[1] // chips
    rows = chips * local_rows
    everyone = 2 * rows
    sides = local_rows // BLK

    sums = 5 * shard + qkv_bias.shape[0] + up_bias.shape[0]
    small = 6 * shard + qkv_bias.shape[0] + up_bias.shape[0]
    rope_r, rope_b = rotary_parts(everyone // BLK)

    inputs = {
        "order": block_order,
        "h": h.reshape(sides, BLK, width),
        "g": g.reshape(sides, BLK, width),
        "wqkv": qkv_weight,
        "wup": up_weight,
        "wdown": down_weight,
        "wout": out_weight,
        **dict(
            zip(
                VECTORS,
                (norm1_gain, attention_norm_bias, norm2_gain, feedforward_norm_bias)
                + (out_bias, down_bias, qkv_bias, up_bias),
            )
        ),
        "rope_r": jnp.asarray(rope_r),
        "rope_b": jnp.asarray(rope_b[:, None, :]),
    }
    outputs = {
        "hidden_out": ((local_rows, width), b16),
        "hidden_grad": ((local_rows, width), f32),
        "fq": ((2, chips, half, 3 * part), b16),
        "fu": ((2, chips, half, hidden), b16),
        "fd": ((2, chips, half, width), b16),
        "fo": ((2, half, width), b16),
        "vsum": ((1, sums), f32),
    }
    scratch = {
        "hall": ((everyone // BLK, BLK, width), b16),
        "gall": ((everyone // BLK, BLK, width), b16),
        "wqs": ((shard, 3 * part), b16),
        "wus": ((shard, hidden), b16),
        "wq4": ((nz, shard, 3 * part), b16),
        "wu4": ((nz, shard, hidden), b16),
        "wd4": ((nz, shard, width), b16),
        "wo1": ((part, width), b16),
        "sm": ((1, small), f32),
        "sm4": ((nz, 1, small), f32),
        "vec": ((8, width), f32),
        "sums": ((8, width), f32),
        "q": ((everyone // BLK, BLK, part), b16),
        "k": ((everyone // BLK, BLK, part), b16),
        "v": ((everyone // BLK, BLK, part), b16),
        "kt": ((everyone // BLK, part, BLK), b16),
        "vt": ((everyone // BLK, part, BLK), b16),
        "att": ((rows, part), b16),
        "attt": ((part, rows), b16),
        "lse": ((8, rows), f32),
        "delta": ((8, rows), f32),
        "datt": ((rows, part), b16),
        "act": ((rows, hidden), b16),
        "du": ((rows, hidden), b16),
        "n": ((rows, width), b16),
        "gl": ((rows, width), b16),
        "outb": ((rows // BLK, BLK, width), b16),
        "e2": ((rows, width), f32),
        "dk": ((everyone, part), f32),
        "dv": ((everyone, part), f32),
        "dqt": ((part, rows), f32),
        "kvin": ((rows, 2 * part), b16),
        "osent": ((rows // BLK, BLK, width), b16),
        "ogot": ((rows // BLK, BLK, width), b16),
        "oland": ((6, BLK, width), b16),
        "eland": ((6, BLK, width), b16),
        "gq": ((nz, shard, 3 * part), b16),
        "gu": ((nz, shard, hidden), b16),
        "gd": ((nz, shard, width), b16),
        "go": ((part, width), b16),
        "tq": ((nz, half, 3 * part), b16),
        "uq": ((nz, half, 3 * part), b16),
        "tu": ((nz, half, hidden), b16),
        "uu": ((nz, half, hidden), b16),
        "td": ((nz, half, width), b16),
        "ud": ((nz, half, width), b16),
        "to": ((half, width), b16),
        "uo": ((nz, half, width), b16),
        "vout": ((nz, 1, sums), f32),
        "vline": ((nz, 1, sums), f32),
        "vsend": ((1, sums), f32),
        "vplane": ((2 * chips, 1, sums), f32),
    }
    names = [*inputs, *outputs, *scratch, "idx", "send_sems", "recv_sems", "local_sem"]
    results = pl.pallas_call(
        functools.partial(layer_kernel, nz, names),
        out_shape=tuple(jax.ShapeDtypeStruct(*leaf) for leaf in outputs.values()),
        in_specs=[SPECS.get(name, VMEM_SPEC) for name in inputs],
        out_specs=(VMEM_SPEC,) * len(outputs),
        scratch_shapes=[pltpu.VMEM(*leaf) for leaf in scratch.values()]
        + [pltpu.SMEM((64,), jnp.int32)]
        + [pltpu.SemaphoreType.DMA((SEMAPHORES,))] * 2
        + [pltpu.SemaphoreType.DMA],
        compiler_params=pltpu.CompilerParams(
            collective_id=0, has_side_effects=True, vmem_limit_bytes=VMEM_LIMIT
        ),
        name="layer",
    )(*inputs.values())
    hidden_out, hidden_grad, fq, fu, fd, fo, vsum = results

    steps = 4
    some, few = shard // steps, local_rows // steps
    inner = half // some

    def pieces(cols):
        return pl.BlockSpec((1, chips, some, cols), lambda i: (i // inner, 0, i % inner, 0))

    def lines(count, cols):
        return pl.BlockSpec((count, cols), lambda i: (i, 0))

    def vector(count):
        return pl.BlockSpec((count,), lambda i: (0,))

    sizes = [shard] * 6 + [qkv_bias.shape[0], up_bias.shape[0]]
    grad_qkv, grad_up, grad_down, grad_out, hidden_out, hidden_grad, *vectors = pl.pallas_call(
        assemble_kernel,
        grid=(steps,),
        out_shape=(
            jax.ShapeDtypeStruct(qkv_weight.shape, f32),
            jax.ShapeDtypeStruct(up_weight.shape, f32),
            jax.ShapeDtypeStruct((chips, steps, some, width), f32),
            jax.ShapeDtypeStruct(out_weight.shape, f32),
            jax.ShapeDtypeStruct(h.shape, b16),
            jax.ShapeDtypeStruct(h.shape, f32),
        )
        + tuple(jax.ShapeDtypeStruct((size,), f32) for size in sizes),
        in_specs=[
            pieces(3 * part),
            pieces(hidden),
            pieces(width),
            pl.BlockSpec((1, some, width), lambda i: (i // inner, i % inner, 0)),
            lines(few, width),
            lines(few, width),
            pl.BlockSpec((1, sums), lambda i: (0, 0)),
        ],
        out_specs=(
            lines(some, qkv_weight.shape[1]),
            lines(some, up_weight.shape[1]),
            pl.BlockSpec((chips, 1, some, width), lambda i: (0, i, 0, 0)),
            lines(some, width),
            lines(few, width),
            lines(few, width),
        )
        + tuple(vector(size) for size in sizes),
        compiler_params=pltpu.CompilerParams(vmem_limit_bytes=56 * 1024 * 1024),
        name="assemble",
    )(fq, fu, fd, fo, hidden_out, hidden_grad, vsum)
    g_gain1, g_shift1, g_gain2, g_shift2, g_bout, g_bdown, g_bqkv, g_bup = vectors
    return (
        hidden_out[None],
        hidden_grad[None],
        g_gain1,
        g_shift1,
        grad_qkv,
        g_bqkv,
        grad_out,
        g_bout,
        g_gain2,
        g_shift2,
        grad_up,
        g_bup,
        grad_down.reshape(down_weight.shape),
        g_bdown,
    )


def sliced_fits(mesh):
    return mesh.shape["ctx"] == 8 and mesh.shape["fsdp"] == 4


def solution(mesh):
    in_specs = (
        P("fsdp", "ctx", None),
        P("fsdp"),
        P("fsdp"),
        P("fsdp", None),
        P("fsdp"),
        P("fsdp", None),
        P("fsdp"),
        P("fsdp"),
        P("fsdp"),
        P("fsdp", None),
        P("fsdp"),
        P("fsdp", None),
        P("fsdp"),
        P("fsdp", "ctx", None),
        P(),
    )
    out_specs = (
        P("fsdp", "ctx", None),
        P("fsdp", "ctx", None),
        P("fsdp"),
        P("fsdp"),
        P("fsdp", None),
        P("fsdp"),
        P("fsdp", None),
        P("fsdp"),
        P("fsdp"),
        P("fsdp"),
        P("fsdp", None),
        P("fsdp"),
        P("fsdp", None),
        P("fsdp"),
    )
    local = whole_parameter_layer
    if sliced_fits(mesh):
        local = functools.partial(sliced_layer, mesh.shape["fsdp"])
    return jax.shard_map(local, mesh=mesh, in_specs=in_specs, out_specs=out_specs, check_vma=False)
```

```python
import functools
import math
import types

import jax
import jax.numpy as jnp
import numpy as np
from jax import lax
from jax.experimental import pallas as pl
from jax.experimental.pallas import tpu as pltpu
from jax.sharding import PartitionSpec as P

H = 12
HD = 64
ROT = 16
BLK = 128


EPS = 1e-05
NEG = -1e30
SQRT_HALF = 0.7071067811865476
INV_ROOT_TWO_PI = 0.3989422804014327


def apply_layer_norm(values_in, norm_gain, norm_bias):
    centre = jnp.mean(values_in, axis=-1, keepdims=True)
    mean_removed = values_in - centre
    inverse_deviation = lax.rsqrt(
        jnp.mean(mean_removed * mean_removed, axis=-1, keepdims=True) + EPS
    )
    standardized = mean_removed * inverse_deviation
    return (standardized * norm_gain + norm_bias, standardized, inverse_deviation)


def layer_norm_backward(output_gradient, standardized, inverse_deviation, norm_gain):
    gain_scaled = output_gradient * norm_gain
    return inverse_deviation * (
        gain_scaled
        - jnp.mean(gain_scaled, axis=-1, keepdims=True)
        - standardized * jnp.mean(gain_scaled * standardized, axis=-1, keepdims=True)
    )


def gelu_exact(values_in):
    return 0.5 * values_in * (1.0 + lax.erf(values_in * SQRT_HALF))


def gelu_slope(values_in):
    return (
        0.5 * (1.0 + lax.erf(values_in * SQRT_HALF))
        + values_in * jnp.exp(-0.5 * values_in * values_in) * INV_ROOT_TWO_PI
    )


def rotary_tables(position_list):
    half_rot = ROT // 2
    inverse = jnp.power(jnp.float32(10000.0), -2.0 * jnp.arange(half_rot, dtype=jnp.float32) / ROT)
    angle = position_list.astype(jnp.float32)[:, None] * inverse[None, :]
    return (jnp.cos(angle)[:, None, :], jnp.sin(angle)[:, None, :])


def rotate(tensor, cosine, sine):
    half_rot = ROT // 2
    first_half = tensor[..., :half_rot]
    second_half = tensor[..., half_rot:ROT]
    return jnp.concatenate(
        [
            first_half * cosine - second_half * sine,
            second_half * cosine + first_half * sine,
            tensor[..., ROT:],
        ],
        axis=-1,
    )


def rotate_back(tensor, cosine, sine):
    half_rot = ROT // 2
    first_half = tensor[..., :half_rot]
    second_half = tensor[..., half_rot:ROT]
    return jnp.concatenate(
        [
            first_half * cosine + second_half * sine,
            second_half * cosine - first_half * sine,
            tensor[..., ROT:],
        ],
        axis=-1,
    )


def masked_logits(query_block, key_block, query_pos, key_pos):
    logits = jnp.einsum(
        "qhd,khd->hqk", query_block, key_block, preferred_element_type=jnp.float32
    ) * (1.0 / math.sqrt(HD))
    return jnp.where(key_pos[None, None, :] <= query_pos[None, :, None], logits, NEG)


def block_terms(
    query_block, dout_block, total_t, delta_t, query_pos, key_block, value_block, key_pos
):
    logits = masked_logits(query_block, key_block, query_pos, key_pos)
    probs_wide = jnp.exp(logits - total_t[:, :, None])
    dprobs = jnp.einsum("qhd,khd->hqk", dout_block, value_block, preferred_element_type=jnp.float32)
    d_logits = (probs_wide * (dprobs - delta_t[:, :, None]) * (1.0 / math.sqrt(HD))).astype(
        jnp.bfloat16
    )
    return (probs_wide.astype(jnp.bfloat16), d_logits)


def keep_state(state_in):
    return state_in


def forward_attention(query, keys_all, values_all, own_pos, all_pos):
    local_rows = query.shape[0]
    seq_rows = keys_all.shape[0]
    qstep = min(512, local_rows)
    kstep = min(512, seq_rows)
    latest = jnp.max(own_pos)

    def stats_step(number, state_in):
        key_block = lax.dynamic_slice_in_dim(keys_all, number * kstep, kstep, 0)
        key_pos = lax.dynamic_slice_in_dim(all_pos, number * kstep, kstep, 0)

        def stats_live(state_now):
            running_max, running_sum = state_now
            logits = masked_logits(query, key_block, own_pos, key_pos)
            new_max = jnp.maximum(running_max, jnp.max(logits, axis=-1))
            running_sum = running_sum * jnp.exp(running_max - new_max) + jnp.sum(
                jnp.exp(logits - new_max[:, :, None]), axis=-1
            )
            return (new_max, running_sum)

        return lax.cond(jnp.min(key_pos) <= latest, stats_live, keep_state, state_in)

    start_state = (jnp.full((H, qstep), NEG, jnp.float32), jnp.zeros((H, qstep), jnp.float32))
    running_max, running_sum = lax.fori_loop(0, seq_rows // kstep, stats_step, start_state)
    total_t = running_max + jnp.log(running_sum)

    def value_step(number, state_in):
        key_block = lax.dynamic_slice_in_dim(keys_all, number * kstep, kstep, 0)
        value_block = lax.dynamic_slice_in_dim(values_all, number * kstep, kstep, 0)
        key_pos = lax.dynamic_slice_in_dim(all_pos, number * kstep, kstep, 0)

        def value_live(state_now):
            logits = masked_logits(query, key_block, own_pos, key_pos)
            attn_probs = jnp.exp(logits - total_t[:, :, None]).astype(jnp.bfloat16)
            return state_now + jnp.einsum(
                "hqk,khd->qhd", attn_probs, value_block, preferred_element_type=jnp.float32
            )

        return lax.cond(jnp.min(key_pos) <= latest, value_live, keep_state, state_in)

    weighted = lax.fori_loop(
        0, seq_rows // kstep, value_step, jnp.zeros((qstep, H, HD), jnp.float32)
    )
    totals = total_t.T
    return (weighted, totals)


def query_grads(query, d_att, log_total, delta, own_pos, keys_all, values_all, all_pos):
    local_rows = query.shape[0]
    seq_rows = keys_all.shape[0]
    qstep = min(512, local_rows)
    kstep = min(512, seq_rows)
    key_grads = jnp.zeros((seq_rows, H, HD), jnp.float32)
    value_grads = jnp.zeros((seq_rows, H, HD), jnp.float32)
    total_t = log_total.T
    delta_t = delta.T
    latest = jnp.max(own_pos)

    def key_step(number, state_in):
        offset = number * kstep
        key_block = lax.dynamic_slice_in_dim(keys_all, offset, kstep, 0)
        value_block = lax.dynamic_slice_in_dim(values_all, offset, kstep, 0)
        key_pos = lax.dynamic_slice_in_dim(all_pos, offset, kstep, 0)

        def key_live(state_now):
            attn_probs, d_logits = block_terms(
                query, d_att, total_t, delta_t, own_pos, key_block, value_block, key_pos
            )
            d_query = state_now[0] + jnp.einsum(
                "hqk,khd->qhd", d_logits, key_block, preferred_element_type=jnp.float32
            )
            key_acc = state_now[1]
            value_acc = state_now[2]
            key_part = jnp.einsum(
                "hqk,qhd->khd", d_logits, query, preferred_element_type=jnp.float32
            )
            value_part = jnp.einsum(
                "hqk,qhd->khd", attn_probs, d_att, preferred_element_type=jnp.float32
            )
            key_acc = lax.dynamic_update_slice_in_dim(
                key_acc, lax.dynamic_slice_in_dim(key_acc, offset, kstep, 0) + key_part, offset, 0
            )
            value_acc = lax.dynamic_update_slice_in_dim(
                value_acc,
                lax.dynamic_slice_in_dim(value_acc, offset, kstep, 0) + value_part,
                offset,
                0,
            )
            return (d_query, key_acc, value_acc)

        return lax.cond(jnp.min(key_pos) <= latest, key_live, keep_state, state_in)

    start_state = (jnp.zeros((qstep, H, HD), jnp.float32),) + (key_grads, value_grads)
    result = lax.fori_loop(0, seq_rows // kstep, key_step, start_state)
    pieces = result[0]
    key_grads = result[1]
    value_grads = result[2]
    return (pieces, key_grads, value_grads)


def whole_parameter_layer(
    hidden_in,
    norm1_gain,
    attention_norm_bias,
    qkv_weight,
    qkv_bias,
    out_weight,
    out_bias,
    norm2_gain,
    feedforward_norm_bias,
    up_weight,
    up_bias,
    down_weight,
    down_bias,
    cotangent,
    block_order,
):
    (
        attention_norm_gain,
        attention_bias_term,
        wqkv,
        bqkv,
        wout,
        bout,
        feedforward_norm_gain,
        feedforward_bias_term,
        wup,
        bup,
        wdown,
        bdown,
    ) = (
        lax.all_gather(norm1_gain, "fsdp", axis=0, tiled=True),
        lax.all_gather(attention_norm_bias, "fsdp", axis=0, tiled=True),
        lax.all_gather(qkv_weight, "fsdp", axis=0, tiled=True),
        lax.all_gather(qkv_bias, "fsdp", axis=0, tiled=True),
        lax.all_gather(out_weight, "fsdp", axis=0, tiled=True),
        lax.all_gather(out_bias, "fsdp", axis=0, tiled=True),
        lax.all_gather(norm2_gain, "fsdp", axis=0, tiled=True),
        lax.all_gather(feedforward_norm_bias, "fsdp", axis=0, tiled=True),
        lax.all_gather(up_weight, "fsdp", axis=0, tiled=True),
        lax.all_gather(up_bias, "fsdp", axis=0, tiled=True),
        lax.all_gather(down_weight, "fsdp", axis=0, tiled=True),
        lax.all_gather(down_bias, "fsdp", axis=0, tiled=True),
    )
    width = H * HD
    hidden_rows = hidden_in[0]
    cotan_rows = cotangent[0]
    local_rows = hidden_rows.shape[0]
    ctx_count = lax.axis_size("ctx")
    ctx_rank = lax.axis_index("ctx")
    seq_rows = local_rows * ctx_count
    all_pos = (block_order[:, None] * BLK + jnp.arange(BLK, dtype=jnp.int32)[None, :]).reshape(
        seq_rows
    )
    own_pos = lax.dynamic_slice_in_dim(all_pos, ctx_rank * local_rows, local_rows, 0)
    cosine, sine = rotary_tables(own_pos)
    attention_norm_gain = attention_norm_gain.astype(jnp.float32)
    feedforward_norm_gain = feedforward_norm_gain.astype(jnp.float32)
    residual_stream = hidden_rows.astype(jnp.float32)
    attention_normed, attention_standardized, attention_inverse_deviation = apply_layer_norm(
        residual_stream, attention_norm_gain, attention_bias_term.astype(jnp.float32)
    )
    normed1_b = attention_normed.astype(jnp.bfloat16)
    projected = jnp.dot(normed1_b, wqkv, preferred_element_type=jnp.float32) + bqkv.astype(
        jnp.float32
    )
    query = rotate(projected[:, :width].reshape(local_rows, H, HD), cosine, sine).astype(
        jnp.bfloat16
    )
    key_rows = rotate(
        projected[:, width : 2 * width].reshape(local_rows, H, HD), cosine, sine
    ).astype(jnp.bfloat16)
    value_rows = projected[:, 2 * width :].astype(jnp.bfloat16)
    keys_all, values_all = (
        lax.all_gather(key_rows.reshape(local_rows, width), "ctx", axis=0, tiled=True),
        lax.all_gather(value_rows, "ctx", axis=0, tiled=True),
    )
    keys_all = keys_all.reshape(seq_rows, H, HD)
    values_all = values_all.reshape(seq_rows, H, HD)
    attended, log_total = forward_attention(query, keys_all, values_all, own_pos, all_pos)
    attended_b = attended.reshape(local_rows, width).astype(jnp.bfloat16)
    attn_out = jnp.dot(attended_b, wout, preferred_element_type=jnp.float32) + bout.astype(
        jnp.float32
    )
    feedforward_normed, feedforward_standardized, feedforward_inverse_deviation = apply_layer_norm(
        residual_stream, feedforward_norm_gain, feedforward_bias_term.astype(jnp.float32)
    )
    normed2_b = feedforward_normed.astype(jnp.bfloat16)
    up_rows = jnp.dot(normed2_b, wup, preferred_element_type=jnp.float32) + bup.astype(jnp.float32)
    act_b = gelu_exact(up_rows).astype(jnp.bfloat16)
    mlp_out = jnp.dot(act_b, wdown, preferred_element_type=jnp.float32) + bdown.astype(jnp.float32)
    hidden_out = (residual_stream + attn_out + mlp_out).astype(jnp.bfloat16)
    cotan_wide = cotan_rows.astype(jnp.float32)
    grad_wdown = jnp.einsum("tk,tn->kn", act_b, cotan_rows, preferred_element_type=jnp.float32)
    grad_bdown = jnp.sum(cotan_wide, axis=0)
    d_up = jnp.einsum(
        "tn,kn->tk", cotan_rows, wdown, preferred_element_type=jnp.float32
    ) * gelu_slope(up_rows)
    d_up16 = d_up.astype(jnp.bfloat16)
    grad_wup = jnp.einsum("tk,tn->kn", normed2_b, d_up16, preferred_element_type=jnp.float32)
    grad_bup = jnp.sum(d_up, axis=0)
    grad_feedforward_normed = jnp.einsum(
        "tn,kn->tk", d_up16, wup, preferred_element_type=jnp.float32
    )
    grad_feedforward_gain = jnp.sum(grad_feedforward_normed * feedforward_standardized, axis=0)
    grad_shift2 = jnp.sum(grad_feedforward_normed, axis=0)
    feedforward_branch_grad = layer_norm_backward(
        grad_feedforward_normed,
        feedforward_standardized,
        feedforward_inverse_deviation,
        feedforward_norm_gain,
    )
    grad_wout = jnp.einsum("tk,tn->kn", attended_b, cotan_rows, preferred_element_type=jnp.float32)
    d_att = jnp.einsum("tn,kn->tk", cotan_rows, wout, preferred_element_type=jnp.float32).astype(
        jnp.bfloat16
    )
    delta = jnp.sum(
        d_att.reshape(local_rows, H, HD).astype(jnp.float32)
        * attended_b.reshape(local_rows, H, HD).astype(jnp.float32),
        axis=-1,
    )
    d_att3 = d_att.reshape(local_rows, H, HD)
    d_query, key_grads, value_grads = query_grads(
        query, d_att3, log_total, delta, own_pos, keys_all, values_all, all_pos
    )
    d_key, d_value = (
        lax.psum_scatter(
            key_grads.reshape(seq_rows, width), "ctx", scatter_dimension=0, tiled=True
        ),
        lax.psum_scatter(
            value_grads.reshape(seq_rows, width), "ctx", scatter_dimension=0, tiled=True
        ),
    )
    d_query = rotate_back(d_query, cosine, sine)
    d_key = rotate_back(d_key.reshape(local_rows, H, HD), cosine, sine)
    d_qkv = jnp.concatenate(
        [d_query.reshape(local_rows, width), d_key.reshape(local_rows, width), d_value], axis=1
    )
    d_qkv16 = d_qkv.astype(jnp.bfloat16)
    grad_wqkv = jnp.einsum("tk,tn->kn", normed1_b, d_qkv16, preferred_element_type=jnp.float32)
    grad_bqkv = jnp.sum(d_qkv, axis=0)
    grad_attention_normed = jnp.einsum(
        "tn,kn->tk", d_qkv16, wqkv, preferred_element_type=jnp.float32
    )
    grad_attention_gain = jnp.sum(grad_attention_normed * attention_standardized, axis=0)
    grad_shift1 = jnp.sum(grad_attention_normed, axis=0)
    attention_branch_grad = layer_norm_backward(
        grad_attention_normed,
        attention_standardized,
        attention_inverse_deviation,
        attention_norm_gain,
    )
    hidden_grad = cotan_wide + attention_branch_grad + feedforward_branch_grad
    terms = (
        grad_attention_gain,
        grad_shift1,
        grad_wqkv,
        grad_bqkv,
        grad_wout,
        grad_bdown,
        grad_feedforward_gain,
        grad_shift2,
        grad_wup,
        grad_bup,
        grad_wdown,
        grad_bdown,
    )
    shares = (
        lax.psum_scatter(terms[0], "fsdp", scatter_dimension=0, tiled=True),
        lax.psum_scatter(terms[1], "fsdp", scatter_dimension=0, tiled=True),
        lax.psum_scatter(terms[2], "fsdp", scatter_dimension=0, tiled=True),
        lax.psum_scatter(terms[3], "fsdp", scatter_dimension=0, tiled=True),
        lax.psum_scatter(terms[4], "fsdp", scatter_dimension=0, tiled=True),
        lax.psum_scatter(terms[5], "fsdp", scatter_dimension=0, tiled=True),
        lax.psum_scatter(terms[6], "fsdp", scatter_dimension=0, tiled=True),
        lax.psum_scatter(terms[7], "fsdp", scatter_dimension=0, tiled=True),
        lax.psum_scatter(terms[8], "fsdp", scatter_dimension=0, tiled=True),
        lax.psum_scatter(terms[9], "fsdp", scatter_dimension=0, tiled=True),
        lax.psum_scatter(terms[10], "fsdp", scatter_dimension=0, tiled=True),
        lax.psum_scatter(terms[11], "fsdp", scatter_dimension=0, tiled=True),
    )
    shares = lax.psum(
        (
            shares[0],
            shares[1],
            shares[2],
            shares[3],
            shares[4],
            shares[5],
            shares[6],
            shares[7],
            shares[8],
            shares[9],
            shares[10],
            shares[11],
        ),
        "ctx",
    )
    return (
        hidden_out[None],
        hidden_grad[None],
        shares[0],
        shares[1],
        shares[2],
        shares[3],
        shares[4],
        shares[5],
        shares[6],
        shares[7],
        shares[8],
        shares[9],
        shares[10],
        shares[11],
    )


MESH_IDS = pl.DeviceIdType.MESH
NN = (((1,), (0,)), ((), ()))
NT = (((1,), (1,)), ((), ()))
TN = (((0,), (0,)), ((), ()))
QTILE = 256
SEMAPHORES = 192


def mm(left, right, dims=NN):
    return lax.dot_general(left, right, dims, preferred_element_type=jnp.float32)


def flip(index, bit):
    return index + bit - 2 * bit * ((index // bit) % 2)


def run_when(condition, action):
    if condition is None:
        action()
    else:
        pl.when(condition)(action)


def narrow(values):
    return values.astype(jnp.bfloat16)


def wide(values):
    return values.astype(jnp.float32)


class Copies:
    def __init__(self, send_sems, recv_sems):
        self.send_sems, self.recv_sems = send_sems, recv_sems
        self.count, self.started, self.numbers = 0, [], {}

    def make(self, source, target, device, when=None, like=None):
        if like is None:
            number = self.count
            self.count += 1
        else:
            number = self.numbers[id(like)]
        copy = pltpu.make_async_remote_copy(
            src_ref=source,
            dst_ref=target,
            send_sem=self.send_sems.at[number],
            recv_sem=self.recv_sems.at[number],
            device_id=device,
            device_id_type=MESH_IDS,
        )
        self.started.append((copy, when))
        self.numbers[id(copy)] = number
        return copy

    def settle(self, chosen):
        numbers = {id(copy) for copy in chosen}
        for copy, when in self.started:
            if id(copy) in numbers:
                run_when(when, copy.wait_send)
        self.started = [entry for entry in self.started if id(entry[0]) not in numbers]

    def finish(self):
        for copy, when in self.started:
            run_when(when, copy.wait_send)


class Place:
    def __init__(self, nz):
        self.nz = nz
        self.c, self.z = lax.axis_index("ctx"), lax.axis_index("fsdp")
        self.k, self.t = self.c % 2, self.c // 2
        self.xn, self.yn, self.pn = flip(self.c, 2), flip(self.c, 4), flip(self.c, 1)
        self.dn = flip(self.xn, 4)
        self.tx, self.ty = flip(self.t, 1), flip(self.t, 2)
        self.td = flip(self.tx, 2)
        self.others = [(self.z + d) % nz for d in range(1, nz)]
        self.plane = [self.xn, self.yn, self.dn, self.pn] + [
            flip(peer, 1) for peer in (self.xn, self.yn, self.dn)
        ]
        self.above, self.below = jnp.minimum(self.z + 1, nz - 1), jnp.maximum(self.z - 1, 0)

    def on_plane(self, c):
        return (c, self.z)

    def on_line(self, z):
        return (self.c, z)

    def greet(self):
        barrier = pltpu.get_barrier_semaphore()
        peers = [self.on_plane(peer) for peer in self.plane] + [self.on_line(z) for z in self.others]
        for peer in peers:
            pl.semaphore_signal(barrier, inc=1, device_id=peer, device_id_type=MESH_IDS)
        pl.semaphore_wait(barrier, len(peers))


class PlaneShare:
    def __init__(self, copies, me, source, slot, rows):
        self.copies, self.me, self.slot = copies, me, slot
        top, bottom = pl.ds(0, rows // 2), pl.ds(rows // 2, rows // 2)
        own = slot(me.k, me.t)
        to_x, to_y = me.on_plane(me.xn), me.on_plane(me.yn)
        self.x_first = copies.make(source.at[top], own.at[top], to_x)
        self.y_first = copies.make(source.at[bottom], own.at[bottom], to_y)
        self.x_second = copies.make(source.at[bottom], own.at[bottom], to_x)
        self.y_second = copies.make(source.at[top], own.at[top], to_y)
        self.to_p = copies.make(source, own, me.on_plane(me.pn))
        through_x, through_y = slot(me.k, me.tx).at[top], slot(me.k, me.ty).at[bottom]
        self.hop_y = copies.make(through_x, through_x, to_y)
        self.hop_x = copies.make(through_y, through_y, to_x)
        self.swaps = []
        for chip in (me.tx, me.ty, me.td):
            place = slot(me.k, chip)
            self.swaps.append(copies.make(place, place, me.on_plane(me.pn)))

    def start(self):
        for copy in (self.x_first, self.y_first, self.x_second, self.y_second, self.to_p):
            copy.start()

    def relay(self):
        self.x_first.wait_recv()
        self.hop_y.start()
        self.y_first.wait_recv()
        self.hop_x.start()

    def swap(self):
        self.x_second.wait_recv()
        self.swaps[0].start()
        self.y_second.wait_recv()
        self.swaps[1].start()

    def on_diagonal(self):
        self.hop_y.wait_recv()
        self.hop_x.wait_recv()
        self.swaps[2].start()

    def finish(self):
        for copy in (self.to_p, *self.swaps):
            copy.wait_recv()


class LineGather:
    def __init__(self, copies, me, source, gathered):
        self.copies, self.me, self.gathered = copies, me, gathered
        rows = gathered.shape[1] // 2
        self.mine = pl.ds(me.k * rows, rows)
        self.moves, self.swaps = {}, []
        for step in range(me.nz - 1):
            for sign in (1, -1):
                shard, target = me.z - sign * step, me.z + sign
                ok = (shard >= 0) & (shard < me.nz) & (target >= 0) & (target < me.nz)
                place = self.slot(shard)
                copy = copies.make(
                    source.at[self.mine] if step == 0 else place,
                    place,
                    me.on_line(jnp.clip(target, 0, me.nz - 1)),
                    when=ok,
                )
                self.moves[step, sign] = (copy, ok)

    def slot(self, shard):
        return self.gathered.at[jnp.clip(shard, 0, self.me.nz - 1), self.mine]

    def start(self):
        for sign in (1, -1):
            copy, ok = self.moves[0, sign]
            run_when(ok, copy.start)

    def advance(self, step):
        me = self.me
        for sign in (1, -1):
            arrived = me.z - sign * (step + 1)
            ok = (arrived >= 0) & (arrived < me.nz)
            run_when(ok, self.moves[step, sign][0].wait_recv)
            if step + 1 < me.nz - 1:
                copy, following = self.moves[step + 1, sign]
                run_when(following, copy.start)
            place = self.slot(arrived)
            swap = self.copies.make(place, place, me.on_plane(me.pn), when=ok)
            run_when(ok, swap.start)
            self.swaps.append((swap, ok))

    def finish(self):
        for swap, ok in self.swaps:
            run_when(ok, swap.wait_recv)


class LineSend:
    def __init__(self, copies, me, source, gathered):
        self.me = me
        rows = gathered.shape[1] // 2
        mine = pl.ds(me.k * rows, rows)
        self.sends, self.swaps = [], []
        for distance, other in enumerate(me.others, 1):
            self.sends.append(
                copies.make(source.at[mine], gathered.at[me.z, mine], me.on_line(other))
            )
            place = gathered.at[(me.z - distance) % me.nz, mine]
            self.swaps.append(copies.make(place, place, me.on_plane(me.pn)))

    def start(self):
        for send in self.sends:
            send.start()

    def advance(self):
        for send, swap in zip(self.sends, self.swaps):
            send.wait_recv()
            swap.start()

    def finish(self):
        for swap in self.swaps:
            swap.wait_recv()


class LineSpread:
    def __init__(self, copies, me, source, target, sem):
        self.me = me
        self.keep = pltpu.make_async_copy(source, target, sem)
        rows = target.shape[0] // 2
        mine = pl.ds(me.k * rows, rows)
        self.here, self.away = me.z == me.t, me.z != me.t
        place = target.at[mine]
        self.sends, self.arrivals = [], []
        for distance in range(1, me.nz):
            target_z = (me.t + distance) % me.nz
            copy = copies.make(source.at[mine], place, me.on_line(target_z), when=self.here)
            self.sends.append(copy)
            self.arrivals.append(me.z == target_z)
        self.swap = copies.make(place, place, me.on_plane(me.pn), when=self.away)

    def start(self):
        @pl.when(self.here)
        def _():
            for copy in self.sends:
                copy.start()
            self.keep.start()

    def advance(self):
        for copy, arrives in zip(self.sends, self.arrivals):
            pl.when(arrives)(copy.wait_recv)
        pl.when(self.away)(self.swap.start)

    def finish(self):
        pl.when(self.here)(self.keep.wait)
        pl.when(self.away)(self.swap.wait_recv)


class LineReduce:
    def __init__(self, copies, me, source, total, landed):
        self.me, self.source, self.total, self.landed = me, source, total, landed
        half = total.shape[1]
        self.mine, theirs = pl.ds(me.k * half, half), pl.ds((1 - me.k) * half, half)
        self.exchange = copies.make(source.at[:, theirs], total, me.on_plane(me.pn))
        self.sends = [
            copies.make(total.at[other], landed.at[me.z], me.on_line(other)) for other in me.others
        ]

    def start(self):
        self.exchange.start()

    def pair(self):
        self.exchange.wait_recv()
        for owner in range(self.me.nz):
            self.total[owner] = narrow(
                wide(self.total[owner]) + wide(self.source[owner, self.mine])
            )
        for send in self.sends:
            send.start()

    def collect(self):
        me = self.me
        result = wide(self.total[me.z])
        for send in self.sends:
            send.wait_recv()
        for other in me.others:
            result = result + wide(self.landed[other])
        self.total[me.z] = narrow(result)


class LineCollect:
    def __init__(self, copies, me, source, total, landed):
        self.me, self.source, self.total, self.landed = me, source, total, landed
        half = total.shape[0]
        self.mine, theirs = pl.ds(me.k * half, half), pl.ds((1 - me.k) * half, half)
        self.exchange = copies.make(source.at[theirs], total, me.on_plane(me.pn))
        self.sends = []
        for distance in range(1, me.nz):
            leaves = (me.z + distance) % me.nz == me.t
            copy = copies.make(total, landed.at[me.z], me.on_line(me.t), when=leaves)
            self.sends.append((copy, leaves))

    def start(self):
        self.exchange.start()

    def pair(self):
        self.exchange.wait_recv()
        self.total[...] = narrow(wide(self.total[...]) + wide(self.source[self.mine]))
        for copy, leaves in self.sends:
            pl.when(leaves)(copy.start)

    def collect(self):
        me = self.me

        @pl.when(me.z == me.t)
        def _():
            result = wide(self.total[...])
            for copy, _ in self.sends:
                copy.wait_recv()
            for other in me.others:
                result = result + wide(self.landed[other])
            self.total[...] = narrow(result)


class PlaneSpread:
    def __init__(self, copies, me, source, target, rows, sem):
        self.me = me
        self.keep = pltpu.make_async_copy(source, target.at[me.k], sem)
        top, bottom = pl.ds(0, rows // 2), pl.ds(rows // 2, rows // 2)
        place = target.at[me.k]
        self.here, self.from_x, self.from_y = me.t == me.z, me.tx == me.z, me.ty == me.z
        self.from_d = me.td == me.z
        self.to_x = copies.make(source, place, me.on_plane(me.xn), when=self.here)
        self.to_y = copies.make(source, place, me.on_plane(me.yn), when=self.here)
        self.to_p = copies.make(source, place, me.on_plane(me.pn), when=self.here)
        self.hop_y = copies.make(place.at[top], place.at[top], me.on_plane(me.yn), when=self.from_x)
        self.hop_x = copies.make(
            place.at[bottom], place.at[bottom], me.on_plane(me.xn), when=self.from_y
        )
        away = self.from_x | self.from_y | self.from_d
        self.away = away
        self.swap = copies.make(place, place, me.on_plane(me.pn), when=away, like=self.to_p)

    def start(self):
        @pl.when(self.here)
        def _():
            self.to_x.start()
            self.to_y.start()
            self.to_p.start()
            self.keep.start()

    def advance(self):
        @pl.when(self.from_x)
        def _():
            self.to_x.wait_recv()
            self.hop_y.start()
            self.swap.start()

        @pl.when(self.from_y)
        def _():
            self.to_y.wait_recv()
            self.hop_x.start()
            self.swap.start()

    def on_diagonal(self):
        @pl.when(self.from_d)
        def _():
            self.hop_y.wait_recv()
            self.hop_x.wait_recv()
            self.swap.start()

    def finish(self):
        pl.when(self.here)(self.keep.wait)
        self.to_p.wait_recv()

def norm_rows(values_in):
    centre = jnp.mean(values_in, axis=-1, keepdims=True)
    mean_removed = values_in - centre
    inverse_deviation = lax.rsqrt(
        jnp.mean(mean_removed * mean_removed, axis=-1, keepdims=True) + EPS
    )
    return mean_removed * inverse_deviation, inverse_deviation


def head_rows(rows, head):
    lanes = lax.broadcasted_iota(jnp.int32, rows.shape, 1)
    inside = (lanes >= head * HD) & (lanes < (head + 1) * HD)
    return jnp.where(inside, rows, jnp.zeros_like(rows))


def rope_lanes(r, blocks, columns, back):
    half_rot = ROT // 2
    tables = [[], [], []]
    row_cos, row_sin = r.rope_r[:, :128], r.rope_r[:, 128:]
    lane = lax.broadcasted_iota(jnp.int32, row_cos.shape, 1) % HD
    for block in blocks:
        both = r.rope_b[block]
        block_cos, block_sin = both[:, :128], both[:, 128:]
        cosine = block_cos * row_cos - block_sin * row_sin
        sine = block_sin * row_cos + block_cos * row_sin
        if back:
            sine = -sine
        tables[0].append(cosine)
        tables[1].append(jnp.where(lane < half_rot, -sine, 0.0))
        tables[2].append(jnp.where(lane >= half_rot, sine, 0.0))
    stacked = [jnp.concatenate(table, axis=0) for table in tables]
    return [jnp.concatenate([table] * (columns // 128), axis=1) for table in stacked]


def turn(values, tables):
    columns, half_rot = values.shape[1], ROT // 2
    return (
        values * tables[0]
        + pltpu.roll(values, columns - half_rot, 1) * tables[1]
        + pltpu.roll(values, half_rot, 1) * tables[2]
    )


def windows(r, me):
    part = r.wqs.shape[1] // 3
    chips, columns = me.nz, r.win.shape[2]
    copies = []
    for source, pieces in ((r.wqkv, 3), (r.wup, r.wus.shape[1] // part)):
        for piece in range(pieces):
            first = (piece * chips + me.t) * part // 128 * 128
            number = len(copies)
            copies.append(
                pltpu.make_async_copy(
                    source.at[:, pl.ds(pl.multiple_of(first, 128), columns)],
                    r.win.at[number],
                    r.window_sems.at[number],
                )
            )
    return copies


def slice_weights(r, me):
    part = r.wqs.shape[1] // 3
    for chip in range(me.nz):

        @pl.when(me.t == chip)
        def _():
            first = chip * part % 128
            number = 0
            for target in (r.wqs, r.wus):
                for piece in range(target.shape[1] // part):
                    target[:, piece * part : (piece + 1) * part] = r.win[
                        number, :, first : first + part
                    ]
                    number += 1


VECTORS = ("gain1", "shift1", "gain2", "shift2", "bout", "bdown", "bqkv", "bup")


def pack_vectors(r):
    first = 0
    for name in VECTORS:
        values = wide(getattr(r, name)[...])
        count = values.shape[0]
        r.sm[0:1, first : first + count] = values.reshape(1, count)
        first += count


def read_vectors(r, me):
    nz, part = me.nz, r.vec.shape[1] // me.nz

    def piece(z, number):
        return r.sm4[z, 0:1, number * part : (number + 1) * part]

    for z in range(nz):
        span = slice(z * part, (z + 1) * part)
        for row in range(4):
            r.vec[row : row + 1, span] = piece(z, row)
        r.vec[4:5, span] = piece(z, 4) + piece(z, 5)
    chips = nz
    for chip in range(chips):

        @pl.when(me.t == chip)
        def _():
            for number in range(3):
                held = number * chips + chip
                r.vec[5:6, number * part : (number + 1) * part] = piece(held // 3, 6 + held % 3)
            for z in range(nz):
                r.vec[6:7, z * part : (z + 1) * part] = piece(z, 9 + chip)


def block_table(r, me):
    count = r.order.shape[0]
    chips, quarter = me.nz, count // 4
    sides = count // (2 * chips)
    held = [r.order[number] for number in range(count)]
    for position in range(count):
        found = 0
        for number in range(1, count):
            found = jnp.where(held[number] == position, number, found)
        r.idx[position] = found
    for chip in range(chips):
        for holder, first in ((me.k, count), (1 - me.k, count + chips * sides)):
            for side in range(sides):
                position = r.order[(2 * chip + me.k) * sides + side]
                low = (position >= quarter * holder) & (position < quarter * (holder + 1))
                near = position - quarter * holder
                high = position - 2 * quarter + quarter * holder
                r.idx[first + chip * sides + side] = jnp.clip(
                    jnp.where(low, near, high), 0, 2 * quarter - 1
                )
        position = r.order[(2 * chip + me.k) * sides]
        outer = jnp.where((position < quarter) | (position >= 3 * quarter), 0, 1)
        r.idx[count + 2 * chips * sides + chip] = jnp.where(outer == me.k, 1, 0)


def sorted_rows(r, source, block, blocks):
    pieces = []
    for number in range(blocks):
        pieces.append(source[r.idx[block + number]])
    return jnp.concatenate(pieces, axis=0)


def flat_rows(values):
    return values.reshape(-1, values.shape[-1])


def put_blocks(target, tile, values):
    blocks = values.shape[0] // BLK
    target[pl.ds(tile * blocks, blocks)] = values.reshape(blocks, BLK, values.shape[1])


def prepare(r, chip, target, at):
    sides = r.h.shape[0]
    rows = sides * BLK

    @pl.loop(0, 2)
    def _(core):
        values = flat_rows(r.hall[pl.ds((2 * chip + core) * sides, sides)])
        standardized, _ = norm_rows(wide(values))
        place = pl.ds(pl.multiple_of(at + core * rows, rows), rows)
        target[place, :] = narrow(standardized * r.vec[0:1, :] + r.vec[1:2, :])


def project(r, chip, source, at):
    part = r.wqs.shape[1] // 3
    blocks = 2 * r.h.shape[0]
    first = chip * blocks
    weight = r.wq4[...].reshape(-1, 3 * part)
    projected = mm(source[at : at + blocks * BLK, :], weight) + r.vec[5:6, : 3 * part]
    positions = [r.order[first + number] for number in range(blocks)]
    turned = turn(projected[:, : 2 * part], rope_lanes(r, positions, 2 * part, False))
    keys, values = turned[:, part:], projected[:, 2 * part :]
    query = narrow(wide(narrow(turned[:, :part])) * HD**-0.5)
    for number in range(blocks):
        own = slice(number * BLK, (number + 1) * BLK)
        r.q[first + number] = query[own]
        r.k[first + number] = narrow(keys[own])
        r.v[first + number] = narrow(values[own])
        r.kt[first + number] = narrow(keys[own].T)
        r.vt[first + number] = narrow(values[own].T)


def sorted_columns(r, source, head, block, blocks):
    lanes = slice(head * HD, (head + 1) * HD)
    return jnp.concatenate(
        [source[r.idx[block + number], lanes, :] for number in range(blocks)], axis=1
    )


def tile_start(r, me, tile):
    quarter = r.k.shape[0] * BLK // 4
    low = tile < quarter // QTILE
    inside = tile * QTILE - jnp.where(low, 0, quarter)
    return jnp.where(low, quarter * me.k, 3 * quarter - quarter * me.k) + inside


def attend(r, me, tile):
    part = r.k.shape[2]
    blocks = QTILE // BLK
    heads = part // HD
    start = tile_start(r, me, tile)
    rows = slice(tile * QTILE, (tile + 1) * QTILE)
    query = sorted_rows(r, r.q, start // BLK, blocks)
    per_head = [head_rows(query, head) for head in range(heads)]

    def visit(number, state, masked):
        keys = sorted_rows(r, r.k, number * blocks, blocks)
        result = []
        for head in range(heads):
            top, total, acc = state[head]
            logits = mm(keys, per_head[head], NT)
            if masked:
                key_row = lax.broadcasted_iota(jnp.int32, logits.shape, 0)
                query_row = lax.broadcasted_iota(jnp.int32, logits.shape, 1)
                logits = jnp.where(key_row <= query_row, logits, NEG)
            new_top = jnp.maximum(top, jnp.max(logits, axis=0, keepdims=True))
            fade = jnp.exp(top - new_top)
            probs = jnp.exp(logits - new_top)
            total = total * fade + jnp.sum(probs, axis=0, keepdims=True)
            values = sorted_columns(r, r.vt, head, number * blocks, blocks)
            acc = acc * fade + mm(values, narrow(probs))
            result.append((new_top, total, acc))
        return tuple(result)

    state = tuple(
        (
            jnp.full((1, QTILE), NEG, jnp.float32),
            jnp.zeros((1, QTILE), jnp.float32),
            jnp.zeros((HD, QTILE), jnp.float32),
        )
        for _ in range(heads)
    )
    last = start // QTILE
    state = lax.fori_loop(0, last, lambda n, s: visit(n, s, False), state)
    state = visit(last, state, True)
    merged = jnp.concatenate([acc / total for _, total, acc in state], axis=0)
    r.att[rows, :] = narrow(merged.T)
    r.attt[:, rows] = narrow(merged)
    for head in range(heads):
        r.lse[head : head + 1, rows] = state[head][0] + jnp.log(state[head][1])


def feed_forward(r, me, tile):
    place = pl.ds(pl.multiple_of(tile * QTILE, QTILE), QTILE)
    blocks = QTILE // BLK
    block = tile_start(r, me, tile) // BLK
    width = r.hall.shape[2]
    standardized, _ = norm_rows(wide(sorted_rows(r, r.hall, block, blocks)))
    cotan = sorted_rows(r, r.gall, block, blocks)
    gain2 = r.vec[2:3, :]
    normed = narrow(standardized * gain2 + r.vec[3:4, :])
    up_weight = r.wu4[...].reshape(width, -1)
    down_weight = r.wd4[...].reshape(-1, width)
    up = mm(normed, up_weight) + r.vec[6:7, :]
    below = 0.5 * (1.0 + lax.erf(up * SQRT_HALF))
    act = narrow(up * below)
    slope = below + up * jnp.exp(-0.5 * up * up) * INV_ROOT_TWO_PI
    d_up = mm(cotan, down_weight, NT) * slope
    d_up16 = narrow(d_up)
    put_blocks(r.outb, tile, narrow(mm(act, down_weight)))
    d_normed = mm(d_up16, up_weight, NT)
    r.sums[2:3, :] += jnp.sum(d_normed * standardized, axis=0, keepdims=True)
    r.sums[3:4, :] += jnp.sum(d_normed, axis=0, keepdims=True)
    r.sums[6:7, :] += jnp.sum(d_up, axis=0, keepdims=True)
    r.e2[place, :] = d_normed * gain2
    r.n[place, :] = normed
    r.gl[place, :] = cotan
    r.act[place, :] = act
    r.du[place, :] = d_up16


def out_project(r, me, tile):
    place = pl.ds(pl.multiple_of(tile * QTILE, QTILE), QTILE)
    blocks = QTILE // BLK
    attended = r.att[place, :]
    mlp = flat_rows(r.outb[pl.ds(tile * blocks, blocks)])
    put_blocks(r.outb, tile, narrow(wide(mlp) + mm(attended, r.wo1[...])))
    cotan = r.gl[place, :]
    r.datt[place, :] = narrow(mm(cotan, r.wo1[...], NT))
    product = wide(narrow(mm(r.wo1[...], cotan, NT))) * wide(r.attt[:, place])
    for head in range(product.shape[0] // HD):
        r.delta[head : head + 1, place] = jnp.sum(
            product[head * HD : (head + 1) * HD], axis=0, keepdims=True
        )


def weight_grad(target, left, right):
    rows, columns = left.shape[1], right.shape[1]
    shard = target.shape[1]
    values = right[...]
    for first in range(0, rows, QTILE):
        result = narrow(mm(left[:, first : first + QTILE], values, TN))
        at = first
        while at < first + QTILE:
            owner, inside = at // shard, at % shard
            until = min((owner + 1) * shard, first + QTILE)
            target[owner, inside : inside + until - at, :] = result[at - first : until - first, :]
            at = until


def attend_grad(r, me, tile):
    part = r.k.shape[2]
    heads = part // HD
    kstep = 2 * QTILE
    start = tile_start(r, me, tile)
    rows = slice(tile * QTILE, (tile + 1) * QTILE)
    blocks = kstep // BLK
    query = sorted_rows(r, r.q, start // BLK, QTILE // BLK)
    d_out = r.datt[rows, :]
    queries = jnp.concatenate([head_rows(query, head) for head in range(heads)], axis=0)
    d_outs = jnp.concatenate([head_rows(d_out, head) for head in range(heads)], axis=0)

    def visit(number, state, masked):
        place = pl.ds(pl.multiple_of(number * kstep, kstep), kstep)
        keys = sorted_rows(r, r.k, number * blocks, blocks)
        values = sorted_rows(r, r.v, number * blocks, blocks)
        probs_all, d_logits_all, result = [], [], []
        for head in range(heads):
            own = slice(head * QTILE, (head + 1) * QTILE)
            logits = mm(keys, queries[own], NT)
            probs = jnp.exp(logits - r.lse[head : head + 1, rows])
            if masked:
                key_row = number * kstep + lax.broadcasted_iota(jnp.int32, logits.shape, 0)
                query_row = start + lax.broadcasted_iota(jnp.int32, logits.shape, 1)
                probs = jnp.where(key_row <= query_row, probs, 0.0)
            d_probs = mm(values, d_outs[own], NT)
            d_logits = narrow(probs * (d_probs - r.delta[head : head + 1, rows]))
            probs_all.append(narrow(probs))
            d_logits_all.append(d_logits)
            columns = sorted_columns(r, r.kt, head, number * blocks, blocks)
            result.append(state[head] + mm(columns, d_logits))
        r.dv[place, :] += mm(jnp.concatenate(probs_all, axis=1), d_outs)
        r.dk[place, :] += mm(jnp.concatenate(d_logits_all, axis=1), queries)
        return tuple(result)

    state = tuple(jnp.zeros((HD, QTILE), jnp.float32) for _ in range(heads))
    last = start // kstep
    state = lax.fori_loop(0, last, lambda n, s: visit(n, s, False), state)
    state = visit(last, state, True)
    r.dqt[:, rows] = jnp.concatenate(state, axis=0)


def qkv_grad(r, me, tile):
    place = pl.ds(pl.multiple_of(tile * QTILE, QTILE), QTILE)
    part = r.k.shape[2]
    blocks = QTILE // BLK
    start = tile_start(r, me, tile)
    block = start // BLK
    held = pl.ds(pl.multiple_of(start, QTILE), QTILE)
    standardized, _ = norm_rows(wide(sorted_rows(r, r.hall, block, blocks)))
    gain1 = r.vec[0:1, :]
    r.n[place, :] = narrow(standardized * gain1 + r.vec[1:2, :])
    d_query = r.dqt[:, place].T * HD**-0.5
    d_key = r.dk[held, :] + wide(r.kvin[place, :part])
    d_value = r.dv[held, :] + wide(r.kvin[place, part:])
    turned = turn(
        jnp.concatenate([d_query, d_key], axis=1),
        rope_lanes(r, [block + n for n in range(blocks)], 2 * part, True),
    )
    d_qkv = jnp.concatenate([turned, d_value], axis=1)
    d_qkv16 = narrow(d_qkv)
    r.du[place, : 3 * part] = d_qkv16
    r.sums[5:6, : 3 * part] += jnp.sum(d_qkv, axis=0, keepdims=True)
    weight = r.wq4[...].reshape(-1, 3 * part)
    d_normed = mm(d_qkv16, weight, NT)
    r.sums[0:1, :] += jnp.sum(d_normed * standardized, axis=0, keepdims=True)
    r.sums[1:2, :] += jnp.sum(d_normed, axis=0, keepdims=True)
    put_blocks(r.outb, tile, narrow(d_normed * gain1 + r.e2[place, :]))


def gather_sums(r, me):
    nz, part = me.nz, r.vec.shape[1] // me.nz
    r.sums[4:5, :] = jnp.sum(wide(flat_rows(r.gown[...])), axis=0, keepdims=True)

    def put(z, number, values):
        r.vout[z, 0:1, number * part : (number + 1) * part] = values

    for z in range(nz):
        for row in range(5):
            put(z, row, r.sums[row : row + 1, z * part : (z + 1) * part])
    for chip in range(nz):

        @pl.when(me.t == chip)
        def _():
            for number in range(3):
                held = number * nz + chip
                put(held // 3, 5 + held % 3, r.sums[5:6, number * part : (number + 1) * part])
            for z in range(nz):
                put(z, 8 + chip, r.sums[6:7, z * part : (z + 1) * part])


class Scatter:
    def __init__(self, copies, me, r, source, theirs, got, landed):
        self.me, self.r, self.source, self.theirs, self.got, self.landed = me, r, source, theirs, got, landed
        self.chips = me.nz
        self.sides = got.shape[0] // self.chips
        self.first = r.k.shape[0]
        self.tiles = source.shape[0] * BLK // QTILE
        self.number = copies.count
        self.send_sems, self.recv_sems = copies.send_sems, copies.recv_sems
        self.exchanges = [
            copies.make(*self.rows(tile), me.on_plane(me.pn)) for tile in range(self.tiles)
        ]
        self.steps = []
        for side, near, far, to_near, to_far in (
            (0, me.tx, me.ty, me.xn, me.yn),
            (1, me.ty, me.tx, me.yn, me.xn),
        ):
            first, last = self.place(near, side), self.place(far, side)
            self.steps.append(
                (
                    copies.make(got.at[self.place(me.td, side)], landed.at[3 * side], me.on_plane(to_near)),
                    copies.make(got.at[first], landed.at[3 * side + 1], me.on_plane(to_near)),
                    copies.make(got.at[last], landed.at[3 * side + 2], me.on_plane(to_far)),
                    last,
                )
            )

    def place(self, chip, side):
        return chip * self.sides + side

    def rows(self, tile):
        blocks = QTILE // BLK
        place = pl.ds(tile * blocks, blocks)
        return self.source.at[place], self.theirs.at[place]

    def exchange(self, tile):
        source, target = self.rows(tile)
        pltpu.make_async_remote_copy(
            src_ref=source,
            dst_ref=target,
            send_sem=self.send_sems.at[self.number + tile],
            recv_sem=self.recv_sems.at[self.number + tile],
            device_id=self.me.on_plane(self.me.pn),
            device_id_type=MESH_IDS,
        ).start()

    def spread(self):
        count = self.chips * self.sides
        for exchange in self.exchanges:
            exchange.wait_recv()
        for number in range(count):
            flag = self.r.idx[self.first + 2 * count + number // self.sides]
            own = wide(self.source[self.r.idx[self.first + number]])
            other = wide(self.theirs[self.r.idx[self.first + count + number]])
            here = jnp.full(own.shape, flag, jnp.int32) > 0
            self.got[number] = narrow(jnp.where(here, own, other))
        for far, _, _, _ in self.steps:
            far.start()
        for _, near, _, _ in self.steps:
            near.start()

    def middle(self):
        for side, (far, _, on, last) in enumerate(self.steps):
            far.wait_recv()
            self.got[last] = narrow(wide(self.got[last]) + wide(self.landed[3 * side]))
            on.start()

    def total(self):
        pieces = []
        for side, (_, near, on, _) in enumerate(self.steps):
            near.wait_recv()
            on.wait_recv()
            pieces.append(
                wide(self.got[self.place(self.me.t, side)])
                + wide(self.landed[3 * side + 1])
                + wide(self.landed[3 * side + 2])
            )
        return jnp.concatenate(pieces, axis=0)


def layer_kernel(nz, names, *refs):
    r = types.SimpleNamespace(**dict(zip(names, refs)))
    me = Place(nz)
    copies = Copies(r.send_sems, r.recv_sems)
    sides = r.h.shape[0]
    shard = r.wqs.shape[0]
    tiles = r.att.shape[0] // QTILE

    kept = []

    def keep(source, target):
        copy = pltpu.make_async_copy(source, target, r.local_sems.at[len(kept)])
        copy.start()
        kept.append(copy)
        return copy

    own_rows = pl.ds(me.c * sides, sides)
    loads = windows(r, me)
    for copy in loads:
        copy.start()
    h_own = keep(r.h, r.hall.at[own_rows])
    keep(r.g, r.gall.at[own_rows])
    keep(r.g, r.gown)
    own_down = keep(r.wdown.at[pl.ds(me.t * shard, shard)], r.wd4.at[me.z])
    pack_vectors(r)
    me.greet()

    def row_slot(array):
        return lambda core, chip: array.at[pl.ds((2 * chip + core) * sides, sides)]

    h_share = PlaneShare(copies, me, r.h, row_slot(r.hall), sides)
    g_share = PlaneShare(copies, me, r.g, row_slot(r.gall), sides)
    wq = LineSend(copies, me, r.wqs, r.wq4)
    wu = LineGather(copies, me, r.wus, r.wu4)
    wd = LineGather(copies, me, r.wdown.at[pl.ds(me.t * shard, shard)], r.wd4)
    wo = LineSpread(copies, me, r.wout, r.wo1, r.window_sems.at[len(loads)])
    small = [copies.make(r.sm, r.sm4.at[me.z], me.on_line(other)) for other in me.others]

    for copy in small:
        copy.start()
    h_share.start()
    for copy in loads:
        copy.wait()
    slice_weights(r, me)
    r.wq4[me.z] = r.wqs[...]
    r.wu4[me.z] = r.wus[...]
    wq.start()
    wu.start()
    wd.start()
    r.sm4[me.z] = r.sm[...]
    block_table(r, me)
    r.sums[...] = jnp.zeros_like(r.sums)
    r.vout[...] = jnp.zeros_like(r.vout)
    r.dk[...] = jnp.zeros_like(r.dk)
    r.dv[...] = jnp.zeros_like(r.dv)
    for copy in small:
        copy.wait_recv()
    read_vectors(r, me)
    h_own.wait()
    h_share.to_p.wait_recv()
    pair = 2 * sides * BLK
    prepare(r, me.t, r.n, 0)
    h_share.relay()
    h_share.swap()
    g_share.start()
    h_share.swaps[0].wait_recv()
    prepare(r, me.tx, r.n, pair)
    h_share.swaps[1].wait_recv()
    wq.advance()
    prepare(r, me.ty, r.gl, 0)
    wq.finish()
    project(r, me.t, r.n, 0)
    wu.advance(0)
    h_share.on_diagonal()
    project(r, me.tx, r.n, pair)
    wd.advance(0)
    project(r, me.ty, r.gl, 0)
    g_share.relay()
    wu.advance(1)
    h_share.swaps[2].wait_recv()
    prepare(r, me.td, r.gl, pair)
    project(r, me.td, r.gl, pair)
    attend(r, me, 1)
    wd.advance(1)
    g_share.swap()
    attend(r, me, 2)
    wu.advance(2)
    g_share.on_diagonal()
    attend(r, me, 0)
    wd.advance(2)
    wo.start()
    for copy in kept[1:]:
        copy.wait()
    settled = len(kept)
    wu.finish()
    wd.finish()
    g_share.finish()

    @pl.loop(0, tiles)
    def _(tile):
        feed_forward(r, me, tile)

    half = shard // 2
    out_scatter = Scatter(copies, me, r, r.outb, r.otheirs, r.ogot, r.oland)
    up_reduce = LineReduce(copies, me, r.gu, r.tu, r.uu)
    down_reduce = LineReduce(copies, me, r.gd, r.td, r.ud)
    out_reduce = LineCollect(copies, me, r.go, r.to, r.uo)
    d_share = PlaneShare(copies, me, r.td.at[me.z], lambda core, chip: r.fd.at[core, chip], half)
    u_share = PlaneShare(copies, me, r.tu.at[me.z], lambda core, chip: r.fu.at[core, chip], half)
    o_spread = PlaneSpread(copies, me, r.to, r.fo, half, r.window_sems.at[len(loads) + 1])

    def share_down():
        d_share.start()
        keep(r.td.at[me.z], r.fd.at[me.k, me.t])

    def share_up():
        u_share.start()
        keep(r.tu.at[me.z], r.fu.at[me.k, me.t])

    weight_grad(r.gd, r.act, r.gl)
    down_reduce.start()
    weight_grad(r.gu, r.n, r.du)
    up_reduce.start()
    wo.advance()
    down_reduce.pair()
    attend(r, me, 3)
    up_reduce.pair()
    wo.finish()

    @pl.loop(0, tiles)
    def _(tile):
        out_project(r, me, tile)
        pl.when(tile > 0)(functools.partial(out_scatter.exchange, tile - 1))

    out_scatter.exchange(tiles - 1)
    r.go[...] = narrow(mm(r.att[...], r.gl[...], TN))
    out_reduce.start()
    attend_grad(r, me, 0)
    out_reduce.pair()
    out_scatter.spread()
    attend_grad(r, me, 3)
    out_scatter.middle()
    attend_grad(r, me, 2)
    down_reduce.collect()
    share_down()
    copies.settle([g_share.hop_x, g_share.hop_y, *g_share.swaps])
    copies.settle(out_scatter.exchanges)

    part = r.k.shape[2]
    quarter = r.k.shape[0] * BLK // 4

    def send_keys(number):
        first = quarter * (1 - me.k) if number == 0 else 3 * quarter - quarter * (1 - me.k)
        theirs = pl.ds(pl.multiple_of(first, quarter), quarter)
        rows = slice(number * quarter, (number + 1) * quarter)
        r.act[rows, :part] = narrow(r.dk[theirs, :])
        r.act[rows, part : 2 * part] = narrow(r.dv[theirs, :])
        copy = copies.make(r.act.at[rows, : 2 * part], r.kvin.at[rows], me.on_plane(me.pn))
        copy.start()
        return copy

    later = send_keys(1)
    attend_grad(r, me, 1)
    sooner = send_keys(0)
    d_share.relay()
    later.wait_recv()
    e_scatter = Scatter(
        copies, me, r, r.outb, r.gall.at[: r.outb.shape[0]], r.gall.at[r.outb.shape[0] :], r.eland
    )

    @pl.loop(0, tiles)
    def _(number):
        pl.when(number == tiles // 2)(sooner.wait_recv)
        qkv_grad(r, me, (number + tiles // 2) % tiles)
        pl.when(number > 0)(
            functools.partial(e_scatter.exchange, (number + tiles // 2 - 1) % tiles)
        )

    up_reduce.collect()
    share_up()
    gather_sums(r, me)
    e_scatter.exchange(tiles // 2 - 1)
    vec_line = [
        copies.make(r.vout.at[other], r.vline.at[me.z], me.on_line(other)) for other in me.others
    ]
    for copy in vec_line:
        copy.start()
    d_share.swap()
    weight_grad(r.gq, r.n, r.du.at[:, : 3 * part])
    qkv_reduce = LineReduce(copies, me, r.gq, r.tq, r.uq)
    qkv_reduce.start()
    e_scatter.spread()
    qkv_reduce.pair()
    u_share.relay()
    out_reduce.collect()
    o_spread.start()
    d_share.on_diagonal()
    u_share.swap()
    e_scatter.middle()
    for copy in vec_line:
        copy.wait_recv()
    vector = r.vout[me.z]
    for other in me.others:
        vector = vector + r.vline[other]
    r.vsend[...] = vector
    vec_plane = [copies.make(r.vsend, r.vplane.at[me.c], me.on_plane(peer)) for peer in me.plane]
    for copy in vec_plane:
        copy.start()
    qkv_reduce.collect()
    q_share = PlaneShare(copies, me, r.tq.at[me.z], lambda core, chip: r.fq.at[core, chip], half)
    q_share.start()
    keep(r.tq.at[me.z], r.fq.at[me.k, me.t])

    residual = wide(flat_rows(r.hall[own_rows]))
    own_standardized, own_deviation = norm_rows(residual)
    rows = sides * BLK
    r.n[:rows, :] = narrow(residual + r.vec[4:5, :] + out_scatter.total())
    keep(r.n.at[:rows], r.hidden_out)
    o_spread.advance()
    u_share.on_diagonal()
    q_share.relay()
    e_total = e_scatter.total()
    r.e2[:rows, :] = wide(flat_rows(r.gown[...])) + own_deviation * (
        e_total
        - jnp.mean(e_total, axis=-1, keepdims=True)
        - own_standardized * jnp.mean(e_total * own_standardized, axis=-1, keepdims=True)
    )
    keep(r.e2.at[:rows], r.hidden_grad)
    q_share.swap()
    o_spread.on_diagonal()
    for copy in vec_plane:
        copy.wait_recv()
    vector = r.vsend[...]
    for peer in me.plane:
        vector = vector + r.vplane[peer]
    r.vlast[...] = vector
    keep(r.vlast, r.vsum)
    q_share.on_diagonal()
    for share in (d_share, u_share, o_spread, q_share):
        share.finish()
    for copy in kept[settled:]:
        copy.wait()
    copies.finish()


def assemble_kernel(
    fq_ref, fu_ref, fd_ref, fo_ref, out_ref, grad_ref, vsum_ref,
    gq_ref, gu_ref, gd_ref, go_ref, hidden_out_ref, hidden_grad_ref, *vector_refs,
):
    _, chips, _, _ = fq_ref.shape
    part = fq_ref.shape[3] // 3
    hidden_out_ref[...] = out_ref[...]
    hidden_grad_ref[...] = grad_ref[...]
    go_ref[...] = wide(fo_ref[0])
    for chip in range(chips):
        for source, target in ((fq_ref, gq_ref), (fu_ref, gu_ref)):
            for piece in range(source.shape[3] // part):
                first = (piece * chips + chip) * part
                target[:, first : first + part] = wide(
                    source[0, chip, :, piece * part : (piece + 1) * part]
                )
        gd_ref[chip, 0] = wide(fd_ref[0, chip])

    @pl.when(pl.program_id(0) == 0)
    def _():
        first = 0
        for number, target in enumerate(vector_refs):
            count = target.shape[0]
            if number == 5:
                first -= count
            target[...] = vsum_ref[0:1, first : first + count].reshape(count)
            first += count


def rotary_parts(block_count):
    half_rot = ROT // 2
    lane = np.arange(128) % HD
    rate = np.where(lane < ROT, 10000.0 ** (-2.0 * (lane % half_rot) / ROT), 0.0)

    def table(places):
        angle = places[:, None].astype(np.float64) * rate[None, :]
        return np.concatenate([np.cos(angle), np.sin(angle)], axis=1).astype(np.float32)

    return table(np.arange(BLK)), table(np.arange(block_count) * BLK)


VMEM_SPEC = pl.BlockSpec(memory_space=pltpu.VMEM)
SPECS = {
    "order": pl.BlockSpec(memory_space=pltpu.SMEM),
    **{
        name: pl.BlockSpec(memory_space=pl.ANY)
        for name in ("h", "g", "wqkv", "wup", "wdown", "wout")
        + ("hidden_out", "hidden_grad", "fq", "fu", "fd", "fo", "vsum")
    },
}
VMEM_LIMIT = 63 * 1024 * 1024


def sliced_layer(
    nz,
    hidden_in,
    norm1_gain,
    attention_norm_bias,
    qkv_weight,
    qkv_bias,
    out_weight,
    out_bias,
    norm2_gain,
    feedforward_norm_bias,
    up_weight,
    up_bias,
    down_weight,
    down_bias,
    cotangent,
    block_order,
):
    f32, b16 = jnp.float32, jnp.bfloat16
    h, g = hidden_in[0], cotangent[0]
    local_rows, width = h.shape
    chips = lax.axis_size("ctx") // 2
    shard = qkv_weight.shape[0]
    half = shard // 2
    part = width // chips
    hidden = up_weight.shape[1] // chips
    rows = chips * local_rows
    everyone = 2 * rows
    sides = local_rows // BLK

    sums = 5 * shard + qkv_bias.shape[0] + up_bias.shape[0]
    slices = 3 + hidden // part
    columns = max(-(-(chip * part % 128 + part) // 128) * 128 for chip in range(chips))
    small = 6 * shard + qkv_bias.shape[0] + up_bias.shape[0]
    rope_r, rope_b = rotary_parts(everyone // BLK)

    inputs = {
        "order": block_order,
        "h": h.reshape(sides, BLK, width),
        "g": g.reshape(sides, BLK, width),
        "wqkv": qkv_weight,
        "wup": up_weight,
        "wdown": down_weight,
        "wout": out_weight,
        **dict(
            zip(
                VECTORS,
                (norm1_gain, attention_norm_bias, norm2_gain, feedforward_norm_bias)
                + (out_bias, down_bias, qkv_bias, up_bias),
            )
        ),
        "rope_r": jnp.asarray(rope_r),
        "rope_b": jnp.asarray(rope_b[:, None, :]),
    }
    outputs = {
        "hidden_out": ((local_rows, width), b16),
        "hidden_grad": ((local_rows, width), f32),
        "fq": ((2, chips, half, 3 * part), b16),
        "fu": ((2, chips, half, hidden), b16),
        "fd": ((2, chips, half, width), b16),
        "fo": ((2, half, width), b16),
        "vsum": ((1, sums), f32),
    }
    scratch = {
        "hall": ((everyone // BLK, BLK, width), b16),
        "gall": ((everyone // BLK, BLK, width), b16),
        "wqs": ((shard, 3 * part), b16),
        "wus": ((shard, hidden), b16),
        "wq4": ((nz, shard, 3 * part), b16),
        "wu4": ((nz, shard, hidden), b16),
        "wd4": ((nz, shard, width), b16),
        "wo1": ((part, width), b16),
        "sm": ((1, small), f32),
        "sm4": ((nz, 1, small), f32),
        "vec": ((8, width), f32),
        "sums": ((8, width), f32),
        "q": ((everyone // BLK, BLK, part), b16),
        "k": ((everyone // BLK, BLK, part), b16),
        "v": ((everyone // BLK, BLK, part), b16),
        "kt": ((everyone // BLK, part, BLK), b16),
        "vt": ((everyone // BLK, part, BLK), b16),
        "att": ((rows, part), b16),
        "attt": ((part, rows), b16),
        "lse": ((8, rows), f32),
        "delta": ((8, rows), f32),
        "datt": ((rows, part), b16),
        "act": ((rows, hidden), b16),
        "du": ((rows, hidden), b16),
        "n": ((rows, width), b16),
        "gl": ((rows, width), b16),
        "outb": ((rows // BLK, BLK, width), b16),
        "e2": ((rows, width), f32),
        "dk": ((everyone, part), f32),
        "dv": ((everyone, part), f32),
        "dqt": ((part, rows), f32),
        "kvin": ((rows, 2 * part), b16),
        "otheirs": ((rows // BLK, BLK, width), b16),
        "ogot": ((rows // BLK, BLK, width), b16),
        "oland": ((6, BLK, width), b16),
        "eland": ((6, BLK, width), b16),
        "gq": ((nz, shard, 3 * part), b16),
        "gu": ((nz, shard, hidden), b16),
        "gd": ((nz, shard, width), b16),
        "go": ((part, width), b16),
        "tq": ((nz, half, 3 * part), b16),
        "uq": ((nz, half, 3 * part), b16),
        "tu": ((nz, half, hidden), b16),
        "uu": ((nz, half, hidden), b16),
        "td": ((nz, half, width), b16),
        "ud": ((nz, half, width), b16),
        "to": ((half, width), b16),
        "uo": ((nz, half, width), b16),
        "vout": ((nz, 1, sums), f32),
        "vline": ((nz, 1, sums), f32),
        "vsend": ((1, sums), f32),
        "vlast": ((1, sums), f32),
        "gown": ((sides, BLK, width), b16),
        "win": ((slices, shard, columns), b16),
        "vplane": ((2 * chips, 1, sums), f32),
    }
    names = [*inputs, *outputs, *scratch, "idx", "send_sems", "recv_sems", "local_sems", "window_sems"]
    results = pl.pallas_call(
        functools.partial(layer_kernel, nz, names),
        out_shape=tuple(jax.ShapeDtypeStruct(*leaf) for leaf in outputs.values()),
        in_specs=[SPECS.get(name, VMEM_SPEC) for name in inputs],
        out_specs=tuple(SPECS.get(name, VMEM_SPEC) for name in outputs),
        scratch_shapes=[pltpu.VMEM(*leaf) for leaf in scratch.values()]
        + [pltpu.SMEM((64,), jnp.int32)]
        + [pltpu.SemaphoreType.DMA((SEMAPHORES,))] * 2
        + [pltpu.SemaphoreType.DMA((16,))] * 2,
        compiler_params=pltpu.CompilerParams(
            collective_id=0, has_side_effects=True, vmem_limit_bytes=VMEM_LIMIT
        ),
        name="layer",
    )(*inputs.values())
    hidden_out, hidden_grad, fq, fu, fd, fo, vsum = results

    steps = 2
    some, few = shard // steps, local_rows // steps
    inner = half // some

    def pieces(cols):
        return pl.BlockSpec((1, chips, some, cols), lambda i: (i // inner, 0, i % inner, 0))

    def lines(count, cols):
        return pl.BlockSpec((count, cols), lambda i: (i, 0))

    def vector(count):
        return pl.BlockSpec((count,), lambda i: (0,))

    sizes = [shard] * 6 + [qkv_bias.shape[0], up_bias.shape[0]]
    grad_qkv, grad_up, grad_down, grad_out, hidden_out, hidden_grad, *vectors = pl.pallas_call(
        assemble_kernel,
        grid=(steps,),
        out_shape=(
            jax.ShapeDtypeStruct(qkv_weight.shape, f32),
            jax.ShapeDtypeStruct(up_weight.shape, f32),
            jax.ShapeDtypeStruct((chips, steps, some, width), f32),
            jax.ShapeDtypeStruct(out_weight.shape, f32),
            jax.ShapeDtypeStruct(h.shape, b16),
            jax.ShapeDtypeStruct(h.shape, f32),
        )
        + tuple(jax.ShapeDtypeStruct((size,), f32) for size in sizes),
        in_specs=[
            pieces(3 * part),
            pieces(hidden),
            pieces(width),
            pl.BlockSpec((1, some, width), lambda i: (i // inner, i % inner, 0)),
            lines(few, width),
            lines(few, width),
            pl.BlockSpec((1, sums), lambda i: (0, 0)),
        ],
        out_specs=(
            lines(some, qkv_weight.shape[1]),
            lines(some, up_weight.shape[1]),
            pl.BlockSpec((chips, 1, some, width), lambda i: (0, i, 0, 0)),
            lines(some, width),
            lines(few, width),
            lines(few, width),
        )
        + tuple(vector(size) for size in sizes),
        compiler_params=pltpu.CompilerParams(vmem_limit_bytes=56 * 1024 * 1024),
        name="assemble",
    )(fq, fu, fd, fo, hidden_out, hidden_grad, vsum)
    g_gain1, g_shift1, g_gain2, g_shift2, g_bout, g_bdown, g_bqkv, g_bup = vectors
    return (
        hidden_out[None],
        hidden_grad[None],
        g_gain1,
        g_shift1,
        grad_qkv,
        g_bqkv,
        grad_out,
        g_bout,
        g_gain2,
        g_shift2,
        grad_up,
        g_bup,
        grad_down.reshape(down_weight.shape),
        g_bdown,
    )


def sliced_fits(mesh):
    return mesh.shape["ctx"] == 8 and mesh.shape["fsdp"] == 4


def solution(mesh):
    in_specs = (
        P("fsdp", "ctx", None),
        P("fsdp"),
        P("fsdp"),
        P("fsdp", None),
        P("fsdp"),
        P("fsdp", None),
        P("fsdp"),
        P("fsdp"),
        P("fsdp"),
        P("fsdp", None),
        P("fsdp"),
        P("fsdp", None),
        P("fsdp"),
        P("fsdp", "ctx", None),
        P(),
    )
    out_specs = (
        P("fsdp", "ctx", None),
        P("fsdp", "ctx", None),
        P("fsdp"),
        P("fsdp"),
        P("fsdp", None),
        P("fsdp"),
        P("fsdp", None),
        P("fsdp"),
        P("fsdp"),
        P("fsdp"),
        P("fsdp", None),
        P("fsdp"),
        P("fsdp", None),
        P("fsdp"),
    )
    local = whole_parameter_layer
    if sliced_fits(mesh):
        local = functools.partial(sliced_layer, mesh.shape["fsdp"])
    return jax.shard_map(local, mesh=mesh, in_specs=in_specs, out_specs=out_specs, check_vma=False)
```

```python
import functools
import math
import types

import jax
import jax.numpy as jnp
import numpy as np
from jax import lax
from jax.experimental import pallas as pl
from jax.experimental.pallas import tpu as pltpu
from jax.sharding import PartitionSpec as P

H = 12
HD = 64
ROT = 16
BLK = 128


EPS = 1e-05
NEG = -1e30
SQRT_HALF = 0.7071067811865476
INV_ROOT_TWO_PI = 0.3989422804014327


def apply_layer_norm(values_in, norm_gain, norm_bias):
    centre = jnp.mean(values_in, axis=-1, keepdims=True)
    mean_removed = values_in - centre
    inverse_deviation = lax.rsqrt(
        jnp.mean(mean_removed * mean_removed, axis=-1, keepdims=True) + EPS
    )
    standardized = mean_removed * inverse_deviation
    return (standardized * norm_gain + norm_bias, standardized, inverse_deviation)


def layer_norm_backward(output_gradient, standardized, inverse_deviation, norm_gain):
    gain_scaled = output_gradient * norm_gain
    return inverse_deviation * (
        gain_scaled
        - jnp.mean(gain_scaled, axis=-1, keepdims=True)
        - standardized * jnp.mean(gain_scaled * standardized, axis=-1, keepdims=True)
    )


def gelu_exact(values_in):
    return 0.5 * values_in * (1.0 + lax.erf(values_in * SQRT_HALF))


def gelu_slope(values_in):
    return (
        0.5 * (1.0 + lax.erf(values_in * SQRT_HALF))
        + values_in * jnp.exp(-0.5 * values_in * values_in) * INV_ROOT_TWO_PI
    )


def rotary_tables(position_list):
    half_rot = ROT // 2
    inverse = jnp.power(jnp.float32(10000.0), -2.0 * jnp.arange(half_rot, dtype=jnp.float32) / ROT)
    angle = position_list.astype(jnp.float32)[:, None] * inverse[None, :]
    return (jnp.cos(angle)[:, None, :], jnp.sin(angle)[:, None, :])


def rotate(tensor, cosine, sine):
    half_rot = ROT // 2
    first_half = tensor[..., :half_rot]
    second_half = tensor[..., half_rot:ROT]
    return jnp.concatenate(
        [
            first_half * cosine - second_half * sine,
            second_half * cosine + first_half * sine,
            tensor[..., ROT:],
        ],
        axis=-1,
    )


def rotate_back(tensor, cosine, sine):
    half_rot = ROT // 2
    first_half = tensor[..., :half_rot]
    second_half = tensor[..., half_rot:ROT]
    return jnp.concatenate(
        [
            first_half * cosine + second_half * sine,
            second_half * cosine - first_half * sine,
            tensor[..., ROT:],
        ],
        axis=-1,
    )


def masked_logits(query_block, key_block, query_pos, key_pos):
    logits = jnp.einsum(
        "qhd,khd->hqk", query_block, key_block, preferred_element_type=jnp.float32
    ) * (1.0 / math.sqrt(HD))
    return jnp.where(key_pos[None, None, :] <= query_pos[None, :, None], logits, NEG)


def block_terms(
    query_block, dout_block, total_t, delta_t, query_pos, key_block, value_block, key_pos
):
    logits = masked_logits(query_block, key_block, query_pos, key_pos)
    probs_wide = jnp.exp(logits - total_t[:, :, None])
    dprobs = jnp.einsum("qhd,khd->hqk", dout_block, value_block, preferred_element_type=jnp.float32)
    d_logits = (probs_wide * (dprobs - delta_t[:, :, None]) * (1.0 / math.sqrt(HD))).astype(
        jnp.bfloat16
    )
    return (probs_wide.astype(jnp.bfloat16), d_logits)


def keep_state(state_in):
    return state_in


def forward_attention(query, keys_all, values_all, own_pos, all_pos):
    local_rows = query.shape[0]
    seq_rows = keys_all.shape[0]
    qstep = min(512, local_rows)
    kstep = min(512, seq_rows)
    latest = jnp.max(own_pos)

    def stats_step(number, state_in):
        key_block = lax.dynamic_slice_in_dim(keys_all, number * kstep, kstep, 0)
        key_pos = lax.dynamic_slice_in_dim(all_pos, number * kstep, kstep, 0)

        def stats_live(state_now):
            running_max, running_sum = state_now
            logits = masked_logits(query, key_block, own_pos, key_pos)
            new_max = jnp.maximum(running_max, jnp.max(logits, axis=-1))
            running_sum = running_sum * jnp.exp(running_max - new_max) + jnp.sum(
                jnp.exp(logits - new_max[:, :, None]), axis=-1
            )
            return (new_max, running_sum)

        return lax.cond(jnp.min(key_pos) <= latest, stats_live, keep_state, state_in)

    start_state = (jnp.full((H, qstep), NEG, jnp.float32), jnp.zeros((H, qstep), jnp.float32))
    running_max, running_sum = lax.fori_loop(0, seq_rows // kstep, stats_step, start_state)
    total_t = running_max + jnp.log(running_sum)

    def value_step(number, state_in):
        key_block = lax.dynamic_slice_in_dim(keys_all, number * kstep, kstep, 0)
        value_block = lax.dynamic_slice_in_dim(values_all, number * kstep, kstep, 0)
        key_pos = lax.dynamic_slice_in_dim(all_pos, number * kstep, kstep, 0)

        def value_live(state_now):
            logits = masked_logits(query, key_block, own_pos, key_pos)
            attn_probs = jnp.exp(logits - total_t[:, :, None]).astype(jnp.bfloat16)
            return state_now + jnp.einsum(
                "hqk,khd->qhd", attn_probs, value_block, preferred_element_type=jnp.float32
            )

        return lax.cond(jnp.min(key_pos) <= latest, value_live, keep_state, state_in)

    weighted = lax.fori_loop(
        0, seq_rows // kstep, value_step, jnp.zeros((qstep, H, HD), jnp.float32)
    )
    totals = total_t.T
    return (weighted, totals)


def query_grads(query, d_att, log_total, delta, own_pos, keys_all, values_all, all_pos):
    local_rows = query.shape[0]
    seq_rows = keys_all.shape[0]
    qstep = min(512, local_rows)
    kstep = min(512, seq_rows)
    key_grads = jnp.zeros((seq_rows, H, HD), jnp.float32)
    value_grads = jnp.zeros((seq_rows, H, HD), jnp.float32)
    total_t = log_total.T
    delta_t = delta.T
    latest = jnp.max(own_pos)

    def key_step(number, state_in):
        offset = number * kstep
        key_block = lax.dynamic_slice_in_dim(keys_all, offset, kstep, 0)
        value_block = lax.dynamic_slice_in_dim(values_all, offset, kstep, 0)
        key_pos = lax.dynamic_slice_in_dim(all_pos, offset, kstep, 0)

        def key_live(state_now):
            attn_probs, d_logits = block_terms(
                query, d_att, total_t, delta_t, own_pos, key_block, value_block, key_pos
            )
            d_query = state_now[0] + jnp.einsum(
                "hqk,khd->qhd", d_logits, key_block, preferred_element_type=jnp.float32
            )
            key_acc = state_now[1]
            value_acc = state_now[2]
            key_part = jnp.einsum(
                "hqk,qhd->khd", d_logits, query, preferred_element_type=jnp.float32
            )
            value_part = jnp.einsum(
                "hqk,qhd->khd", attn_probs, d_att, preferred_element_type=jnp.float32
            )
            key_acc = lax.dynamic_update_slice_in_dim(
                key_acc, lax.dynamic_slice_in_dim(key_acc, offset, kstep, 0) + key_part, offset, 0
            )
            value_acc = lax.dynamic_update_slice_in_dim(
                value_acc,
                lax.dynamic_slice_in_dim(value_acc, offset, kstep, 0) + value_part,
                offset,
                0,
            )
            return (d_query, key_acc, value_acc)

        return lax.cond(jnp.min(key_pos) <= latest, key_live, keep_state, state_in)

    start_state = (jnp.zeros((qstep, H, HD), jnp.float32),) + (key_grads, value_grads)
    result = lax.fori_loop(0, seq_rows // kstep, key_step, start_state)
    pieces = result[0]
    key_grads = result[1]
    value_grads = result[2]
    return (pieces, key_grads, value_grads)


def whole_parameter_layer(
    hidden_in,
    norm1_gain,
    attention_norm_bias,
    qkv_weight,
    qkv_bias,
    out_weight,
    out_bias,
    norm2_gain,
    feedforward_norm_bias,
    up_weight,
    up_bias,
    down_weight,
    down_bias,
    cotangent,
    block_order,
):
    (
        attention_norm_gain,
        attention_bias_term,
        wqkv,
        bqkv,
        wout,
        bout,
        feedforward_norm_gain,
        feedforward_bias_term,
        wup,
        bup,
        wdown,
        bdown,
    ) = (
        lax.all_gather(norm1_gain, "fsdp", axis=0, tiled=True),
        lax.all_gather(attention_norm_bias, "fsdp", axis=0, tiled=True),
        lax.all_gather(qkv_weight, "fsdp", axis=0, tiled=True),
        lax.all_gather(qkv_bias, "fsdp", axis=0, tiled=True),
        lax.all_gather(out_weight, "fsdp", axis=0, tiled=True),
        lax.all_gather(out_bias, "fsdp", axis=0, tiled=True),
        lax.all_gather(norm2_gain, "fsdp", axis=0, tiled=True),
        lax.all_gather(feedforward_norm_bias, "fsdp", axis=0, tiled=True),
        lax.all_gather(up_weight, "fsdp", axis=0, tiled=True),
        lax.all_gather(up_bias, "fsdp", axis=0, tiled=True),
        lax.all_gather(down_weight, "fsdp", axis=0, tiled=True),
        lax.all_gather(down_bias, "fsdp", axis=0, tiled=True),
    )
    width = H * HD
    hidden_rows = hidden_in[0]
    cotan_rows = cotangent[0]
    local_rows = hidden_rows.shape[0]
    ctx_count = lax.axis_size("ctx")
    ctx_rank = lax.axis_index("ctx")
    seq_rows = local_rows * ctx_count
    all_pos = (block_order[:, None] * BLK + jnp.arange(BLK, dtype=jnp.int32)[None, :]).reshape(
        seq_rows
    )
    own_pos = lax.dynamic_slice_in_dim(all_pos, ctx_rank * local_rows, local_rows, 0)
    cosine, sine = rotary_tables(own_pos)
    attention_norm_gain = attention_norm_gain.astype(jnp.float32)
    feedforward_norm_gain = feedforward_norm_gain.astype(jnp.float32)
    residual_stream = hidden_rows.astype(jnp.float32)
    attention_normed, attention_standardized, attention_inverse_deviation = apply_layer_norm(
        residual_stream, attention_norm_gain, attention_bias_term.astype(jnp.float32)
    )
    normed1_b = attention_normed.astype(jnp.bfloat16)
    projected = jnp.dot(normed1_b, wqkv, preferred_element_type=jnp.float32) + bqkv.astype(
        jnp.float32
    )
    query = rotate(projected[:, :width].reshape(local_rows, H, HD), cosine, sine).astype(
        jnp.bfloat16
    )
    key_rows = rotate(
        projected[:, width : 2 * width].reshape(local_rows, H, HD), cosine, sine
    ).astype(jnp.bfloat16)
    value_rows = projected[:, 2 * width :].astype(jnp.bfloat16)
    keys_all, values_all = (
        lax.all_gather(key_rows.reshape(local_rows, width), "ctx", axis=0, tiled=True),
        lax.all_gather(value_rows, "ctx", axis=0, tiled=True),
    )
    keys_all = keys_all.reshape(seq_rows, H, HD)
    values_all = values_all.reshape(seq_rows, H, HD)
    attended, log_total = forward_attention(query, keys_all, values_all, own_pos, all_pos)
    attended_b = attended.reshape(local_rows, width).astype(jnp.bfloat16)
    attn_out = jnp.dot(attended_b, wout, preferred_element_type=jnp.float32) + bout.astype(
        jnp.float32
    )
    feedforward_normed, feedforward_standardized, feedforward_inverse_deviation = apply_layer_norm(
        residual_stream, feedforward_norm_gain, feedforward_bias_term.astype(jnp.float32)
    )
    normed2_b = feedforward_normed.astype(jnp.bfloat16)
    up_rows = jnp.dot(normed2_b, wup, preferred_element_type=jnp.float32) + bup.astype(jnp.float32)
    act_b = gelu_exact(up_rows).astype(jnp.bfloat16)
    mlp_out = jnp.dot(act_b, wdown, preferred_element_type=jnp.float32) + bdown.astype(jnp.float32)
    hidden_out = (residual_stream + attn_out + mlp_out).astype(jnp.bfloat16)
    cotan_wide = cotan_rows.astype(jnp.float32)
    grad_wdown = jnp.einsum("tk,tn->kn", act_b, cotan_rows, preferred_element_type=jnp.float32)
    grad_bdown = jnp.sum(cotan_wide, axis=0)
    d_up = jnp.einsum(
        "tn,kn->tk", cotan_rows, wdown, preferred_element_type=jnp.float32
    ) * gelu_slope(up_rows)
    d_up16 = d_up.astype(jnp.bfloat16)
    grad_wup = jnp.einsum("tk,tn->kn", normed2_b, d_up16, preferred_element_type=jnp.float32)
    grad_bup = jnp.sum(d_up, axis=0)
    grad_feedforward_normed = jnp.einsum(
        "tn,kn->tk", d_up16, wup, preferred_element_type=jnp.float32
    )
    grad_feedforward_gain = jnp.sum(grad_feedforward_normed * feedforward_standardized, axis=0)
    grad_shift2 = jnp.sum(grad_feedforward_normed, axis=0)
    feedforward_branch_grad = layer_norm_backward(
        grad_feedforward_normed,
        feedforward_standardized,
        feedforward_inverse_deviation,
        feedforward_norm_gain,
    )
    grad_wout = jnp.einsum("tk,tn->kn", attended_b, cotan_rows, preferred_element_type=jnp.float32)
    d_att = jnp.einsum("tn,kn->tk", cotan_rows, wout, preferred_element_type=jnp.float32).astype(
        jnp.bfloat16
    )
    delta = jnp.sum(
        d_att.reshape(local_rows, H, HD).astype(jnp.float32)
        * attended_b.reshape(local_rows, H, HD).astype(jnp.float32),
        axis=-1,
    )
    d_att3 = d_att.reshape(local_rows, H, HD)
    d_query, key_grads, value_grads = query_grads(
        query, d_att3, log_total, delta, own_pos, keys_all, values_all, all_pos
    )
    d_key, d_value = (
        lax.psum_scatter(
            key_grads.reshape(seq_rows, width), "ctx", scatter_dimension=0, tiled=True
        ),
        lax.psum_scatter(
            value_grads.reshape(seq_rows, width), "ctx", scatter_dimension=0, tiled=True
        ),
    )
    d_query = rotate_back(d_query, cosine, sine)
    d_key = rotate_back(d_key.reshape(local_rows, H, HD), cosine, sine)
    d_qkv = jnp.concatenate(
        [d_query.reshape(local_rows, width), d_key.reshape(local_rows, width), d_value], axis=1
    )
    d_qkv16 = d_qkv.astype(jnp.bfloat16)
    grad_wqkv = jnp.einsum("tk,tn->kn", normed1_b, d_qkv16, preferred_element_type=jnp.float32)
    grad_bqkv = jnp.sum(d_qkv, axis=0)
    grad_attention_normed = jnp.einsum(
        "tn,kn->tk", d_qkv16, wqkv, preferred_element_type=jnp.float32
    )
    grad_attention_gain = jnp.sum(grad_attention_normed * attention_standardized, axis=0)
    grad_shift1 = jnp.sum(grad_attention_normed, axis=0)
    attention_branch_grad = layer_norm_backward(
        grad_attention_normed,
        attention_standardized,
        attention_inverse_deviation,
        attention_norm_gain,
    )
    hidden_grad = cotan_wide + attention_branch_grad + feedforward_branch_grad
    terms = (
        grad_attention_gain,
        grad_shift1,
        grad_wqkv,
        grad_bqkv,
        grad_wout,
        grad_bdown,
        grad_feedforward_gain,
        grad_shift2,
        grad_wup,
        grad_bup,
        grad_wdown,
        grad_bdown,
    )
    shares = (
        lax.psum_scatter(terms[0], "fsdp", scatter_dimension=0, tiled=True),
        lax.psum_scatter(terms[1], "fsdp", scatter_dimension=0, tiled=True),
        lax.psum_scatter(terms[2], "fsdp", scatter_dimension=0, tiled=True),
        lax.psum_scatter(terms[3], "fsdp", scatter_dimension=0, tiled=True),
        lax.psum_scatter(terms[4], "fsdp", scatter_dimension=0, tiled=True),
        lax.psum_scatter(terms[5], "fsdp", scatter_dimension=0, tiled=True),
        lax.psum_scatter(terms[6], "fsdp", scatter_dimension=0, tiled=True),
        lax.psum_scatter(terms[7], "fsdp", scatter_dimension=0, tiled=True),
        lax.psum_scatter(terms[8], "fsdp", scatter_dimension=0, tiled=True),
        lax.psum_scatter(terms[9], "fsdp", scatter_dimension=0, tiled=True),
        lax.psum_scatter(terms[10], "fsdp", scatter_dimension=0, tiled=True),
        lax.psum_scatter(terms[11], "fsdp", scatter_dimension=0, tiled=True),
    )
    shares = lax.psum(
        (
            shares[0],
            shares[1],
            shares[2],
            shares[3],
            shares[4],
            shares[5],
            shares[6],
            shares[7],
            shares[8],
            shares[9],
            shares[10],
            shares[11],
        ),
        "ctx",
    )
    return (
        hidden_out[None],
        hidden_grad[None],
        shares[0],
        shares[1],
        shares[2],
        shares[3],
        shares[4],
        shares[5],
        shares[6],
        shares[7],
        shares[8],
        shares[9],
        shares[10],
        shares[11],
    )


MESH_IDS = pl.DeviceIdType.MESH
NN = (((1,), (0,)), ((), ()))
NT = (((1,), (1,)), ((), ()))
TN = (((0,), (0,)), ((), ()))
QTILE = 256
SEMAPHORES = 192


def mm(left, right, dims=NN):
    return lax.dot_general(left, right, dims, preferred_element_type=jnp.float32)


def flip(index, bit):
    return index + bit - 2 * bit * ((index // bit) % 2)


def run_when(condition, action):
    if condition is None:
        action()
    else:
        pl.when(condition)(action)


def narrow(values):
    return values.astype(jnp.bfloat16)


def wide(values):
    return values.astype(jnp.float32)


class Copies:
    def __init__(self, send_sems, recv_sems):
        self.send_sems, self.recv_sems = send_sems, recv_sems
        self.count, self.started, self.numbers = 0, [], {}

    def make(self, source, target, device, when=None, like=None):
        if like is None:
            number = self.count
            self.count += 1
        else:
            number = self.numbers[id(like)]
        copy = pltpu.make_async_remote_copy(
            src_ref=source,
            dst_ref=target,
            send_sem=self.send_sems.at[number],
            recv_sem=self.recv_sems.at[number],
            device_id=device,
            device_id_type=MESH_IDS,
        )
        self.started.append((copy, when))
        self.numbers[id(copy)] = number
        return copy

    def settle(self, chosen):
        numbers = {id(copy) for copy in chosen}
        for copy, when in self.started:
            if id(copy) in numbers:
                run_when(when, copy.wait_send)
        self.started = [entry for entry in self.started if id(entry[0]) not in numbers]

    def finish(self):
        for copy, when in self.started:
            run_when(when, copy.wait_send)


class Place:
    def __init__(self, nz):
        self.nz = nz
        self.c, self.z = lax.axis_index("ctx"), lax.axis_index("fsdp")
        self.k, self.t = self.c % 2, self.c // 2
        self.xn, self.yn, self.pn = flip(self.c, 2), flip(self.c, 4), flip(self.c, 1)
        self.dn = flip(self.xn, 4)
        self.tx, self.ty = flip(self.t, 1), flip(self.t, 2)
        self.td = flip(self.tx, 2)
        self.others = [(self.z + d) % nz for d in range(1, nz)]
        self.plane = [self.xn, self.yn, self.dn, self.pn] + [
            flip(peer, 1) for peer in (self.xn, self.yn, self.dn)
        ]
        self.above, self.below = jnp.minimum(self.z + 1, nz - 1), jnp.maximum(self.z - 1, 0)

    def on_plane(self, c):
        return (c, self.z)

    def on_line(self, z):
        return (self.c, z)

    def greet(self):
        barrier = pltpu.get_barrier_semaphore()
        peers = [self.on_plane(peer) for peer in self.plane] + [self.on_line(z) for z in self.others]
        for peer in peers:
            pl.semaphore_signal(barrier, inc=1, device_id=peer, device_id_type=MESH_IDS)
        pl.semaphore_wait(barrier, len(peers))


class PlaneShare:
    def __init__(self, copies, me, source, slot, rows):
        self.copies, self.me, self.slot = copies, me, slot
        top, bottom = pl.ds(0, rows // 2), pl.ds(rows // 2, rows // 2)
        own = slot(me.k, me.t)
        to_x, to_y = me.on_plane(me.xn), me.on_plane(me.yn)
        self.x_first = copies.make(source.at[top], own.at[top], to_x)
        self.y_first = copies.make(source.at[bottom], own.at[bottom], to_y)
        self.x_second = copies.make(source.at[bottom], own.at[bottom], to_x)
        self.y_second = copies.make(source.at[top], own.at[top], to_y)
        self.to_p = copies.make(source, own, me.on_plane(me.pn))
        through_x, through_y = slot(me.k, me.tx).at[top], slot(me.k, me.ty).at[bottom]
        self.hop_y = copies.make(through_x, through_x, to_y)
        self.hop_x = copies.make(through_y, through_y, to_x)
        self.swaps = []
        for chip in (me.tx, me.ty, me.td):
            place = slot(me.k, chip)
            self.swaps.append(copies.make(place, place, me.on_plane(me.pn)))

    def start(self):
        for copy in (self.x_first, self.y_first, self.x_second, self.y_second, self.to_p):
            copy.start()

    def relay(self):
        self.x_first.wait_recv()
        self.hop_y.start()
        self.y_first.wait_recv()
        self.hop_x.start()

    def swap(self):
        self.x_second.wait_recv()
        self.swaps[0].start()
        self.y_second.wait_recv()
        self.swaps[1].start()

    def on_diagonal(self):
        self.hop_y.wait_recv()
        self.hop_x.wait_recv()
        self.swaps[2].start()

    def finish(self):
        for copy in (self.to_p, *self.swaps):
            copy.wait_recv()


class LineGather:
    def __init__(self, copies, me, source, gathered):
        self.copies, self.me, self.gathered = copies, me, gathered
        rows = gathered.shape[1] // 2
        self.mine = pl.ds(me.k * rows, rows)
        self.moves, self.swaps = {}, []
        for step in range(me.nz - 1):
            for sign in (1, -1):
                shard, target = me.z - sign * step, me.z + sign
                ok = (shard >= 0) & (shard < me.nz) & (target >= 0) & (target < me.nz)
                place = self.slot(shard)
                copy = copies.make(
                    source.at[self.mine] if step == 0 else place,
                    place,
                    me.on_line(jnp.clip(target, 0, me.nz - 1)),
                    when=ok,
                )
                self.moves[step, sign] = (copy, ok)

    def slot(self, shard):
        return self.gathered.at[jnp.clip(shard, 0, self.me.nz - 1), self.mine]

    def start(self):
        for sign in (1, -1):
            copy, ok = self.moves[0, sign]
            run_when(ok, copy.start)

    def advance(self, step):
        me = self.me
        for sign in (1, -1):
            arrived = me.z - sign * (step + 1)
            ok = (arrived >= 0) & (arrived < me.nz)
            run_when(ok, self.moves[step, sign][0].wait_recv)
            if step + 1 < me.nz - 1:
                copy, following = self.moves[step + 1, sign]
                run_when(following, copy.start)
            place = self.slot(arrived)
            swap = self.copies.make(place, place, me.on_plane(me.pn), when=ok)
            run_when(ok, swap.start)
            self.swaps.append((swap, ok))

    def finish(self):
        for swap, ok in self.swaps:
            run_when(ok, swap.wait_recv)


class LineSend:
    def __init__(self, copies, me, source, gathered):
        self.me = me
        rows = gathered.shape[1] // 2
        mine = pl.ds(me.k * rows, rows)
        self.sends, self.swaps = [], []
        for distance, other in enumerate(me.others, 1):
            self.sends.append(
                copies.make(source.at[mine], gathered.at[me.z, mine], me.on_line(other))
            )
            place = gathered.at[(me.z - distance) % me.nz, mine]
            self.swaps.append(copies.make(place, place, me.on_plane(me.pn)))

    def start(self):
        for send in self.sends:
            send.start()

    def advance(self):
        for send, swap in zip(self.sends, self.swaps):
            send.wait_recv()
            swap.start()

    def finish(self):
        for swap in self.swaps:
            swap.wait_recv()


class LineSpread:
    def __init__(self, copies, me, source, target, sem):
        self.me = me
        self.keep = pltpu.make_async_copy(source, target, sem)
        rows = target.shape[0] // 2
        mine = pl.ds(me.k * rows, rows)
        self.here, self.away = me.z == me.t, me.z != me.t
        place = target.at[mine]
        self.sends, self.arrivals = [], []
        for distance in range(1, me.nz):
            target_z = (me.t + distance) % me.nz
            copy = copies.make(source.at[mine], place, me.on_line(target_z), when=self.here)
            self.sends.append(copy)
            self.arrivals.append(me.z == target_z)
        self.swap = copies.make(place, place, me.on_plane(me.pn), when=self.away)

    def start(self):
        @pl.when(self.here)
        def _():
            for copy in self.sends:
                copy.start()
            self.keep.start()

    def advance(self):
        for copy, arrives in zip(self.sends, self.arrivals):
            pl.when(arrives)(copy.wait_recv)
        pl.when(self.away)(self.swap.start)

    def finish(self):
        pl.when(self.here)(self.keep.wait)
        pl.when(self.away)(self.swap.wait_recv)


class LineReduce:
    def __init__(self, copies, me, source, total, landed):
        self.me, self.source, self.total, self.landed = me, source, total, landed
        half = total.shape[1]
        self.mine, theirs = pl.ds(me.k * half, half), pl.ds((1 - me.k) * half, half)
        self.exchange = copies.make(source.at[:, theirs], total, me.on_plane(me.pn))
        self.sends = [
            copies.make(total.at[other], landed.at[me.z], me.on_line(other)) for other in me.others
        ]

    def start(self):
        self.exchange.start()

    def pair(self):
        self.exchange.wait_recv()
        for owner in range(self.me.nz):
            self.total[owner] = narrow(
                wide(self.total[owner]) + wide(self.source[owner, self.mine])
            )
        for send in self.sends:
            send.start()

    def collect(self):
        me = self.me
        result = wide(self.total[me.z])
        for send in self.sends:
            send.wait_recv()
        for other in me.others:
            result = result + wide(self.landed[other])
        self.total[me.z] = narrow(result)


class LineCollect:
    def __init__(self, copies, me, source, total, landed):
        self.me, self.source, self.total, self.landed = me, source, total, landed
        half = total.shape[0]
        self.mine, theirs = pl.ds(me.k * half, half), pl.ds((1 - me.k) * half, half)
        self.exchange = copies.make(source.at[theirs], total, me.on_plane(me.pn))
        self.sends = []
        for distance in range(1, me.nz):
            leaves = (me.z + distance) % me.nz == me.t
            copy = copies.make(total, landed.at[me.z], me.on_line(me.t), when=leaves)
            self.sends.append((copy, leaves))

    def start(self):
        self.exchange.start()

    def pair(self):
        self.exchange.wait_recv()
        self.total[...] = narrow(wide(self.total[...]) + wide(self.source[self.mine]))
        for copy, leaves in self.sends:
            pl.when(leaves)(copy.start)

    def collect(self):
        me = self.me

        @pl.when(me.z == me.t)
        def _():
            result = wide(self.total[...])
            for copy, _ in self.sends:
                copy.wait_recv()
            for other in me.others:
                result = result + wide(self.landed[other])
            self.total[...] = narrow(result)


class PlaneSpread:
    def __init__(self, copies, me, source, target, rows, sem):
        self.me = me
        self.keep = pltpu.make_async_copy(source, target.at[me.k], sem)
        top, bottom = pl.ds(0, rows // 2), pl.ds(rows // 2, rows // 2)
        place = target.at[me.k]
        self.here, self.from_x, self.from_y = me.t == me.z, me.tx == me.z, me.ty == me.z
        self.from_d = me.td == me.z
        self.to_x = copies.make(source, place, me.on_plane(me.xn), when=self.here)
        self.to_y = copies.make(source, place, me.on_plane(me.yn), when=self.here)
        self.to_p = copies.make(source, place, me.on_plane(me.pn), when=self.here)
        self.hop_y = copies.make(place.at[top], place.at[top], me.on_plane(me.yn), when=self.from_x)
        self.hop_x = copies.make(
            place.at[bottom], place.at[bottom], me.on_plane(me.xn), when=self.from_y
        )
        away = self.from_x | self.from_y | self.from_d
        self.away = away
        self.swap = copies.make(place, place, me.on_plane(me.pn), when=away, like=self.to_p)

    def start(self):
        @pl.when(self.here)
        def _():
            self.to_x.start()
            self.to_y.start()
            self.to_p.start()
            self.keep.start()

    def advance(self):
        @pl.when(self.from_x)
        def _():
            self.to_x.wait_recv()
            self.hop_y.start()
            self.swap.start()

        @pl.when(self.from_y)
        def _():
            self.to_y.wait_recv()
            self.hop_x.start()
            self.swap.start()

    def on_diagonal(self):
        @pl.when(self.from_d)
        def _():
            self.hop_y.wait_recv()
            self.hop_x.wait_recv()
            self.swap.start()

    def finish(self):
        pl.when(self.here)(self.keep.wait)
        self.to_p.wait_recv()

def norm_rows(values_in):
    centre = jnp.mean(values_in, axis=-1, keepdims=True)
    mean_removed = values_in - centre
    inverse_deviation = lax.rsqrt(
        jnp.mean(mean_removed * mean_removed, axis=-1, keepdims=True) + EPS
    )
    return mean_removed * inverse_deviation, inverse_deviation


def head_rows(rows, head):
    lanes = lax.broadcasted_iota(jnp.int32, rows.shape, 1)
    inside = (lanes >= head * HD) & (lanes < (head + 1) * HD)
    return jnp.where(inside, rows, jnp.zeros_like(rows))


def rope_lanes(r, blocks, columns, back):
    half_rot = ROT // 2
    tables = [[], [], []]
    row_cos, row_sin = r.rope_r[:, :128], r.rope_r[:, 128:]
    lane = lax.broadcasted_iota(jnp.int32, row_cos.shape, 1) % HD
    for block in blocks:
        both = r.rope_b[block]
        block_cos, block_sin = both[:, :128], both[:, 128:]
        cosine = block_cos * row_cos - block_sin * row_sin
        sine = block_sin * row_cos + block_cos * row_sin
        if back:
            sine = -sine
        tables[0].append(cosine)
        tables[1].append(jnp.where(lane < half_rot, -sine, 0.0))
        tables[2].append(jnp.where(lane >= half_rot, sine, 0.0))
    stacked = [jnp.concatenate(table, axis=0) for table in tables]
    return [jnp.concatenate([table] * (columns // 128), axis=1) for table in stacked]


def turn(values, tables):
    columns, half_rot = values.shape[1], ROT // 2
    return (
        values * tables[0]
        + pltpu.roll(values, columns - half_rot, 1) * tables[1]
        + pltpu.roll(values, half_rot, 1) * tables[2]
    )


def windows(r, me):
    part = r.wqs.shape[1] // 3
    chips, columns = me.nz, r.win.shape[2]
    copies = []
    for source, pieces in ((r.wqkv, 3), (r.wup, r.wus.shape[1] // part)):
        for piece in range(pieces):
            first = (piece * chips + me.t) * part // 128 * 128
            number = len(copies)
            copies.append(
                pltpu.make_async_copy(
                    source.at[:, pl.ds(pl.multiple_of(first, 128), columns)],
                    r.win.at[number],
                    r.window_sems.at[number],
                )
            )
    return copies


def slice_weights(r, me):
    part = r.wqs.shape[1] // 3
    for chip in range(me.nz):

        @pl.when(me.t == chip)
        def _():
            first = chip * part % 128
            number = 0
            for target in (r.wqs, r.wus):
                for piece in range(target.shape[1] // part):
                    target[:, piece * part : (piece + 1) * part] = r.win[
                        number, :, first : first + part
                    ]
                    number += 1


VECTORS = ("gain1", "shift1", "gain2", "shift2", "bout", "bdown", "bqkv", "bup")


def pack_vectors(r):
    first = 0
    for name in VECTORS:
        values = wide(getattr(r, name)[...])
        count = values.shape[0]
        r.sm[0:1, first : first + count] = values.reshape(1, count)
        first += count


def read_vectors(r, me):
    nz, part = me.nz, r.vec.shape[1] // me.nz

    def piece(z, number):
        return r.sm4[z, 0:1, number * part : (number + 1) * part]

    for z in range(nz):
        span = slice(z * part, (z + 1) * part)
        for row in range(4):
            r.vec[row : row + 1, span] = piece(z, row)
        r.vec[4:5, span] = piece(z, 4) + piece(z, 5)
    chips = nz
    for chip in range(chips):

        @pl.when(me.t == chip)
        def _():
            for number in range(3):
                held = number * chips + chip
                r.vec[5:6, number * part : (number + 1) * part] = piece(held // 3, 6 + held % 3)
            for z in range(nz):
                r.vec[6:7, z * part : (z + 1) * part] = piece(z, 9 + chip)


def block_table(r, me):
    count = r.order.shape[0]
    chips, quarter = me.nz, count // 4
    sides = count // (2 * chips)
    held = [r.order[number] for number in range(count)]
    for position in range(count):
        found = 0
        for number in range(1, count):
            found = jnp.where(held[number] == position, number, found)
        r.idx[position] = found
    for chip in range(chips):
        for holder, first in ((me.k, count), (1 - me.k, count + chips * sides)):
            for side in range(sides):
                position = r.order[(2 * chip + me.k) * sides + side]
                low = (position >= quarter * holder) & (position < quarter * (holder + 1))
                near = position - quarter * holder
                high = position - 2 * quarter + quarter * holder
                r.idx[first + chip * sides + side] = jnp.clip(
                    jnp.where(low, near, high), 0, 2 * quarter - 1
                )
        position = r.order[(2 * chip + me.k) * sides]
        outer = jnp.where((position < quarter) | (position >= 3 * quarter), 0, 1)
        r.idx[count + 2 * chips * sides + chip] = jnp.where(outer == me.k, 1, 0)


def sorted_rows(r, source, block, blocks):
    pieces = []
    for number in range(blocks):
        pieces.append(source[r.idx[block + number]])
    return jnp.concatenate(pieces, axis=0)


def flat_rows(values):
    return values.reshape(-1, values.shape[-1])


def put_blocks(target, tile, values):
    blocks = values.shape[0] // BLK
    target[pl.ds(tile * blocks, blocks)] = values.reshape(blocks, BLK, values.shape[1])


def prepare(r, chip, target, at):
    sides = r.h.shape[0]
    rows = sides * BLK

    @pl.loop(0, 2)
    def _(core):
        values = flat_rows(r.hall[pl.ds((2 * chip + core) * sides, sides)])
        standardized, _ = norm_rows(wide(values))
        place = pl.ds(pl.multiple_of(at + core * rows, rows), rows)
        target[place, :] = narrow(standardized * r.vec[0:1, :] + r.vec[1:2, :])


def project(r, chip, source, at):
    part = r.wqs.shape[1] // 3
    blocks = 2 * r.h.shape[0]
    first = chip * blocks
    weight = r.wq4[...].reshape(-1, 3 * part)
    projected = mm(source[at : at + blocks * BLK, :], weight) + r.vec[5:6, : 3 * part]
    positions = [r.order[first + number] for number in range(blocks)]
    turned = turn(projected[:, : 2 * part], rope_lanes(r, positions, 2 * part, False))
    keys, values = turned[:, part:], projected[:, 2 * part :]
    query = narrow(wide(narrow(turned[:, :part])) * HD**-0.5)
    for number in range(blocks):
        own = slice(number * BLK, (number + 1) * BLK)
        r.q[first + number] = query[own]
        r.k[first + number] = narrow(keys[own])
        r.v[first + number] = narrow(values[own])
        r.kt[first + number] = narrow(keys[own].T)
        r.vt[first + number] = narrow(values[own].T)


def sorted_columns(r, source, head, block, blocks):
    lanes = slice(head * HD, (head + 1) * HD)
    return jnp.concatenate(
        [source[r.idx[block + number], lanes, :] for number in range(blocks)], axis=1
    )


def tile_start(r, me, tile):
    quarter = r.k.shape[0] * BLK // 4
    low = tile < quarter // QTILE
    inside = tile * QTILE - jnp.where(low, 0, quarter)
    return jnp.where(low, quarter * me.k, 3 * quarter - quarter * me.k) + inside


def attend(r, me, tile):
    part = r.k.shape[2]
    blocks = QTILE // BLK
    heads = part // HD
    start = tile_start(r, me, tile)
    rows = slice(tile * QTILE, (tile + 1) * QTILE)
    query = sorted_rows(r, r.q, start // BLK, blocks)
    per_head = [head_rows(query, head) for head in range(heads)]

    def visit(number, state, masked):
        keys = sorted_rows(r, r.k, number * blocks, blocks)
        result = []
        for head in range(heads):
            top, total, acc = state[head]
            logits = mm(keys, per_head[head], NT)
            if masked:
                key_row = lax.broadcasted_iota(jnp.int32, logits.shape, 0)
                query_row = lax.broadcasted_iota(jnp.int32, logits.shape, 1)
                logits = jnp.where(key_row <= query_row, logits, NEG)
            new_top = jnp.maximum(top, jnp.max(logits, axis=0, keepdims=True))
            fade = jnp.exp(top - new_top)
            probs = jnp.exp(logits - new_top)
            total = total * fade + jnp.sum(probs, axis=0, keepdims=True)
            values = sorted_columns(r, r.vt, head, number * blocks, blocks)
            acc = acc * fade + mm(values, narrow(probs))
            result.append((new_top, total, acc))
        return tuple(result)

    state = tuple(
        (
            jnp.full((1, QTILE), NEG, jnp.float32),
            jnp.zeros((1, QTILE), jnp.float32),
            jnp.zeros((HD, QTILE), jnp.float32),
        )
        for _ in range(heads)
    )
    last = start // QTILE
    state = lax.fori_loop(0, last, lambda n, s: visit(n, s, False), state)
    state = visit(last, state, True)
    merged = jnp.concatenate([acc / total for _, total, acc in state], axis=0)
    r.att[rows, :] = narrow(merged.T)
    r.attt[:, rows] = narrow(merged)
    for head in range(heads):
        r.lse[head : head + 1, rows] = state[head][0] + jnp.log(state[head][1])


def feed_forward(r, me, tile):
    place = pl.ds(pl.multiple_of(tile * QTILE, QTILE), QTILE)
    blocks = QTILE // BLK
    block = tile_start(r, me, tile) // BLK
    width = r.hall.shape[2]
    standardized, _ = norm_rows(wide(sorted_rows(r, r.hall, block, blocks)))
    cotan = sorted_rows(r, r.gall, block, blocks)
    gain2 = r.vec[2:3, :]
    normed = narrow(standardized * gain2 + r.vec[3:4, :])
    up_weight = r.wu4[...].reshape(width, -1)
    down_weight = r.wd4[...].reshape(-1, width)
    up = mm(normed, up_weight) + r.vec[6:7, :]
    below = 0.5 * (1.0 + lax.erf(up * SQRT_HALF))
    act = narrow(up * below)
    slope = below + up * jnp.exp(-0.5 * up * up) * INV_ROOT_TWO_PI
    d_up = mm(cotan, down_weight, NT) * slope
    d_up16 = narrow(d_up)
    put_blocks(r.outb, tile, narrow(mm(act, down_weight)))
    d_normed = mm(d_up16, up_weight, NT)
    r.sums[2:3, :] += jnp.sum(d_normed * standardized, axis=0, keepdims=True)
    r.sums[3:4, :] += jnp.sum(d_normed, axis=0, keepdims=True)
    r.sums[6:7, :] += jnp.sum(d_up, axis=0, keepdims=True)
    r.e2[place, :] = d_normed * gain2
    r.n[place, :] = normed
    r.gl[place, :] = cotan
    r.act[place, :] = act
    r.du[place, :] = d_up16


def out_project(r, me, tile):
    place = pl.ds(pl.multiple_of(tile * QTILE, QTILE), QTILE)
    blocks = QTILE // BLK
    attended = r.att[place, :]
    mlp = flat_rows(r.outb[pl.ds(tile * blocks, blocks)])
    put_blocks(r.outb, tile, narrow(wide(mlp) + mm(attended, r.wo1[...])))
    cotan = r.gl[place, :]
    r.datt[place, :] = narrow(mm(cotan, r.wo1[...], NT))
    product = wide(narrow(mm(r.wo1[...], cotan, NT))) * wide(r.attt[:, place])
    for head in range(product.shape[0] // HD):
        r.delta[head : head + 1, place] = jnp.sum(
            product[head * HD : (head + 1) * HD], axis=0, keepdims=True
        )


def weight_grad(target, left, right):
    rows, columns = left.shape[1], right.shape[1]
    shard = target.shape[1]
    values = right[...]
    for first in range(0, rows, QTILE):
        result = narrow(mm(left[:, first : first + QTILE], values, TN))
        at = first
        while at < first + QTILE:
            owner, inside = at // shard, at % shard
            until = min((owner + 1) * shard, first + QTILE)
            target[owner, inside : inside + until - at, :] = result[at - first : until - first, :]
            at = until


def attend_grad(r, me, tile):
    part = r.k.shape[2]
    heads = part // HD
    kstep = 2 * QTILE
    start = tile_start(r, me, tile)
    rows = slice(tile * QTILE, (tile + 1) * QTILE)
    blocks = kstep // BLK
    query = sorted_rows(r, r.q, start // BLK, QTILE // BLK)
    d_out = r.datt[rows, :]
    queries = jnp.concatenate([head_rows(query, head) for head in range(heads)], axis=0)
    d_outs = jnp.concatenate([head_rows(d_out, head) for head in range(heads)], axis=0)

    def visit(number, state, masked):
        place = pl.ds(pl.multiple_of(number * kstep, kstep), kstep)
        keys = sorted_rows(r, r.k, number * blocks, blocks)
        values = sorted_rows(r, r.v, number * blocks, blocks)
        probs_all, d_logits_all, result = [], [], []
        for head in range(heads):
            own = slice(head * QTILE, (head + 1) * QTILE)
            logits = mm(keys, queries[own], NT)
            probs = jnp.exp(logits - r.lse[head : head + 1, rows])
            if masked:
                key_row = number * kstep + lax.broadcasted_iota(jnp.int32, logits.shape, 0)
                query_row = start + lax.broadcasted_iota(jnp.int32, logits.shape, 1)
                probs = jnp.where(key_row <= query_row, probs, 0.0)
            d_probs = mm(values, d_outs[own], NT)
            d_logits = narrow(probs * (d_probs - r.delta[head : head + 1, rows]))
            probs_all.append(narrow(probs))
            d_logits_all.append(d_logits)
            columns = sorted_columns(r, r.kt, head, number * blocks, blocks)
            result.append(state[head] + mm(columns, d_logits))
        r.dv[place, :] += mm(jnp.concatenate(probs_all, axis=1), d_outs)
        r.dk[place, :] += mm(jnp.concatenate(d_logits_all, axis=1), queries)
        return tuple(result)

    state = tuple(jnp.zeros((HD, QTILE), jnp.float32) for _ in range(heads))
    last = start // kstep
    state = lax.fori_loop(0, last, lambda n, s: visit(n, s, False), state)
    state = visit(last, state, True)
    r.dqt[:, rows] = jnp.concatenate(state, axis=0)


def qkv_grad(r, me, tile):
    place = pl.ds(pl.multiple_of(tile * QTILE, QTILE), QTILE)
    part = r.k.shape[2]
    blocks = QTILE // BLK
    start = tile_start(r, me, tile)
    block = start // BLK
    held = pl.ds(pl.multiple_of(start, QTILE), QTILE)
    standardized, _ = norm_rows(wide(sorted_rows(r, r.hall, block, blocks)))
    gain1 = r.vec[0:1, :]
    r.n[place, :] = narrow(standardized * gain1 + r.vec[1:2, :])
    d_query = r.dqt[:, place].T * HD**-0.5
    d_key = r.dk[held, :] + wide(r.kvin[place, :part])
    d_value = r.dv[held, :] + wide(r.kvin[place, part:])
    turned = turn(
        jnp.concatenate([d_query, d_key], axis=1),
        rope_lanes(r, [block + n for n in range(blocks)], 2 * part, True),
    )
    d_qkv = jnp.concatenate([turned, d_value], axis=1)
    d_qkv16 = narrow(d_qkv)
    r.du[place, : 3 * part] = d_qkv16
    r.sums[5:6, : 3 * part] += jnp.sum(d_qkv, axis=0, keepdims=True)
    weight = r.wq4[...].reshape(-1, 3 * part)
    d_normed = mm(d_qkv16, weight, NT)
    r.sums[0:1, :] += jnp.sum(d_normed * standardized, axis=0, keepdims=True)
    r.sums[1:2, :] += jnp.sum(d_normed, axis=0, keepdims=True)
    put_blocks(r.outb, tile, narrow(d_normed * gain1 + r.e2[place, :]))


def gather_sums(r, me):
    nz, part = me.nz, r.vec.shape[1] // me.nz
    r.sums[4:5, :] = jnp.sum(wide(flat_rows(r.gown[...])), axis=0, keepdims=True)

    def put(z, number, values):
        r.vout[z, 0:1, number * part : (number + 1) * part] = values

    for z in range(nz):
        for row in range(5):
            put(z, row, r.sums[row : row + 1, z * part : (z + 1) * part])
    for chip in range(nz):

        @pl.when(me.t == chip)
        def _():
            for number in range(3):
                held = number * nz + chip
                put(held // 3, 5 + held % 3, r.sums[5:6, number * part : (number + 1) * part])
            for z in range(nz):
                put(z, 8 + chip, r.sums[6:7, z * part : (z + 1) * part])


class Scatter:
    def __init__(self, copies, me, r, source, theirs, got, landed):
        self.me, self.r, self.source, self.theirs, self.got, self.landed = me, r, source, theirs, got, landed
        self.chips = me.nz
        self.sides = got.shape[0] // self.chips
        self.first = r.k.shape[0]
        self.tiles = source.shape[0] * BLK // QTILE
        self.number = copies.count
        self.send_sems, self.recv_sems = copies.send_sems, copies.recv_sems
        self.exchanges = [
            copies.make(*self.rows(tile), me.on_plane(me.pn)) for tile in range(self.tiles)
        ]
        self.steps = []
        for side, near, far, to_near, to_far in (
            (0, me.tx, me.ty, me.xn, me.yn),
            (1, me.ty, me.tx, me.yn, me.xn),
        ):
            first, last = self.place(near, side), self.place(far, side)
            self.steps.append(
                (
                    copies.make(got.at[self.place(me.td, side)], landed.at[3 * side], me.on_plane(to_near)),
                    copies.make(got.at[first], landed.at[3 * side + 1], me.on_plane(to_near)),
                    copies.make(got.at[last], landed.at[3 * side + 2], me.on_plane(to_far)),
                    last,
                )
            )

    def place(self, chip, side):
        return chip * self.sides + side

    def rows(self, tile):
        blocks = QTILE // BLK
        place = pl.ds(tile * blocks, blocks)
        return self.source.at[place], self.theirs.at[place]

    def exchange(self, tile):
        source, target = self.rows(tile)
        pltpu.make_async_remote_copy(
            src_ref=source,
            dst_ref=target,
            send_sem=self.send_sems.at[self.number + tile],
            recv_sem=self.recv_sems.at[self.number + tile],
            device_id=self.me.on_plane(self.me.pn),
            device_id_type=MESH_IDS,
        ).start()

    def spread(self):
        count = self.chips * self.sides
        for exchange in self.exchanges:
            exchange.wait_recv()
        for number in range(count):
            flag = self.r.idx[self.first + 2 * count + number // self.sides]
            own = wide(self.source[self.r.idx[self.first + number]])
            other = wide(self.theirs[self.r.idx[self.first + count + number]])
            here = jnp.full(own.shape, flag, jnp.int32) > 0
            self.got[number] = narrow(jnp.where(here, own, other))
        for far, _, _, _ in self.steps:
            far.start()
        for _, near, _, _ in self.steps:
            near.start()

    def middle(self):
        for side, (far, _, on, last) in enumerate(self.steps):
            far.wait_recv()
            self.got[last] = narrow(wide(self.got[last]) + wide(self.landed[3 * side]))
            on.start()

    def total(self):
        pieces = []
        for side, (_, near, on, _) in enumerate(self.steps):
            near.wait_recv()
            on.wait_recv()
            pieces.append(
                wide(self.got[self.place(self.me.t, side)])
                + wide(self.landed[3 * side + 1])
                + wide(self.landed[3 * side + 2])
            )
        return jnp.concatenate(pieces, axis=0)


def layer_kernel(nz, names, *refs):
    r = types.SimpleNamespace(**dict(zip(names, refs)))
    me = Place(nz)
    copies = Copies(r.send_sems, r.recv_sems)
    sides = r.h.shape[0]
    shard = r.wqs.shape[0]
    tiles = r.att.shape[0] // QTILE

    kept = []

    def keep(source, target):
        copy = pltpu.make_async_copy(source, target, r.local_sems.at[len(kept)])
        copy.start()
        kept.append(copy)
        return copy

    own_rows = pl.ds(me.c * sides, sides)
    loads = windows(r, me)
    for copy in loads:
        copy.start()
    h_own = keep(r.h, r.hall.at[own_rows])
    keep(r.g, r.gall.at[own_rows])
    keep(r.g, r.gown)
    own_down = keep(r.wdown.at[pl.ds(me.t * shard, shard)], r.wd4.at[me.z])
    pack_vectors(r)
    me.greet()

    def row_slot(array):
        return lambda core, chip: array.at[pl.ds((2 * chip + core) * sides, sides)]

    h_share = PlaneShare(copies, me, r.h, row_slot(r.hall), sides)
    g_share = PlaneShare(copies, me, r.g, row_slot(r.gall), sides)
    wq = LineSend(copies, me, r.wqs, r.wq4)
    wu = LineGather(copies, me, r.wus, r.wu4)
    wd = LineGather(copies, me, r.wdown.at[pl.ds(me.t * shard, shard)], r.wd4)
    wo = LineSpread(copies, me, r.wout, r.wo1, r.window_sems.at[len(loads)])
    small = [copies.make(r.sm, r.sm4.at[me.z], me.on_line(other)) for other in me.others]

    for copy in small:
        copy.start()
    h_share.start()
    for copy in loads:
        copy.wait()
    slice_weights(r, me)
    r.wq4[me.z] = r.wqs[...]
    r.wu4[me.z] = r.wus[...]
    wq.start()
    wu.start()
    wd.start()
    r.sm4[me.z] = r.sm[...]
    block_table(r, me)
    r.sums[...] = jnp.zeros_like(r.sums)
    r.vout[...] = jnp.zeros_like(r.vout)
    r.dk[...] = jnp.zeros_like(r.dk)
    r.dv[...] = jnp.zeros_like(r.dv)
    for copy in small:
        copy.wait_recv()
    read_vectors(r, me)
    h_own.wait()
    h_share.to_p.wait_recv()
    pair = 2 * sides * BLK
    prepare(r, me.t, r.n, 0)
    h_share.relay()
    h_share.swap()
    g_share.start()
    h_share.swaps[0].wait_recv()
    prepare(r, me.tx, r.n, pair)
    h_share.swaps[1].wait_recv()
    wq.advance()
    prepare(r, me.ty, r.gl, 0)
    wq.finish()
    project(r, me.t, r.n, 0)
    wu.advance(0)
    h_share.on_diagonal()
    project(r, me.tx, r.n, pair)
    wd.advance(0)
    project(r, me.ty, r.gl, 0)
    g_share.relay()
    wu.advance(1)
    h_share.swaps[2].wait_recv()
    prepare(r, me.td, r.gl, pair)
    project(r, me.td, r.gl, pair)
    attend(r, me, 1)
    wd.advance(1)
    g_share.swap()
    attend(r, me, 2)
    wu.advance(2)
    g_share.on_diagonal()
    wd.advance(2)
    wo.start()
    for copy in kept[1:]:
        copy.wait()
    settled = len(kept)
    wu.finish()
    wd.finish()
    g_share.finish()

    @pl.loop(0, tiles)
    def _(tile):
        feed_forward(r, me, tile)

    half = shard // 2
    out_scatter = Scatter(copies, me, r, r.outb, r.otheirs, r.ogot, r.oland)
    up_reduce = LineReduce(copies, me, r.gu, r.tu, r.uu)
    down_reduce = LineReduce(copies, me, r.gd, r.td, r.ud)
    out_reduce = LineCollect(copies, me, r.go, r.to, r.uo)
    d_share = PlaneShare(copies, me, r.td.at[me.z], lambda core, chip: r.fd.at[core, chip], half)
    u_share = PlaneShare(copies, me, r.tu.at[me.z], lambda core, chip: r.fu.at[core, chip], half)
    o_spread = PlaneSpread(copies, me, r.to, r.fo, half, r.window_sems.at[len(loads) + 1])

    def share_down():
        d_share.start()
        keep(r.td.at[me.z], r.fd.at[me.k, me.t])

    def share_up():
        u_share.start()
        keep(r.tu.at[me.z], r.fu.at[me.k, me.t])

    weight_grad(r.gd, r.act, r.gl)
    down_reduce.start()
    weight_grad(r.gu, r.n, r.du)
    up_reduce.start()
    wo.advance()
    down_reduce.pair()
    attend(r, me, 0)
    attend(r, me, 3)
    up_reduce.pair()
    wo.finish()

    @pl.loop(0, tiles)
    def _(tile):
        out_project(r, me, tile)
        pl.when(tile > 0)(functools.partial(out_scatter.exchange, tile - 1))

    out_scatter.exchange(tiles - 1)
    r.go[...] = narrow(mm(r.att[...], r.gl[...], TN))
    out_reduce.start()
    attend_grad(r, me, 0)
    out_reduce.pair()
    out_scatter.spread()
    attend_grad(r, me, 3)
    out_scatter.middle()
    attend_grad(r, me, 2)
    down_reduce.collect()
    share_down()
    copies.settle([g_share.hop_x, g_share.hop_y, *g_share.swaps])
    copies.settle(out_scatter.exchanges)

    part = r.k.shape[2]
    quarter = r.k.shape[0] * BLK // 4

    def send_keys(number):
        first = quarter * (1 - me.k) if number == 0 else 3 * quarter - quarter * (1 - me.k)
        theirs = pl.ds(pl.multiple_of(first, quarter), quarter)
        rows = slice(number * quarter, (number + 1) * quarter)
        r.act[rows, :part] = narrow(r.dk[theirs, :])
        r.act[rows, part : 2 * part] = narrow(r.dv[theirs, :])
        copy = copies.make(r.act.at[rows, : 2 * part], r.kvin.at[rows], me.on_plane(me.pn))
        copy.start()
        return copy

    later = send_keys(1)
    attend_grad(r, me, 1)
    sooner = send_keys(0)
    later.wait_recv()
    e_scatter = Scatter(
        copies, me, r, r.outb, r.gall.at[: r.outb.shape[0]], r.gall.at[r.outb.shape[0] :], r.eland
    )

    @pl.loop(0, tiles)
    def _(number):
        pl.when(number == tiles // 2)(sooner.wait_recv)
        pl.when(number == tiles // 2)(d_share.relay)
        qkv_grad(r, me, (number + tiles // 2) % tiles)
        pl.when(number > 0)(
            functools.partial(e_scatter.exchange, (number + tiles // 2 - 1) % tiles)
        )

    up_reduce.collect()
    share_up()
    gather_sums(r, me)
    e_scatter.exchange(tiles // 2 - 1)
    vec_line = [
        copies.make(r.vout.at[other], r.vline.at[me.z], me.on_line(other)) for other in me.others
    ]
    for copy in vec_line:
        copy.start()
    d_share.swap()
    weight_grad(r.gq, r.n, r.du.at[:, : 3 * part])
    qkv_reduce = LineReduce(copies, me, r.gq, r.tq, r.uq)
    qkv_reduce.start()
    e_scatter.spread()
    qkv_reduce.pair()
    u_share.relay()
    out_reduce.collect()
    o_spread.start()
    d_share.on_diagonal()
    u_share.swap()
    e_scatter.middle()
    for copy in vec_line:
        copy.wait_recv()
    vector = r.vout[me.z]
    for other in me.others:
        vector = vector + r.vline[other]
    r.vsend[...] = vector
    vec_plane = [copies.make(r.vsend, r.vplane.at[me.c], me.on_plane(peer)) for peer in me.plane]
    for copy in vec_plane:
        copy.start()
    qkv_reduce.collect()
    q_share = PlaneShare(copies, me, r.tq.at[me.z], lambda core, chip: r.fq.at[core, chip], half)
    q_share.start()
    keep(r.tq.at[me.z], r.fq.at[me.k, me.t])

    residual = wide(flat_rows(r.hall[own_rows]))
    own_standardized, own_deviation = norm_rows(residual)
    rows = sides * BLK
    r.n[:rows, :] = narrow(residual + r.vec[4:5, :] + out_scatter.total())
    keep(r.n.at[:rows], r.hidden_out)
    o_spread.advance()
    u_share.on_diagonal()
    q_share.relay()
    e_total = e_scatter.total()
    r.e2[:rows, :] = wide(flat_rows(r.gown[...])) + own_deviation * (
        e_total
        - jnp.mean(e_total, axis=-1, keepdims=True)
        - own_standardized * jnp.mean(e_total * own_standardized, axis=-1, keepdims=True)
    )
    keep(r.e2.at[:rows], r.hidden_grad)
    q_share.swap()
    o_spread.on_diagonal()
    for copy in vec_plane:
        copy.wait_recv()
    vector = r.vsend[...]
    for peer in me.plane:
        vector = vector + r.vplane[peer]
    r.vlast[...] = vector
    keep(r.vlast, r.vsum)
    q_share.on_diagonal()
    for share in (d_share, u_share, o_spread, q_share):
        share.finish()
    for copy in kept[settled:]:
        copy.wait()
    copies.finish()


def assemble_kernel(
    fq_ref, fu_ref, fd_ref, fo_ref, out_ref, grad_ref, vsum_ref,
    gq_ref, gu_ref, gd_ref, go_ref, hidden_out_ref, hidden_grad_ref, *vector_refs,
):
    _, chips, _, _ = fq_ref.shape
    part = fq_ref.shape[3] // 3
    hidden_out_ref[...] = out_ref[...]
    hidden_grad_ref[...] = grad_ref[...]
    go_ref[...] = wide(fo_ref[0])
    for chip in range(chips):
        for source, target in ((fq_ref, gq_ref), (fu_ref, gu_ref)):
            for piece in range(source.shape[3] // part):
                first = (piece * chips + chip) * part
                target[:, first : first + part] = wide(
                    source[0, chip, :, piece * part : (piece + 1) * part]
                )
        gd_ref[chip, 0] = wide(fd_ref[0, chip])

    @pl.when(pl.program_id(0) == 0)
    def _():
        first = 0
        for number, target in enumerate(vector_refs):
            count = target.shape[0]
            if number == 5:
                first -= count
            target[...] = vsum_ref[0:1, first : first + count].reshape(count)
            first += count


def rotary_parts(block_count):
    half_rot = ROT // 2
    lane = np.arange(128) % HD
    rate = np.where(lane < ROT, 10000.0 ** (-2.0 * (lane % half_rot) / ROT), 0.0)

    def table(places):
        angle = places[:, None].astype(np.float64) * rate[None, :]
        return np.concatenate([np.cos(angle), np.sin(angle)], axis=1).astype(np.float32)

    return table(np.arange(BLK)), table(np.arange(block_count) * BLK)


VMEM_SPEC = pl.BlockSpec(memory_space=pltpu.VMEM)
SPECS = {
    "order": pl.BlockSpec(memory_space=pltpu.SMEM),
    **{
        name: pl.BlockSpec(memory_space=pl.ANY)
        for name in ("h", "g", "wqkv", "wup", "wdown", "wout")
        + ("hidden_out", "hidden_grad", "fq", "fu", "fd", "fo", "vsum")
    },
}
VMEM_LIMIT = 63 * 1024 * 1024


def sliced_layer(
    nz,
    hidden_in,
    norm1_gain,
    attention_norm_bias,
    qkv_weight,
    qkv_bias,
    out_weight,
    out_bias,
    norm2_gain,
    feedforward_norm_bias,
    up_weight,
    up_bias,
    down_weight,
    down_bias,
    cotangent,
    block_order,
):
    f32, b16 = jnp.float32, jnp.bfloat16
    h, g = hidden_in[0], cotangent[0]
    local_rows, width = h.shape
    chips = lax.axis_size("ctx") // 2
    shard = qkv_weight.shape[0]
    half = shard // 2
    part = width // chips
    hidden = up_weight.shape[1] // chips
    rows = chips * local_rows
    everyone = 2 * rows
    sides = local_rows // BLK

    sums = 5 * shard + qkv_bias.shape[0] + up_bias.shape[0]
    slices = 3 + hidden // part
    columns = max(-(-(chip * part % 128 + part) // 128) * 128 for chip in range(chips))
    small = 6 * shard + qkv_bias.shape[0] + up_bias.shape[0]
    rope_r, rope_b = rotary_parts(everyone // BLK)

    inputs = {
        "order": block_order,
        "h": h.reshape(sides, BLK, width),
        "g": g.reshape(sides, BLK, width),
        "wqkv": qkv_weight,
        "wup": up_weight,
        "wdown": down_weight,
        "wout": out_weight,
        **dict(
            zip(
                VECTORS,
                (norm1_gain, attention_norm_bias, norm2_gain, feedforward_norm_bias)
                + (out_bias, down_bias, qkv_bias, up_bias),
            )
        ),
        "rope_r": jnp.asarray(rope_r),
        "rope_b": jnp.asarray(rope_b[:, None, :]),
    }
    outputs = {
        "hidden_out": ((local_rows, width), b16),
        "hidden_grad": ((local_rows, width), f32),
        "fq": ((2, chips, half, 3 * part), b16),
        "fu": ((2, chips, half, hidden), b16),
        "fd": ((2, chips, half, width), b16),
        "fo": ((2, half, width), b16),
        "vsum": ((1, sums), f32),
    }
    scratch = {
        "hall": ((everyone // BLK, BLK, width), b16),
        "gall": ((everyone // BLK, BLK, width), b16),
        "wqs": ((shard, 3 * part), b16),
        "wus": ((shard, hidden), b16),
        "wq4": ((nz, shard, 3 * part), b16),
        "wu4": ((nz, shard, hidden), b16),
        "wd4": ((nz, shard, width), b16),
        "wo1": ((part, width), b16),
        "sm": ((1, small), f32),
        "sm4": ((nz, 1, small), f32),
        "vec": ((8, width), f32),
        "sums": ((8, width), f32),
        "q": ((everyone // BLK, BLK, part), b16),
        "k": ((everyone // BLK, BLK, part), b16),
        "v": ((everyone // BLK, BLK, part), b16),
        "kt": ((everyone // BLK, part, BLK), b16),
        "vt": ((everyone // BLK, part, BLK), b16),
        "att": ((rows, part), b16),
        "attt": ((part, rows), b16),
        "lse": ((8, rows), f32),
        "delta": ((8, rows), f32),
        "datt": ((rows, part), b16),
        "act": ((rows, hidden), b16),
        "du": ((rows, hidden), b16),
        "n": ((rows, width), b16),
        "gl": ((rows, width), b16),
        "outb": ((rows // BLK, BLK, width), b16),
        "e2": ((rows, width), f32),
        "dk": ((everyone, part), f32),
        "dv": ((everyone, part), f32),
        "dqt": ((part, rows), f32),
        "kvin": ((rows, 2 * part), b16),
        "otheirs": ((rows // BLK, BLK, width), b16),
        "ogot": ((rows // BLK, BLK, width), b16),
        "oland": ((6, BLK, width), b16),
        "eland": ((6, BLK, width), b16),
        "gq": ((nz, shard, 3 * part), b16),
        "gu": ((nz, shard, hidden), b16),
        "gd": ((nz, shard, width), b16),
        "go": ((part, width), b16),
        "tq": ((nz, half, 3 * part), b16),
        "uq": ((nz, half, 3 * part), b16),
        "tu": ((nz, half, hidden), b16),
        "uu": ((nz, half, hidden), b16),
        "td": ((nz, half, width), b16),
        "ud": ((nz, half, width), b16),
        "to": ((half, width), b16),
        "uo": ((nz, half, width), b16),
        "vout": ((nz, 1, sums), f32),
        "vline": ((nz, 1, sums), f32),
        "vsend": ((1, sums), f32),
        "vlast": ((1, sums), f32),
        "gown": ((sides, BLK, width), b16),
        "win": ((slices, shard, columns), b16),
        "vplane": ((2 * chips, 1, sums), f32),
    }
    names = [*inputs, *outputs, *scratch, "idx", "send_sems", "recv_sems", "local_sems", "window_sems"]
    results = pl.pallas_call(
        functools.partial(layer_kernel, nz, names),
        out_shape=tuple(jax.ShapeDtypeStruct(*leaf) for leaf in outputs.values()),
        in_specs=[SPECS.get(name, VMEM_SPEC) for name in inputs],
        out_specs=tuple(SPECS.get(name, VMEM_SPEC) for name in outputs),
        scratch_shapes=[pltpu.VMEM(*leaf) for leaf in scratch.values()]
        + [pltpu.SMEM((64,), jnp.int32)]
        + [pltpu.SemaphoreType.DMA((SEMAPHORES,))] * 2
        + [pltpu.SemaphoreType.DMA((16,))] * 2,
        compiler_params=pltpu.CompilerParams(
            collective_id=0, has_side_effects=True, vmem_limit_bytes=VMEM_LIMIT
        ),
        name="layer",
    )(*inputs.values())
    hidden_out, hidden_grad, fq, fu, fd, fo, vsum = results

    steps = 2
    some, few = shard // steps, local_rows // steps
    inner = half // some

    def pieces(cols):
        return pl.BlockSpec((1, chips, some, cols), lambda i: (i // inner, 0, i % inner, 0))

    def lines(count, cols):
        return pl.BlockSpec((count, cols), lambda i: (i, 0))

    def vector(count):
        return pl.BlockSpec((count,), lambda i: (0,))

    sizes = [shard] * 6 + [qkv_bias.shape[0], up_bias.shape[0]]
    grad_qkv, grad_up, grad_down, grad_out, hidden_out, hidden_grad, *vectors = pl.pallas_call(
        assemble_kernel,
        grid=(steps,),
        out_shape=(
            jax.ShapeDtypeStruct(qkv_weight.shape, f32),
            jax.ShapeDtypeStruct(up_weight.shape, f32),
            jax.ShapeDtypeStruct((chips, steps, some, width), f32),
            jax.ShapeDtypeStruct(out_weight.shape, f32),
            jax.ShapeDtypeStruct(h.shape, b16),
            jax.ShapeDtypeStruct(h.shape, f32),
        )
        + tuple(jax.ShapeDtypeStruct((size,), f32) for size in sizes),
        in_specs=[
            pieces(3 * part),
            pieces(hidden),
            pieces(width),
            pl.BlockSpec((1, some, width), lambda i: (i // inner, i % inner, 0)),
            lines(few, width),
            lines(few, width),
            pl.BlockSpec((1, sums), lambda i: (0, 0)),
        ],
        out_specs=(
            lines(some, qkv_weight.shape[1]),
            lines(some, up_weight.shape[1]),
            pl.BlockSpec((chips, 1, some, width), lambda i: (0, i, 0, 0)),
            lines(some, width),
            lines(few, width),
            lines(few, width),
        )
        + tuple(vector(size) for size in sizes),
        compiler_params=pltpu.CompilerParams(vmem_limit_bytes=56 * 1024 * 1024),
        name="assemble",
    )(fq, fu, fd, fo, hidden_out, hidden_grad, vsum)
    g_gain1, g_shift1, g_gain2, g_shift2, g_bout, g_bdown, g_bqkv, g_bup = vectors
    return (
        hidden_out[None],
        hidden_grad[None],
        g_gain1,
        g_shift1,
        grad_qkv,
        g_bqkv,
        grad_out,
        g_bout,
        g_gain2,
        g_shift2,
        grad_up,
        g_bup,
        grad_down.reshape(down_weight.shape),
        g_bdown,
    )


def sliced_fits(mesh):
    return mesh.shape["ctx"] == 8 and mesh.shape["fsdp"] == 4


def solution(mesh):
    in_specs = (
        P("fsdp", "ctx", None),
        P("fsdp"),
        P("fsdp"),
        P("fsdp", None),
        P("fsdp"),
        P("fsdp", None),
        P("fsdp"),
        P("fsdp"),
        P("fsdp"),
        P("fsdp", None),
        P("fsdp"),
        P("fsdp", None),
        P("fsdp"),
        P("fsdp", "ctx", None),
        P(),
    )
    out_specs = (
        P("fsdp", "ctx", None),
        P("fsdp", "ctx", None),
        P("fsdp"),
        P("fsdp"),
        P("fsdp", None),
        P("fsdp"),
        P("fsdp", None),
        P("fsdp"),
        P("fsdp"),
        P("fsdp"),
        P("fsdp", None),
        P("fsdp"),
        P("fsdp", None),
        P("fsdp"),
    )
    local = whole_parameter_layer
    if sliced_fits(mesh):
        local = functools.partial(sliced_layer, mesh.shape["fsdp"])
    return jax.shard_map(local, mesh=mesh, in_specs=in_specs, out_specs=out_specs, check_vma=False)
```

```python
import functools
import math
import types

import jax
import jax.numpy as jnp
import numpy as np
from jax import lax
from jax.experimental import pallas as pl
from jax.experimental.pallas import tpu as pltpu
from jax.sharding import PartitionSpec as P

H = 12
HD = 64
ROT = 16
BLK = 128


EPS = 1e-05
NEG = -1e30
SQRT_HALF = 0.7071067811865476
INV_ROOT_TWO_PI = 0.3989422804014327


def apply_layer_norm(values_in, norm_gain, norm_bias):
    centre = jnp.mean(values_in, axis=-1, keepdims=True)
    mean_removed = values_in - centre
    inverse_deviation = lax.rsqrt(
        jnp.mean(mean_removed * mean_removed, axis=-1, keepdims=True) + EPS
    )
    standardized = mean_removed * inverse_deviation
    return (standardized * norm_gain + norm_bias, standardized, inverse_deviation)


def layer_norm_backward(output_gradient, standardized, inverse_deviation, norm_gain):
    gain_scaled = output_gradient * norm_gain
    return inverse_deviation * (
        gain_scaled
        - jnp.mean(gain_scaled, axis=-1, keepdims=True)
        - standardized * jnp.mean(gain_scaled * standardized, axis=-1, keepdims=True)
    )


def gelu_exact(values_in):
    return 0.5 * values_in * (1.0 + lax.erf(values_in * SQRT_HALF))


def gelu_slope(values_in):
    return (
        0.5 * (1.0 + lax.erf(values_in * SQRT_HALF))
        + values_in * jnp.exp(-0.5 * values_in * values_in) * INV_ROOT_TWO_PI
    )


def rotary_tables(position_list):
    half_rot = ROT // 2
    inverse = jnp.power(jnp.float32(10000.0), -2.0 * jnp.arange(half_rot, dtype=jnp.float32) / ROT)
    angle = position_list.astype(jnp.float32)[:, None] * inverse[None, :]
    return (jnp.cos(angle)[:, None, :], jnp.sin(angle)[:, None, :])


def rotate(tensor, cosine, sine):
    half_rot = ROT // 2
    first_half = tensor[..., :half_rot]
    second_half = tensor[..., half_rot:ROT]
    return jnp.concatenate(
        [
            first_half * cosine - second_half * sine,
            second_half * cosine + first_half * sine,
            tensor[..., ROT:],
        ],
        axis=-1,
    )


def rotate_back(tensor, cosine, sine):
    half_rot = ROT // 2
    first_half = tensor[..., :half_rot]
    second_half = tensor[..., half_rot:ROT]
    return jnp.concatenate(
        [
            first_half * cosine + second_half * sine,
            second_half * cosine - first_half * sine,
            tensor[..., ROT:],
        ],
        axis=-1,
    )


def masked_logits(query_block, key_block, query_pos, key_pos):
    logits = jnp.einsum(
        "qhd,khd->hqk", query_block, key_block, preferred_element_type=jnp.float32
    ) * (1.0 / math.sqrt(HD))
    return jnp.where(key_pos[None, None, :] <= query_pos[None, :, None], logits, NEG)


def block_terms(
    query_block, dout_block, total_t, delta_t, query_pos, key_block, value_block, key_pos
):
    logits = masked_logits(query_block, key_block, query_pos, key_pos)
    probs_wide = jnp.exp(logits - total_t[:, :, None])
    dprobs = jnp.einsum("qhd,khd->hqk", dout_block, value_block, preferred_element_type=jnp.float32)
    d_logits = (probs_wide * (dprobs - delta_t[:, :, None]) * (1.0 / math.sqrt(HD))).astype(
        jnp.bfloat16
    )
    return (probs_wide.astype(jnp.bfloat16), d_logits)


def keep_state(state_in):
    return state_in


def forward_attention(query, keys_all, values_all, own_pos, all_pos):
    local_rows = query.shape[0]
    seq_rows = keys_all.shape[0]
    qstep = min(512, local_rows)
    kstep = min(512, seq_rows)
    latest = jnp.max(own_pos)

    def stats_step(number, state_in):
        key_block = lax.dynamic_slice_in_dim(keys_all, number * kstep, kstep, 0)
        key_pos = lax.dynamic_slice_in_dim(all_pos, number * kstep, kstep, 0)

        def stats_live(state_now):
            running_max, running_sum = state_now
            logits = masked_logits(query, key_block, own_pos, key_pos)
            new_max = jnp.maximum(running_max, jnp.max(logits, axis=-1))
            running_sum = running_sum * jnp.exp(running_max - new_max) + jnp.sum(
                jnp.exp(logits - new_max[:, :, None]), axis=-1
            )
            return (new_max, running_sum)

        return lax.cond(jnp.min(key_pos) <= latest, stats_live, keep_state, state_in)

    start_state = (jnp.full((H, qstep), NEG, jnp.float32), jnp.zeros((H, qstep), jnp.float32))
    running_max, running_sum = lax.fori_loop(0, seq_rows // kstep, stats_step, start_state)
    total_t = running_max + jnp.log(running_sum)

    def value_step(number, state_in):
        key_block = lax.dynamic_slice_in_dim(keys_all, number * kstep, kstep, 0)
        value_block = lax.dynamic_slice_in_dim(values_all, number * kstep, kstep, 0)
        key_pos = lax.dynamic_slice_in_dim(all_pos, number * kstep, kstep, 0)

        def value_live(state_now):
            logits = masked_logits(query, key_block, own_pos, key_pos)
            attn_probs = jnp.exp(logits - total_t[:, :, None]).astype(jnp.bfloat16)
            return state_now + jnp.einsum(
                "hqk,khd->qhd", attn_probs, value_block, preferred_element_type=jnp.float32
            )

        return lax.cond(jnp.min(key_pos) <= latest, value_live, keep_state, state_in)

    weighted = lax.fori_loop(
        0, seq_rows // kstep, value_step, jnp.zeros((qstep, H, HD), jnp.float32)
    )
    totals = total_t.T
    return (weighted, totals)


def query_grads(query, d_att, log_total, delta, own_pos, keys_all, values_all, all_pos):
    local_rows = query.shape[0]
    seq_rows = keys_all.shape[0]
    qstep = min(512, local_rows)
    kstep = min(512, seq_rows)
    key_grads = jnp.zeros((seq_rows, H, HD), jnp.float32)
    value_grads = jnp.zeros((seq_rows, H, HD), jnp.float32)
    total_t = log_total.T
    delta_t = delta.T
    latest = jnp.max(own_pos)

    def key_step(number, state_in):
        offset = number * kstep
        key_block = lax.dynamic_slice_in_dim(keys_all, offset, kstep, 0)
        value_block = lax.dynamic_slice_in_dim(values_all, offset, kstep, 0)
        key_pos = lax.dynamic_slice_in_dim(all_pos, offset, kstep, 0)

        def key_live(state_now):
            attn_probs, d_logits = block_terms(
                query, d_att, total_t, delta_t, own_pos, key_block, value_block, key_pos
            )
            d_query = state_now[0] + jnp.einsum(
                "hqk,khd->qhd", d_logits, key_block, preferred_element_type=jnp.float32
            )
            key_acc = state_now[1]
            value_acc = state_now[2]
            key_part = jnp.einsum(
                "hqk,qhd->khd", d_logits, query, preferred_element_type=jnp.float32
            )
            value_part = jnp.einsum(
                "hqk,qhd->khd", attn_probs, d_att, preferred_element_type=jnp.float32
            )
            key_acc = lax.dynamic_update_slice_in_dim(
                key_acc, lax.dynamic_slice_in_dim(key_acc, offset, kstep, 0) + key_part, offset, 0
            )
            value_acc = lax.dynamic_update_slice_in_dim(
                value_acc,
                lax.dynamic_slice_in_dim(value_acc, offset, kstep, 0) + value_part,
                offset,
                0,
            )
            return (d_query, key_acc, value_acc)

        return lax.cond(jnp.min(key_pos) <= latest, key_live, keep_state, state_in)

    start_state = (jnp.zeros((qstep, H, HD), jnp.float32),) + (key_grads, value_grads)
    result = lax.fori_loop(0, seq_rows // kstep, key_step, start_state)
    pieces = result[0]
    key_grads = result[1]
    value_grads = result[2]
    return (pieces, key_grads, value_grads)


def whole_parameter_layer(
    hidden_in,
    norm1_gain,
    attention_norm_bias,
    qkv_weight,
    qkv_bias,
    out_weight,
    out_bias,
    norm2_gain,
    feedforward_norm_bias,
    up_weight,
    up_bias,
    down_weight,
    down_bias,
    cotangent,
    block_order,
):
    (
        attention_norm_gain,
        attention_bias_term,
        wqkv,
        bqkv,
        wout,
        bout,
        feedforward_norm_gain,
        feedforward_bias_term,
        wup,
        bup,
        wdown,
        bdown,
    ) = (
        lax.all_gather(norm1_gain, "fsdp", axis=0, tiled=True),
        lax.all_gather(attention_norm_bias, "fsdp", axis=0, tiled=True),
        lax.all_gather(qkv_weight, "fsdp", axis=0, tiled=True),
        lax.all_gather(qkv_bias, "fsdp", axis=0, tiled=True),
        lax.all_gather(out_weight, "fsdp", axis=0, tiled=True),
        lax.all_gather(out_bias, "fsdp", axis=0, tiled=True),
        lax.all_gather(norm2_gain, "fsdp", axis=0, tiled=True),
        lax.all_gather(feedforward_norm_bias, "fsdp", axis=0, tiled=True),
        lax.all_gather(up_weight, "fsdp", axis=0, tiled=True),
        lax.all_gather(up_bias, "fsdp", axis=0, tiled=True),
        lax.all_gather(down_weight, "fsdp", axis=0, tiled=True),
        lax.all_gather(down_bias, "fsdp", axis=0, tiled=True),
    )
    width = H * HD
    hidden_rows = hidden_in[0]
    cotan_rows = cotangent[0]
    local_rows = hidden_rows.shape[0]
    ctx_count = lax.axis_size("ctx")
    ctx_rank = lax.axis_index("ctx")
    seq_rows = local_rows * ctx_count
    all_pos = (block_order[:, None] * BLK + jnp.arange(BLK, dtype=jnp.int32)[None, :]).reshape(
        seq_rows
    )
    own_pos = lax.dynamic_slice_in_dim(all_pos, ctx_rank * local_rows, local_rows, 0)
    cosine, sine = rotary_tables(own_pos)
    attention_norm_gain = attention_norm_gain.astype(jnp.float32)
    feedforward_norm_gain = feedforward_norm_gain.astype(jnp.float32)
    residual_stream = hidden_rows.astype(jnp.float32)
    attention_normed, attention_standardized, attention_inverse_deviation = apply_layer_norm(
        residual_stream, attention_norm_gain, attention_bias_term.astype(jnp.float32)
    )
    normed1_b = attention_normed.astype(jnp.bfloat16)
    projected = jnp.dot(normed1_b, wqkv, preferred_element_type=jnp.float32) + bqkv.astype(
        jnp.float32
    )
    query = rotate(projected[:, :width].reshape(local_rows, H, HD), cosine, sine).astype(
        jnp.bfloat16
    )
    key_rows = rotate(
        projected[:, width : 2 * width].reshape(local_rows, H, HD), cosine, sine
    ).astype(jnp.bfloat16)
    value_rows = projected[:, 2 * width :].astype(jnp.bfloat16)
    keys_all, values_all = (
        lax.all_gather(key_rows.reshape(local_rows, width), "ctx", axis=0, tiled=True),
        lax.all_gather(value_rows, "ctx", axis=0, tiled=True),
    )
    keys_all = keys_all.reshape(seq_rows, H, HD)
    values_all = values_all.reshape(seq_rows, H, HD)
    attended, log_total = forward_attention(query, keys_all, values_all, own_pos, all_pos)
    attended_b = attended.reshape(local_rows, width).astype(jnp.bfloat16)
    attn_out = jnp.dot(attended_b, wout, preferred_element_type=jnp.float32) + bout.astype(
        jnp.float32
    )
    feedforward_normed, feedforward_standardized, feedforward_inverse_deviation = apply_layer_norm(
        residual_stream, feedforward_norm_gain, feedforward_bias_term.astype(jnp.float32)
    )
    normed2_b = feedforward_normed.astype(jnp.bfloat16)
    up_rows = jnp.dot(normed2_b, wup, preferred_element_type=jnp.float32) + bup.astype(jnp.float32)
    act_b = gelu_exact(up_rows).astype(jnp.bfloat16)
    mlp_out = jnp.dot(act_b, wdown, preferred_element_type=jnp.float32) + bdown.astype(jnp.float32)
    hidden_out = (residual_stream + attn_out + mlp_out).astype(jnp.bfloat16)
    cotan_wide = cotan_rows.astype(jnp.float32)
    grad_wdown = jnp.einsum("tk,tn->kn", act_b, cotan_rows, preferred_element_type=jnp.float32)
    grad_bdown = jnp.sum(cotan_wide, axis=0)
    d_up = jnp.einsum(
        "tn,kn->tk", cotan_rows, wdown, preferred_element_type=jnp.float32
    ) * gelu_slope(up_rows)
    d_up16 = d_up.astype(jnp.bfloat16)
    grad_wup = jnp.einsum("tk,tn->kn", normed2_b, d_up16, preferred_element_type=jnp.float32)
    grad_bup = jnp.sum(d_up, axis=0)
    grad_feedforward_normed = jnp.einsum(
        "tn,kn->tk", d_up16, wup, preferred_element_type=jnp.float32
    )
    grad_feedforward_gain = jnp.sum(grad_feedforward_normed * feedforward_standardized, axis=0)
    grad_shift2 = jnp.sum(grad_feedforward_normed, axis=0)
    feedforward_branch_grad = layer_norm_backward(
        grad_feedforward_normed,
        feedforward_standardized,
        feedforward_inverse_deviation,
        feedforward_norm_gain,
    )
    grad_wout = jnp.einsum("tk,tn->kn", attended_b, cotan_rows, preferred_element_type=jnp.float32)
    d_att = jnp.einsum("tn,kn->tk", cotan_rows, wout, preferred_element_type=jnp.float32).astype(
        jnp.bfloat16
    )
    delta = jnp.sum(
        d_att.reshape(local_rows, H, HD).astype(jnp.float32)
        * attended_b.reshape(local_rows, H, HD).astype(jnp.float32),
        axis=-1,
    )
    d_att3 = d_att.reshape(local_rows, H, HD)
    d_query, key_grads, value_grads = query_grads(
        query, d_att3, log_total, delta, own_pos, keys_all, values_all, all_pos
    )
    d_key, d_value = (
        lax.psum_scatter(
            key_grads.reshape(seq_rows, width), "ctx", scatter_dimension=0, tiled=True
        ),
        lax.psum_scatter(
            value_grads.reshape(seq_rows, width), "ctx", scatter_dimension=0, tiled=True
        ),
    )
    d_query = rotate_back(d_query, cosine, sine)
    d_key = rotate_back(d_key.reshape(local_rows, H, HD), cosine, sine)
    d_qkv = jnp.concatenate(
        [d_query.reshape(local_rows, width), d_key.reshape(local_rows, width), d_value], axis=1
    )
    d_qkv16 = d_qkv.astype(jnp.bfloat16)
    grad_wqkv = jnp.einsum("tk,tn->kn", normed1_b, d_qkv16, preferred_element_type=jnp.float32)
    grad_bqkv = jnp.sum(d_qkv, axis=0)
    grad_attention_normed = jnp.einsum(
        "tn,kn->tk", d_qkv16, wqkv, preferred_element_type=jnp.float32
    )
    grad_attention_gain = jnp.sum(grad_attention_normed * attention_standardized, axis=0)
    grad_shift1 = jnp.sum(grad_attention_normed, axis=0)
    attention_branch_grad = layer_norm_backward(
        grad_attention_normed,
        attention_standardized,
        attention_inverse_deviation,
        attention_norm_gain,
    )
    hidden_grad = cotan_wide + attention_branch_grad + feedforward_branch_grad
    terms = (
        grad_attention_gain,
        grad_shift1,
        grad_wqkv,
        grad_bqkv,
        grad_wout,
        grad_bdown,
        grad_feedforward_gain,
        grad_shift2,
        grad_wup,
        grad_bup,
        grad_wdown,
        grad_bdown,
    )
    shares = (
        lax.psum_scatter(terms[0], "fsdp", scatter_dimension=0, tiled=True),
        lax.psum_scatter(terms[1], "fsdp", scatter_dimension=0, tiled=True),
        lax.psum_scatter(terms[2], "fsdp", scatter_dimension=0, tiled=True),
        lax.psum_scatter(terms[3], "fsdp", scatter_dimension=0, tiled=True),
        lax.psum_scatter(terms[4], "fsdp", scatter_dimension=0, tiled=True),
        lax.psum_scatter(terms[5], "fsdp", scatter_dimension=0, tiled=True),
        lax.psum_scatter(terms[6], "fsdp", scatter_dimension=0, tiled=True),
        lax.psum_scatter(terms[7], "fsdp", scatter_dimension=0, tiled=True),
        lax.psum_scatter(terms[8], "fsdp", scatter_dimension=0, tiled=True),
        lax.psum_scatter(terms[9], "fsdp", scatter_dimension=0, tiled=True),
        lax.psum_scatter(terms[10], "fsdp", scatter_dimension=0, tiled=True),
        lax.psum_scatter(terms[11], "fsdp", scatter_dimension=0, tiled=True),
    )
    shares = lax.psum(
        (
            shares[0],
            shares[1],
            shares[2],
            shares[3],
            shares[4],
            shares[5],
            shares[6],
            shares[7],
            shares[8],
            shares[9],
            shares[10],
            shares[11],
        ),
        "ctx",
    )
    return (
        hidden_out[None],
        hidden_grad[None],
        shares[0],
        shares[1],
        shares[2],
        shares[3],
        shares[4],
        shares[5],
        shares[6],
        shares[7],
        shares[8],
        shares[9],
        shares[10],
        shares[11],
    )


MESH_IDS = pl.DeviceIdType.MESH
NN = (((1,), (0,)), ((), ()))
NT = (((1,), (1,)), ((), ()))
TN = (((0,), (0,)), ((), ()))
QTILE = 256
SEMAPHORES = 192


def mm(left, right, dims=NN):
    return lax.dot_general(left, right, dims, preferred_element_type=jnp.float32)


def flip(index, bit):
    return index + bit - 2 * bit * ((index // bit) % 2)


def run_when(condition, action):
    if condition is None:
        action()
    else:
        pl.when(condition)(action)


def narrow(values):
    return values.astype(jnp.bfloat16)


def wide(values):
    return values.astype(jnp.float32)


class Copies:
    def __init__(self, send_sems, recv_sems):
        self.send_sems, self.recv_sems = send_sems, recv_sems
        self.count, self.started, self.numbers = 0, [], {}

    def make(self, source, target, device, when=None, like=None):
        if like is None:
            number = self.count
            self.count += 1
        else:
            number = self.numbers[id(like)]
        copy = pltpu.make_async_remote_copy(
            src_ref=source,
            dst_ref=target,
            send_sem=self.send_sems.at[number],
            recv_sem=self.recv_sems.at[number],
            device_id=device,
            device_id_type=MESH_IDS,
        )
        self.started.append((copy, when))
        self.numbers[id(copy)] = number
        return copy

    def settle(self, chosen):
        numbers = {id(copy) for copy in chosen}
        for copy, when in self.started:
            if id(copy) in numbers:
                run_when(when, copy.wait_send)
        self.started = [entry for entry in self.started if id(entry[0]) not in numbers]

    def finish(self):
        for copy, when in self.started:
            run_when(when, copy.wait_send)


class Place:
    def __init__(self, nz):
        self.nz = nz
        self.c, self.z = lax.axis_index("ctx"), lax.axis_index("fsdp")
        self.k, self.t = self.c % 2, self.c // 2
        self.xn, self.yn, self.pn = flip(self.c, 2), flip(self.c, 4), flip(self.c, 1)
        self.dn = flip(self.xn, 4)
        self.tx, self.ty = flip(self.t, 1), flip(self.t, 2)
        self.td = flip(self.tx, 2)
        self.others = [(self.z + d) % nz for d in range(1, nz)]
        self.plane = [self.xn, self.yn, self.dn, self.pn] + [
            flip(peer, 1) for peer in (self.xn, self.yn, self.dn)
        ]
        self.above, self.below = jnp.minimum(self.z + 1, nz - 1), jnp.maximum(self.z - 1, 0)

    def on_plane(self, c):
        return (c, self.z)

    def on_line(self, z):
        return (self.c, z)

    def greet(self):
        barrier = pltpu.get_barrier_semaphore()
        peers = [self.on_plane(peer) for peer in self.plane] + [self.on_line(z) for z in self.others]
        for peer in peers:
            pl.semaphore_signal(barrier, inc=1, device_id=peer, device_id_type=MESH_IDS)
        pl.semaphore_wait(barrier, len(peers))


class PlaneShare:
    def __init__(self, copies, me, source, slot, rows):
        self.copies, self.me, self.slot = copies, me, slot
        top, bottom = pl.ds(0, rows // 2), pl.ds(rows // 2, rows // 2)
        own = slot(me.k, me.t)
        to_x, to_y = me.on_plane(me.xn), me.on_plane(me.yn)
        self.x_first = copies.make(source.at[top], own.at[top], to_x)
        self.y_first = copies.make(source.at[bottom], own.at[bottom], to_y)
        self.x_second = copies.make(source.at[bottom], own.at[bottom], to_x)
        self.y_second = copies.make(source.at[top], own.at[top], to_y)
        self.to_p = copies.make(source, own, me.on_plane(me.pn))
        through_x, through_y = slot(me.k, me.tx).at[top], slot(me.k, me.ty).at[bottom]
        self.hop_y = copies.make(through_x, through_x, to_y)
        self.hop_x = copies.make(through_y, through_y, to_x)
        self.swaps = []
        for chip in (me.tx, me.ty, me.td):
            place = slot(me.k, chip)
            self.swaps.append(copies.make(place, place, me.on_plane(me.pn)))

    def start(self):
        for copy in (self.x_first, self.y_first, self.x_second, self.y_second, self.to_p):
            copy.start()

    def relay(self):
        self.x_first.wait_recv()
        self.hop_y.start()
        self.y_first.wait_recv()
        self.hop_x.start()

    def swap(self):
        self.x_second.wait_recv()
        self.swaps[0].start()
        self.y_second.wait_recv()
        self.swaps[1].start()

    def on_diagonal(self):
        self.hop_y.wait_recv()
        self.hop_x.wait_recv()
        self.swaps[2].start()

    def finish(self):
        for copy in (self.to_p, *self.swaps):
            copy.wait_recv()


class LineGather:
    def __init__(self, copies, me, source, gathered):
        self.copies, self.me, self.gathered = copies, me, gathered
        rows = gathered.shape[1] // 2
        self.mine = pl.ds(me.k * rows, rows)
        self.moves, self.swaps = {}, []
        for step in range(me.nz - 1):
            for sign in (1, -1):
                shard, target = me.z - sign * step, me.z + sign
                ok = (shard >= 0) & (shard < me.nz) & (target >= 0) & (target < me.nz)
                place = self.slot(shard)
                copy = copies.make(
                    source.at[self.mine] if step == 0 else place,
                    place,
                    me.on_line(jnp.clip(target, 0, me.nz - 1)),
                    when=ok,
                )
                self.moves[step, sign] = (copy, ok)

    def slot(self, shard):
        return self.gathered.at[jnp.clip(shard, 0, self.me.nz - 1), self.mine]

    def start(self):
        for sign in (1, -1):
            copy, ok = self.moves[0, sign]
            run_when(ok, copy.start)

    def advance(self, step):
        me = self.me
        for sign in (1, -1):
            arrived = me.z - sign * (step + 1)
            ok = (arrived >= 0) & (arrived < me.nz)
            run_when(ok, self.moves[step, sign][0].wait_recv)
            if step + 1 < me.nz - 1:
                copy, following = self.moves[step + 1, sign]
                run_when(following, copy.start)
            place = self.slot(arrived)
            swap = self.copies.make(place, place, me.on_plane(me.pn), when=ok)
            run_when(ok, swap.start)
            self.swaps.append((swap, ok))

    def finish(self):
        for swap, ok in self.swaps:
            run_when(ok, swap.wait_recv)


class LineSend:
    def __init__(self, copies, me, source, gathered):
        self.me = me
        rows = gathered.shape[1] // 2
        mine = pl.ds(me.k * rows, rows)
        self.sends, self.swaps = [], []
        for distance, other in enumerate(me.others, 1):
            self.sends.append(
                copies.make(source.at[mine], gathered.at[me.z, mine], me.on_line(other))
            )
            place = gathered.at[(me.z - distance) % me.nz, mine]
            self.swaps.append(copies.make(place, place, me.on_plane(me.pn)))

    def start(self):
        for send in self.sends:
            send.start()

    def advance(self):
        for send, swap in zip(self.sends, self.swaps):
            send.wait_recv()
            swap.start()

    def finish(self):
        for swap in self.swaps:
            swap.wait_recv()


class LineSpread:
    def __init__(self, copies, me, source, target, sem):
        self.me = me
        self.keep = pltpu.make_async_copy(source, target, sem)
        rows = target.shape[0] // 2
        mine = pl.ds(me.k * rows, rows)
        self.here, self.away = me.z == me.t, me.z != me.t
        place = target.at[mine]
        self.sends, self.arrivals = [], []
        for distance in range(1, me.nz):
            target_z = (me.t + distance) % me.nz
            copy = copies.make(source.at[mine], place, me.on_line(target_z), when=self.here)
            self.sends.append(copy)
            self.arrivals.append(me.z == target_z)
        self.swap = copies.make(place, place, me.on_plane(me.pn), when=self.away)

    def start(self):
        @pl.when(self.here)
        def _():
            for copy in self.sends:
                copy.start()
            self.keep.start()

    def advance(self):
        for copy, arrives in zip(self.sends, self.arrivals):
            pl.when(arrives)(copy.wait_recv)
        pl.when(self.away)(self.swap.start)

    def finish(self):
        pl.when(self.here)(self.keep.wait)
        pl.when(self.away)(self.swap.wait_recv)


class LineReduce:
    def __init__(self, copies, me, source, total, landed):
        self.me, self.source, self.total, self.landed = me, source, total, landed
        half = total.shape[1]
        self.mine, theirs = pl.ds(me.k * half, half), pl.ds((1 - me.k) * half, half)
        self.exchange = copies.make(source.at[:, theirs], total, me.on_plane(me.pn))
        self.sends = [
            copies.make(total.at[other], landed.at[me.z], me.on_line(other)) for other in me.others
        ]

    def start(self):
        self.exchange.start()

    def pair(self):
        self.exchange.wait_recv()
        for owner in range(self.me.nz):
            self.total[owner] = narrow(
                wide(self.total[owner]) + wide(self.source[owner, self.mine])
            )
        for send in self.sends:
            send.start()

    def collect(self):
        me = self.me
        result = wide(self.total[me.z])
        for send in self.sends:
            send.wait_recv()
        for other in me.others:
            result = result + wide(self.landed[other])
        self.total[me.z] = narrow(result)


class LineCollect:
    def __init__(self, copies, me, source, total, landed):
        self.me, self.source, self.total, self.landed = me, source, total, landed
        half = total.shape[0]
        self.mine, theirs = pl.ds(me.k * half, half), pl.ds((1 - me.k) * half, half)
        self.exchange = copies.make(source.at[theirs], total, me.on_plane(me.pn))
        self.sends = []
        for distance in range(1, me.nz):
            leaves = (me.z + distance) % me.nz == me.t
            copy = copies.make(total, landed.at[me.z], me.on_line(me.t), when=leaves)
            self.sends.append((copy, leaves))

    def start(self):
        self.exchange.start()

    def pair(self):
        self.exchange.wait_recv()
        self.total[...] = narrow(wide(self.total[...]) + wide(self.source[self.mine]))
        for copy, leaves in self.sends:
            pl.when(leaves)(copy.start)

    def collect(self):
        me = self.me

        @pl.when(me.z == me.t)
        def _():
            result = wide(self.total[...])
            for copy, _ in self.sends:
                copy.wait_recv()
            for other in me.others:
                result = result + wide(self.landed[other])
            self.total[...] = narrow(result)


class PlaneSpread:
    def __init__(self, copies, me, source, target, rows, sem):
        self.me = me
        self.keep = pltpu.make_async_copy(source, target.at[me.k], sem)
        top, bottom = pl.ds(0, rows // 2), pl.ds(rows // 2, rows // 2)
        place = target.at[me.k]
        self.here, self.from_x, self.from_y = me.t == me.z, me.tx == me.z, me.ty == me.z
        self.from_d = me.td == me.z
        self.to_x = copies.make(source, place, me.on_plane(me.xn), when=self.here)
        self.to_y = copies.make(source, place, me.on_plane(me.yn), when=self.here)
        self.to_p = copies.make(source, place, me.on_plane(me.pn), when=self.here)
        self.hop_y = copies.make(place.at[top], place.at[top], me.on_plane(me.yn), when=self.from_x)
        self.hop_x = copies.make(
            place.at[bottom], place.at[bottom], me.on_plane(me.xn), when=self.from_y
        )
        away = self.from_x | self.from_y | self.from_d
        self.away = away
        self.swap = copies.make(place, place, me.on_plane(me.pn), when=away, like=self.to_p)

    def start(self):
        @pl.when(self.here)
        def _():
            self.to_x.start()
            self.to_y.start()
            self.to_p.start()
            self.keep.start()

    def advance(self):
        @pl.when(self.from_x)
        def _():
            self.to_x.wait_recv()
            self.hop_y.start()
            self.swap.start()

        @pl.when(self.from_y)
        def _():
            self.to_y.wait_recv()
            self.hop_x.start()
            self.swap.start()

    def on_diagonal(self):
        @pl.when(self.from_d)
        def _():
            self.hop_y.wait_recv()
            self.hop_x.wait_recv()
            self.swap.start()

    def finish(self):
        pl.when(self.here)(self.keep.wait)
        self.to_p.wait_recv()

def norm_rows(values_in):
    centre = jnp.mean(values_in, axis=-1, keepdims=True)
    mean_removed = values_in - centre
    inverse_deviation = lax.rsqrt(
        jnp.mean(mean_removed * mean_removed, axis=-1, keepdims=True) + EPS
    )
    return mean_removed * inverse_deviation, inverse_deviation


def head_rows(rows, head):
    lanes = lax.broadcasted_iota(jnp.int32, rows.shape, 1)
    inside = (lanes >= head * HD) & (lanes < (head + 1) * HD)
    return jnp.where(inside, rows, jnp.zeros_like(rows))


def rope_lanes(r, blocks, columns, back):
    half_rot = ROT // 2
    tables = [[], [], []]
    row_cos, row_sin = r.rope_r[:, :128], r.rope_r[:, 128:]
    lane = lax.broadcasted_iota(jnp.int32, row_cos.shape, 1) % HD
    for block in blocks:
        both = r.rope_b[block]
        block_cos, block_sin = both[:, :128], both[:, 128:]
        cosine = block_cos * row_cos - block_sin * row_sin
        sine = block_sin * row_cos + block_cos * row_sin
        if back:
            sine = -sine
        tables[0].append(cosine)
        tables[1].append(jnp.where(lane < half_rot, -sine, 0.0))
        tables[2].append(jnp.where(lane >= half_rot, sine, 0.0))
    stacked = [jnp.concatenate(table, axis=0) for table in tables]
    return [jnp.concatenate([table] * (columns // 128), axis=1) for table in stacked]


def turn(values, tables):
    columns, half_rot = values.shape[1], ROT // 2
    return (
        values * tables[0]
        + pltpu.roll(values, columns - half_rot, 1) * tables[1]
        + pltpu.roll(values, half_rot, 1) * tables[2]
    )


def windows(r, me):
    part = r.wqs.shape[1] // 3
    chips, columns = me.nz, r.win.shape[2]
    copies = []
    for source, pieces in ((r.wqkv, 3), (r.wup, r.wus.shape[1] // part)):
        for piece in range(pieces):
            first = (piece * chips + me.t) * part // 128 * 128
            number = len(copies)
            copies.append(
                pltpu.make_async_copy(
                    source.at[:, pl.ds(pl.multiple_of(first, 128), columns)],
                    r.win.at[number],
                    r.window_sems.at[number],
                )
            )
    return copies


def slice_weights(r, me):
    part = r.wqs.shape[1] // 3
    for chip in range(me.nz):

        @pl.when(me.t == chip)
        def _():
            first = chip * part % 128
            number = 0
            for target in (r.wqs, r.wus):
                for piece in range(target.shape[1] // part):
                    target[:, piece * part : (piece + 1) * part] = r.win[
                        number, :, first : first + part
                    ]
                    number += 1


VECTORS = ("gain1", "shift1", "gain2", "shift2", "bout", "bdown", "bqkv", "bup")


def pack_vectors(r):
    first = 0
    for name in VECTORS:
        values = wide(getattr(r, name)[...])
        count = values.shape[0]
        r.sm[0:1, first : first + count] = values.reshape(1, count)
        first += count


def read_vectors(r, me):
    nz, part = me.nz, r.vec.shape[1] // me.nz

    def piece(z, number):
        return r.sm4[z, 0:1, number * part : (number + 1) * part]

    for z in range(nz):
        span = slice(z * part, (z + 1) * part)
        for row in range(4):
            r.vec[row : row + 1, span] = piece(z, row)
        r.vec[4:5, span] = piece(z, 4) + piece(z, 5)
    chips = nz
    for chip in range(chips):

        @pl.when(me.t == chip)
        def _():
            for number in range(3):
                held = number * chips + chip
                r.vec[5:6, number * part : (number + 1) * part] = piece(held // 3, 6 + held % 3)
            for z in range(nz):
                r.vec[6:7, z * part : (z + 1) * part] = piece(z, 9 + chip)


def block_table(r, me):
    count = r.order.shape[0]
    chips, quarter = me.nz, count // 4
    sides = count // (2 * chips)
    held = [r.order[number] for number in range(count)]
    for position in range(count):
        found = 0
        for number in range(1, count):
            found = jnp.where(held[number] == position, number, found)
        r.idx[position] = found
    for chip in range(chips):
        for holder, first in ((me.k, count), (1 - me.k, count + chips * sides)):
            for side in range(sides):
                position = r.order[(2 * chip + me.k) * sides + side]
                low = (position >= quarter * holder) & (position < quarter * (holder + 1))
                near = position - quarter * holder
                high = position - 2 * quarter + quarter * holder
                r.idx[first + chip * sides + side] = jnp.clip(
                    jnp.where(low, near, high), 0, 2 * quarter - 1
                )
        position = r.order[(2 * chip + me.k) * sides]
        outer = jnp.where((position < quarter) | (position >= 3 * quarter), 0, 1)
        r.idx[count + 2 * chips * sides + chip] = jnp.where(outer == me.k, 1, 0)


def sorted_rows(r, source, block, blocks):
    pieces = []
    for number in range(blocks):
        pieces.append(source[r.idx[block + number]])
    return jnp.concatenate(pieces, axis=0)


def flat_rows(values):
    return values.reshape(-1, values.shape[-1])


def put_blocks(target, tile, values):
    blocks = values.shape[0] // BLK
    target[pl.ds(tile * blocks, blocks)] = values.reshape(blocks, BLK, values.shape[1])


def prepare(r, chip, target, at):
    sides = r.h.shape[0]
    rows = sides * BLK

    @pl.loop(0, 2)
    def _(core):
        values = flat_rows(r.hall[pl.ds((2 * chip + core) * sides, sides)])
        standardized, _ = norm_rows(wide(values))
        place = pl.ds(pl.multiple_of(at + core * rows, rows), rows)
        target[place, :] = narrow(standardized * r.vec[0:1, :] + r.vec[1:2, :])


def project(r, chip, source, at):
    part = r.wqs.shape[1] // 3
    blocks = 2 * r.h.shape[0]
    first = chip * blocks
    weight = r.wq4[...].reshape(-1, 3 * part)
    projected = mm(source[at : at + blocks * BLK, :], weight) + r.vec[5:6, : 3 * part]
    positions = [r.order[first + number] for number in range(blocks)]
    turned = turn(projected[:, : 2 * part], rope_lanes(r, positions, 2 * part, False))
    keys, values = turned[:, part:], projected[:, 2 * part :]
    query = narrow(wide(narrow(turned[:, :part])) * HD**-0.5)
    for number in range(blocks):
        own = slice(number * BLK, (number + 1) * BLK)
        r.q[first + number] = query[own]
        r.k[first + number] = narrow(keys[own])
        r.v[first + number] = narrow(values[own])
        r.kt[first + number] = narrow(keys[own].T)
        r.vt[first + number] = narrow(values[own].T)


def sorted_columns(r, source, head, block, blocks):
    lanes = slice(head * HD, (head + 1) * HD)
    return jnp.concatenate(
        [source[r.idx[block + number], lanes, :] for number in range(blocks)], axis=1
    )


def tile_start(r, me, tile):
    quarter = r.k.shape[0] * BLK // 4
    low = tile < quarter // QTILE
    inside = tile * QTILE - jnp.where(low, 0, quarter)
    return jnp.where(low, quarter * me.k, 3 * quarter - quarter * me.k) + inside


def attend(r, me, tile):
    part = r.k.shape[2]
    blocks = QTILE // BLK
    heads = part // HD
    start = tile_start(r, me, tile)
    rows = slice(tile * QTILE, (tile + 1) * QTILE)
    query = sorted_rows(r, r.q, start // BLK, blocks)
    per_head = [head_rows(query, head) for head in range(heads)]

    def visit(number, state, masked):
        keys = sorted_rows(r, r.k, number * blocks, blocks)
        result = []
        for head in range(heads):
            top, total, acc = state[head]
            logits = mm(keys, per_head[head], NT)
            if masked:
                key_row = lax.broadcasted_iota(jnp.int32, logits.shape, 0)
                query_row = lax.broadcasted_iota(jnp.int32, logits.shape, 1)
                logits = jnp.where(key_row <= query_row, logits, NEG)
            new_top = jnp.maximum(top, jnp.max(logits, axis=0, keepdims=True))
            fade = jnp.exp(top - new_top)
            probs = jnp.exp(logits - new_top)
            total = total * fade + jnp.sum(probs, axis=0, keepdims=True)
            values = sorted_columns(r, r.vt, head, number * blocks, blocks)
            acc = acc * fade + mm(values, narrow(probs))
            result.append((new_top, total, acc))
        return tuple(result)

    state = tuple(
        (
            jnp.full((1, QTILE), NEG, jnp.float32),
            jnp.zeros((1, QTILE), jnp.float32),
            jnp.zeros((HD, QTILE), jnp.float32),
        )
        for _ in range(heads)
    )
    last = start // QTILE
    state = lax.fori_loop(0, last, lambda n, s: visit(n, s, False), state)
    state = visit(last, state, True)
    merged = jnp.concatenate([acc / total for _, total, acc in state], axis=0)
    r.att[rows, :] = narrow(merged.T)
    r.attt[:, rows] = narrow(merged)
    for head in range(heads):
        r.lse[head : head + 1, rows] = state[head][0] + jnp.log(state[head][1])


def feed_forward(r, me, tile):
    place = pl.ds(pl.multiple_of(tile * QTILE, QTILE), QTILE)
    blocks = QTILE // BLK
    block = tile_start(r, me, tile) // BLK
    width = r.hall.shape[2]
    standardized, _ = norm_rows(wide(sorted_rows(r, r.hall, block, blocks)))
    cotan = sorted_rows(r, r.gall, block, blocks)
    gain2 = r.vec[2:3, :]
    normed = narrow(standardized * gain2 + r.vec[3:4, :])
    up_weight = r.wu4[...].reshape(width, -1)
    down_weight = r.wd4[...].reshape(-1, width)
    up = mm(normed, up_weight) + r.vec[6:7, :]
    below = 0.5 * (1.0 + lax.erf(up * SQRT_HALF))
    act = narrow(up * below)
    slope = below + up * jnp.exp(-0.5 * up * up) * INV_ROOT_TWO_PI
    d_up = mm(cotan, down_weight, NT) * slope
    d_up16 = narrow(d_up)
    put_blocks(r.outb, tile, narrow(mm(act, down_weight)))
    d_normed = mm(d_up16, up_weight, NT)
    r.sums[2:3, :] += jnp.sum(d_normed * standardized, axis=0, keepdims=True)
    r.sums[3:4, :] += jnp.sum(d_normed, axis=0, keepdims=True)
    r.sums[6:7, :] += jnp.sum(d_up, axis=0, keepdims=True)
    r.e2[place, :] = d_normed * gain2
    r.n[place, :] = normed
    r.gl[place, :] = cotan
    r.act[place, :] = act
    r.du[place, :] = d_up16


def out_project(r, me, tile):
    place = pl.ds(pl.multiple_of(tile * QTILE, QTILE), QTILE)
    blocks = QTILE // BLK
    attended = r.att[place, :]
    mlp = flat_rows(r.outb[pl.ds(tile * blocks, blocks)])
    put_blocks(r.outb, tile, narrow(wide(mlp) + mm(attended, r.wo1[...])))
    cotan = r.gl[place, :]
    r.datt[place, :] = narrow(mm(cotan, r.wo1[...], NT))
    product = wide(narrow(mm(r.wo1[...], cotan, NT))) * wide(r.attt[:, place])
    for head in range(product.shape[0] // HD):
        r.delta[head : head + 1, place] = jnp.sum(
            product[head * HD : (head + 1) * HD], axis=0, keepdims=True
        )


def weight_grad(target, left, right):
    rows, columns = left.shape[1], right.shape[1]
    shard = target.shape[1]
    values = right[...]
    for first in range(0, rows, QTILE):
        result = narrow(mm(left[:, first : first + QTILE], values, TN))
        at = first
        while at < first + QTILE:
            owner, inside = at // shard, at % shard
            until = min((owner + 1) * shard, first + QTILE)
            target[owner, inside : inside + until - at, :] = result[at - first : until - first, :]
            at = until


def attend_grad(r, me, tile):
    part = r.k.shape[2]
    heads = part // HD
    kstep = 2 * QTILE
    start = tile_start(r, me, tile)
    rows = slice(tile * QTILE, (tile + 1) * QTILE)
    blocks = kstep // BLK
    query = sorted_rows(r, r.q, start // BLK, QTILE // BLK)
    d_out = r.datt[rows, :]
    queries = jnp.concatenate([head_rows(query, head) for head in range(heads)], axis=0)
    d_outs = jnp.concatenate([head_rows(d_out, head) for head in range(heads)], axis=0)

    def visit(number, state, masked):
        place = pl.ds(pl.multiple_of(number * kstep, kstep), kstep)
        keys = sorted_rows(r, r.k, number * blocks, blocks)
        values = sorted_rows(r, r.v, number * blocks, blocks)
        probs_all, d_logits_all, result = [], [], []
        for head in range(heads):
            own = slice(head * QTILE, (head + 1) * QTILE)
            logits = mm(keys, queries[own], NT)
            probs = jnp.exp(logits - r.lse[head : head + 1, rows])
            if masked:
                key_row = number * kstep + lax.broadcasted_iota(jnp.int32, logits.shape, 0)
                query_row = start + lax.broadcasted_iota(jnp.int32, logits.shape, 1)
                probs = jnp.where(key_row <= query_row, probs, 0.0)
            d_probs = mm(values, d_outs[own], NT)
            d_logits = narrow(probs * (d_probs - r.delta[head : head + 1, rows]))
            probs_all.append(narrow(probs))
            d_logits_all.append(d_logits)
            columns = sorted_columns(r, r.kt, head, number * blocks, blocks)
            result.append(state[head] + mm(columns, d_logits))
        r.dv[place, :] += mm(jnp.concatenate(probs_all, axis=1), d_outs)
        r.dk[place, :] += mm(jnp.concatenate(d_logits_all, axis=1), queries)
        return tuple(result)

    state = tuple(jnp.zeros((HD, QTILE), jnp.float32) for _ in range(heads))
    last = start // kstep
    state = lax.fori_loop(0, last, lambda n, s: visit(n, s, False), state)
    state = visit(last, state, True)
    r.dqt[:, rows] = jnp.concatenate(state, axis=0)


def qkv_grad(r, me, tile):
    place = pl.ds(pl.multiple_of(tile * QTILE, QTILE), QTILE)
    part = r.k.shape[2]
    blocks = QTILE // BLK
    start = tile_start(r, me, tile)
    block = start // BLK
    held = pl.ds(pl.multiple_of(start, QTILE), QTILE)
    standardized, _ = norm_rows(wide(sorted_rows(r, r.hall, block, blocks)))
    gain1 = r.vec[0:1, :]
    r.n[place, :] = narrow(standardized * gain1 + r.vec[1:2, :])
    d_query = r.dqt[:, place].T * HD**-0.5
    d_key = r.dk[held, :] + wide(r.kvin[place, :part])
    d_value = r.dv[held, :] + wide(r.kvin[place, part:])
    turned = turn(
        jnp.concatenate([d_query, d_key], axis=1),
        rope_lanes(r, [block + n for n in range(blocks)], 2 * part, True),
    )
    d_qkv = jnp.concatenate([turned, d_value], axis=1)
    d_qkv16 = narrow(d_qkv)
    r.du[place, : 3 * part] = d_qkv16
    r.sums[5:6, : 3 * part] += jnp.sum(d_qkv, axis=0, keepdims=True)
    weight = r.wq4[...].reshape(-1, 3 * part)
    d_normed = mm(d_qkv16, weight, NT)
    r.sums[0:1, :] += jnp.sum(d_normed * standardized, axis=0, keepdims=True)
    r.sums[1:2, :] += jnp.sum(d_normed, axis=0, keepdims=True)
    put_blocks(r.outb, tile, narrow(d_normed * gain1 + r.e2[place, :]))


def gather_sums(r, me):
    nz, part = me.nz, r.vec.shape[1] // me.nz
    r.sums[4:5, :] = jnp.sum(wide(flat_rows(r.gown[...])), axis=0, keepdims=True)

    def put(z, number, values):
        r.vout[z, 0:1, number * part : (number + 1) * part] = values

    for z in range(nz):
        for row in range(5):
            put(z, row, r.sums[row : row + 1, z * part : (z + 1) * part])
    for chip in range(nz):

        @pl.when(me.t == chip)
        def _():
            for number in range(3):
                held = number * nz + chip
                put(held // 3, 5 + held % 3, r.sums[5:6, number * part : (number + 1) * part])
            for z in range(nz):
                put(z, 8 + chip, r.sums[6:7, z * part : (z + 1) * part])


class Scatter:
    def __init__(self, copies, me, r, source, theirs, got, landed):
        self.me, self.r, self.source, self.theirs, self.got, self.landed = me, r, source, theirs, got, landed
        self.chips = me.nz
        self.sides = got.shape[0] // self.chips
        self.first = r.k.shape[0]
        self.tiles = source.shape[0] * BLK // QTILE
        self.number = copies.count
        self.send_sems, self.recv_sems = copies.send_sems, copies.recv_sems
        self.exchanges = [
            copies.make(*self.rows(tile), me.on_plane(me.pn)) for tile in range(self.tiles)
        ]
        self.steps = []
        for side, near, far, to_near, to_far in (
            (0, me.tx, me.ty, me.xn, me.yn),
            (1, me.ty, me.tx, me.yn, me.xn),
        ):
            first, last = self.place(near, side), self.place(far, side)
            self.steps.append(
                (
                    copies.make(got.at[self.place(me.td, side)], landed.at[3 * side], me.on_plane(to_near)),
                    copies.make(got.at[first], landed.at[3 * side + 1], me.on_plane(to_near)),
                    copies.make(got.at[last], landed.at[3 * side + 2], me.on_plane(to_far)),
                    last,
                )
            )

    def place(self, chip, side):
        return chip * self.sides + side

    def rows(self, tile):
        blocks = QTILE // BLK
        place = pl.ds(tile * blocks, blocks)
        return self.source.at[place], self.theirs.at[place]

    def exchange(self, tile):
        source, target = self.rows(tile)
        pltpu.make_async_remote_copy(
            src_ref=source,
            dst_ref=target,
            send_sem=self.send_sems.at[self.number + tile],
            recv_sem=self.recv_sems.at[self.number + tile],
            device_id=self.me.on_plane(self.me.pn),
            device_id_type=MESH_IDS,
        ).start()

    def spread(self):
        count = self.chips * self.sides
        for exchange in self.exchanges:
            exchange.wait_recv()
        for number in range(count):
            flag = self.r.idx[self.first + 2 * count + number // self.sides]
            own = wide(self.source[self.r.idx[self.first + number]])
            other = wide(self.theirs[self.r.idx[self.first + count + number]])
            here = jnp.full(own.shape, flag, jnp.int32) > 0
            self.got[number] = narrow(jnp.where(here, own, other))
        for far, _, _, _ in self.steps:
            far.start()
        for _, near, _, _ in self.steps:
            near.start()

    def middle(self):
        for side, (far, _, on, last) in enumerate(self.steps):
            far.wait_recv()
            self.got[last] = narrow(wide(self.got[last]) + wide(self.landed[3 * side]))
            on.start()

    def total(self):
        pieces = []
        for side, (_, near, on, _) in enumerate(self.steps):
            near.wait_recv()
            on.wait_recv()
            pieces.append(
                wide(self.got[self.place(self.me.t, side)])
                + wide(self.landed[3 * side + 1])
                + wide(self.landed[3 * side + 2])
            )
        return jnp.concatenate(pieces, axis=0)


def layer_kernel(nz, names, *refs):
    r = types.SimpleNamespace(**dict(zip(names, refs)))
    me = Place(nz)
    copies = Copies(r.send_sems, r.recv_sems)
    sides = r.h.shape[0]
    shard = r.wqs.shape[0]
    tiles = r.att.shape[0] // QTILE

    kept = []

    def keep(source, target):
        copy = pltpu.make_async_copy(source, target, r.local_sems.at[len(kept)])
        copy.start()
        kept.append(copy)
        return copy

    own_rows = pl.ds(me.c * sides, sides)
    loads = windows(r, me)
    for copy in loads:
        copy.start()
    h_own = keep(r.h, r.hall.at[own_rows])
    keep(r.g, r.gall.at[own_rows])
    keep(r.g, r.gown)
    own_down = keep(r.wdown.at[pl.ds(me.t * shard, shard)], r.wd4.at[me.z])
    pack_vectors(r)
    me.greet()

    def row_slot(array):
        return lambda core, chip: array.at[pl.ds((2 * chip + core) * sides, sides)]

    h_share = PlaneShare(copies, me, r.h, row_slot(r.hall), sides)
    g_share = PlaneShare(copies, me, r.g, row_slot(r.gall), sides)
    wq = LineSend(copies, me, r.wqs, r.wq4)
    wu = LineGather(copies, me, r.wus, r.wu4)
    wd = LineGather(copies, me, r.wdown.at[pl.ds(me.t * shard, shard)], r.wd4)
    wo = LineSpread(copies, me, r.wout, r.wo1, r.window_sems.at[len(loads)])
    small = [copies.make(r.sm, r.sm4.at[me.z], me.on_line(other)) for other in me.others]

    for copy in small:
        copy.start()
    h_share.start()
    for copy in loads:
        copy.wait()
    slice_weights(r, me)
    r.wq4[me.z] = r.wqs[...]
    r.wu4[me.z] = r.wus[...]
    wq.start()
    wu.start()
    wd.start()
    r.sm4[me.z] = r.sm[...]
    block_table(r, me)
    r.sums[...] = jnp.zeros_like(r.sums)
    r.vout[...] = jnp.zeros_like(r.vout)
    r.dk[...] = jnp.zeros_like(r.dk)
    r.dv[...] = jnp.zeros_like(r.dv)
    for copy in small:
        copy.wait_recv()
    read_vectors(r, me)
    h_own.wait()
    h_share.to_p.wait_recv()
    pair = 2 * sides * BLK
    prepare(r, me.t, r.n, 0)
    h_share.relay()
    h_share.swap()
    g_share.start()
    h_share.swaps[0].wait_recv()
    prepare(r, me.tx, r.n, pair)
    h_share.swaps[1].wait_recv()
    wq.advance()
    prepare(r, me.ty, r.gl, 0)
    wq.finish()
    project(r, me.t, r.n, 0)
    wu.advance(0)
    h_share.on_diagonal()
    project(r, me.tx, r.n, pair)
    wd.advance(0)
    project(r, me.ty, r.gl, 0)
    g_share.relay()
    wu.advance(1)
    h_share.swaps[2].wait_recv()
    prepare(r, me.td, r.gl, pair)
    project(r, me.td, r.gl, pair)
    attend(r, me, 1)
    wd.advance(1)
    g_share.swap()
    attend(r, me, 2)
    wu.advance(2)
    g_share.on_diagonal()
    wd.advance(2)
    wo.start()
    for copy in kept[1:]:
        copy.wait()
    settled = len(kept)
    wu.finish()
    wd.finish()
    g_share.finish()

    @pl.loop(0, tiles)
    def _(tile):
        feed_forward(r, me, tile)

    half = shard // 2
    out_scatter = Scatter(copies, me, r, r.outb, r.otheirs, r.ogot, r.oland)
    up_reduce = LineReduce(copies, me, r.gu, r.tu, r.uu)
    down_reduce = LineReduce(copies, me, r.gd, r.td, r.ud)
    out_reduce = LineCollect(copies, me, r.go, r.to, r.uo)
    d_share = PlaneShare(copies, me, r.td.at[me.z], lambda core, chip: r.fd.at[core, chip], half)
    u_share = PlaneShare(copies, me, r.tu.at[me.z], lambda core, chip: r.fu.at[core, chip], half)
    o_spread = PlaneSpread(copies, me, r.to, r.fo, half, r.window_sems.at[len(loads) + 1])

    def share_down():
        d_share.start()
        keep(r.td.at[me.z], r.fd.at[me.k, me.t])

    weight_grad(r.gd, r.act, r.gl)
    down_reduce.start()
    weight_grad(r.gu, r.n, r.du)
    up_reduce.start()
    wo.advance()
    down_reduce.pair()
    attend(r, me, 0)
    attend(r, me, 3)
    up_reduce.pair()
    wo.finish()

    @pl.loop(0, tiles)
    def _(tile):
        out_project(r, me, tile)
        pl.when(tile > 0)(functools.partial(out_scatter.exchange, tile - 1))

    out_scatter.exchange(tiles - 1)
    r.go[...] = narrow(mm(r.att[...], r.gl[...], TN))
    out_reduce.start()
    attend_grad(r, me, 0)
    out_scatter.spread()
    attend_grad(r, me, 3)
    out_scatter.middle()
    attend_grad(r, me, 2)
    out_reduce.pair()
    down_reduce.collect()
    share_down()
    copies.settle([g_share.hop_x, g_share.hop_y, *g_share.swaps])
    copies.settle(out_scatter.exchanges)

    part = r.k.shape[2]
    quarter = r.k.shape[0] * BLK // 4

    def send_keys(number):
        first = quarter * (1 - me.k) if number == 0 else 3 * quarter - quarter * (1 - me.k)
        theirs = pl.ds(pl.multiple_of(first, quarter), quarter)
        rows = slice(number * quarter, (number + 1) * quarter)
        r.act[rows, :part] = narrow(r.dk[theirs, :])
        r.act[rows, part : 2 * part] = narrow(r.dv[theirs, :])
        copy = copies.make(r.act.at[rows, : 2 * part], r.kvin.at[rows], me.on_plane(me.pn))
        copy.start()
        return copy

    later = send_keys(1)
    attend_grad(r, me, 1)
    sooner = send_keys(0)
    later.wait_recv()
    e_scatter = Scatter(
        copies, me, r, r.outb, r.gall.at[: r.outb.shape[0]], r.gall.at[r.outb.shape[0] :], r.eland
    )

    @pl.loop(0, tiles)
    def _(number):
        pl.when(number == tiles // 2)(sooner.wait_recv)
        pl.when(number == tiles // 2)(d_share.relay)
        pl.when(number == tiles - 1)(up_reduce.collect)
        pl.when(number == tiles - 1)(u_share.start)
        qkv_grad(r, me, (number + tiles // 2) % tiles)
        pl.when(number > 0)(
            functools.partial(e_scatter.exchange, (number + tiles // 2 - 1) % tiles)
        )

    keep(r.tu.at[me.z], r.fu.at[me.k, me.t])
    gather_sums(r, me)
    e_scatter.exchange(tiles // 2 - 1)
    vec_line = [
        copies.make(r.vout.at[other], r.vline.at[me.z], me.on_line(other)) for other in me.others
    ]
    for copy in vec_line:
        copy.start()
    d_share.swap()
    weight_grad(r.gq, r.n, r.du.at[:, : 3 * part])
    qkv_reduce = LineReduce(copies, me, r.gq, r.tq, r.uq)
    qkv_reduce.start()
    e_scatter.spread()
    qkv_reduce.pair()
    u_share.relay()
    out_reduce.collect()
    o_spread.start()
    d_share.on_diagonal()
    u_share.swap()
    e_scatter.middle()
    for copy in vec_line:
        copy.wait_recv()
    vector = r.vout[me.z]
    for other in me.others:
        vector = vector + r.vline[other]
    r.vsend[...] = vector
    vec_plane = [copies.make(r.vsend, r.vplane.at[me.c], me.on_plane(peer)) for peer in me.plane]
    for copy in vec_plane:
        copy.start()
    qkv_reduce.collect()
    q_share = PlaneShare(copies, me, r.tq.at[me.z], lambda core, chip: r.fq.at[core, chip], half)
    q_share.start()
    keep(r.tq.at[me.z], r.fq.at[me.k, me.t])

    residual = wide(flat_rows(r.hall[own_rows]))
    own_standardized, own_deviation = norm_rows(residual)
    rows = sides * BLK
    r.n[:rows, :] = narrow(residual + r.vec[4:5, :] + out_scatter.total())
    keep(r.n.at[:rows], r.hidden_out)
    o_spread.advance()
    u_share.on_diagonal()
    q_share.relay()
    e_total = e_scatter.total()
    r.e2[:rows, :] = wide(flat_rows(r.gown[...])) + own_deviation * (
        e_total
        - jnp.mean(e_total, axis=-1, keepdims=True)
        - own_standardized * jnp.mean(e_total * own_standardized, axis=-1, keepdims=True)
    )
    keep(r.e2.at[:rows], r.hidden_grad)
    q_share.swap()
    o_spread.on_diagonal()
    for copy in vec_plane:
        copy.wait_recv()
    vector = r.vsend[...]
    for peer in me.plane:
        vector = vector + r.vplane[peer]
    r.vlast[...] = vector
    keep(r.vlast, r.vsum)
    q_share.on_diagonal()
    for share in (d_share, u_share, o_spread, q_share):
        share.finish()
    for copy in kept[settled:]:
        copy.wait()
    copies.finish()


def assemble_kernel(
    fq_ref, fu_ref, fd_ref, fo_ref, out_ref, grad_ref, vsum_ref,
    gq_ref, gu_ref, gd_ref, go_ref, hidden_out_ref, hidden_grad_ref, *vector_refs,
):
    _, chips, _, _ = fq_ref.shape
    part = fq_ref.shape[3] // 3
    hidden_out_ref[...] = out_ref[...]
    hidden_grad_ref[...] = grad_ref[...]
    go_ref[...] = wide(fo_ref[0])
    for chip in range(chips):
        for source, target in ((fq_ref, gq_ref), (fu_ref, gu_ref)):
            for piece in range(source.shape[3] // part):
                first = (piece * chips + chip) * part
                target[:, first : first + part] = wide(
                    source[0, chip, :, piece * part : (piece + 1) * part]
                )
        gd_ref[chip, 0] = wide(fd_ref[0, chip])

    @pl.when(pl.program_id(0) == 0)
    def _():
        first = 0
        for number, target in enumerate(vector_refs):
            count = target.shape[0]
            if number == 5:
                first -= count
            target[...] = vsum_ref[0:1, first : first + count].reshape(count)
            first += count


def rotary_parts(block_count):
    half_rot = ROT // 2
    lane = np.arange(128) % HD
    rate = np.where(lane < ROT, 10000.0 ** (-2.0 * (lane % half_rot) / ROT), 0.0)

    def table(places):
        angle = places[:, None].astype(np.float64) * rate[None, :]
        return np.concatenate([np.cos(angle), np.sin(angle)], axis=1).astype(np.float32)

    return table(np.arange(BLK)), table(np.arange(block_count) * BLK)


VMEM_SPEC = pl.BlockSpec(memory_space=pltpu.VMEM)
SPECS = {
    "order": pl.BlockSpec(memory_space=pltpu.SMEM),
    **{
        name: pl.BlockSpec(memory_space=pl.ANY)
        for name in ("h", "g", "wqkv", "wup", "wdown", "wout")
        + ("hidden_out", "hidden_grad", "fq", "fu", "fd", "fo", "vsum")
    },
}
VMEM_LIMIT = 63 * 1024 * 1024


def sliced_layer(
    nz,
    hidden_in,
    norm1_gain,
    attention_norm_bias,
    qkv_weight,
    qkv_bias,
    out_weight,
    out_bias,
    norm2_gain,
    feedforward_norm_bias,
    up_weight,
    up_bias,
    down_weight,
    down_bias,
    cotangent,
    block_order,
):
    f32, b16 = jnp.float32, jnp.bfloat16
    h, g = hidden_in[0], cotangent[0]
    local_rows, width = h.shape
    chips = lax.axis_size("ctx") // 2
    shard = qkv_weight.shape[0]
    half = shard // 2
    part = width // chips
    hidden = up_weight.shape[1] // chips
    rows = chips * local_rows
    everyone = 2 * rows
    sides = local_rows // BLK

    sums = 5 * shard + qkv_bias.shape[0] + up_bias.shape[0]
    slices = 3 + hidden // part
    columns = max(-(-(chip * part % 128 + part) // 128) * 128 for chip in range(chips))
    small = 6 * shard + qkv_bias.shape[0] + up_bias.shape[0]
    rope_r, rope_b = rotary_parts(everyone // BLK)

    inputs = {
        "order": block_order,
        "h": h.reshape(sides, BLK, width),
        "g": g.reshape(sides, BLK, width),
        "wqkv": qkv_weight,
        "wup": up_weight,
        "wdown": down_weight,
        "wout": out_weight,
        **dict(
            zip(
                VECTORS,
                (norm1_gain, attention_norm_bias, norm2_gain, feedforward_norm_bias)
                + (out_bias, down_bias, qkv_bias, up_bias),
            )
        ),
        "rope_r": jnp.asarray(rope_r),
        "rope_b": jnp.asarray(rope_b[:, None, :]),
    }
    outputs = {
        "hidden_out": ((local_rows, width), b16),
        "hidden_grad": ((local_rows, width), f32),
        "fq": ((2, chips, half, 3 * part), b16),
        "fu": ((2, chips, half, hidden), b16),
        "fd": ((2, chips, half, width), b16),
        "fo": ((2, half, width), b16),
        "vsum": ((1, sums), f32),
    }
    scratch = {
        "hall": ((everyone // BLK, BLK, width), b16),
        "gall": ((everyone // BLK, BLK, width), b16),
        "wqs": ((shard, 3 * part), b16),
        "wus": ((shard, hidden), b16),
        "wq4": ((nz, shard, 3 * part), b16),
        "wu4": ((nz, shard, hidden), b16),
        "wd4": ((nz, shard, width), b16),
        "wo1": ((part, width), b16),
        "sm": ((1, small), f32),
        "sm4": ((nz, 1, small), f32),
        "vec": ((8, width), f32),
        "sums": ((8, width), f32),
        "q": ((everyone // BLK, BLK, part), b16),
        "k": ((everyone // BLK, BLK, part), b16),
        "v": ((everyone // BLK, BLK, part), b16),
        "kt": ((everyone // BLK, part, BLK), b16),
        "vt": ((everyone // BLK, part, BLK), b16),
        "att": ((rows, part), b16),
        "attt": ((part, rows), b16),
        "lse": ((8, rows), f32),
        "delta": ((8, rows), f32),
        "datt": ((rows, part), b16),
        "act": ((rows, hidden), b16),
        "du": ((rows, hidden), b16),
        "n": ((rows, width), b16),
        "gl": ((rows, width), b16),
        "outb": ((rows // BLK, BLK, width), b16),
        "e2": ((rows, width), f32),
        "dk": ((everyone, part), f32),
        "dv": ((everyone, part), f32),
        "dqt": ((part, rows), f32),
        "kvin": ((rows, 2 * part), b16),
        "otheirs": ((rows // BLK, BLK, width), b16),
        "ogot": ((rows // BLK, BLK, width), b16),
        "oland": ((6, BLK, width), b16),
        "eland": ((6, BLK, width), b16),
        "gq": ((nz, shard, 3 * part), b16),
        "gu": ((nz, shard, hidden), b16),
        "gd": ((nz, shard, width), b16),
        "go": ((part, width), b16),
        "tq": ((nz, half, 3 * part), b16),
        "uq": ((nz, half, 3 * part), b16),
        "tu": ((nz, half, hidden), b16),
        "uu": ((nz, half, hidden), b16),
        "td": ((nz, half, width), b16),
        "ud": ((nz, half, width), b16),
        "to": ((half, width), b16),
        "uo": ((nz, half, width), b16),
        "vout": ((nz, 1, sums), f32),
        "vline": ((nz, 1, sums), f32),
        "vsend": ((1, sums), f32),
        "vlast": ((1, sums), f32),
        "gown": ((sides, BLK, width), b16),
        "win": ((slices, shard, columns), b16),
        "vplane": ((2 * chips, 1, sums), f32),
    }
    names = [*inputs, *outputs, *scratch, "idx", "send_sems", "recv_sems", "local_sems", "window_sems"]
    results = pl.pallas_call(
        functools.partial(layer_kernel, nz, names),
        out_shape=tuple(jax.ShapeDtypeStruct(*leaf) for leaf in outputs.values()),
        in_specs=[SPECS.get(name, VMEM_SPEC) for name in inputs],
        out_specs=tuple(SPECS.get(name, VMEM_SPEC) for name in outputs),
        scratch_shapes=[pltpu.VMEM(*leaf) for leaf in scratch.values()]
        + [pltpu.SMEM((64,), jnp.int32)]
        + [pltpu.SemaphoreType.DMA((SEMAPHORES,))] * 2
        + [pltpu.SemaphoreType.DMA((16,))] * 2,
        compiler_params=pltpu.CompilerParams(
            collective_id=0, has_side_effects=True, vmem_limit_bytes=VMEM_LIMIT
        ),
        name="layer",
    )(*inputs.values())
    hidden_out, hidden_grad, fq, fu, fd, fo, vsum = results

    steps = 2
    some, few = shard // steps, local_rows // steps
    inner = half // some

    def pieces(cols):
        return pl.BlockSpec((1, chips, some, cols), lambda i: (i // inner, 0, i % inner, 0))

    def lines(count, cols):
        return pl.BlockSpec((count, cols), lambda i: (i, 0))

    def vector(count):
        return pl.BlockSpec((count,), lambda i: (0,))

    sizes = [shard] * 6 + [qkv_bias.shape[0], up_bias.shape[0]]
    grad_qkv, grad_up, grad_down, grad_out, hidden_out, hidden_grad, *vectors = pl.pallas_call(
        assemble_kernel,
        grid=(steps,),
        out_shape=(
            jax.ShapeDtypeStruct(qkv_weight.shape, f32),
            jax.ShapeDtypeStruct(up_weight.shape, f32),
            jax.ShapeDtypeStruct((chips, steps, some, width), f32),
            jax.ShapeDtypeStruct(out_weight.shape, f32),
            jax.ShapeDtypeStruct(h.shape, b16),
            jax.ShapeDtypeStruct(h.shape, f32),
        )
        + tuple(jax.ShapeDtypeStruct((size,), f32) for size in sizes),
        in_specs=[
            pieces(3 * part),
            pieces(hidden),
            pieces(width),
            pl.BlockSpec((1, some, width), lambda i: (i // inner, i % inner, 0)),
            lines(few, width),
            lines(few, width),
            pl.BlockSpec((1, sums), lambda i: (0, 0)),
        ],
        out_specs=(
            lines(some, qkv_weight.shape[1]),
            lines(some, up_weight.shape[1]),
            pl.BlockSpec((chips, 1, some, width), lambda i: (0, i, 0, 0)),
            lines(some, width),
            lines(few, width),
            lines(few, width),
        )
        + tuple(vector(size) for size in sizes),
        compiler_params=pltpu.CompilerParams(vmem_limit_bytes=56 * 1024 * 1024),
        name="assemble",
    )(fq, fu, fd, fo, hidden_out, hidden_grad, vsum)
    g_gain1, g_shift1, g_gain2, g_shift2, g_bout, g_bdown, g_bqkv, g_bup = vectors
    return (
        hidden_out[None],
        hidden_grad[None],
        g_gain1,
        g_shift1,
        grad_qkv,
        g_bqkv,
        grad_out,
        g_bout,
        g_gain2,
        g_shift2,
        grad_up,
        g_bup,
        grad_down.reshape(down_weight.shape),
        g_bdown,
    )


def sliced_fits(mesh):
    return mesh.shape["ctx"] == 8 and mesh.shape["fsdp"] == 4


def solution(mesh):
    in_specs = (
        P("fsdp", "ctx", None),
        P("fsdp"),
        P("fsdp"),
        P("fsdp", None),
        P("fsdp"),
        P("fsdp", None),
        P("fsdp"),
        P("fsdp"),
        P("fsdp"),
        P("fsdp", None),
        P("fsdp"),
        P("fsdp", None),
        P("fsdp"),
        P("fsdp", "ctx", None),
        P(),
    )
    out_specs = (
        P("fsdp", "ctx", None),
        P("fsdp", "ctx", None),
        P("fsdp"),
        P("fsdp"),
        P("fsdp", None),
        P("fsdp"),
        P("fsdp", None),
        P("fsdp"),
        P("fsdp"),
        P("fsdp"),
        P("fsdp", None),
        P("fsdp"),
        P("fsdp", None),
        P("fsdp"),
    )
    local = whole_parameter_layer
    if sliced_fits(mesh):
        local = functools.partial(sliced_layer, mesh.shape["fsdp"])
    return jax.shard_map(local, mesh=mesh, in_specs=in_specs, out_specs=out_specs, check_vma=False)
```
